128 devices in a mesh: gy: 16 (over z, x), gz: 8 (over y, core).
Axes of the slice: x: 4, y: 4, z: 4, core: 2. Of those that a mesh axis runs over, the one named last changes fastest.
Arguments:
- fraction: float32 [128, 128, 1024], P('gz', 'gy'), may hold values from 0 to 1
- velocity_x: float32 [128, 128, 1024], P('gz', 'gy'), may hold values from -9 to 9
- velocity_y: float32 [128, 128, 1024], P('gz', 'gy'), may hold values from -9 to 9
- velocity_z: float32 [128, 128, 1024], P('gz', 'gy'), may hold values from -9 to 9
Outputs:
- advected: float32 [128, 128, 1024], P('gz', 'gy')
- time_step: float32 [], replicated
The draws below stay inside these ranges and needn't reach their ends.
All inputs are finite; a program needn't handle non-finite values. Where the reference program divides by a largest or mean magnitude, that divisor is 1e-20 or more.
Results may differ from the reference program's by a relative error of at most 0.0003.
Values sent between devices are 32-bit elements; how exact they have to be, the bound alone decides.
A program may use at most 64 MiB of HBM per device.

```python
import jax
import jax.numpy as jnp

NX = 1024
CY = 8
CZ = 16
NEWTON = 5
NY = 128
NZ = 128
N_GY = 16
N_GZ = 8


def block_linear():
    plane_owner = jnp.arange(NZ) // CZ
    row_owner = jnp.arange(NY) // CY
    return row_owner[None, :] * N_GZ + plane_owner[:, None]


def spread_blocks(values):
    return values[block_linear()][:, :, None]


def draw_fraction(key, part):
    key_pick, key_coin, key_value, key_level, key_jitter, key_power = jax.random.split(key, 6)
    count = N_GY * N_GZ
    linear = jnp.arange(count).astype(jnp.float32)
    rise = 0.5 + linear / (count - 1)
    level = jax.random.uniform(key_level, (), jnp.float32, 0.15, 0.45)
    jitter = jnp.exp(jax.random.uniform(key_jitter, (count,), jnp.float32, jnp.log(0.6), jnp.log(1.4)))
    mixed_rate = spread_blocks(level * rise * jitter)
    power = jax.random.uniform(key_power, (count,), jnp.float32, 1.0, 2.0)
    chooser = jax.random.uniform(key_pick, (NZ, NY, NX), jnp.float32)
    pure_value = (jax.random.uniform(key_coin, (NZ, NY, NX), jnp.float32) < 0.5).astype(jnp.float32)
    mixture = jax.random.uniform(key_value, (NZ, NY, NX), jnp.float32)
    mixture = jnp.power(mixture, spread_blocks(power))
    return jnp.where(chooser < mixed_rate, mixture, pure_value)


def speed_field(key, which):
    local_key = jax.random.fold_in(key, which)
    key_values, key_peak, key_lower, key_upper = jax.random.split(local_key, 4)
    count = N_GY * N_GZ
    half = count // 2
    ranks = jnp.concatenate([jax.random.permutation(key_lower, half), half + jax.random.permutation(key_upper, count - half)]).astype(jnp.float32)
    peak = jax.random.uniform(key_peak, (), jnp.float32, 3.0, 9.0)
    amplitude = peak * (1.0 + 2.0 * ranks / (count - 1)) / 3.0
    values = jnp.clip(jax.random.normal(key_values, (NZ, NY, NX), jnp.float32), -3.0, 3.0) / 3.0
    return values * spread_blocks(amplitude)


def draw_velocity_x(key, part):
    return speed_field(key, 11)


def draw_velocity_y(key, part):
    return speed_field(key, 23)


def draw_velocity_z(key, part):
    return speed_field(key, 37)


def setup_inputs(seed: int = 0) -> dict:
    key_of = jax.random.split(jax.random.key(seed), 5)
    fraction = draw_fraction(jax.random.fold_in(key_of[4], 71), 0)
    velocity_x = draw_velocity_x(jax.random.fold_in(key_of[4], 71), 0)
    velocity_y = draw_velocity_y(jax.random.fold_in(key_of[4], 71), 0)
    velocity_z = draw_velocity_z(jax.random.fold_in(key_of[4], 71), 0)
    return dict(fraction=fraction, velocity_x=velocity_x, velocity_y=velocity_y, velocity_z=velocity_z)


tilt_floor = 0.1
courant = 0.45
epsilon = 1e-6


def cube_step(reach, height):
    safe = jnp.where(height > 0, height, 1.0)
    whole = 3.0 * reach * reach - 3.0 * reach * height + height * height
    partial_part = reach * reach * reach / safe
    return jnp.where(reach - height >= 0, whole, jnp.where(reach >= 0, partial_part, 0.0))


def cube_rate(reach, height):
    safe = jnp.where(height > 0, height, 1.0)
    whole = 6.0 * reach - 3.0 * height
    partial_part = 3.0 * reach * reach / safe
    return jnp.where(reach - height >= 0, whole, jnp.where(reach >= 0, partial_part, 0.0))


def region_volume(offset, tilt_a, tilt_b, height, extent):
    combo = cube_step(offset, height) - cube_step(offset - tilt_a, height) - cube_step(offset - tilt_b, height) + cube_step(offset - tilt_a - tilt_b, height)
    return extent * combo / (6.0 * tilt_a * tilt_b)


def section_area(offset, tilt_a, tilt_b, height):
    combo = cube_rate(offset, height) - cube_rate(offset - tilt_a, height) - cube_rate(offset - tilt_b, height) + cube_rate(offset - tilt_a - tilt_b, height)
    return combo / (6.0 * tilt_a * tilt_b)


def youngs_slope(padded):
    def smooth_zero(arr):
        return arr[:-2] + 2.0 * arr[1:-1] + arr[2:]

    def smooth_one(arr):
        return arr[:, :-2] + 2.0 * arr[:, 1:-1] + arr[:, 2:]

    def smooth_cells(arr):
        return jnp.roll(arr, 1, 2) + 2.0 * arr + jnp.roll(arr, -1, 2)

    diff_zero = padded[2:] - padded[:-2]
    diff_one = padded[:, 2:] - padded[:, :-2]
    diff_cells = jnp.roll(padded, -1, 2) - jnp.roll(padded, 1, 2)
    grad_zero = smooth_cells(smooth_one(diff_zero)) / 32.0
    grad_one = smooth_cells(smooth_zero(diff_one)) / 32.0
    grad_cells = smooth_one(smooth_zero(diff_cells)) / 32.0
    return (grad_zero, grad_one, grad_cells)


def plane_for(fraction, slopes, axis_dim):
    slope_d = slopes[axis_dim]
    across = [slopes[index] for index in range(3) if index != axis_dim]
    tilt_d = jnp.abs(slope_d)
    tilt_a = jnp.abs(across[0]) + tilt_floor
    tilt_b = jnp.abs(across[1]) + tilt_floor
    volume = jnp.clip(fraction, 0.0, 1.0)
    lesser = jnp.minimum(volume, 1.0 - volume)
    summed = tilt_a + tilt_b + tilt_d
    offset = 0.5 * summed
    for repeat in range(NEWTON):
        offset = offset - (region_volume(offset, tilt_a, tilt_b, tilt_d, 1.0) - lesser) / section_area(offset, tilt_a, tilt_b, tilt_d)
    offset = jnp.where(volume > 0.5, summed - offset, offset)
    return (offset, tilt_a, tilt_b, tilt_d, slope_d > 0)


def outflow(planes, width, upward):
    offset, tilt_a, tilt_b, tilt_d, mirrored = planes
    if upward:
        start_at = jnp.where(mirrored, 0.0, 1.0 - width)
    else:
        start_at = jnp.where(mirrored, 1.0 - width, 0.0)
    return region_volume(offset - tilt_d * start_at, tilt_a, tilt_b, tilt_d * width, width)


def sweep(fraction, velocity, axis_dim, time_step):
    padded = jnp.pad(fraction, ((1, 1), (1, 1), (0, 0)), mode="wrap")
    planes = plane_for(fraction, youngs_slope(padded), axis_dim)
    velocity_low = jnp.roll(velocity, 1, axis_dim)
    out_upper = outflow(planes, jnp.maximum(time_step * velocity, 0.0), True)
    out_lower = outflow(planes, jnp.maximum(-time_step * velocity_low, 0.0), False)
    from_below = jnp.roll(out_upper, 1, axis_dim)
    from_above = jnp.roll(out_lower, -1, axis_dim)
    divisor = 1.0 - time_step * velocity + time_step * velocity_low
    return (fraction - out_upper - out_lower + from_below + from_above) / divisor


def reference(fraction, velocity_x, velocity_y, velocity_z):
    umax = jnp.maximum(jnp.maximum(jnp.max(jnp.abs(velocity_x)), jnp.max(jnp.abs(velocity_y))), jnp.max(jnp.abs(velocity_z)))
    share = jnp.sum(4.0 * fraction * (1.0 - fraction)) / (NX * NY * NZ)
    time_step = courant / ((umax + epsilon) * (1.0 + share))
    field = sweep(fraction, velocity_x, 2, time_step)
    field = sweep(field, velocity_y, 1, time_step)
    field = sweep(field, velocity_z, 0, time_step)
    return field, time_step
```

```python
import jax
import jax.numpy as jnp
from jax import lax
from jax.experimental import pallas as pl
from jax.experimental.pallas import tpu as pltpu
from jax.sharding import PartitionSpec as P

NEWTON = 5
TILT_FLOOR = 3.2
TINY = 1e-18
COURANT = 0.45
EPSILON = 1e-6
THIRD = 1.0 / 3.0

NZ, NY, J, LN = 16, 8, 8, 128
N_GY, N_GZ = 16, 8
RING = 4
F32 = jnp.float32

HALO = (0, 8, 16)
VEL = 24
FLUX_Y = 26
FLUX_Z = 28
STAT_A = 30
STAT_X = 37
STAT_Z = 40
N_SEMS = 43


def lanes(u):
    return lax.broadcasted_iota(jnp.int32, u.shape, u.ndim - 1)


def at_next(u):
    moved = pltpu.roll(u, LN - 1, u.ndim - 1)
    return jnp.where(lanes(u) == LN - 1, pltpu.roll(moved, J - 1, u.ndim - 2), moved)


def at_prev(u):
    moved = pltpu.roll(u, 1, u.ndim - 1)
    return jnp.where(lanes(u) == 0, pltpu.roll(moved, 1, u.ndim - 2), moved)


def plane(g, slope_d, slope_a, slope_b):
    tilt_a = jnp.abs(slope_a) + TILT_FLOOR
    tilt_b = jnp.abs(slope_b) + TILT_FLOOR
    lo, hi = jnp.minimum(tilt_a, tilt_b), jnp.maximum(tilt_a, tilt_b)
    slope_d = jnp.where(jnp.abs(slope_d) < TINY, TINY, slope_d)
    tilt_d = jnp.abs(slope_d)
    m1, rest = jnp.minimum(lo, tilt_d), jnp.maximum(lo, tilt_d)
    m2, m3 = jnp.minimum(rest, hi), jnp.maximum(rest, hi)
    volume = jnp.clip(g, 0.0, 1.0)
    lesser = jnp.minimum(volume, 1.0 - volume)
    m12 = m1 * m2
    product = m12 * m3
    target = lesser * product
    both = target + target
    summed = lo + hi + tilt_d
    w = 0.5 * jnp.maximum(m1 + m2 - m3, 0.0)
    a = 0.5 * summed - (0.5 * product - target) / (m12 - w * w)
    for _ in range(NEWTON - 1):
        q0 = jnp.minimum(a, m1)
        r0 = a - q0
        p2 = jnp.maximum(a - m2, 0.0)
        q2 = jnp.minimum(p2, m1)
        r2 = p2 - q2
        p3 = jnp.maximum(a - m3, 0.0)
        s3 = p3 * p3
        value = q0 * (q0 * q0 * THIRD + a * r0) - q2 * (q2 * q2 * THIRD + p2 * r2) - s3 * (p3 * THIRD) - both
        rate = q0 * (a + r0) - q2 * (p2 + r2) - s3
        a = a - value / rate
    return jnp.where(volume > 0.5, summed - a, a), lo, hi, slope_d, 0.5 / product


def cube_part(s, h):
    p = jnp.maximum(s, 0.0)
    q = jnp.minimum(p, h)
    r = p - q
    return q * (q * q * THIRD + p * r)


def flow(offset, lo, hi, slope_d, scale, c):
    signed = c * slope_d
    h = jnp.abs(signed)
    s = offset - jnp.where(signed < 0, jnp.abs(slope_d) - h, 0.0)
    t = s - hi
    return scale * ((cube_part(s, h) - cube_part(s - lo, h)) - (cube_part(t, h) - cube_part(t - lo, h)))


def rows(ref, where):
    parts = [ref[z, pl.ds(y, n)] for z, y, n in where]
    return parts[0] if len(parts) == 1 else jnp.concatenate(parts, axis=0)


def put(ref, where, value):
    start = 0
    for z, y, n in where:
        ref[z, pl.ds(y, n)] = value[start : start + n]
        start += n


def moved(where, dz, dy):
    return [(z + dz, y + dy, n) for z, y, n in where]


def loop(first, last, body):
    def step(i, carry):
        body(i)
        return carry

    lax.fori_loop(first, last, step, 0)


def kernel(
    f_hbm, vx_hbm, vy_hbm, vz_hbm, out_hbm, dt_out,
    f_ext, g1_ext, g2_ext, vx, vy, vz, smooth, diff, sum_y, dif_y, sum_d,
    off, lo, hi, slope, scale, face_y, face_z, edge_y, edge_z,
    stat_a, stat_x, stat_z, dt_vec, out_buf,
    load_sem, out_sem, send_sem, recv_sem,
):
    gy, gz = lax.axis_index("gy"), lax.axis_index("gz")
    chip_z, chip_x = gy // RING, lax.rem(gy, RING)

    def neighbour(dy, dz):
        return {"gy": lax.rem(gy + dy + N_GY, N_GY), "gz": lax.rem(gz + dz + N_GZ, N_GZ)}

    def along_x(k):
        return {"gy": chip_z * RING + lax.rem(chip_x + k, RING), "gz": gz}

    def along_z(k):
        return {"gy": lax.rem(chip_z + k, RING) * RING + chip_x, "gz": gz}

    corners = [(1, 1), (1, -1), (-1, 1), (-1, -1)]

    loads = []
    for source, target in (
        (f_hbm, lambda y: f_ext.at[pl.ds(1, NZ), 1 + y]),
        (vx_hbm, lambda y: vx.at[:, y]),
        (vy_hbm, lambda y: vy.at[:, 1 + y]),
        (vz_hbm, lambda y: vz.at[pl.ds(1, NZ), y]),
    ):
        loads.append([
            pltpu.make_async_copy(source.at[:, :, y, :], target(y), load_sem.at[len(loads), y])
            for y in range(NY)
        ])
    for group in loads:
        for copy in group:
            copy.start()
    barrier = pltpu.get_barrier_semaphore()
    greeted = [neighbour(0, k) for k in range(1, N_GZ)]
    greeted += [neighbour(1, 0), neighbour(-1, 0)] + [neighbour(*c) for c in corners]
    greeted += [along_x(k) for k in range(1, RING)] + [along_z(k) for k in range(1, RING)]
    for device in greeted:
        pl.semaphore_signal(barrier, inc=1, device_id=device, device_id_type=pl.DeviceIdType.MESH)

    def remote(source, target, k, device):
        return pltpu.make_async_remote_copy(
            src_ref=source, dst_ref=target, send_sem=send_sem.at[k], recv_sem=recv_sem.at[k],
            device_id=device, device_id_type=pl.DeviceIdType.MESH,
        )

    def halo(g, base):
        inner_z, inner_y = pl.ds(1, NZ), pl.ds(1, NY)
        copies = [
            remote(g.at[inner_z, NY], g.at[inner_z, 0], base, neighbour(1, 0)),
            remote(g.at[inner_z, 1], g.at[inner_z, NY + 1], base + 1, neighbour(-1, 0)),
            remote(g.at[NZ, inner_y], g.at[0, inner_y], base + 2, neighbour(0, 1)),
            remote(g.at[1, inner_y], g.at[NZ + 1, inner_y], base + 3, neighbour(0, -1)),
        ]
        for k, (dy, dz) in enumerate(corners):
            source = g.at[NZ if dz > 0 else 1, NY if dy > 0 else 1]
            target = g.at[0 if dz > 0 else NZ + 1, 0 if dy > 0 else NY + 1]
            copies.append(remote(source, target, base + 4 + k, neighbour(dy, dz)))
        return copies

    sent = []

    def send(copies):
        for copy in copies:
            copy.start()
        sent.extend(copies)

    def arrive(copies):
        for copy in copies:
            copy.wait_recv()

    def put_shifts(g, where):
        before, after = at_prev(g), at_next(g)
        put(smooth, where, before + 2.0 * g + after)
        put(diff, where, after - before)

    for copy in loads[0]:
        copy.wait()

    def scan_fraction(z, total):
        g = f_ext[z, pl.ds(1, NY)]
        put_shifts(g, [(z, 1, NY)])
        return total + g * (1.0 - g)

    total = lax.fori_loop(1, NZ + 1, scan_fraction, jnp.zeros((NY, J, LN), F32))
    for group in loads[1:]:
        for copy in group:
            copy.wait()

    def scan_velocity(z, peak):
        own = jnp.maximum(jnp.abs(vx[z]), jnp.abs(vy[z, pl.ds(1, NY)]))
        return jnp.maximum(peak, jnp.maximum(own, jnp.abs(vz[z + 1])))

    peak = lax.fori_loop(0, NZ, scan_velocity, jnp.zeros((NY, J, LN), F32))
    first_row = lax.broadcasted_iota(jnp.int32, (J, LN), 0) == 0

    def stat_tile(peak_rows, total_rows):
        return jnp.where(
            first_row,
            jnp.broadcast_to(jnp.max(peak_rows, axis=0, keepdims=True), (J, LN)),
            jnp.broadcast_to(jnp.sum(total_rows, axis=0, keepdims=True), (J, LN)),
        )

    def combined(ref, n):
        top, add = ref[0], ref[0]
        for k in range(1, n):
            top, add = jnp.maximum(top, ref[k]), add + ref[k]
        return jnp.where(first_row, top, add)

    stat_a[gz] = stat_tile(jnp.max(peak, axis=0), jnp.sum(total, axis=0))

    pl.semaphore_wait(barrier, len(greeted))
    halo_f = halo(f_ext, HALO[0])
    stats_a = [
        remote(stat_a.at[gz], stat_a.at[gz], STAT_A + k - 1, neighbour(0, k)) for k in range(1, N_GZ)
    ]
    stats_x = [
        remote(stat_x.at[chip_x], stat_x.at[chip_x], STAT_X + k - 1, along_x(k)) for k in range(1, RING)
    ]
    stats_z = [
        remote(stat_z.at[chip_z], stat_z.at[chip_z], STAT_Z + k - 1, along_z(k)) for k in range(1, RING)
    ]
    velocity = [
        remote(vy.at[:, NY], vy.at[:, 0], VEL, neighbour(1, 0)),
        remote(vz.at[NZ], vz.at[0], VEL + 1, neighbour(0, 1)),
    ]
    send(stats_a)
    send(halo_f)
    send(velocity)

    def put_sums(z, y, n):
        s = smooth[z, pl.ds(y - 1, n + 2)]
        d = diff[z, pl.ds(y - 1, n + 2)]
        where = [(z, y - 1, n)]
        put(sum_y, where, s[:-2] + 2.0 * s[1:-1] + s[2:])
        put(dif_y, where, s[2:] - s[:-2])
        put(sum_d, where, d[:-2] + 2.0 * d[1:-1] + d[2:])

    def put_planes(g_ext, where, dim):
        at = moved(where, 0, -1)
        below, above = moved(at, -1, 0), moved(at, 1, 0)
        along_z = rows(sum_y, above) - rows(sum_y, below)
        along_y = rows(dif_y, below) + 2.0 * rows(dif_y, at) + rows(dif_y, above)
        along_x = rows(sum_d, below) + 2.0 * rows(sum_d, at) + rows(sum_d, above)
        slopes = [along_z, along_y, along_x]
        across = [slopes[k] for k in range(3) if k != dim]
        found = plane(rows(g_ext, where), slopes[dim], *across)
        for ref, value in zip((off, lo, hi, slope, scale), found):
            put(ref, moved(where, -1, -1), value)

    inner = (2, NY - 2)

    def sums_inner():
        loop(1, NZ + 1, lambda z: put_sums(z, *inner))

    def planes_inner(g_ext, dim, first, last):
        loop(first, last, lambda z: put_planes(g_ext, [(z, *inner)], dim))

    def y_edge(i):
        z = 2 * i + 1
        return [(z, 1, 1), (z, NY, 1), (z + 1, 1, 1), (z + 1, NY, 1)]

    def z_edge(i):
        return [(1 + i * (NZ - 1), *inner)]

    def sums_outer(g_ext):
        def sides(i):
            z = 2 * i + 1
            where = [(z, 0, 1), (z, NY + 1, 1), (z + 1, 0, 1), (z + 1, NY + 1, 1)]
            put_shifts(rows(g_ext, where), where)

        def ends(i):
            where = [(i * (NZ + 1), 0, NY + 2)]
            put_shifts(rows(g_ext, where), where)

        loop(0, NZ // 2, sides)
        loop(0, 2, ends)

        def side_sums(z):
            put_sums(z, 1, 1)
            put_sums(z, NY, 1)

        loop(1, NZ + 1, side_sums)
        loop(0, 2, lambda i: put_sums(i * (NZ + 1), 1, NY))

    def donors(upward, here, there):
        picked = []
        for ref in (off, lo, hi, slope):
            picked.append(jnp.where(upward, rows(ref, here), rows(ref, there)))
        picked.append(jnp.where(upward, rows(scale, here), -rows(scale, there)))
        return picked

    sums_inner()
    planes_inner(f_ext, 2, 2, 6)
    arrive(stats_a)
    stat_x[chip_x] = combined(stat_a, N_GZ)
    planes_inner(f_ext, 2, 6, 7)
    send(stats_x)
    planes_inner(f_ext, 2, 7, 11)
    arrive(stats_x)
    stat_z[chip_z] = combined(stat_x, RING)
    planes_inner(f_ext, 2, 11, 12)
    send(stats_z)
    planes_inner(f_ext, 2, 12, NZ)
    arrive(halo_f)
    arrive(velocity)
    sums_outer(f_ext)
    loop(0, NZ // 2, lambda i: put_planes(f_ext, y_edge(i), 2))
    loop(0, 2, lambda i: put_planes(f_ext, z_edge(i), 2))
    arrive(stats_z)
    stats = combined(stat_z, RING)
    umax = jnp.max(stats[0:1], axis=1, keepdims=True)
    share = jnp.sum(stats[1:2], axis=1, keepdims=True) * (4.0 / (N_GZ * NZ * N_GY * NY * J * LN))
    step = COURANT / ((umax + EPSILON) * (1.0 + share))
    dt_vec[...] = jnp.broadcast_to(step, (J, LN))
    dt_out[0, 0] = jnp.max(step)

    def sweep_x(where):
        here = moved(where, -1, -1)
        c = dt_vec[...] * rows(vx, here)
        upward = c > 0
        picked = []
        for ref in (off, lo, hi, slope, scale):
            own = rows(ref, here)
            other = at_next(own)
            picked.append(jnp.where(upward, own, -other if ref is scale else other))
        out = flow(*picked, c)
        g = (rows(f_ext, where) - out + at_prev(out)) / (1.0 - c + at_prev(c))
        put(g1_ext, where, g)
        put_shifts(g, where)

    loop(0, NZ // 2, lambda i: sweep_x(y_edge(i)))
    loop(0, 2, lambda i: sweep_x(z_edge(i)))
    halo_1 = halo(g1_ext, HALO[1])
    send(halo_1)
    loop(2, NZ, lambda z: sweep_x([(z, *inner)]))

    half = NZ // 2 + 1
    sums_inner()
    planes_inner(g1_ext, 1, 2, half)
    arrive(halo_1)
    sums_outer(g1_ext)
    loop(0, NZ // 2, lambda i: put_planes(g1_ext, y_edge(i), 1))

    def half_faces_y(i):
        where = moved(y_edge(i), -1, -1)
        at_face = [(2 * i, 0, 1), (2 * i, NY, 1), (2 * i + 1, 0, 1), (2 * i + 1, NY, 1)]
        c = dt_vec[...] * rows(vy, at_face)
        out = flow(*[rows(ref, where) for ref in (off, lo, hi, slope, scale)], c)
        for k in range(2):
            edge_y[0, 2 * i + k] = jnp.where(c[2 * k + 1] > 0, out[2 * k + 1], 0.0)
            edge_y[1, 2 * i + k] = jnp.where(c[2 * k] < 0, out[2 * k], 0.0)

    loop(0, NZ // 2, half_faces_y)
    flux_y = [
        remote(edge_y.at[0], edge_y.at[2], FLUX_Y, neighbour(1, 0)),
        remote(edge_y.at[1], edge_y.at[3], FLUX_Y + 1, neighbour(-1, 0)),
    ]
    loop(0, 2, lambda i: put_planes(g1_ext, z_edge(i), 1))
    send(flux_y)
    planes_inner(g1_ext, 1, half, NZ)

    def faces_y(z):
        c = dt_vec[...] * vy[z, pl.ds(1, NY - 1)]
        face_y[z, pl.ds(1, NY - 1)] = flow(*donors(c > 0, [(z, 0, NY - 1)], [(z, 1, NY - 1)]), c)

    loop(0, NZ, faces_y)
    arrive(flux_y)

    def update_y(z):
        face_y[z, 0] = edge_y[2, z] - edge_y[1, z]
        face_y[z, NY] = edge_y[0, z] - edge_y[3, z]
        out, q = face_y[z], vy[z]
        g = (g1_ext[z + 1, pl.ds(1, NY)] - out[1:] + out[:-1]) / (1.0 - dt_vec[...] * (q[1:] - q[:-1]))
        where = [(z + 1, 1, NY)]
        put(g2_ext, where, g)
        put_shifts(g, where)

    loop(0, NZ, update_y)
    halo_2 = halo(g2_ext, HALO[2])

    sums_inner()
    send(halo_2)
    planes_inner(g2_ext, 0, 2, half)
    arrive(halo_2)
    sums_outer(g2_ext)
    loop(0, NZ // 2, lambda i: put_planes(g2_ext, y_edge(i), 0))
    loop(0, 2, lambda i: put_planes(g2_ext, z_edge(i), 0))

    def half_faces_z(i):
        c = dt_vec[...] * vz[i * NZ]
        where = [(i * (NZ - 1), 0, NY)]
        out = flow(*[rows(ref, where) for ref in (off, lo, hi, slope, scale)], c)
        toward = jnp.where(i == 0, -c, c)
        edge_z[1 - i] = jnp.where(toward > 0, out, 0.0)

    loop(0, 2, half_faces_z)
    flux_z = [
        remote(edge_z.at[0], edge_z.at[2], FLUX_Z, neighbour(0, 1)),
        remote(edge_z.at[1], edge_z.at[3], FLUX_Z + 1, neighbour(0, -1)),
    ]
    planes_inner(g2_ext, 0, half, half + 1)
    send(flux_z)
    planes_inner(g2_ext, 0, half + 1, NZ)

    def faces_z(z):
        c = dt_vec[...] * vz[z]
        face_z[z] = flow(*donors(c > 0, [(z - 1, 0, NY)], [(z, 0, NY)]), c)

    loop(1, NZ, faces_z)
    arrive(flux_z)
    face_z[0] = edge_z[2] - edge_z[1]
    face_z[NZ] = edge_z[0] - edge_z[3]

    def update_z(z):
        g = g2_ext[z + 1, pl.ds(1, NY)] - face_z[z + 1] + face_z[z]
        out_buf[z] = g / (1.0 - dt_vec[...] * (vz[z + 1] - vz[z]))

    loop(0, NZ, update_z)
    stores = [
        pltpu.make_async_copy(out_buf.at[:, y], out_hbm.at[:, :, y, :], out_sem.at[y]) for y in range(NY)
    ]
    for copy in stores:
        copy.start()
    for copy in sent:
        copy.wait_send()
    for copy in stores:
        copy.wait()


def shards(*blocks):
    tiled = [b.reshape(NZ, NY, J, LN).transpose(0, 2, 1, 3) for b in blocks]
    row = (J, LN)
    ext = pltpu.VMEM((NZ + 2, NY + 2, *row), F32)
    sums = pltpu.VMEM((NZ + 2, NY, *row), F32)
    own = pltpu.VMEM((NZ, NY, *row), F32)
    anywhere = pl.BlockSpec(memory_space=pl.ANY)
    field, step = pl.pallas_call(
        kernel,
        out_shape=(jax.ShapeDtypeStruct((NZ, J, NY, LN), F32), jax.ShapeDtypeStruct((1, 1), F32)),
        in_specs=[anywhere] * 4,
        out_specs=(anywhere, pl.BlockSpec(memory_space=pltpu.SMEM)),
        scratch_shapes=[
            ext, ext, ext,
            own, pltpu.VMEM((NZ, NY + 1, *row), F32), pltpu.VMEM((NZ + 1, NY, *row), F32),
            ext, ext, sums, sums, sums,
            own, own, own, own, own,
            pltpu.VMEM((NZ, NY + 1, *row), F32), pltpu.VMEM((NZ + 1, NY, *row), F32),
            pltpu.VMEM((4, NZ, *row), F32), pltpu.VMEM((4, NY, *row), F32),
            pltpu.VMEM((N_GZ, *row), F32), pltpu.VMEM((RING, *row), F32), pltpu.VMEM((RING, *row), F32),
            pltpu.VMEM(row, F32), own,
            pltpu.SemaphoreType.DMA((4, NY)), pltpu.SemaphoreType.DMA((NY,)),
            pltpu.SemaphoreType.DMA((N_SEMS,)), pltpu.SemaphoreType.DMA((N_SEMS,)),
        ],
        compiler_params=pltpu.CompilerParams(collective_id=0, has_side_effects=True),
        name="advect",
    )(*tiled)
    return field.transpose(0, 2, 1, 3).reshape(NZ, NY, J * LN), step.reshape(())


def solution(mesh):
    spec = P("gz", "gy", None)
    return jax.shard_map(shards, mesh=mesh, in_specs=(spec,) * 4, out_specs=(spec, P()), check_vma=False)
```

```python
import jax
import jax.numpy as jnp
from jax import lax
from jax.experimental import pallas as pl
from jax.experimental.pallas import tpu as pltpu
from jax.sharding import PartitionSpec as P

NEWTON = 5
TILT_FLOOR = 3.2
TINY = 1e-18
COURANT = 0.45
EPSILON = 1e-6
THIRD = 1.0 / 3.0

NZ, NY, J, LN = 16, 8, 8, 128
N_GY, N_GZ = 16, 8
RING = 4
F32 = jnp.float32

EZ, EY = NZ + 4, NY + 4
Z0, Y0 = 2, 2
Z1, Y1 = Z0 + NZ, Y0 + NY

HALO_F, HALO_V, HALO_G = 0, 8, 16
VEL = 24
FLUX_Y = 26
STAT_A = 28
STAT_X = 35
STAT_Z = 38
N_SEMS = 41


def lanes(u):
    return lax.broadcasted_iota(jnp.int32, u.shape, u.ndim - 1)


def at_next(u):
    moved = pltpu.roll(u, LN - 1, u.ndim - 1)
    return jnp.where(lanes(u) == LN - 1, pltpu.roll(moved, J - 1, u.ndim - 2), moved)


def at_prev(u):
    moved = pltpu.roll(u, 1, u.ndim - 1)
    return jnp.where(lanes(u) == 0, pltpu.roll(moved, 1, u.ndim - 2), moved)


def plane(g, slope_d, slope_a, slope_b):
    tilt_a = jnp.abs(slope_a) + TILT_FLOOR
    tilt_b = jnp.abs(slope_b) + TILT_FLOOR
    lo, hi = jnp.minimum(tilt_a, tilt_b), jnp.maximum(tilt_a, tilt_b)
    slope_d = jnp.where(jnp.abs(slope_d) < TINY, TINY, slope_d)
    tilt_d = jnp.abs(slope_d)
    m1, rest = jnp.minimum(lo, tilt_d), jnp.maximum(lo, tilt_d)
    m2, m3 = jnp.minimum(rest, hi), jnp.maximum(rest, hi)
    volume = jnp.clip(g, 0.0, 1.0)
    lesser = jnp.minimum(volume, 1.0 - volume)
    m12 = m1 * m2
    product = m12 * m3
    target = lesser * product
    both = target + target
    summed = lo + hi + tilt_d
    w = 0.5 * jnp.maximum(m1 + m2 - m3, 0.0)
    a = 0.5 * summed - (0.5 * product - target) / (m12 - w * w)
    for _ in range(NEWTON - 1):
        q0 = jnp.minimum(a, m1)
        r0 = a - q0
        p2 = jnp.maximum(a - m2, 0.0)
        q2 = jnp.minimum(p2, m1)
        r2 = p2 - q2
        p3 = jnp.maximum(a - m3, 0.0)
        s3 = p3 * p3
        value = q0 * (q0 * q0 * THIRD + a * r0) - q2 * (q2 * q2 * THIRD + p2 * r2) - s3 * (p3 * THIRD) - both
        rate = q0 * (a + r0) - q2 * (p2 + r2) - s3
        a = a - value / rate
    return jnp.where(volume > 0.5, summed - a, a), lo, hi, slope_d, 0.5 / product


def cube_part(s, h):
    p = jnp.maximum(s, 0.0)
    q = jnp.minimum(p, h)
    r = p - q
    return q * (q * q * THIRD + p * r)


def flow(offset, lo, hi, slope_d, scale, c):
    signed = c * slope_d
    h = jnp.abs(signed)
    s = offset - jnp.where(signed < 0, jnp.abs(slope_d) - h, 0.0)
    t = s - hi
    return scale * ((cube_part(s, h) - cube_part(s - lo, h)) - (cube_part(t, h) - cube_part(t - lo, h)))


def rows(ref, where):
    parts = [ref[z, pl.ds(y, n)] for z, y, n in where]
    return parts[0] if len(parts) == 1 else jnp.concatenate(parts, axis=0)


def put(ref, where, value):
    start = 0
    for z, y, n in where:
        ref[z, pl.ds(y, n)] = value[start : start + n]
        start += n


def moved(where, dz, dy):
    return [(z + dz, y + dy, n) for z, y, n in where]


def loop(first, last, body):
    def step(i, carry):
        body(i)
        return carry

    lax.fori_loop(first, last, step, 0)


def pipelined(count, where_of, *stages):
    depth = len(stages)

    def run(i, live):
        for store in reversed([stages[k](where_of(i - k)) for k in live]):
            store()

    for i in range(depth - 1):
        run(i, range(i + 1))
    loop(depth - 1, count, lambda i: run(i, range(depth)))
    for i in range(count, count + depth - 1):
        run(i, range(i - count + 1, depth))


def kernel(
    f_hbm, vx_hbm, vy_hbm, vz_hbm, out_hbm, dt_out,
    f_ext, g1_ext, g2_ext, vx, vy, vz, vx_diff, smooth, diff, sum_y, dif_y, sum_d,
    off, lo, hi, slope, scale, face, edge_y, stat_a, stat_x, stat_z, dt_vec, out_buf,
    load_sem, out_sem, send_sem, recv_sem,
):
    gy, gz = lax.axis_index("gy"), lax.axis_index("gz")
    chip_z, chip_x = gy // RING, lax.rem(gy, RING)

    def neighbour(dy, dz):
        return {"gy": lax.rem(gy + dy + N_GY, N_GY), "gz": lax.rem(gz + dz + N_GZ, N_GZ)}

    def along_x(k):
        return {"gy": chip_z * RING + lax.rem(chip_x + k, RING), "gz": gz}

    def along_z(k):
        return {"gy": lax.rem(chip_z + k, RING) * RING + chip_x, "gz": gz}

    corners = [(1, 1), (1, -1), (-1, 1), (-1, -1)]
    own_z, own_y = pl.ds(Z0, NZ), pl.ds(Y0, NY)

    loads = []
    for source, target in ((f_hbm, f_ext), (vx_hbm, vx), (vy_hbm, vy), (vz_hbm, vz)):
        for y in range(NY):
            semaphore = load_sem.at[len(loads)]
            loads.append(pltpu.make_async_copy(source.at[:, :, y, :], target.at[own_z, Y0 + y], semaphore))
    for copy in loads:
        copy.start()
    barrier = pltpu.get_barrier_semaphore()
    greeted = [neighbour(0, k) for k in range(1, N_GZ)]
    greeted += [neighbour(1, 0), neighbour(-1, 0)] + [neighbour(*c) for c in corners]
    greeted += [along_x(k) for k in range(1, RING)] + [along_z(k) for k in range(1, RING)]
    for device in greeted:
        pl.semaphore_signal(barrier, inc=1, device_id=device, device_id_type=pl.DeviceIdType.MESH)

    def remote(source, target, k, device):
        return pltpu.make_async_remote_copy(
            src_ref=source, dst_ref=target, send_sem=send_sem.at[k], recv_sem=recv_sem.at[k],
            device_id=device, device_id_type=pl.DeviceIdType.MESH,
        )

    def halo(g, base, wide_z, wide_y):
        from_z = {1: pl.ds(Z1 - wide_z, wide_z), -1: pl.ds(Z0, wide_z), 0: own_z}
        from_y = {1: pl.ds(Y1 - wide_y, wide_y), -1: pl.ds(Y0, wide_y), 0: own_y}
        to_z = {1: pl.ds(Z0 - wide_z, wide_z), -1: pl.ds(Z1, wide_z), 0: own_z}
        to_y = {1: pl.ds(Y0 - wide_y, wide_y), -1: pl.ds(Y1, wide_y), 0: own_y}
        return [
            remote(g.at[from_z[dz], from_y[dy]], g.at[to_z[dz], to_y[dy]], base + k, neighbour(dy, dz))
            for k, (dy, dz) in enumerate([(1, 0), (-1, 0), (0, 1), (0, -1)] + corners)
        ]

    sent = []

    def send(copies):
        for copy in copies:
            copy.start()
        sent.extend(copies)

    def arrive(copies):
        for copy in copies:
            copy.wait_recv()

    for copy in loads:
        copy.wait()

    def scan(i, found):
        z = i + Z0
        peak, total = found
        g = f_ext[z, own_y]
        own = jnp.maximum(jnp.abs(vx[z, own_y]), jnp.abs(vy[z, own_y]))
        return jnp.maximum(peak, jnp.maximum(own, jnp.abs(vz[z, own_y]))), total + g * (1.0 - g)

    zeros = jnp.zeros((NY, J, LN), F32)
    peak, total = lax.fori_loop(0, NZ, scan, (zeros, zeros))
    first_row = lax.broadcasted_iota(jnp.int32, (J, LN), 0) == 0

    def stat_tile(peak_rows, total_rows):
        return jnp.where(
            first_row,
            jnp.broadcast_to(jnp.max(peak_rows, axis=0, keepdims=True), (J, LN)),
            jnp.broadcast_to(jnp.sum(total_rows, axis=0, keepdims=True), (J, LN)),
        )

    def combined(ref, n):
        top, add = ref[0], ref[0]
        for k in range(1, n):
            top, add = jnp.maximum(top, ref[k]), add + ref[k]
        return jnp.where(first_row, top, add)

    stat_a[gz] = stat_tile(jnp.max(peak, axis=0), jnp.sum(total, axis=0))

    pl.semaphore_wait(barrier, len(greeted))
    halo_f = halo(f_ext, HALO_F, 2, 2)
    halo_v = halo(vx, HALO_V, 1, 1)
    stats_a = [
        remote(stat_a.at[gz], stat_a.at[gz], STAT_A + k - 1, neighbour(0, k)) for k in range(1, N_GZ)
    ]
    stats_x = [
        remote(stat_x.at[chip_x], stat_x.at[chip_x], STAT_X + k - 1, along_x(k)) for k in range(1, RING)
    ]
    stats_z = [
        remote(stat_z.at[chip_z], stat_z.at[chip_z], STAT_Z + k - 1, along_z(k)) for k in range(1, RING)
    ]
    velocity = [
        remote(vy.at[own_z, Y1 - 1], vy.at[own_z, Y0 - 1], VEL, neighbour(1, 0)),
        remote(vz.at[Z1 - 1, own_y], vz.at[Z0 - 1, own_y], VEL + 1, neighbour(0, 1)),
    ]
    send(stats_a)
    send(halo_f)

    def put_shifts(g, where):
        before, after = at_prev(g), at_next(g)
        put(smooth, where, before + 2.0 * g + after)
        put(diff, where, after - before)

    def shift_rows(g_ext, where):
        put_shifts(rows(g_ext, where), where)

    def put_sums(z, y, n):
        s = smooth[z, pl.ds(y - 1, n + 2)]
        d = diff[z, pl.ds(y - 1, n + 2)]
        where = [(z, y, n)]
        put(sum_y, where, s[:-2] + 2.0 * s[1:-1] + s[2:])
        put(dif_y, where, s[2:] - s[:-2])
        put(sum_d, where, d[:-2] + 2.0 * d[1:-1] + d[2:])

    planes = (off, lo, hi, slope, scale)

    def planes_of(g_ext, dim):
        def stage(where):
            below, above = moved(where, -1, 0), moved(where, 1, 0)
            along_z = rows(sum_y, above) - rows(sum_y, below)
            along_y = rows(dif_y, below) + 2.0 * rows(dif_y, where) + rows(dif_y, above)
            along_x = rows(sum_d, below) + 2.0 * rows(sum_d, where) + rows(sum_d, above)
            slopes = [along_z, along_y, along_x]
            across = [slopes[k] for k in range(3) if k != dim]
            g = rows(g_ext, where)

            def store():
                for ref, value in zip(planes, plane(g, slopes[dim], *across)):
                    put(ref, where, value)

            return store

        return stage

    def put_planes(g_ext, dim, where):
        planes_of(g_ext, dim)(where)()

    def donors_x(where):
        found = [rows(ref, where) for ref in planes]
        q = rows(vx, where)
        others = [at_next(value) for value in found]
        before = at_prev(q)

        def store():
            upward = q > 0
            others[-1] = -others[-1]
            for ref, value, other in zip(planes, found, others):
                put(ref, where, jnp.where(upward, value, other))
            put(vx_diff, where, q - before)

        return store

    def donors(upward, here, there):
        picked = [jnp.where(upward, rows(ref, here), rows(ref, there)) for ref in planes[:-1]]
        return picked + [jnp.where(upward, rows(scale, here), -rows(scale, there))]

    inner = (Y0 + 1, NY - 2)

    loop(0, NZ // 2, lambda i: shift_rows(f_ext, [(Z0 + 2 * i, Y0, NY), (Z0 + 2 * i + 1, Y0, NY)]))
    loop(Z0, Z1, lambda z: put_sums(z, *inner))
    pipelined(NZ - 2, lambda i: [(Z0 + 1 + i, *inner)], planes_of(f_ext, 2), donors_x)
    arrive(stats_a)
    stat_x[chip_x] = combined(stat_a, N_GZ)
    arrive(halo_f[:2])
    send(stats_x)
    send(halo_v)
    send(velocity)

    def shift_sides(i):
        z = Z0 + 2 * i
        shift_rows(f_ext, [(z, 0, 2), (z, Y1, 2), (z + 1, 0, 2), (z + 1, Y1, 2)])

    def shift_ends(i):
        z = i + (i // 2) * (EZ - 4)
        shift_rows(f_ext, [(z, 0, EY)])

    def sums_side(z):
        put_sums(z, 1, 2)
        put_sums(z, Y1 - 1, 2)

    loop(0, NZ // 2, shift_sides)
    arrive(halo_f[2:])
    loop(0, 4, shift_ends)
    loop(Z0, Z1, sums_side)
    loop(0, 4, lambda i: put_sums(i + (i // 2) * (EZ - 4), 1, EY - 2))
    arrive(stats_x)
    stat_z[chip_z] = combined(stat_x, RING)

    def sides(i):
        z = 1 + 2 * i
        return [(z, 1, 2), (z, Y1 - 1, 2), (z + 1, 1, 2), (z + 1, Y1 - 1, 2)]

    def ends(i):
        return [(1 + i + (i // 2) * (NZ - 2), *inner)]

    loop(0, 4, lambda i: put_planes(f_ext, 2, ends(i)))
    send(stats_z)
    arrive(halo_v)
    loop(0, 4, lambda i: donors_x(ends(i))())
    pipelined(NZ // 2 + 1, sides, planes_of(f_ext, 2), donors_x)
    arrive(stats_z)
    arrive(velocity)
    stats = combined(stat_z, RING)
    umax = jnp.max(stats[0:1], axis=1, keepdims=True)
    share = jnp.sum(stats[1:2], axis=1, keepdims=True) * (4.0 / (N_GZ * NZ * N_GY * NY * J * LN))
    step = COURANT / ((umax + EPSILON) * (1.0 + share))
    dt_vec[...] = jnp.broadcast_to(step, (J, LN))
    dt_out[0, 0] = jnp.max(step)

    def flow_x(where):
        found = [rows(ref, where) for ref in planes]
        q = rows(vx, where)
        return lambda: put(face, where, flow(*found, dt_vec[...] * q))

    def update_x(where):
        out = rows(face, where)
        before = at_prev(out)
        g, change = rows(f_ext, where), rows(vx_diff, where)
        return lambda: put(g1_ext, where, (g - out + before) / (1.0 - dt_vec[...] * change))

    def shifts_of(g_ext):
        def stage(where):
            g = rows(g_ext, where)
            before, after = at_prev(g), at_next(g)

            def store():
                put(smooth, where, before + 2.0 * g + after)
                put(diff, where, after - before)

            return store

        return stage

    x_stages = (flow_x, update_x, shifts_of(g1_ext))
    pipelined(NZ + 2, lambda i: [(1 + i, 1, 3), (1 + i, Y1 - 2, 3)], *x_stages)

    def sums_edge(z):
        put_sums(z, Y0, 1)
        put_sums(z, Y1 - 1, 1)

    def y_edge(i):
        z = Z0 + 2 * i
        return [(z, Y0, 1), (z, Y1 - 1, 1), (z + 1, Y0, 1), (z + 1, Y1 - 1, 1)]

    def half_faces_y(i):
        z = Z0 + 2 * i
        at_face = [(z, Y0 - 1, 1), (z, Y1 - 1, 1), (z + 1, Y0 - 1, 1), (z + 1, Y1 - 1, 1)]
        c = dt_vec[...] * rows(vy, at_face)
        out = flow(*[rows(ref, y_edge(i)) for ref in planes], c)
        for k in range(2):
            edge_y[0, 2 * i + k] = jnp.where(c[2 * k + 1] > 0, out[2 * k + 1], 0.0)
            edge_y[1, 2 * i + k] = jnp.where(c[2 * k] < 0, out[2 * k], 0.0)

    flux_y = [
        remote(edge_y.at[0], edge_y.at[2], FLUX_Y, neighbour(1, 0)),
        remote(edge_y.at[1], edge_y.at[3], FLUX_Y + 1, neighbour(-1, 0)),
    ]
    loop(Z0 - 1, Z1 + 1, sums_edge)
    loop(0, NZ // 2, lambda i: put_planes(g1_ext, 1, y_edge(i)))
    loop(0, NZ // 2, half_faces_y)
    send(flux_y)

    def middle(i):
        return [(1 + 2 * i, Y0 + 2, NY - 4), (2 + 2 * i, Y0 + 2, NY - 4)]

    def faces_y(z):
        c = dt_vec[...] * vy[z, pl.ds(Y0, NY - 1)]
        picked = donors(c > 0, [(z, Y0, NY - 1)], [(z, Y0 + 1, NY - 1)])
        put(face, [(z, Y0, NY - 1)], flow(*picked, c))

    pipelined(NZ // 2 + 1, middle, *x_stages)
    loop(Z0 - 1, Z1 + 1, lambda z: put_sums(z, *inner))
    loop(Z0, Z1, lambda z: put_planes(g1_ext, 1, [(z, *inner)]))
    loop(Z0, Z1, faces_y)
    arrive(flux_y)

    def update_y(z):
        face[z, Y0 - 1] = edge_y[2, z - Z0] - edge_y[1, z - Z0]
        face[z, Y1 - 1] = edge_y[0, z - Z0] - edge_y[3, z - Z0]
        out, q = face[z, pl.ds(Y0 - 1, NY + 1)], vy[z, pl.ds(Y0 - 1, NY + 1)]
        g2_ext[z, own_y] = (g1_ext[z, own_y] - out[1:] + out[:-1]) / (1.0 - dt_vec[...] * (q[1:] - q[:-1]))

    loop(Z0, Z1, update_y)
    halo_g = halo(g2_ext, HALO_G, 2, 1)

    def faces_z(where):
        c = dt_vec[...] * rows(vz, where)
        put(face, where, flow(*donors(c > 0, where, moved(where, 1, 0)), c))

    loop(0, 1, lambda i: shift_rows(g2_ext, [(Z0 + 2 * i, Y0, NY), (Z0 + 2 * i + 1, Y0, NY)]))
    send(halo_g)
    loop(1, NZ // 2, lambda i: shift_rows(g2_ext, [(Z0 + 2 * i, Y0, NY), (Z0 + 2 * i + 1, Y0, NY)]))
    loop(Z0, Z1, lambda z: put_sums(z, *inner))
    loop(Z0 + 1, Z1 - 1, lambda z: put_planes(g2_ext, 0, [(z, *inner)]))
    loop(Z0 + 1, Z1 - 2, lambda z: faces_z([(z, *inner)]))
    arrive(halo_g)

    def shift_sides_g(i):
        z = Z0 + 4 * i
        shift_rows(g2_ext, [w for k in range(4) for w in ((z + k, Y0 - 1, 1), (z + k, Y1, 1))])

    def z_sides(i):
        z = 1 + 2 * i
        return [(z, Y0, 1), (z, Y1 - 1, 1), (z + 1, Y0, 1), (z + 1, Y1 - 1, 1)]

    loop(0, NZ // 4, shift_sides_g)
    loop(0, 4, lambda i: shift_rows(g2_ext, [(i + (i // 2) * (EZ - 4), 1, EY - 2)]))
    loop(Z0, Z1, sums_edge)
    loop(0, 4, lambda i: put_sums(i + (i // 2) * (EZ - 4), Y0, NY))
    loop(0, NZ // 2 + 1, lambda i: put_planes(g2_ext, 0, z_sides(i)))
    loop(0, 4, lambda i: put_planes(g2_ext, 0, ends(i)))
    loop(0, NZ // 2, lambda i: faces_z(z_sides(i)))
    faces_z([(Z1 - 1, Y0, 1), (Z1 - 1, Y1 - 1, 1)])
    loop(0, 4, lambda i: faces_z([(1 + i + (i // 2) * (NZ - 3), *inner)]))

    def update_z(z):
        g = g2_ext[z, own_y] - face[z, own_y] + face[z - 1, own_y]
        out_buf[z - Z0] = g / (1.0 - dt_vec[...] * (vz[z, own_y] - vz[z - 1, own_y]))

    loop(Z0, Z1, update_z)
    stores = [
        pltpu.make_async_copy(out_buf.at[:, y], out_hbm.at[:, :, y, :], out_sem.at[y]) for y in range(NY)
    ]
    for copy in stores:
        copy.start()
    for copy in sent:
        copy.wait_send()
    for copy in stores:
        copy.wait()


def shards(*blocks):
    tiled = [b.reshape(NZ, NY, J, LN).transpose(0, 2, 1, 3) for b in blocks]
    row = (J, LN)
    ext = pltpu.VMEM((EZ, EY, *row), F32)
    anywhere = pl.BlockSpec(memory_space=pl.ANY)
    field, step = pl.pallas_call(
        kernel,
        out_shape=(jax.ShapeDtypeStruct((NZ, J, NY, LN), F32), jax.ShapeDtypeStruct((1, 1), F32)),
        in_specs=[anywhere] * 4,
        out_specs=(anywhere, pl.BlockSpec(memory_space=pltpu.SMEM)),
        scratch_shapes=[ext] * 18 + [
            pltpu.VMEM((4, NZ, *row), F32),
            pltpu.VMEM((N_GZ, *row), F32), pltpu.VMEM((RING, *row), F32), pltpu.VMEM((RING, *row), F32),
            pltpu.VMEM(row, F32), pltpu.VMEM((NZ, NY, *row), F32),
            pltpu.SemaphoreType.DMA((4 * NY,)), pltpu.SemaphoreType.DMA((NY,)),
            pltpu.SemaphoreType.DMA((N_SEMS,)), pltpu.SemaphoreType.DMA((N_SEMS,)),
        ],
        compiler_params=pltpu.CompilerParams(collective_id=0, has_side_effects=True),
        name="advect",
    )(*tiled)
    return field.transpose(0, 2, 1, 3).reshape(NZ, NY, J * LN), step.reshape(())


def solution(mesh):
    spec = P("gz", "gy", None)
    return jax.shard_map(shards, mesh=mesh, in_specs=(spec,) * 4, out_specs=(spec, P()), check_vma=False)
```

```python
import jax
import jax.numpy as jnp
from jax import lax
from jax.experimental import pallas as pl
from jax.experimental.pallas import tpu as pltpu
from jax.sharding import PartitionSpec as P

NEWTON = 5
TILT_FLOOR = 3.2
TINY = 1e-18
COURANT = 0.45
EPSILON = 1e-6
THIRD = 1.0 / 3.0

NZ, NY, J, LN = 16, 8, 8, 128
N_GY, N_GZ = 16, 8
RING = 4
F32 = jnp.float32

EZ, EY = NZ + 4, NY + 4
Z0, Y0 = 2, 2
Z1, Y1 = Z0 + NZ, Y0 + NY

HALO_F, HALO_V, HALO_G = 0, 8, 16
VEL = 24
FLUX_Y = 26
STAT_A = 28
STAT_X = 35
STAT_Z = 38
N_SEMS = 41


def lanes(u):
    return lax.broadcasted_iota(jnp.int32, u.shape, u.ndim - 1)


def at_next(u):
    moved = pltpu.roll(u, LN - 1, u.ndim - 1)
    return jnp.where(lanes(u) == LN - 1, pltpu.roll(moved, J - 1, u.ndim - 2), moved)


def at_prev(u):
    moved = pltpu.roll(u, 1, u.ndim - 1)
    return jnp.where(lanes(u) == 0, pltpu.roll(moved, 1, u.ndim - 2), moved)


def plane(g, slope_d, slope_a, slope_b):
    tilt_a = jnp.abs(slope_a) + TILT_FLOOR
    tilt_b = jnp.abs(slope_b) + TILT_FLOOR
    lo, hi = jnp.minimum(tilt_a, tilt_b), jnp.maximum(tilt_a, tilt_b)
    slope_d = jnp.where(jnp.abs(slope_d) < TINY, TINY, slope_d)
    tilt_d = jnp.abs(slope_d)
    m1, rest = jnp.minimum(lo, tilt_d), jnp.maximum(lo, tilt_d)
    m2, m3 = jnp.minimum(rest, hi), jnp.maximum(rest, hi)
    volume = jnp.clip(g, 0.0, 1.0)
    lesser = jnp.minimum(volume, 1.0 - volume)
    m12 = m1 * m2
    product = m12 * m3
    target = lesser * product
    both = target + target
    summed = lo + hi + tilt_d
    w = 0.5 * jnp.maximum(m1 + m2 - m3, 0.0)
    a = 0.5 * summed - (0.5 * product - target) / (m12 - w * w)
    for _ in range(NEWTON - 1):
        q0 = jnp.minimum(a, m1)
        r0 = a - q0
        p2 = jnp.maximum(a - m2, 0.0)
        q2 = jnp.minimum(p2, m1)
        r2 = p2 - q2
        p3 = jnp.maximum(a - m3, 0.0)
        s3 = p3 * p3
        value = q0 * (q0 * q0 * THIRD + a * r0) - q2 * (q2 * q2 * THIRD + p2 * r2) - s3 * (p3 * THIRD) - both
        rate = q0 * (a + r0) - q2 * (p2 + r2) - s3
        a = a - value / rate
    return jnp.where(volume > 0.5, summed - a, a), lo, hi, slope_d, 0.5 / product


def cube_part(s, h):
    p = jnp.maximum(s, 0.0)
    q = jnp.minimum(p, h)
    r = p - q
    return q * (q * q * THIRD + p * r)


def flow(offset, lo, hi, slope_d, scale, c):
    signed = c * slope_d
    h = jnp.abs(signed)
    s = offset - jnp.where(signed < 0, jnp.abs(slope_d) - h, 0.0)
    t = s - hi
    return scale * ((cube_part(s, h) - cube_part(s - lo, h)) - (cube_part(t, h) - cube_part(t - lo, h)))


def rows(ref, where):
    parts = [ref[z, pl.ds(y, n)] for z, y, n in where]
    return parts[0] if len(parts) == 1 else jnp.concatenate(parts, axis=0)


def put(ref, where, value):
    start = 0
    for z, y, n in where:
        ref[z, pl.ds(y, n)] = value[start : start + n]
        start += n


def moved(where, dz, dy):
    return [(z + dz, y + dy, n) for z, y, n in where]


def loop(first, last, body):
    def step(i, carry):
        body(i)
        return carry

    lax.fori_loop(first, last, step, 0)


def pipelined(count, where_of, *stages):
    depth = len(stages)

    def run(i, live):
        for store in reversed([stages[k](where_of(i - k)) for k in live]):
            store()

    for i in range(depth - 1):
        run(i, range(i + 1))
    loop(depth - 1, count, lambda i: run(i, range(depth)))
    for i in range(count, count + depth - 1):
        run(i, range(i - count + 1, depth))


def kernel(
    f_hbm, vx_hbm, vy_hbm, vz_hbm, out_hbm, dt_out,
    f_ext, g1_ext, g2_ext, vx, vy, vz, vx_diff, smooth, diff, sum_y, dif_y, sum_d,
    off, lo, hi, slope, scale, face, edge_y, stat_a, stat_x, stat_z, dt_vec, dt_cell, out_buf,
    load_sem, out_sem, send_sem, recv_sem,
):
    gy, gz = lax.axis_index("gy"), lax.axis_index("gz")
    chip_z, chip_x = gy // RING, lax.rem(gy, RING)

    def neighbour(dy, dz):
        return {"gy": lax.rem(gy + dy + N_GY, N_GY), "gz": lax.rem(gz + dz + N_GZ, N_GZ)}

    def along_x(k):
        return {"gy": chip_z * RING + lax.rem(chip_x + k, RING), "gz": gz}

    def along_z(k):
        return {"gy": lax.rem(chip_z + k, RING) * RING + chip_x, "gz": gz}

    corners = [(1, 1), (1, -1), (-1, 1), (-1, -1)]
    own_z, own_y = pl.ds(Z0, NZ), pl.ds(Y0, NY)

    loads = []
    for source, target in ((f_hbm, f_ext), (vx_hbm, vx), (vy_hbm, vy), (vz_hbm, vz)):
        for y in range(NY):
            semaphore = load_sem.at[len(loads)]
            loads.append(pltpu.make_async_copy(source.at[:, :, y, :], target.at[own_z, Y0 + y], semaphore))
    for copy in loads:
        copy.start()
    barrier = pltpu.get_barrier_semaphore()
    greeted = [neighbour(0, k) for k in range(1, N_GZ)]
    greeted += [neighbour(1, 0), neighbour(-1, 0)] + [neighbour(*c) for c in corners]
    greeted += [along_x(k) for k in range(1, RING)] + [along_z(k) for k in range(1, RING)]
    for device in greeted:
        pl.semaphore_signal(barrier, inc=1, device_id=device, device_id_type=pl.DeviceIdType.MESH)

    def remote(source, target, k, device):
        return pltpu.make_async_remote_copy(
            src_ref=source, dst_ref=target, send_sem=send_sem.at[k], recv_sem=recv_sem.at[k],
            device_id=device, device_id_type=pl.DeviceIdType.MESH,
        )

    def halo(g, base, wide_z, wide_y):
        from_z = {1: pl.ds(Z1 - wide_z, wide_z), -1: pl.ds(Z0, wide_z), 0: own_z}
        from_y = {1: pl.ds(Y1 - wide_y, wide_y), -1: pl.ds(Y0, wide_y), 0: own_y}
        to_z = {1: pl.ds(Z0 - wide_z, wide_z), -1: pl.ds(Z1, wide_z), 0: own_z}
        to_y = {1: pl.ds(Y0 - wide_y, wide_y), -1: pl.ds(Y1, wide_y), 0: own_y}
        return [
            remote(g.at[from_z[dz], from_y[dy]], g.at[to_z[dz], to_y[dy]], base + k, neighbour(dy, dz))
            for k, (dy, dz) in enumerate([(1, 0), (-1, 0), (0, 1), (0, -1)] + corners)
        ]

    sent = []

    def send(copies):
        for copy in copies:
            copy.start()
        sent.extend(copies)

    def arrive(copies):
        for copy in copies:
            copy.wait_recv()

    for copy in loads:
        copy.wait()

    def scan(i, found):
        z = i + Z0
        peak, total = found
        g = f_ext[z, own_y]
        own = jnp.maximum(jnp.abs(vx[z, own_y]), jnp.abs(vy[z, own_y]))
        return jnp.maximum(peak, jnp.maximum(own, jnp.abs(vz[z, own_y]))), total + g * (1.0 - g)

    zeros = jnp.zeros((NY, J, LN), F32)
    peak, total = lax.fori_loop(0, NZ, scan, (zeros, zeros))
    first_row = lax.broadcasted_iota(jnp.int32, (J, LN), 0) == 0

    def stat_tile(peak_rows, total_rows):
        return jnp.where(
            first_row,
            jnp.broadcast_to(jnp.max(peak_rows, axis=0, keepdims=True), (J, LN)),
            jnp.broadcast_to(jnp.sum(total_rows, axis=0, keepdims=True), (J, LN)),
        )

    def combined(ref, n):
        top, add = ref[0], ref[0]
        for k in range(1, n):
            top, add = jnp.maximum(top, ref[k]), add + ref[k]
        return jnp.where(first_row, top, add)

    stat_x[chip_x] = stat_tile(jnp.max(peak, axis=0), jnp.sum(total, axis=0))

    pl.semaphore_wait(barrier, len(greeted))
    halo_f = halo(f_ext, HALO_F, 2, 2)
    halo_v = halo(vx, HALO_V, 1, 1)
    stats_a = [
        remote(stat_a.at[gz], stat_a.at[gz], STAT_A + k - 1, neighbour(0, k)) for k in range(1, N_GZ)
    ]
    stats_x = [
        remote(stat_x.at[chip_x], stat_x.at[chip_x], STAT_X + k - 1, along_x(k)) for k in range(1, RING)
    ]
    stats_z = [
        remote(stat_z.at[chip_z], stat_z.at[chip_z], STAT_Z + k - 1, along_z(k)) for k in range(1, RING)
    ]
    velocity = [
        remote(vy.at[own_z, Y1 - 1], vy.at[own_z, Y0 - 1], VEL, neighbour(1, 0)),
        remote(vz.at[Z1 - 1, own_y], vz.at[Z0 - 1, own_y], VEL + 1, neighbour(0, 1)),
    ]
    send(stats_x)
    send(halo_f)
    send(halo_v)
    send(velocity)

    def put_shifts(g, where):
        before, after = at_prev(g), at_next(g)
        put(smooth, where, before + 2.0 * g + after)
        put(diff, where, after - before)

    def shift_rows(g_ext, where):
        put_shifts(rows(g_ext, where), where)

    def sums_of(z, y, n):
        s = smooth[z, pl.ds(y - 1, n + 2)]
        d = diff[z, pl.ds(y - 1, n + 2)]

        def store():
            where = [(z, y, n)]
            put(sum_y, where, s[:-2] + 2.0 * s[1:-1] + s[2:])
            put(dif_y, where, s[2:] - s[:-2])
            put(sum_d, where, d[:-2] + 2.0 * d[1:-1] + d[2:])

        return store

    def put_sums(z, y, n):
        sums_of(z, y, n)()

    planes = (off, lo, hi, slope, scale)

    def planes_of(g_ext, dim):
        def stage(where):
            below, above = moved(where, -1, 0), moved(where, 1, 0)
            along_z = rows(sum_y, above) - rows(sum_y, below)
            along_y = rows(dif_y, below) + 2.0 * rows(dif_y, where) + rows(dif_y, above)
            along_x = rows(sum_d, below) + 2.0 * rows(sum_d, where) + rows(sum_d, above)
            slopes = [along_z, along_y, along_x]
            across = [slopes[k] for k in range(3) if k != dim]
            g = rows(g_ext, where)

            def store():
                for ref, value in zip(planes, plane(g, slopes[dim], *across)):
                    put(ref, where, value)

            return store

        return stage

    def put_planes(g_ext, dim, where):
        planes_of(g_ext, dim)(where)()

    def donors_x(where):
        found = [rows(ref, where) for ref in planes]
        q = rows(vx, where)
        others = [at_next(value) for value in found]
        before = at_prev(q)

        def store():
            upward = q > 0
            others[-1] = -others[-1]
            for ref, value, other in zip(planes, found, others):
                put(ref, where, jnp.where(upward, value, other))
            put(vx_diff, where, q - before)

        return store

    def donors(upward, here, there):
        picked = [jnp.where(upward, rows(ref, here), rows(ref, there)) for ref in planes[:-1]]
        return picked + [jnp.where(upward, rows(scale, here), -rows(scale, there))]

    inner = (Y0 + 1, NY - 2)

    def x_inner(first, count):
        pipelined(count, lambda i: [(first + i, *inner)], planes_of(f_ext, 2), donors_x)

    loop(0, NZ // 2, lambda i: shift_rows(f_ext, [(Z0 + 2 * i, Y0, NY), (Z0 + 2 * i + 1, Y0, NY)]))
    loop(Z0, Z1, lambda z: put_sums(z, *inner))
    x_inner(Z0 + 1, 6)
    arrive(stats_x)
    stat_z[chip_z] = combined(stat_x, RING)
    x_inner(Z0 + 7, 2)
    send(stats_z)
    x_inner(Z0 + 9, NZ - 10)
    arrive(halo_f[:2])

    def shift_sides(i):
        z = Z0 + 2 * i
        shift_rows(f_ext, [(z, 0, 2), (z, Y1, 2), (z + 1, 0, 2), (z + 1, Y1, 2)])

    def shift_ends(i):
        z = i + (i // 2) * (EZ - 4)
        shift_rows(f_ext, [(z, 0, EY)])

    def sums_side(z):
        put_sums(z, 1, 2)
        put_sums(z, Y1 - 1, 2)

    loop(0, NZ // 2, shift_sides)
    arrive(halo_f[2:])
    loop(0, 4, shift_ends)
    loop(Z0, Z1, sums_side)
    loop(0, 4, lambda i: put_sums(i + (i // 2) * (EZ - 4), 1, EY - 2))
    def sides(i):
        z = 1 + 2 * i
        return [(z, 1, 2), (z, Y1 - 1, 2), (z + 1, 1, 2), (z + 1, Y1 - 1, 2)]

    def ends(i):
        return [(1 + i + (i // 2) * (NZ - 2), *inner)]

    arrive(stats_z)
    stat_a[gz] = combined(stat_z, RING)
    loop(0, 4, lambda i: put_planes(f_ext, 2, ends(i)))
    send(stats_a)
    arrive(halo_v)
    loop(0, 4, lambda i: donors_x(ends(i))())
    pipelined(NZ // 2 + 1, sides, planes_of(f_ext, 2), donors_x)
    arrive(stats_a)
    arrive(velocity)
    stats = combined(stat_a, N_GZ)
    umax = jnp.max(stats[0:1], axis=1, keepdims=True)
    share = jnp.sum(stats[1:2], axis=1, keepdims=True) * (4.0 / (N_GZ * NZ * N_GY * NY * J * LN))
    step = COURANT / ((umax + EPSILON) * (1.0 + share))
    dt_vec[...] = jnp.broadcast_to(step, (J, LN))
    dt_cell[...] = step

    def flow_x(where):
        found = [rows(ref, where) for ref in planes]
        q = rows(vx, where)
        return lambda: put(face, where, flow(*found, dt_vec[...] * q))

    def update_x(where):
        out = rows(face, where)
        before = at_prev(out)
        g, change = rows(f_ext, where), rows(vx_diff, where)
        return lambda: put(g1_ext, where, (g - out + before) / (1.0 - dt_vec[...] * change))

    def shifts_of(g_ext):
        def stage(where):
            g = rows(g_ext, where)
            before, after = at_prev(g), at_next(g)

            def store():
                put(smooth, where, before + 2.0 * g + after)
                put(diff, where, after - before)

            return store

        return stage

    dt_copy = pltpu.make_async_copy(dt_cell, dt_out, out_sem.at[NY])
    x_stages = (flow_x, update_x, shifts_of(g1_ext))
    pipelined(NZ + 2, lambda i: [(1 + i, 1, 3), (1 + i, Y1 - 2, 3)], *x_stages)

    dt_copy.start()

    def sums_edge(z):
        put_sums(z, Y0, 1)
        put_sums(z, Y1 - 1, 1)

    def y_edge(i):
        z = Z0 + 2 * i
        return [(z, Y0, 1), (z, Y1 - 1, 1), (z + 1, Y0, 1), (z + 1, Y1 - 1, 1)]

    def half_faces_y(i):
        z = Z0 + 2 * i
        at_face = [(z, Y0 - 1, 1), (z, Y1 - 1, 1), (z + 1, Y0 - 1, 1), (z + 1, Y1 - 1, 1)]
        c = dt_vec[...] * rows(vy, at_face)
        out = flow(*[rows(ref, y_edge(i)) for ref in planes], c)
        for k in range(2):
            edge_y[0, 2 * i + k] = jnp.where(c[2 * k + 1] > 0, out[2 * k + 1], 0.0)
            edge_y[1, 2 * i + k] = jnp.where(c[2 * k] < 0, out[2 * k], 0.0)

    flux_y = [
        remote(edge_y.at[0], edge_y.at[2], FLUX_Y, neighbour(1, 0)),
        remote(edge_y.at[1], edge_y.at[3], FLUX_Y + 1, neighbour(-1, 0)),
    ]
    loop(Z0 - 1, Z1 + 1, sums_edge)
    loop(0, NZ // 2, lambda i: put_planes(g1_ext, 1, y_edge(i)))
    loop(0, NZ // 2, half_faces_y)
    send(flux_y)

    def middle(i):
        return [(1 + 2 * i, Y0 + 2, NY - 4), (2 + 2 * i, Y0 + 2, NY - 4)]

    def faces_y(z):
        c = dt_vec[...] * vy[z, pl.ds(Y0, NY - 1)]
        picked = donors(c > 0, [(z, Y0, NY - 1)], [(z, Y0 + 1, NY - 1)])
        put(face, [(z, Y0, NY - 1)], flow(*picked, c))

    pipelined(NZ // 2 + 1, middle, *x_stages)
    loop(Z0 - 1, Z0 + 2, lambda z: put_sums(z, *inner))

    def y_inner(z):
        stores = planes_of(g1_ext, 1)([(z, *inner)]), sums_of(z + 2, *inner)
        for store in stores:
            store()

    loop(Z0, Z1 - 1, y_inner)
    put_planes(g1_ext, 1, [(Z1 - 1, *inner)])
    loop(Z0, Z1, faces_y)
    arrive(flux_y)

    def update_y(z):
        face[z, Y0 - 1] = edge_y[2, z - Z0] - edge_y[1, z - Z0]
        face[z, Y1 - 1] = edge_y[0, z - Z0] - edge_y[3, z - Z0]
        out, q = face[z, pl.ds(Y0 - 1, NY + 1)], vy[z, pl.ds(Y0 - 1, NY + 1)]
        g2_ext[z, own_y] = (g1_ext[z, own_y] - out[1:] + out[:-1]) / (1.0 - dt_vec[...] * (q[1:] - q[:-1]))

    loop(Z0, Z1, update_y)
    halo_g = halo(g2_ext, HALO_G, 2, 1)

    def faces_z(where):
        c = dt_vec[...] * rows(vz, where)
        put(face, where, flow(*donors(c > 0, where, moved(where, 1, 0)), c))

    shift_rows(g2_ext, [(Z0, Y0, NY), (Z0 + 1, Y0, NY)])
    send(halo_g)
    shift_rows(g2_ext, [(Z0 + 2, Y0, NY), (Z0 + 3, Y0, NY)])
    loop(Z0, Z0 + 3, lambda z: put_sums(z, *inner))

    def z_inner(z):
        stores = (
            shifts_of(g2_ext)([(z + 3, Y0, NY)]),
            planes_of(g2_ext, 0)([(z, *inner)]),
            sums_of(z + 2, *inner),
        )
        for store in reversed(stores):
            store()

    loop(Z0 + 1, Z1 - 3, z_inner)
    put_sums(Z1 - 1, *inner)
    loop(Z1 - 3, Z1 - 1, lambda z: put_planes(g2_ext, 0, [(z, *inner)]))
    loop(Z0 + 1, Z1 - 2, lambda z: faces_z([(z, *inner)]))
    arrive(halo_g)

    def shift_sides_g(i):
        z = Z0 + 4 * i
        shift_rows(g2_ext, [w for k in range(4) for w in ((z + k, Y0 - 1, 1), (z + k, Y1, 1))])

    def z_sides(i):
        z = 1 + 2 * i
        return [(z, Y0, 1), (z, Y1 - 1, 1), (z + 1, Y0, 1), (z + 1, Y1 - 1, 1)]

    loop(0, NZ // 4, shift_sides_g)
    loop(0, 4, lambda i: shift_rows(g2_ext, [(i + (i // 2) * (EZ - 4), 1, EY - 2)]))
    loop(Z0, Z1, sums_edge)
    loop(0, 4, lambda i: put_sums(i + (i // 2) * (EZ - 4), Y0, NY))
    loop(0, NZ // 2 + 1, lambda i: put_planes(g2_ext, 0, z_sides(i)))
    loop(0, 4, lambda i: put_planes(g2_ext, 0, ends(i)))
    loop(0, NZ // 2, lambda i: faces_z(z_sides(i)))
    faces_z([(Z1 - 1, Y0, 1), (Z1 - 1, Y1 - 1, 1)])
    loop(0, 4, lambda i: faces_z([(1 + i + (i // 2) * (NZ - 3), *inner)]))

    def update_z(z):
        g = g2_ext[z, own_y] - face[z, own_y] + face[z - 1, own_y]
        out_buf[z - Z0] = g / (1.0 - dt_vec[...] * (vz[z, own_y] - vz[z - 1, own_y]))

    loop(Z0, Z1, update_z)
    stores = [
        pltpu.make_async_copy(out_buf.at[:, y], out_hbm.at[:, :, y, :], out_sem.at[y]) for y in range(NY)
    ]
    for copy in stores:
        copy.start()
    for copy in sent:
        copy.wait_send()
    for copy in [*stores, dt_copy]:
        copy.wait()


def shards(*blocks):
    tiled = [b.reshape(NZ, NY, J, LN).transpose(0, 2, 1, 3) for b in blocks]
    row = (J, LN)
    ext = pltpu.VMEM((EZ, EY, *row), F32)
    anywhere = pl.BlockSpec(memory_space=pl.ANY)
    field, step = pl.pallas_call(
        kernel,
        out_shape=(jax.ShapeDtypeStruct((NZ, J, NY, LN), F32), jax.ShapeDtypeStruct((1, 1), F32)),
        in_specs=[anywhere] * 4,
        out_specs=(anywhere, anywhere),
        scratch_shapes=[ext] * 18 + [
            pltpu.VMEM((4, NZ, *row), F32),
            pltpu.VMEM((N_GZ, *row), F32), pltpu.VMEM((RING, *row), F32), pltpu.VMEM((RING, *row), F32),
            pltpu.VMEM(row, F32), pltpu.VMEM((1, 1), F32), pltpu.VMEM((NZ, NY, *row), F32),
            pltpu.SemaphoreType.DMA((4 * NY,)), pltpu.SemaphoreType.DMA((NY + 1,)),
            pltpu.SemaphoreType.DMA((N_SEMS,)), pltpu.SemaphoreType.DMA((N_SEMS,)),
        ],
        compiler_params=pltpu.CompilerParams(collective_id=0, has_side_effects=True),
        name="advect",
    )(*tiled)
    return field.transpose(0, 2, 1, 3).reshape(NZ, NY, J * LN), step.reshape(())


def solution(mesh):
    spec = P("gz", "gy", None)
    return jax.shard_map(shards, mesh=mesh, in_specs=(spec,) * 4, out_specs=(spec, P()), check_vma=False)
```

```python
import jax
import jax.numpy as jnp
from jax import lax
from jax.experimental import pallas as pl
from jax.experimental.pallas import tpu as pltpu
from jax.sharding import PartitionSpec as P

NEWTON = 5
TILT_FLOOR = 3.2
TINY = 1e-18
COURANT = 0.45
EPSILON = 1e-6
THIRD = 1.0 / 3.0

NZ, NY, J, LN = 16, 8, 8, 128
N_GY, N_GZ = 16, 8
F32 = jnp.float32

EZ, EY = NZ + 4, NY + 4
Z0, Y0 = 2, 2
Z1, Y1 = Z0 + NZ, Y0 + NY

HALO_F, HALO_V, HALO_G = 0, 8, 16
VEL = 24
FLUX_Y = 26
STAT_Y = 28
STAT_Z = STAT_Y + N_GY - 1
N_SEMS = STAT_Z + N_GZ - 1


def lanes(u):
    return lax.broadcasted_iota(jnp.int32, u.shape, u.ndim - 1)


def at_next(u):
    moved = pltpu.roll(u, LN - 1, u.ndim - 1)
    return jnp.where(lanes(u) == LN - 1, pltpu.roll(moved, J - 1, u.ndim - 2), moved)


def at_prev(u):
    moved = pltpu.roll(u, 1, u.ndim - 1)
    return jnp.where(lanes(u) == 0, pltpu.roll(moved, 1, u.ndim - 2), moved)


def plane(g, slope_d, slope_a, slope_b):
    tilt_a = jnp.abs(slope_a) + TILT_FLOOR
    tilt_b = jnp.abs(slope_b) + TILT_FLOOR
    lo, hi = jnp.minimum(tilt_a, tilt_b), jnp.maximum(tilt_a, tilt_b)
    slope_d = jnp.where(jnp.abs(slope_d) < TINY, TINY, slope_d)
    tilt_d = jnp.abs(slope_d)
    m1, rest = jnp.minimum(lo, tilt_d), jnp.maximum(lo, tilt_d)
    m2, m3 = jnp.minimum(rest, hi), jnp.maximum(rest, hi)
    lesser = jnp.maximum(jnp.minimum(g, 1.0 - g), 0.0)
    m12 = m1 * m2
    product = m12 * m3
    target = lesser * product
    both = target + target
    summed = lo + hi + tilt_d
    w = 0.5 * jnp.maximum(m1 + m2 - m3, 0.0)
    a = 0.5 * summed - (0.5 * product - target) / (m12 - w * w)
    for _ in range(NEWTON - 1):
        q0 = jnp.minimum(a, m1)
        r0 = a - q0
        p2 = jnp.maximum(a - m2, 0.0)
        q2 = jnp.minimum(p2, m1)
        r2 = p2 - q2
        p3 = jnp.maximum(a - m3, 0.0)
        s3 = p3 * p3
        value = q0 * (q0 * q0 * THIRD + a * r0) - q2 * (q2 * q2 * THIRD + p2 * r2) - s3 * (p3 * THIRD) - both
        rate = q0 * (a + r0) - q2 * (p2 + r2) - s3
        a = a - value / rate
    return jnp.where(g > 0.5, summed - a, a), lo, hi, slope_d, 0.5 / product


def cube_part(s, h):
    p = jnp.maximum(s, 0.0)
    q = jnp.minimum(p, h)
    r = p - q
    return q * (q * q * THIRD + p * r)


def flow(offset, lo, hi, slope_d, scale, c):
    signed = c * slope_d
    h = jnp.abs(signed)
    s = offset - jnp.where(signed < 0, jnp.abs(slope_d) - h, 0.0)
    t = s - hi
    return scale * ((cube_part(s, h) - cube_part(s - lo, h)) - (cube_part(t, h) - cube_part(t - lo, h)))


def rows(ref, where):
    parts = [ref[z, pl.ds(y, n)] for z, y, n in where]
    return parts[0] if len(parts) == 1 else jnp.concatenate(parts, axis=0)


def put(ref, where, value):
    start = 0
    for z, y, n in where:
        ref[z, pl.ds(y, n)] = value[start : start + n]
        start += n


def moved(where, dz, dy):
    return [(z + dz, y + dy, n) for z, y, n in where]


def loop(first, last, body):
    def step(i, carry):
        body(i)
        return carry

    lax.fori_loop(first, last, step, 0)


def pipelined(count, where_of, *stages):
    depth = len(stages)

    def run(i, live):
        for store in reversed([stages[k](where_of(i - k)) for k in live]):
            store()

    for i in range(depth - 1):
        run(i, range(i + 1))
    loop(depth - 1, count, lambda i: run(i, range(depth)))
    for i in range(count, count + depth - 1):
        run(i, range(i - count + 1, depth))


def kernel(
    f_hbm, vx_hbm, vy_hbm, vz_hbm, out_hbm, dt_out,
    f_ext, g1_ext, g2_ext, vx, vy, vz, vx_diff, smooth, diff, sum_y, dif_y, sum_d,
    off, lo, hi, slope, scale, face, edge_y, stat_y, stat_z, dt_vec, dt_cell, out_buf,
    load_sem, out_sem, send_sem, recv_sem,
):
    gy, gz = lax.axis_index("gy"), lax.axis_index("gz")

    def neighbour(dy, dz):
        return {"gy": lax.rem(gy + dy + N_GY, N_GY), "gz": lax.rem(gz + dz + N_GZ, N_GZ)}

    corners = [(1, 1), (1, -1), (-1, 1), (-1, -1)]
    own_z, own_y = pl.ds(Z0, NZ), pl.ds(Y0, NY)

    loads = []
    for source, target in ((f_hbm, f_ext), (vx_hbm, vx), (vy_hbm, vy), (vz_hbm, vz)):
        for y in range(NY):
            semaphore = load_sem.at[len(loads)]
            loads.append(pltpu.make_async_copy(source.at[:, :, y, :], target.at[own_z, Y0 + y], semaphore))
    for copy in loads:
        copy.start()
    barrier = pltpu.get_barrier_semaphore()
    greeted = [neighbour(0, k) for k in range(1, N_GZ)]
    greeted += [neighbour(k, 0) for k in range(1, N_GY)] + [neighbour(*c) for c in corners]
    for device in greeted:
        pl.semaphore_signal(barrier, inc=1, device_id=device, device_id_type=pl.DeviceIdType.MESH)

    def remote(source, target, k, device):
        return pltpu.make_async_remote_copy(
            src_ref=source, dst_ref=target, send_sem=send_sem.at[k], recv_sem=recv_sem.at[k],
            device_id=device, device_id_type=pl.DeviceIdType.MESH,
        )

    def halo(g, base, wide_z, wide_y):
        from_z = {1: pl.ds(Z1 - wide_z, wide_z), -1: pl.ds(Z0, wide_z), 0: own_z}
        from_y = {1: pl.ds(Y1 - wide_y, wide_y), -1: pl.ds(Y0, wide_y), 0: own_y}
        to_z = {1: pl.ds(Z0 - wide_z, wide_z), -1: pl.ds(Z1, wide_z), 0: own_z}
        to_y = {1: pl.ds(Y0 - wide_y, wide_y), -1: pl.ds(Y1, wide_y), 0: own_y}
        return [
            remote(g.at[from_z[dz], from_y[dy]], g.at[to_z[dz], to_y[dy]], base + k, neighbour(dy, dz))
            for k, (dy, dz) in enumerate([(1, 0), (-1, 0), (0, 1), (0, -1)] + corners)
        ]

    sent = []

    def send(copies):
        for copy in copies:
            copy.start()
        sent.extend(copies)

    def arrive(copies):
        for copy in copies:
            copy.wait_recv()

    for copy in loads:
        copy.wait()

    def scan(i, found):
        z = i + Z0
        peak, total = found
        g = f_ext[z, own_y]
        own = jnp.maximum(jnp.abs(vx[z, own_y]), jnp.abs(vy[z, own_y]))
        return jnp.maximum(peak, jnp.maximum(own, jnp.abs(vz[z, own_y]))), total + g * (1.0 - g)

    zeros = jnp.zeros((NY, J, LN), F32)
    peak, total = lax.fori_loop(0, NZ, scan, (zeros, zeros))
    top_row = lax.broadcasted_iota(jnp.int32, (2, LN), 0) == 0

    def combined(ref, n):
        top, add = ref[0], ref[0]
        for k in range(1, n):
            top, add = jnp.maximum(top, ref[k]), add + ref[k]
        return jnp.where(top_row, top, add)

    top, add = jnp.max(peak, axis=0), jnp.sum(total, axis=0)
    stat_y[gy] = jnp.concatenate([jnp.max(top, axis=0, keepdims=True), jnp.sum(add, axis=0, keepdims=True)], axis=0)

    pl.semaphore_wait(barrier, len(greeted))
    halo_f = halo(f_ext, HALO_F, 2, 2)
    halo_v = halo(vx, HALO_V, 1, 1)
    stats_y = [remote(stat_y.at[gy], stat_y.at[gy], STAT_Y + k - 1, neighbour(k, 0)) for k in range(1, N_GY)]
    stats_z = [remote(stat_z.at[gz], stat_z.at[gz], STAT_Z + k - 1, neighbour(0, k)) for k in range(1, N_GZ)]
    velocity = [
        remote(vy.at[own_z, Y1 - 1], vy.at[own_z, Y0 - 1], VEL, neighbour(1, 0)),
        remote(vz.at[Z1 - 1, own_y], vz.at[Z0 - 1, own_y], VEL + 1, neighbour(0, 1)),
    ]
    send(stats_y)
    send(halo_f)
    send(halo_v)
    send(velocity)

    def put_shifts(g, where):
        before, after = at_prev(g), at_next(g)
        put(smooth, where, before + 2.0 * g + after)
        put(diff, where, after - before)

    def shift_rows(g_ext, where):
        put_shifts(rows(g_ext, where), where)

    def sums_of(z, y, n):
        s = smooth[z, pl.ds(y - 1, n + 2)]
        d = diff[z, pl.ds(y - 1, n + 2)]

        def store():
            where = [(z, y, n)]
            put(sum_y, where, s[:-2] + 2.0 * s[1:-1] + s[2:])
            put(dif_y, where, s[2:] - s[:-2])
            put(sum_d, where, d[:-2] + 2.0 * d[1:-1] + d[2:])

        return store

    def put_sums(z, y, n):
        sums_of(z, y, n)()

    planes = (off, lo, hi, slope, scale)

    def planes_of(g_ext, dim):
        def stage(where):
            below, above = moved(where, -1, 0), moved(where, 1, 0)
            along_z = rows(sum_y, above) - rows(sum_y, below)
            along_y = rows(dif_y, below) + 2.0 * rows(dif_y, where) + rows(dif_y, above)
            along_x = rows(sum_d, below) + 2.0 * rows(sum_d, where) + rows(sum_d, above)
            slopes = [along_z, along_y, along_x]
            across = [slopes[k] for k in range(3) if k != dim]
            g = rows(g_ext, where)

            def store():
                for ref, value in zip(planes, plane(g, slopes[dim], *across)):
                    put(ref, where, value)

            return store

        return stage

    def put_planes(g_ext, dim, where):
        planes_of(g_ext, dim)(where)()

    def donors_x(where):
        found = [rows(ref, where) for ref in planes]
        q = rows(vx, where)
        others = [at_next(value) for value in found]
        before = at_prev(q)

        def store():
            upward = q > 0
            others[-1] = -others[-1]
            for ref, value, other in zip(planes, found, others):
                put(ref, where, jnp.where(upward, value, other))
            put(vx_diff, where, q - before)

        return store

    def donors(upward, here, there):
        picked = [jnp.where(upward, rows(ref, here), rows(ref, there)) for ref in planes[:-1]]
        return picked + [jnp.where(upward, rows(scale, here), -rows(scale, there))]

    inner = (Y0 + 1, NY - 2)

    def x_inner(first, count):
        pipelined(count, lambda i: [(first + i, *inner)], planes_of(f_ext, 2), donors_x)

    loop(0, NZ // 2, lambda i: shift_rows(f_ext, [(Z0 + 2 * i, Y0, NY), (Z0 + 2 * i + 1, Y0, NY)]))
    loop(Z0, Z1, lambda z: put_sums(z, *inner))
    x_inner(Z0 + 1, 9)
    arrive(stats_y)
    stat_z[gz] = combined(stat_y, N_GY)
    send(stats_z)
    x_inner(Z0 + 10, NZ - 11)
    arrive(halo_f[:2])

    def shift_sides(i):
        z = Z0 + 2 * i
        shift_rows(f_ext, [(z, 0, 2), (z, Y1, 2), (z + 1, 0, 2), (z + 1, Y1, 2)])

    def shift_ends(i):
        z = i + (i // 2) * (EZ - 4)
        shift_rows(f_ext, [(z, 0, EY)])

    def sums_side(z):
        put_sums(z, 1, 2)
        put_sums(z, Y1 - 1, 2)

    loop(0, NZ // 2, shift_sides)
    arrive(halo_f[2:])
    loop(0, 4, shift_ends)
    loop(Z0, Z1, sums_side)
    loop(0, 4, lambda i: put_sums(i + (i // 2) * (EZ - 4), 1, EY - 2))
    def sides(i):
        z = 1 + 2 * i
        return [(z, 1, 2), (z, Y1 - 1, 2), (z + 1, 1, 2), (z + 1, Y1 - 1, 2)]

    def ends(i):
        return [(1 + i + (i // 2) * (NZ - 2), *inner)]

    loop(0, 4, lambda i: put_planes(f_ext, 2, ends(i)))
    arrive(halo_v)
    loop(0, 4, lambda i: donors_x(ends(i))())
    pipelined(NZ // 2 + 1, sides, planes_of(f_ext, 2), donors_x)
    arrive(stats_z)
    arrive(velocity)
    stats = combined(stat_z, N_GZ)
    umax = jnp.max(stats[0:1], axis=1, keepdims=True)
    share = jnp.sum(stats[1:2], axis=1, keepdims=True) * (4.0 / (N_GZ * NZ * N_GY * NY * J * LN))
    step = COURANT / ((umax + EPSILON) * (1.0 + share))
    dt_vec[...] = jnp.broadcast_to(step, (J, LN))
    dt_cell[...] = step

    def flow_x(where):
        found = [rows(ref, where) for ref in planes]
        q = rows(vx, where)
        return lambda: put(face, where, flow(*found, dt_vec[...] * q))

    def update_x(where):
        out = rows(face, where)
        before = at_prev(out)
        g, change = rows(f_ext, where), rows(vx_diff, where)
        return lambda: put(g1_ext, where, (g - out + before) / (1.0 - dt_vec[...] * change))

    def shifts_of(g_ext):
        def stage(where):
            g = rows(g_ext, where)
            before, after = at_prev(g), at_next(g)

            def store():
                put(smooth, where, before + 2.0 * g + after)
                put(diff, where, after - before)

            return store

        return stage

    dt_copy = pltpu.make_async_copy(dt_cell, dt_out, out_sem.at[NY])
    x_stages = (flow_x, update_x, shifts_of(g1_ext))
    pipelined(
        NZ // 2 + 1,
        lambda i: [w for z in (1 + 2 * i, 2 + 2 * i) for w in ((z, 1, 3), (z, Y1 - 2, 3))],
        *x_stages,
    )

    dt_copy.start()

    def sums_edge(first, n):
        for z in range(n):
            put_sums(first + z, Y0, 1)
            put_sums(first + z, Y1 - 1, 1)

    def edges(first, n):
        return [w for k in range(n) for w in ((first + k, Y0, 1), (first + k, Y1 - 1, 1))]

    def half_faces_y(i):
        z = Z0 + 4 * i
        at_face = [w for k in range(4) for w in ((z + k, Y0 - 1, 1), (z + k, Y1 - 1, 1))]
        c = dt_vec[...] * rows(vy, at_face)
        out = flow(*[rows(ref, edges(z, 4)) for ref in planes], c)
        for k in range(4):
            edge_y[0, 4 * i + k] = jnp.where(c[2 * k + 1] > 0, out[2 * k + 1], 0.0)
            edge_y[1, 4 * i + k] = jnp.where(c[2 * k] < 0, out[2 * k], 0.0)

    flux_y = [
        remote(edge_y.at[0], edge_y.at[2], FLUX_Y, neighbour(1, 0)),
        remote(edge_y.at[1], edge_y.at[3], FLUX_Y + 1, neighbour(-1, 0)),
    ]
    loop(0, (NZ + 2) // 3, lambda i: sums_edge(Z0 - 1 + 3 * i, 3))
    loop(0, NZ // 4, lambda i: put_planes(g1_ext, 1, edges(Z0 + 4 * i, 4)))
    loop(0, NZ // 4, half_faces_y)
    send(flux_y)

    def middle(i):
        return [(1 + 3 * i + k, Y0 + 2, NY - 4) for k in range(3)]

    def faces_y(z):
        c = dt_vec[...] * vy[z, pl.ds(Y0, NY - 1)]
        picked = donors(c > 0, [(z, Y0, NY - 1)], [(z, Y0 + 1, NY - 1)])
        put(face, [(z, Y0, NY - 1)], flow(*picked, c))

    pipelined((NZ + 2) // 3, middle, *x_stages)
    loop(Z0 - 1, Z0 + 2, lambda z: put_sums(z, *inner))

    def y_inner(z):
        stores = planes_of(g1_ext, 1)([(z, *inner)]), sums_of(z + 2, *inner)
        for store in stores:
            store()

    loop(Z0, Z1 - 1, y_inner)
    put_planes(g1_ext, 1, [(Z1 - 1, *inner)])
    loop(Z0, Z1, faces_y)
    arrive(flux_y)

    def update_y(z):
        face[z, Y0 - 1] = edge_y[2, z - Z0] - edge_y[1, z - Z0]
        face[z, Y1 - 1] = edge_y[0, z - Z0] - edge_y[3, z - Z0]
        out, q = face[z, pl.ds(Y0 - 1, NY + 1)], vy[z, pl.ds(Y0 - 1, NY + 1)]
        g2_ext[z, own_y] = (g1_ext[z, own_y] - out[1:] + out[:-1]) / (1.0 - dt_vec[...] * (q[1:] - q[:-1]))

    loop(Z0, Z1, update_y)
    halo_g = halo(g2_ext, HALO_G, 2, 1)

    def faces_z(where):
        c = dt_vec[...] * rows(vz, where)
        put(face, where, flow(*donors(c > 0, where, moved(where, 1, 0)), c))

    shift_rows(g2_ext, [(Z0, Y0, NY), (Z0 + 1, Y0, NY)])
    send(halo_g)
    shift_rows(g2_ext, [(Z0 + 2, Y0, NY), (Z0 + 3, Y0, NY)])
    loop(Z0, Z0 + 3, lambda z: put_sums(z, *inner))

    def z_inner(z):
        stores = (
            shifts_of(g2_ext)([(z + 3, Y0, NY)]),
            planes_of(g2_ext, 0)([(z, *inner)]),
            sums_of(z + 2, *inner),
        )
        for store in reversed(stores):
            store()

    loop(Z0 + 1, Z1 - 3, z_inner)
    put_sums(Z1 - 1, *inner)
    loop(Z1 - 3, Z1 - 1, lambda z: put_planes(g2_ext, 0, [(z, *inner)]))
    loop(Z0 + 1, Z1 - 2, lambda z: faces_z([(z, *inner)]))
    arrive(halo_g[2:4])
    loop(0, 2, lambda i: shift_rows(g2_ext, [(i * Z1, Y0, NY), (i * Z1 + 1, Y0, NY)]))
    loop(0, 4, lambda i: put_sums(i + (i // 2) * (EZ - 4), *inner))
    loop(0, 4, lambda i: put_planes(g2_ext, 0, ends(i)))
    loop(0, 4, lambda i: faces_z([(1 + i + (i // 2) * (NZ - 3), *inner)]))
    arrive(halo_g[:2] + halo_g[4:])
    loop(0, 2, lambda i: shift_rows(
        g2_ext, [w for k in range(EZ // 2) for w in ((i * (EZ // 2) + k, Y0 - 1, 1), (i * (EZ // 2) + k, Y1, 1))]
    ))
    loop(0, EZ // 4, lambda i: sums_edge(4 * i, 4))
    loop(0, (NZ + 2) // 3, lambda i: put_planes(g2_ext, 0, edges(1 + 3 * i, 3)))
    loop(0, NZ // 3, lambda i: faces_z(edges(1 + 3 * i, 3)))
    faces_z(edges(Z1 - 2, 2))

    def update_z(z):
        g = g2_ext[z, own_y] - face[z, own_y] + face[z - 1, own_y]
        out_buf[z - Z0] = g / (1.0 - dt_vec[...] * (vz[z, own_y] - vz[z - 1, own_y]))

    loop(Z0, Z1, update_z)
    stores = [
        pltpu.make_async_copy(out_buf.at[:, y], out_hbm.at[:, :, y, :], out_sem.at[y]) for y in range(NY)
    ]
    for copy in stores:
        copy.start()
    for copy in sent:
        copy.wait_send()
    for copy in [*stores, dt_copy]:
        copy.wait()


def shards(*blocks):
    tiled = [b.reshape(NZ, NY, J, LN).transpose(0, 2, 1, 3) for b in blocks]
    row = (J, LN)
    ext = pltpu.VMEM((EZ, EY, *row), F32)
    anywhere = pl.BlockSpec(memory_space=pl.ANY)
    field, step = pl.pallas_call(
        kernel,
        out_shape=(jax.ShapeDtypeStruct((NZ, J, NY, LN), F32), jax.ShapeDtypeStruct((1, 1), F32)),
        in_specs=[anywhere] * 4,
        out_specs=(anywhere, anywhere),
        scratch_shapes=[ext] * 18 + [
            pltpu.VMEM((4, NZ, *row), F32),
            pltpu.VMEM((N_GY, 2, LN), F32), pltpu.VMEM((N_GZ, 2, LN), F32),
            pltpu.VMEM(row, F32), pltpu.VMEM((1, 1), F32), pltpu.VMEM((NZ, NY, *row), F32),
            pltpu.SemaphoreType.DMA((4 * NY,)), pltpu.SemaphoreType.DMA((NY + 1,)),
            pltpu.SemaphoreType.DMA((N_SEMS,)), pltpu.SemaphoreType.DMA((N_SEMS,)),
        ],
        compiler_params=pltpu.CompilerParams(collective_id=0, has_side_effects=True),
        name="advect",
    )(*tiled)
    return field.transpose(0, 2, 1, 3).reshape(NZ, NY, J * LN), step.reshape(())


def solution(mesh):
    spec = P("gz", "gy", None)
    return jax.shard_map(shards, mesh=mesh, in_specs=(spec,) * 4, out_specs=(spec, P()), check_vma=False)
```

```python
import jax
import jax.numpy as jnp
from jax import lax
from jax.experimental import pallas as pl
from jax.experimental.pallas import tpu as pltpu
from jax.sharding import PartitionSpec as P

NEWTON = 5
TILT_FLOOR = 3.2
TINY = 1e-18
COURANT = 0.45
EPSILON = 1e-6
THIRD = 1.0 / 3.0

NZ, NY, J, LN = 16, 8, 8, 128
N_GY, N_GZ = 16, 8
F32 = jnp.float32

EZ, EY = NZ + 4, NY + 4
Z0, Y0 = 2, 2
Z1, Y1 = Z0 + NZ, Y0 + NY

HALO_F, HALO_V, HALO_G = 0, 8, 16
VEL = 24
FLUX_Y = 26
STAT_Y = 30
STAT_Z = STAT_Y + N_GY - 1
N_SEMS = STAT_Z + N_GZ - 1


def lanes(u):
    return lax.broadcasted_iota(jnp.int32, u.shape, u.ndim - 1)


def at_next(u):
    moved = pltpu.roll(u, LN - 1, u.ndim - 1)
    return jnp.where(lanes(u) == LN - 1, pltpu.roll(moved, J - 1, u.ndim - 2), moved)


def at_prev(u):
    moved = pltpu.roll(u, 1, u.ndim - 1)
    return jnp.where(lanes(u) == 0, pltpu.roll(moved, 1, u.ndim - 2), moved)


def plane(g, slope_d, slope_a, slope_b):
    tilt_a = jnp.abs(slope_a) + TILT_FLOOR
    tilt_b = jnp.abs(slope_b) + TILT_FLOOR
    lo, hi = jnp.minimum(tilt_a, tilt_b), jnp.maximum(tilt_a, tilt_b)
    slope_d = jnp.where(jnp.abs(slope_d) < TINY, TINY, slope_d)
    tilt_d = jnp.abs(slope_d)
    m1, rest = jnp.minimum(lo, tilt_d), jnp.maximum(lo, tilt_d)
    m2, m3 = jnp.minimum(rest, hi), jnp.maximum(rest, hi)
    lesser = jnp.maximum(jnp.minimum(g, 1.0 - g), 0.0)
    m12 = m1 * m2
    product = m12 * m3
    target = lesser * product
    both = target + target
    summed = lo + hi + tilt_d
    w = 0.5 * jnp.maximum(m1 + m2 - m3, 0.0)
    a = 0.5 * summed - (0.5 * product - target) / (m12 - w * w)
    for _ in range(NEWTON - 1):
        q0 = jnp.minimum(a, m1)
        r0 = a - q0
        p2 = jnp.maximum(a - m2, 0.0)
        q2 = jnp.minimum(p2, m1)
        r2 = p2 - q2
        p3 = jnp.maximum(a - m3, 0.0)
        s3 = p3 * p3
        value = q0 * (q0 * q0 * THIRD + a * r0) - q2 * (q2 * q2 * THIRD + p2 * r2) - s3 * (p3 * THIRD) - both
        rate = q0 * (a + r0) - q2 * (p2 + r2) - s3
        a = a - value / rate
    return jnp.where(g > 0.5, summed - a, a), lo, hi, slope_d, 0.5 / product


def cube_part(s, h):
    p = jnp.maximum(s, 0.0)
    q = jnp.minimum(p, h)
    r = p - q
    return q * (q * q * THIRD + p * r)


def flow(offset, lo, hi, slope_d, scale, c):
    signed = c * slope_d
    h = jnp.abs(signed)
    s = offset - jnp.where(signed < 0, jnp.abs(slope_d) - h, 0.0)
    t = s - hi
    return scale * ((cube_part(s, h) - cube_part(s - lo, h)) - (cube_part(t, h) - cube_part(t - lo, h)))


def rows(ref, where):
    parts = [ref[z, pl.ds(y, n)] for z, y, n in where]
    return parts[0] if len(parts) == 1 else jnp.concatenate(parts, axis=0)


def put(ref, where, value):
    start = 0
    for z, y, n in where:
        ref[z, pl.ds(y, n)] = value[start : start + n]
        start += n


def moved(where, dz, dy):
    return [(z + dz, y + dy, n) for z, y, n in where]


def loop(first, last, body):
    def step(i, carry):
        body(i)
        return carry

    lax.fori_loop(first, last, step, 0)


def pipelined(count, where_of, *stages):
    depth = len(stages)

    def run(i, live):
        for store in reversed([stages[k](where_of(i - k)) for k in live]):
            store()

    for i in range(depth - 1):
        run(i, range(i + 1))
    loop(depth - 1, count, lambda i: run(i, range(depth)))
    for i in range(count, count + depth - 1):
        run(i, range(i - count + 1, depth))


def kernel(
    f_hbm, vx_hbm, vy_hbm, vz_hbm, out_ref, dt_out,
    f_ext, g1_ext, g2_ext, vx, vy, vz, vx_diff, smooth, diff, sum_y, dif_y, sum_d,
    off, lo, hi, slope, scale, face, edge_y, stat_y, stat_z, dt_vec, dt_cell,
    load_sem, out_sem, send_sem, recv_sem,
):
    gy, gz = lax.axis_index("gy"), lax.axis_index("gz")

    def neighbour(dy, dz):
        return {"gy": lax.rem(gy + dy + N_GY, N_GY), "gz": lax.rem(gz + dz + N_GZ, N_GZ)}

    corners = [(1, 1), (1, -1), (-1, 1), (-1, -1)]
    own_z, own_y = pl.ds(Z0, NZ), pl.ds(Y0, NY)

    loads = []
    for source, target in ((f_hbm, f_ext), (vx_hbm, vx), (vy_hbm, vy), (vz_hbm, vz)):
        for y in range(NY):
            semaphore = load_sem.at[len(loads)]
            loads.append(pltpu.make_async_copy(source.at[:, :, y, :], target.at[own_z, Y0 + y], semaphore))
    for copy in loads:
        copy.start()
    barrier = pltpu.get_barrier_semaphore()
    greeted = [neighbour(0, k) for k in range(1, N_GZ)]
    greeted += [neighbour(k, 0) for k in range(1, N_GY)] + [neighbour(*c) for c in corners]
    for device in greeted:
        pl.semaphore_signal(barrier, inc=1, device_id=device, device_id_type=pl.DeviceIdType.MESH)

    def remote(source, target, k, device):
        return pltpu.make_async_remote_copy(
            src_ref=source, dst_ref=target, send_sem=send_sem.at[k], recv_sem=recv_sem.at[k],
            device_id=device, device_id_type=pl.DeviceIdType.MESH,
        )

    def halo(g, base, wide_z, wide_y):
        from_z = {1: pl.ds(Z1 - wide_z, wide_z), -1: pl.ds(Z0, wide_z), 0: own_z}
        from_y = {1: pl.ds(Y1 - wide_y, wide_y), -1: pl.ds(Y0, wide_y), 0: own_y}
        to_z = {1: pl.ds(Z0 - wide_z, wide_z), -1: pl.ds(Z1, wide_z), 0: own_z}
        to_y = {1: pl.ds(Y0 - wide_y, wide_y), -1: pl.ds(Y1, wide_y), 0: own_y}
        return [
            remote(g.at[from_z[dz], from_y[dy]], g.at[to_z[dz], to_y[dy]], base + k, neighbour(dy, dz))
            for k, (dy, dz) in enumerate([(1, 0), (-1, 0), (0, 1), (0, -1)] + corners)
        ]

    sent = []

    def send(copies):
        for copy in copies:
            copy.start()
        sent.extend(copies)

    def arrive(copies):
        for copy in copies:
            copy.wait_recv()

    for copy in loads:
        copy.wait()

    def scan(i, found):
        z = i + Z0
        peak, total = found
        g = f_ext[z, own_y]
        own = jnp.maximum(jnp.abs(vx[z, own_y]), jnp.abs(vy[z, own_y]))
        return jnp.maximum(peak, jnp.maximum(own, jnp.abs(vz[z, own_y]))), total + g * (1.0 - g)

    zeros = jnp.zeros((NY, J, LN), F32)
    peak, total = lax.fori_loop(0, NZ, scan, (zeros, zeros))
    top_row = lax.broadcasted_iota(jnp.int32, (2, LN), 0) == 0

    def combined(ref, n):
        top, add = ref[0], ref[0]
        for k in range(1, n):
            top, add = jnp.maximum(top, ref[k]), add + ref[k]
        return jnp.where(top_row, top, add)

    top, add = jnp.max(peak, axis=0), jnp.sum(total, axis=0)
    stat_y[gy] = jnp.concatenate([jnp.max(top, axis=0, keepdims=True), jnp.sum(add, axis=0, keepdims=True)], axis=0)

    pl.semaphore_wait(barrier, len(greeted))
    halo_f = halo(f_ext, HALO_F, 2, 2)
    halo_v = halo(vx, HALO_V, 1, 1)
    stats_y = [remote(stat_y.at[gy], stat_y.at[gy], STAT_Y + k - 1, neighbour(k, 0)) for k in range(1, N_GY)]
    stats_z = [remote(stat_z.at[gz], stat_z.at[gz], STAT_Z + k - 1, neighbour(0, k)) for k in range(1, N_GZ)]
    velocity = [
        remote(vy.at[own_z, Y1 - 1], vy.at[own_z, Y0 - 1], VEL, neighbour(1, 0)),
        remote(vz.at[Z1 - 1, own_y], vz.at[Z0 - 1, own_y], VEL + 1, neighbour(0, 1)),
    ]
    send(stats_y)
    send(halo_f)
    send(halo_v)
    send(velocity)

    def put_shifts(g, where):
        before, after = at_prev(g), at_next(g)
        put(smooth, where, before + 2.0 * g + after)
        put(diff, where, after - before)

    def shift_rows(g_ext, where):
        put_shifts(rows(g_ext, where), where)

    def sums_of(z, y, n):
        s = smooth[z, pl.ds(y - 1, n + 2)]
        d = diff[z, pl.ds(y - 1, n + 2)]

        def store():
            where = [(z, y, n)]
            put(sum_y, where, s[:-2] + 2.0 * s[1:-1] + s[2:])
            put(dif_y, where, s[2:] - s[:-2])
            put(sum_d, where, d[:-2] + 2.0 * d[1:-1] + d[2:])

        return store

    def put_sums(z, y, n):
        sums_of(z, y, n)()

    planes = (off, lo, hi, slope, scale)

    def planes_of(g_ext, dim):
        def stage(where):
            below, above = moved(where, -1, 0), moved(where, 1, 0)
            along_z = rows(sum_y, above) - rows(sum_y, below)
            along_y = rows(dif_y, below) + 2.0 * rows(dif_y, where) + rows(dif_y, above)
            along_x = rows(sum_d, below) + 2.0 * rows(sum_d, where) + rows(sum_d, above)
            slopes = [along_z, along_y, along_x]
            across = [slopes[k] for k in range(3) if k != dim]
            g = rows(g_ext, where)

            def store():
                for ref, value in zip(planes, plane(g, slopes[dim], *across)):
                    put(ref, where, value)

            return store

        return stage

    def put_planes(g_ext, dim, where):
        planes_of(g_ext, dim)(where)()

    def donors_x(where):
        found = [rows(ref, where) for ref in planes]
        q = rows(vx, where)
        others = [at_next(value) for value in found]
        before = at_prev(q)

        def store():
            upward = q > 0
            others[-1] = -others[-1]
            for ref, value, other in zip(planes, found, others):
                put(ref, where, jnp.where(upward, value, other))
            put(vx_diff, where, q - before)

        return store

    def donors(upward, here, there):
        picked = [jnp.where(upward, rows(ref, here), rows(ref, there)) for ref in planes[:-1]]
        return picked + [jnp.where(upward, rows(scale, here), -rows(scale, there))]

    inner = (Y0 + 1, NY - 2)

    loop(0, NZ // 2, lambda i: shift_rows(f_ext, [(Z0 + 2 * i, Y0, NY), (Z0 + 2 * i + 1, Y0, NY)]))
    loop(Z0, Z1, lambda z: put_sums(z, *inner))
    pipelined(NZ - 2, lambda i: [(Z0 + 1 + i, *inner)], planes_of(f_ext, 2), donors_x)
    arrive(halo_f[:2])

    def shift_sides(i):
        z = Z0 + 4 * i
        shift_rows(f_ext, [w for k in range(4) for w in ((z + k, 0, 2), (z + k, Y1, 2))])

    def sums_side(z):
        put_sums(z, 1, 2)
        put_sums(z, Y1 - 1, 2)

    loop(0, NZ // 4, shift_sides)
    loop(Z0, Z1, sums_side)
    arrive(stats_y)
    stat_z[gz] = combined(stat_y, N_GY)
    send(stats_z)
    arrive(halo_f[2:])

    loop(0, 2, lambda i: shift_rows(f_ext, [(i * Z1, 0, EY), (i * Z1 + 1, 0, EY)]))
    loop(0, 4, lambda i: put_sums(i + (i // 2) * (EZ - 4), 1, EY - 2))

    def sides(i):
        high = i // (NZ // 3 + 1)
        z, y = 1 + 3 * (i - high * (NZ // 3 + 1)), 1 + high * (Y1 - 2)
        return [(z + k, y, 2) for k in range(3)]

    def ends(i):
        return [(1 + i + (i // 2) * (NZ - 2), *inner)]

    loop(0, 4, lambda i: put_planes(f_ext, 2, ends(i)))
    arrive(halo_v)
    loop(0, 4, lambda i: donors_x(ends(i))())
    pipelined(2 * (NZ // 3 + 1), sides, planes_of(f_ext, 2), donors_x)
    arrive(stats_z)
    arrive(velocity)
    stats = combined(stat_z, N_GZ)
    umax = jnp.max(stats[0:1], axis=1, keepdims=True)
    share = jnp.sum(stats[1:2], axis=1, keepdims=True) * (4.0 / (N_GZ * NZ * N_GY * NY * J * LN))
    step = COURANT / ((umax + EPSILON) * (1.0 + share))
    dt_vec[...] = jnp.broadcast_to(step, (J, LN))
    dt_cell[...] = step

    def flow_x(where):
        found = [rows(ref, where) for ref in planes]
        q = rows(vx, where)
        return lambda: put(face, where, flow(*found, dt_vec[...] * q))

    def update_x(where):
        out = rows(face, where)
        before = at_prev(out)
        g, change = rows(f_ext, where), rows(vx_diff, where)
        return lambda: put(g1_ext, where, (g - out + before) / (1.0 - dt_vec[...] * change))

    def shifts_of(g_ext):
        def stage(where):
            g = rows(g_ext, where)
            before, after = at_prev(g), at_next(g)

            def store():
                put(smooth, where, before + 2.0 * g + after)
                put(diff, where, after - before)

            return store

        return stage

    dt_copy = pltpu.make_async_copy(dt_cell, dt_out, out_sem)
    x_stages = (flow_x, update_x, shifts_of(g1_ext))
    pipelined(
        NZ // 2 + 1,
        lambda i: [w for z in (1 + 2 * i, 2 + 2 * i) for w in ((z, 1, 3), (z, Y1 - 2, 3))],
        *x_stages,
    )

    dt_copy.start()

    def sums_edge(first, n):
        for z in range(n):
            put_sums(first + z, Y0, 1)
            put_sums(first + z, Y1 - 1, 1)

    def edges(first, n):
        return [w for k in range(n) for w in ((first + k, Y0, 1), (first + k, Y1 - 1, 1))]

    def half_faces_y(i):
        z = Z0 + 4 * i
        at_face = [w for k in range(4) for w in ((z + k, Y0 - 1, 1), (z + k, Y1 - 1, 1))]
        c = dt_vec[...] * rows(vy, at_face)
        out = flow(*[rows(ref, edges(z, 4)) for ref in planes], c)
        for k in range(4):
            edge_y[0, 4 * i + k] = jnp.where(c[2 * k + 1] > 0, out[2 * k + 1], 0.0)
            edge_y[1, 4 * i + k] = jnp.where(c[2 * k] < 0, out[2 * k], 0.0)

    flux_y = []
    for k in range(2):
        part = pl.ds(k * (NZ // 2), NZ // 2)
        flux_y += [
            remote(edge_y.at[0, part], edge_y.at[2, part], FLUX_Y + 2 * k, neighbour(1, 0)),
            remote(edge_y.at[1, part], edge_y.at[3, part], FLUX_Y + 2 * k + 1, neighbour(-1, 0)),
        ]
    loop(0, (NZ + 2) // 3, lambda i: sums_edge(Z0 - 1 + 3 * i, 3))
    for k in range(2):
        loop(2 * k, 2 * k + 2, lambda i: put_planes(g1_ext, 1, edges(Z0 + 4 * i, 4)))
        loop(2 * k, 2 * k + 2, half_faces_y)
        send(flux_y[2 * k : 2 * k + 2])

    def middle(i):
        return [(1 + 3 * i + k, Y0 + 2, NY - 4) for k in range(3)]

    def faces_y(z):
        c = dt_vec[...] * vy[z, pl.ds(Y0, NY - 1)]
        picked = donors(c > 0, [(z, Y0, NY - 1)], [(z, Y0 + 1, NY - 1)])
        put(face, [(z, Y0, NY - 1)], flow(*picked, c))

    pipelined((NZ + 2) // 3, middle, *x_stages)
    loop(Z0 - 1, Z0 + 2, lambda z: put_sums(z, *inner))

    def y_inner(z):
        stores = planes_of(g1_ext, 1)([(z, *inner)]), sums_of(z + 2, *inner)
        for store in stores:
            store()

    loop(Z0, Z1 - 1, y_inner)
    put_planes(g1_ext, 1, [(Z1 - 1, *inner)])
    loop(Z0, Z1, faces_y)
    def update_y(where):
        before, q = moved(where, 0, -1), dt_vec[...]
        g = rows(g1_ext, where) - rows(face, where) + rows(face, before)
        put(g2_ext, where, g / (1.0 - q * (rows(vy, where) - rows(vy, before))))

    loop(Z0, Z1, lambda z: update_y([(z, *inner)]))
    arrive(flux_y)

    def update_y_edge(i):
        for k in range(4):
            z, at = Z0 + 4 * i + k, 4 * i + k
            face[z, Y0 - 1] = edge_y[2, at] - edge_y[1, at]
            face[z, Y1 - 1] = edge_y[0, at] - edge_y[3, at]
        update_y(edges(Z0 + 4 * i, 4))

    loop(0, NZ // 4, update_y_edge)
    halo_g = halo(g2_ext, HALO_G, 2, 1)

    def faces_z(where):
        c = dt_vec[...] * rows(vz, where)
        put(face, where, flow(*donors(c > 0, where, moved(where, 1, 0)), c))

    shift_rows(g2_ext, [(Z0, Y0, NY), (Z0 + 1, Y0, NY)])
    send(halo_g[:2] + halo_g[4:] + halo_g[2:4])
    shift_rows(g2_ext, [(Z0 + 2, Y0, NY), (Z0 + 3, Y0, NY)])
    loop(Z0, Z0 + 3, lambda z: put_sums(z, *inner))

    def z_inner(z):
        stores = (
            shifts_of(g2_ext)([(z + 3, Y0, NY)]),
            planes_of(g2_ext, 0)([(z, *inner)]),
            sums_of(z + 2, *inner),
        )
        for store in reversed(stores):
            store()

    loop(Z0 + 1, Z1 - 3, z_inner)
    put_sums(Z1 - 1, *inner)
    loop(Z1 - 3, Z1 - 1, lambda z: put_planes(g2_ext, 0, [(z, *inner)]))
    loop(Z0 + 1, Z1 - 2, lambda z: faces_z([(z, *inner)]))
    arrive(halo_g[2:4])
    loop(0, 2, lambda i: shift_rows(g2_ext, [(i * Z1, Y0, NY), (i * Z1 + 1, Y0, NY)]))
    loop(0, 4, lambda i: put_sums(i + (i // 2) * (EZ - 4), *inner))
    loop(0, 4, lambda i: put_planes(g2_ext, 0, ends(i)))
    loop(0, 4, lambda i: faces_z([(1 + i + (i // 2) * (NZ - 3), *inner)]))
    arrive(halo_g[:2] + halo_g[4:])
    loop(0, 2, lambda i: shift_rows(
        g2_ext, [w for k in range(EZ // 2) for w in ((i * (EZ // 2) + k, Y0 - 1, 1), (i * (EZ // 2) + k, Y1, 1))]
    ))
    loop(0, EZ // 4, lambda i: sums_edge(4 * i, 4))
    loop(0, (NZ + 2) // 3, lambda i: put_planes(g2_ext, 0, edges(1 + 3 * i, 3)))
    loop(0, NZ // 3, lambda i: faces_z(edges(1 + 3 * i, 3)))
    faces_z(edges(Z1 - 2, 2))

    def update_z(z):
        g = g2_ext[z, own_y] - face[z, own_y] + face[z - 1, own_y]
        g = g / (1.0 - dt_vec[...] * (vz[z, own_y] - vz[z - 1, own_y]))
        for y in range(NY):
            out_ref[z - Z0, :, y, :] = g[y]

    loop(Z0, Z1, update_z)
    for copy in sent:
        copy.wait_send()
    dt_copy.wait()


def shards(*blocks):
    tiled = [b.reshape(NZ, NY, J, LN).transpose(0, 2, 1, 3) for b in blocks]
    row = (J, LN)
    ext = pltpu.VMEM((EZ, EY, *row), F32)
    anywhere = pl.BlockSpec(memory_space=pl.ANY)
    field, step = pl.pallas_call(
        kernel,
        out_shape=(pltpu.VMEM((NZ, J, NY, LN), F32), jax.ShapeDtypeStruct((1, 1), F32)),
        in_specs=[anywhere] * 4,
        out_specs=(pl.BlockSpec(memory_space=pltpu.VMEM), anywhere),
        scratch_shapes=[ext] * 18 + [
            pltpu.VMEM((4, NZ, *row), F32),
            pltpu.VMEM((N_GY, 2, LN), F32), pltpu.VMEM((N_GZ, 2, LN), F32),
            pltpu.VMEM(row, F32), pltpu.VMEM((1, 1), F32),
            pltpu.SemaphoreType.DMA((4 * NY,)), pltpu.SemaphoreType.DMA(()),
            pltpu.SemaphoreType.DMA((N_SEMS,)), pltpu.SemaphoreType.DMA((N_SEMS,)),
        ],
        compiler_params=pltpu.CompilerParams(collective_id=0, has_side_effects=True),
        name="advect",
    )(*tiled)
    return field.transpose(0, 2, 1, 3).reshape(NZ, NY, J * LN), step.reshape(())


def solution(mesh):
    spec = P("gz", "gy", None)
    return jax.shard_map(shards, mesh=mesh, in_specs=(spec,) * 4, out_specs=(spec, P()), check_vma=False)
```

```python
import jax
import jax.numpy as jnp
from jax import lax
from jax.experimental import pallas as pl
from jax.experimental.pallas import tpu as pltpu
from jax.sharding import PartitionSpec as P

NEWTON = 5
TILT_FLOOR = 3.2
TINY = 1e-18
COURANT = 0.45
EPSILON = 1e-6
THIRD = 1.0 / 3.0

NZ, NY, J, LN = 16, 8, 8, 128
N_GY, N_GZ = 16, 8
F32 = jnp.float32

EZ, EY = NZ + 4, NY + 4
Z0, Y0 = 2, 2
Z1, Y1 = Z0 + NZ, Y0 + NY

HALO_F, HALO_V, HALO_G, VEL, FLUX, STAT_Y, STAT_Z = range(7)
HALO_F_FAR, HALO_G_NEAR = 7, 8
N_SEND, N_RECV = 7, 9


def lanes(u):
    return lax.broadcasted_iota(jnp.int32, u.shape, u.ndim - 1)


def at_next(u):
    moved = pltpu.roll(u, LN - 1, u.ndim - 1)
    return jnp.where(lanes(u) == LN - 1, pltpu.roll(moved, J - 1, u.ndim - 2), moved)


def at_prev(u):
    moved = pltpu.roll(u, 1, u.ndim - 1)
    return jnp.where(lanes(u) == 0, pltpu.roll(moved, 1, u.ndim - 2), moved)


def plane(g, slope_d, slope_a, slope_b):
    tilt_a = jnp.abs(slope_a) + TILT_FLOOR
    tilt_b = jnp.abs(slope_b) + TILT_FLOOR
    lo, hi = jnp.minimum(tilt_a, tilt_b), jnp.maximum(tilt_a, tilt_b)
    slope_d = jnp.where(jnp.abs(slope_d) < TINY, TINY, slope_d)
    tilt_d = jnp.abs(slope_d)
    m1, rest = jnp.minimum(lo, tilt_d), jnp.maximum(lo, tilt_d)
    m2, m3 = jnp.minimum(rest, hi), jnp.maximum(rest, hi)
    lesser = jnp.maximum(jnp.minimum(g, 1.0 - g), 0.0)
    m12 = m1 * m2
    product = m12 * m3
    target = lesser * product
    both = target + target
    summed = lo + hi + tilt_d
    w = 0.5 * jnp.maximum(m1 + m2 - m3, 0.0)
    a = 0.5 * summed - (0.5 * product - target) / (m12 - w * w)
    for _ in range(NEWTON - 1):
        q0 = jnp.minimum(a, m1)
        r0 = a - q0
        p2 = jnp.maximum(a - m2, 0.0)
        q2 = jnp.minimum(p2, m1)
        r2 = p2 - q2
        p3 = jnp.maximum(a - m3, 0.0)
        s3 = p3 * p3
        value = q0 * (q0 * q0 * THIRD + a * r0) - q2 * (q2 * q2 * THIRD + p2 * r2) - s3 * (p3 * THIRD) - both
        rate = q0 * (a + r0) - q2 * (p2 + r2) - s3
        a = a - value / rate
    return jnp.where(g > 0.5, summed - a, a), lo, hi, slope_d, 0.5 / product


def cube_part(s, h):
    p = jnp.maximum(s, 0.0)
    q = jnp.minimum(p, h)
    r = p - q
    return q * (q * q * THIRD + p * r)


def flow(offset, lo, hi, slope_d, scale, c):
    signed = c * slope_d
    h = jnp.abs(signed)
    s = offset - jnp.where(signed < 0, jnp.abs(slope_d) - h, 0.0)
    t = s - hi
    return scale * ((cube_part(s, h) - cube_part(s - lo, h)) - (cube_part(t, h) - cube_part(t - lo, h)))


def rows(ref, where):
    parts = [ref[z, pl.ds(y, n)] for z, y, n in where]
    return parts[0] if len(parts) == 1 else jnp.concatenate(parts, axis=0)


def put(ref, where, value):
    start = 0
    for z, y, n in where:
        ref[z, pl.ds(y, n)] = value[start : start + n]
        start += n


def moved(where, dz, dy):
    return [(z + dz, y + dy, n) for z, y, n in where]


def loop(first, last, body):
    def step(i, carry):
        body(i)
        return carry

    lax.fori_loop(first, last, step, 0)


def pipelined(count, where_of, *stages):
    depth = len(stages)

    def run(i, live):
        for store in reversed([stages[k](where_of(i - k)) for k in live]):
            store()

    for i in range(depth - 1):
        run(i, range(i + 1))
    loop(depth - 1, count, lambda i: run(i, range(depth)))
    for i in range(count, count + depth - 1):
        run(i, range(i - count + 1, depth))


def kernel(
    f_hbm, vx_hbm, vy_hbm, vz_hbm, out_ref, dt_out,
    f_ext, g1_ext, g2_ext, vx, vy, vz, vx_diff, smooth, diff, sum_y, dif_y, sum_d,
    off, lo, hi, slope, scale, face, edge_y, stat_y, stat_z, dt_vec, dt_cell,
    load_sem, out_sem, send_sem, recv_sem,
):
    gy, gz = lax.axis_index("gy"), lax.axis_index("gz")

    def neighbour(dy, dz):
        return {"gy": lax.rem(gy + dy + N_GY, N_GY), "gz": lax.rem(gz + dz + N_GZ, N_GZ)}

    corners = [(1, 1), (1, -1), (-1, 1), (-1, -1)]
    own_z, own_y = pl.ds(Z0, NZ), pl.ds(Y0, NY)

    arrays = [(f_hbm, f_ext), (vx_hbm, vx), (vy_hbm, vy), (vz_hbm, vz)]
    for k, (source, target) in enumerate(arrays):
        for y in range(NY):
            pltpu.make_async_copy(source.at[:, :, y, :], target.at[own_z, Y0 + y], load_sem.at[k]).start()
    barrier = pltpu.get_barrier_semaphore()
    greeted = [neighbour(0, k) for k in range(1, N_GZ)]
    greeted += [neighbour(k, 0) for k in range(1, N_GY)] + [neighbour(*c) for c in corners]
    for device in greeted:
        pl.semaphore_signal(barrier, inc=1, device_id=device, device_id_type=pl.DeviceIdType.MESH)

    def remote(source, target, sends, receives, device):
        return pltpu.make_async_remote_copy(
            src_ref=source, dst_ref=target, send_sem=send_sem.at[sends], recv_sem=recv_sem.at[receives],
            device_id=device, device_id_type=pl.DeviceIdType.MESH,
        )

    def halo(g, sends, receives, wide_z, wide_y):
        from_z = {1: pl.ds(Z1 - wide_z, wide_z), -1: pl.ds(Z0, wide_z), 0: own_z}
        from_y = {1: pl.ds(Y1 - wide_y, wide_y), -1: pl.ds(Y0, wide_y), 0: own_y}
        to_z = {1: pl.ds(Z0 - wide_z, wide_z), -1: pl.ds(Z1, wide_z), 0: own_z}
        to_y = {1: pl.ds(Y0 - wide_y, wide_y), -1: pl.ds(Y1, wide_y), 0: own_y}
        return [
            remote(g.at[from_z[dz], from_y[dy]], g.at[to_z[dz], to_y[dy]], sends, receives[k], neighbour(dy, dz))
            for k, (dy, dz) in enumerate([(1, 0), (-1, 0), (0, 1), (0, -1)] + corners)
        ]

    def send(copies):
        for copy in copies:
            copy.start()

    def arrive(part, receives):
        remote(part, part, 0, receives, neighbour(1, 0)).wait_recv()

    def left(part, sends):
        remote(part, part, sends, 0, neighbour(1, 0)).wait_send()

    def some(ref, z, y):
        return ref.at[pl.ds(0, z), pl.ds(0, y)]

    for k, (source, target) in enumerate(arrays):
        pltpu.make_async_copy(source, target.at[own_z, own_y], load_sem.at[k]).wait()

    def scan(i, found):
        z = i + Z0
        peak, total = found
        g = f_ext[z, own_y]
        own = jnp.maximum(jnp.abs(vx[z, own_y]), jnp.abs(vy[z, own_y]))
        return jnp.maximum(peak, jnp.maximum(own, jnp.abs(vz[z, own_y]))), total + g * (1.0 - g)

    zeros = jnp.zeros((NY, J, LN), F32)
    peak, total = lax.fori_loop(0, NZ, scan, (zeros, zeros))
    top_row = lax.broadcasted_iota(jnp.int32, (2, LN), 0) == 0

    def combined(ref, n):
        top, add = ref[0], ref[0]
        for k in range(1, n):
            top, add = jnp.maximum(top, ref[k]), add + ref[k]
        return jnp.where(top_row, top, add)

    top, add = jnp.max(peak, axis=0), jnp.sum(total, axis=0)
    stat_y[gy] = jnp.concatenate([jnp.max(top, axis=0, keepdims=True), jnp.sum(add, axis=0, keepdims=True)], axis=0)

    pl.semaphore_wait(barrier, len(greeted))
    halo_f = halo(f_ext, HALO_F, 2 * [HALO_F] + 6 * [HALO_F_FAR], 2, 2)
    halo_v = halo(vx, HALO_V, 8 * [HALO_V], 1, 1)
    stats_y = [remote(stat_y.at[gy], stat_y.at[gy], STAT_Y, STAT_Y, neighbour(k, 0)) for k in range(1, N_GY)]
    stats_z = [remote(stat_z.at[gz], stat_z.at[gz], STAT_Z, STAT_Z, neighbour(0, k)) for k in range(1, N_GZ)]
    velocity = [
        remote(vy.at[own_z, Y1 - 1], vy.at[own_z, Y0 - 1], VEL, VEL, neighbour(1, 0)),
        remote(vz.at[Z1 - 1, own_y], vz.at[Z0 - 1, own_y], VEL, VEL, neighbour(0, 1)),
    ]
    send(stats_y)
    send(halo_f)

    def put_shifts(g, where):
        before, after = at_prev(g), at_next(g)
        put(smooth, where, before + 2.0 * g + after)
        put(diff, where, after - before)

    def shift_rows(g_ext, where):
        put_shifts(rows(g_ext, where), where)

    def sums_of(z, y, n):
        s = smooth[z, pl.ds(y - 1, n + 2)]
        d = diff[z, pl.ds(y - 1, n + 2)]

        def store():
            where = [(z, y, n)]
            put(sum_y, where, s[:-2] + 2.0 * s[1:-1] + s[2:])
            put(dif_y, where, s[2:] - s[:-2])
            put(sum_d, where, d[:-2] + 2.0 * d[1:-1] + d[2:])

        return store

    def put_sums(z, y, n):
        sums_of(z, y, n)()

    planes = (off, lo, hi, slope, scale)

    def planes_of(g_ext, dim):
        def stage(where):
            below, above = moved(where, -1, 0), moved(where, 1, 0)
            along_z = rows(sum_y, above) - rows(sum_y, below)
            along_y = rows(dif_y, below) + 2.0 * rows(dif_y, where) + rows(dif_y, above)
            along_x = rows(sum_d, below) + 2.0 * rows(sum_d, where) + rows(sum_d, above)
            slopes = [along_z, along_y, along_x]
            across = [slopes[k] for k in range(3) if k != dim]
            g = rows(g_ext, where)

            def store():
                for ref, value in zip(planes, plane(g, slopes[dim], *across)):
                    put(ref, where, value)

            return store

        return stage

    def put_planes(g_ext, dim, where):
        planes_of(g_ext, dim)(where)()

    def donors_x(where):
        found = [rows(ref, where) for ref in planes]
        q = rows(vx, where)
        others = [at_next(value) for value in found]
        before = at_prev(q)

        def store():
            upward = q > 0
            others[-1] = -others[-1]
            for ref, value, other in zip(planes, found, others):
                put(ref, where, jnp.where(upward, value, other))
            put(vx_diff, where, q - before)

        return store

    def donors(upward, here, there):
        picked = [jnp.where(upward, rows(ref, here), rows(ref, there)) for ref in planes[:-1]]
        return picked + [jnp.where(upward, rows(scale, here), -rows(scale, there))]

    inner = (Y0 + 1, NY - 2)

    loop(0, NZ // 2, lambda i: shift_rows(f_ext, [(Z0 + 2 * i, Y0, NY), (Z0 + 2 * i + 1, Y0, NY)]))
    loop(Z0, Z1, lambda z: put_sums(z, *inner))
    pipelined(NZ - 2, lambda i: [(Z0 + 1 + i, *inner)], planes_of(f_ext, 2), donors_x)
    send(halo_v)
    arrive(some(f_ext, NZ, 4), HALO_F)

    def shift_sides(i):
        z = Z0 + 4 * i
        shift_rows(f_ext, [w for k in range(4) for w in ((z + k, 0, 2), (z + k, Y1, 2))])

    def sums_side(z):
        put_sums(z, 1, 2)
        put_sums(z, Y1 - 1, 2)

    loop(0, NZ // 4, shift_sides)
    loop(Z0, Z1, sums_side)
    arrive(stat_y.at[pl.ds(0, N_GY - 1)], STAT_Y)
    stat_z[gz] = combined(stat_y, N_GY)
    send(stats_z)
    send(velocity)
    arrive(some(f_ext, 12, 4), HALO_F_FAR)

    loop(0, 2, lambda i: shift_rows(f_ext, [(i * Z1, 0, EY), (i * Z1 + 1, 0, EY)]))
    loop(0, 4, lambda i: put_sums(i + (i // 2) * (EZ - 4), 1, EY - 2))

    def sides(i):
        high = i // (NZ // 3 + 1)
        z, y = 1 + 3 * (i - high * (NZ // 3 + 1)), 1 + high * (Y1 - 2)
        return [(z + k, y, 2) for k in range(3)]

    def ends(i):
        return [(1 + i + (i // 2) * (NZ - 2), *inner)]

    loop(0, 4, lambda i: put_planes(f_ext, 2, ends(i)))
    arrive(some(vx, 13, 4), HALO_V)
    loop(0, 2, lambda i: donors_x([(1 + i * NZ + k, *inner) for k in range(2)])())
    pipelined(2 * (NZ // 3 + 1), sides, planes_of(f_ext, 2), donors_x)
    arrive(stat_z.at[pl.ds(0, N_GZ - 1)], STAT_Z)
    stats = combined(stat_z, N_GZ)
    umax = jnp.max(stats[0:1], axis=1, keepdims=True)
    share = jnp.sum(stats[1:2], axis=1, keepdims=True) * (4.0 / (N_GZ * NZ * N_GY * NY * J * LN))
    step = COURANT / ((umax + EPSILON) * (1.0 + share))
    dt_vec[...] = jnp.broadcast_to(step, (J, LN))
    dt_cell[...] = step

    def flow_x(where):
        found = [rows(ref, where) for ref in planes]
        q = rows(vx, where)
        return lambda: put(face, where, flow(*found, dt_vec[...] * q))

    def update_x(where):
        out = rows(face, where)
        before = at_prev(out)
        g, change = rows(f_ext, where), rows(vx_diff, where)
        return lambda: put(g1_ext, where, (g - out + before) / (1.0 - dt_vec[...] * change))

    def shifts_of(g_ext):
        def stage(where):
            g = rows(g_ext, where)
            before, after = at_prev(g), at_next(g)

            def store():
                put(smooth, where, before + 2.0 * g + after)
                put(diff, where, after - before)

            return store

        return stage

    dt_copy = pltpu.make_async_copy(dt_cell, dt_out, out_sem)
    x_stages = (flow_x, update_x, shifts_of(g1_ext))
    pipelined(
        NZ // 2 + 1,
        lambda i: [w for z in (1 + 2 * i, 2 + 2 * i) for w in ((z, 1, 3), (z, Y1 - 2, 3))],
        *x_stages,
    )

    dt_copy.start()

    def sums_edge(first, n):
        for z in range(n):
            put_sums(first + z, Y0, 1)
            put_sums(first + z, Y1 - 1, 1)

    def edges(first, n):
        return [w for k in range(n) for w in ((first + k, Y0, 1), (first + k, Y1 - 1, 1))]

    def half_faces_y(i):
        z = Z0 + 4 * i
        at_face = [w for k in range(4) for w in ((z + k, Y0 - 1, 1), (z + k, Y1 - 1, 1))]
        c = dt_vec[...] * rows(vy, at_face)
        out = flow(*[rows(ref, edges(z, 4)) for ref in planes], c)
        for k in range(4):
            edge_y[0, 4 * i + k] = jnp.where(c[2 * k + 1] > 0, out[2 * k + 1], 0.0)
            edge_y[1, 4 * i + k] = jnp.where(c[2 * k] < 0, out[2 * k], 0.0)

    flux_y = []
    for k in range(2):
        part = pl.ds(k * (NZ // 2), NZ // 2)
        flux_y += [
            remote(edge_y.at[0, part], edge_y.at[2, part], FLUX, FLUX, neighbour(1, 0)),
            remote(edge_y.at[1, part], edge_y.at[3, part], FLUX, FLUX, neighbour(-1, 0)),
        ]
    arrive(some(vy, 6, 4), VEL)
    loop(0, (NZ + 2) // 3, lambda i: sums_edge(Z0 - 1 + 3 * i, 3))
    for k in range(2):
        loop(2 * k, 2 * k + 2, lambda i: put_planes(g1_ext, 1, edges(Z0 + 4 * i, 4)))
        loop(2 * k, 2 * k + 2, half_faces_y)
        send(flux_y[2 * k : 2 * k + 2])

    def middle(i):
        return [(1 + 3 * i + k, Y0 + 2, NY - 4) for k in range(3)]

    def faces_y(z):
        c = dt_vec[...] * vy[z, pl.ds(Y0, NY - 1)]
        picked = donors(c > 0, [(z, Y0, NY - 1)], [(z, Y0 + 1, NY - 1)])
        put(face, [(z, Y0, NY - 1)], flow(*picked, c))

    pipelined((NZ + 2) // 3, middle, *x_stages)
    loop(Z0 - 1, Z0 + 2, lambda z: put_sums(z, *inner))

    def y_inner(z):
        stores = planes_of(g1_ext, 1)([(z, *inner)]), sums_of(z + 2, *inner)
        for store in stores:
            store()

    loop(Z0, Z1 - 1, y_inner)
    put_planes(g1_ext, 1, [(Z1 - 1, *inner)])
    loop(Z0, Z1, faces_y)
    def update_y(where):
        before, q = moved(where, 0, -1), dt_vec[...]
        g = rows(g1_ext, where) - rows(face, where) + rows(face, before)
        put(g2_ext, where, g / (1.0 - q * (rows(vy, where) - rows(vy, before))))

    loop(Z0, Z1, lambda z: update_y([(z, *inner)]))
    arrive(edge_y.at[pl.ds(2, 2)], FLUX)

    def update_y_edge(i):
        for k in range(4):
            z, at = Z0 + 4 * i + k, 4 * i + k
            face[z, Y0 - 1] = edge_y[2, at] - edge_y[1, at]
            face[z, Y1 - 1] = edge_y[0, at] - edge_y[3, at]
        update_y(edges(Z0 + 4 * i, 4))

    loop(0, NZ // 4, update_y_edge)
    near = [HALO_G, HALO_G, HALO_G_NEAR, HALO_G_NEAR] + 4 * [HALO_G]
    halo_g = halo(g2_ext, HALO_G, near, 2, 1)

    def faces_z(where):
        c = dt_vec[...] * rows(vz, where)
        put(face, where, flow(*donors(c > 0, where, moved(where, 1, 0)), c))

    shift_rows(g2_ext, [(Z0, Y0, NY), (Z0 + 1, Y0, NY)])
    send(halo_g[:2] + halo_g[4:] + halo_g[2:4])
    shift_rows(g2_ext, [(Z0 + 2, Y0, NY), (Z0 + 3, Y0, NY)])
    loop(Z0, Z0 + 3, lambda z: put_sums(z, *inner))

    def z_inner(z):
        stores = (
            shifts_of(g2_ext)([(z + 3, Y0, NY)]),
            planes_of(g2_ext, 0)([(z, *inner)]),
            sums_of(z + 2, *inner),
        )
        for store in reversed(stores):
            store()

    loop(Z0 + 1, Z1 - 3, z_inner)
    put_sums(Z1 - 1, *inner)
    loop(Z1 - 3, Z1 - 1, lambda z: put_planes(g2_ext, 0, [(z, *inner)]))
    loop(Z0 + 1, Z1 - 2, lambda z: faces_z([(z, *inner)]))
    arrive(some(g2_ext, 8, 4), HALO_G_NEAR)
    loop(0, 2, lambda i: shift_rows(g2_ext, [(i * Z1, Y0, NY), (i * Z1 + 1, Y0, NY)]))
    loop(0, 4, lambda i: put_sums(i + (i // 2) * (EZ - 4), *inner))
    loop(0, 4, lambda i: put_planes(g2_ext, 0, ends(i)))
    loop(0, 4, lambda i: faces_z([(1 + i + (i // 2) * (NZ - 3), *inner)]))
    arrive(some(g2_ext, 10, 4), HALO_G)
    loop(0, 2, lambda i: shift_rows(
        g2_ext, [w for k in range(EZ // 2) for w in ((i * (EZ // 2) + k, Y0 - 1, 1), (i * (EZ // 2) + k, Y1, 1))]
    ))
    loop(0, EZ // 4, lambda i: sums_edge(4 * i, 4))
    loop(0, (NZ + 2) // 3, lambda i: put_planes(g2_ext, 0, edges(1 + 3 * i, 3)))
    loop(0, NZ // 3, lambda i: faces_z(edges(1 + 3 * i, 3)))
    faces_z(edges(Z1 - 2, 2))

    def update_z(z):
        g = g2_ext[z, own_y] - face[z, own_y] + face[z - 1, own_y]
        g = g / (1.0 - dt_vec[...] * (vz[z, own_y] - vz[z - 1, own_y]))
        for y in range(NY):
            out_ref[z - Z0, :, y, :] = g[y]

    loop(Z0, Z1, update_z)
    left(some(f_ext, 14, 8), HALO_F)
    left(some(vx, 13, 4), HALO_V)
    left(some(g2_ext, 9, 8), HALO_G)
    left(some(vy, 6, 4), VEL)
    left(edge_y.at[pl.ds(0, 2)], FLUX)
    left(stat_y.at[pl.ds(0, N_GY - 1)], STAT_Y)
    left(stat_z.at[pl.ds(0, N_GZ - 1)], STAT_Z)
    dt_copy.wait()


def shards(*blocks):
    tiled = [b.reshape(NZ, NY, J, LN).transpose(0, 2, 1, 3) for b in blocks]
    row = (J, LN)
    ext = pltpu.VMEM((EZ, EY, *row), F32)
    anywhere = pl.BlockSpec(memory_space=pl.ANY)
    field, step = pl.pallas_call(
        kernel,
        out_shape=(pltpu.VMEM((NZ, J, NY, LN), F32), jax.ShapeDtypeStruct((1, 1), F32)),
        in_specs=[anywhere] * 4,
        out_specs=(pl.BlockSpec(memory_space=pltpu.VMEM), anywhere),
        scratch_shapes=[ext] * 18 + [
            pltpu.VMEM((4, NZ, *row), F32),
            pltpu.VMEM((N_GY, 2, LN), F32), pltpu.VMEM((N_GZ, 2, LN), F32),
            pltpu.VMEM(row, F32), pltpu.VMEM((1, 1), F32),
            pltpu.SemaphoreType.DMA((4,)), pltpu.SemaphoreType.DMA(()),
            pltpu.SemaphoreType.DMA((N_SEND,)), pltpu.SemaphoreType.DMA((N_RECV,)),
        ],
        compiler_params=pltpu.CompilerParams(collective_id=0, has_side_effects=True),
        name="advect",
    )(*tiled)
    return field.transpose(0, 2, 1, 3).reshape(NZ, NY, J * LN), step.reshape(())


def solution(mesh):
    spec = P("gz", "gy", None)
    return jax.shard_map(shards, mesh=mesh, in_specs=(spec,) * 4, out_specs=(spec, P()), check_vma=False)
```

```python
import jax
import jax.numpy as jnp
from jax import lax
from jax.experimental import pallas as pl
from jax.experimental.pallas import tpu as pltpu
from jax.sharding import PartitionSpec as P

NEWTON = 5
TILT_FLOOR = 3.2
TINY = 1e-18
COURANT = 0.45
EPSILON = 1e-6
THIRD = 1.0 / 3.0

NZ, NY, J, LN = 16, 8, 8, 128
N_GY, N_GZ = 16, 8
F32 = jnp.float32

EZ, EY = NZ + 4, NY + 4
Z0, Y0 = 2, 2
Z1, Y1 = Z0 + NZ, Y0 + NY

HALO_F, HALO_V, HALO_G, VEL, FLUX, STAT_Y, STAT_Z = range(7)
HALO_F_FAR, HALO_G_NEAR = 7, 8
N_SEND, N_RECV = 7, 9


def lanes(u):
    return lax.broadcasted_iota(jnp.int32, u.shape, u.ndim - 1)


def at_next(u):
    moved = pltpu.roll(u, LN - 1, u.ndim - 1)
    return jnp.where(lanes(u) == LN - 1, pltpu.roll(moved, J - 1, u.ndim - 2), moved)


def at_prev(u):
    moved = pltpu.roll(u, 1, u.ndim - 1)
    return jnp.where(lanes(u) == 0, pltpu.roll(moved, 1, u.ndim - 2), moved)


def plane(g, slope_d, slope_a, slope_b):
    tilt_a = jnp.abs(slope_a) + TILT_FLOOR
    tilt_b = jnp.abs(slope_b) + TILT_FLOOR
    lo, hi = jnp.minimum(tilt_a, tilt_b), jnp.maximum(tilt_a, tilt_b)
    slope_d = jnp.where(jnp.abs(slope_d) < TINY, TINY, slope_d)
    tilt_d = jnp.abs(slope_d)
    m1, rest = jnp.minimum(lo, tilt_d), jnp.maximum(lo, tilt_d)
    m2, m3 = jnp.minimum(rest, hi), jnp.maximum(rest, hi)
    lesser = jnp.maximum(jnp.minimum(g, 1.0 - g), 0.0)
    m12 = m1 * m2
    product = m12 * m3
    target = lesser * product
    both = target + target
    summed = lo + hi + tilt_d
    w = 0.5 * jnp.maximum(m1 + m2 - m3, 0.0)
    a = 0.5 * summed - (0.5 * product - target) / (m12 - w * w)
    for _ in range(NEWTON - 1):
        q0 = jnp.minimum(a, m1)
        r0 = a - q0
        p2 = jnp.maximum(a - m2, 0.0)
        q2 = jnp.minimum(p2, m1)
        r2 = p2 - q2
        p3 = jnp.maximum(a - m3, 0.0)
        s3 = p3 * p3
        value = q0 * (q0 * q0 * THIRD + a * r0) - q2 * (q2 * q2 * THIRD + p2 * r2) - s3 * (p3 * THIRD) - both
        rate = q0 * (a + r0) - q2 * (p2 + r2) - s3
        a = a - value / rate
    return jnp.where(g > 0.5, summed - a, a), lo, hi, slope_d, 0.5 / product


def cube_part(s, h):
    p = jnp.maximum(s, 0.0)
    q = jnp.minimum(p, h)
    r = p - q
    return q * (q * q * THIRD + p * r)


def flow(offset, lo, hi, slope_d, scale, c):
    signed = c * slope_d
    h = jnp.abs(signed)
    s = offset - jnp.where(signed < 0, jnp.abs(slope_d) - h, 0.0)
    t = s - hi
    return scale * ((cube_part(s, h) - cube_part(s - lo, h)) - (cube_part(t, h) - cube_part(t - lo, h)))


def rows(ref, where):
    parts = [ref[z, pl.ds(y, n)] for z, y, n in where]
    return parts[0] if len(parts) == 1 else jnp.concatenate(parts, axis=0)


def put(ref, where, value):
    start = 0
    for z, y, n in where:
        ref[z, pl.ds(y, n)] = value[start : start + n]
        start += n


def moved(where, dz, dy):
    return [(z + dz, y + dy, n) for z, y, n in where]


def loop(first, last, body):
    def step(i, carry):
        body(i)
        return carry

    lax.fori_loop(first, last, step, 0)


def pipelined(count, where_of, *stages):
    depth = len(stages)

    def run(i, live):
        for store in reversed([stages[k](where_of(i - k)) for k in live]):
            store()

    for i in range(depth - 1):
        run(i, range(i + 1))
    loop(depth - 1, count, lambda i: run(i, range(depth)))
    for i in range(count, count + depth - 1):
        run(i, range(i - count + 1, depth))


def kernel(
    f_hbm, vx_hbm, vy_hbm, vz_hbm, out_ref, dt_out,
    f_ext, g1_ext, g2_ext, vx, vy, vz, vx_diff, smooth, diff, sum_y, dif_y, sum_d,
    off, lo, hi, slope, scale, face, edge_y, stat_y, stat_z, dt_vec, dt_cell,
    load_sem, out_sem, send_sem, recv_sem,
):
    gy, gz = lax.axis_index("gy"), lax.axis_index("gz")

    def neighbour(dy, dz):
        return {"gy": lax.rem(gy + dy + N_GY, N_GY), "gz": lax.rem(gz + dz + N_GZ, N_GZ)}

    corners = [(1, 1), (1, -1), (-1, 1), (-1, -1)]
    own_z, own_y = pl.ds(Z0, NZ), pl.ds(Y0, NY)

    arrays = [(f_hbm, f_ext), (vx_hbm, vx), (vy_hbm, vy), (vz_hbm, vz)]

    def load(k):
        source, target = arrays[k]
        for y in range(NY):
            pltpu.make_async_copy(source.at[:, :, y, :], target.at[own_z, Y0 + y], load_sem.at[k]).start()

    load(0)
    barrier = pltpu.get_barrier_semaphore()
    greeted = [neighbour(k, 0) for k in range(1, N_GY)]
    greeted += [neighbour(0, k) for k in range(1, N_GZ)] + [neighbour(*c) for c in corners]
    for device in greeted:
        pl.semaphore_signal(barrier, inc=1, device_id=device, device_id_type=pl.DeviceIdType.MESH)
    for k in (1, 2, 3):
        load(k)

    def remote(source, target, sends, receives, device):
        return pltpu.make_async_remote_copy(
            src_ref=source, dst_ref=target, send_sem=send_sem.at[sends], recv_sem=recv_sem.at[receives],
            device_id=device, device_id_type=pl.DeviceIdType.MESH,
        )

    def halo(g, sends, receives, wide_z, wide_y):
        from_z = {1: pl.ds(Z1 - wide_z, wide_z), -1: pl.ds(Z0, wide_z), 0: own_z}
        from_y = {1: pl.ds(Y1 - wide_y, wide_y), -1: pl.ds(Y0, wide_y), 0: own_y}
        to_z = {1: pl.ds(Z0 - wide_z, wide_z), -1: pl.ds(Z1, wide_z), 0: own_z}
        to_y = {1: pl.ds(Y0 - wide_y, wide_y), -1: pl.ds(Y1, wide_y), 0: own_y}
        return [
            remote(g.at[from_z[dz], from_y[dy]], g.at[to_z[dz], to_y[dy]], sends, receives[k], neighbour(dy, dz))
            for k, (dy, dz) in enumerate([(1, 0), (-1, 0), (0, 1), (0, -1)] + corners)
        ]

    def send(copies):
        for copy in copies:
            copy.start()

    def arrive(part, receives):
        remote(part, part, 0, receives, neighbour(1, 0)).wait_recv()

    def left(part, sends):
        remote(part, part, sends, 0, neighbour(1, 0)).wait_send()

    def some(ref, z, y):
        return ref.at[pl.ds(0, z), pl.ds(0, y)]

    def loaded(k):
        source, target = arrays[k]
        pltpu.make_async_copy(source, target.at[own_z, own_y], load_sem.at[k]).wait()

    def scan_fraction(i, total):
        g = f_ext[i + Z0, own_y]
        return total + g * (1.0 - g)

    loaded(0)
    total = lax.fori_loop(0, NZ, scan_fraction, jnp.zeros((NY, J, LN), F32))
    peak = jnp.zeros((NY, J, LN), F32)
    for k in (1, 2, 3):
        loaded(k)
        speeds = arrays[k][1]
        peak = lax.fori_loop(0, NZ, lambda i, peak: jnp.maximum(peak, jnp.abs(speeds[i + Z0, own_y])), peak)
    top_row = lax.broadcasted_iota(jnp.int32, (2, LN), 0) == 0

    def combined(ref, n):
        top, add = ref[0], ref[0]
        for k in range(1, n):
            top, add = jnp.maximum(top, ref[k]), add + ref[k]
        return jnp.where(top_row, top, add)

    top, add = jnp.max(peak, axis=0), jnp.sum(total, axis=0)
    stat_y[gy] = jnp.concatenate([jnp.max(top, axis=0, keepdims=True), jnp.sum(add, axis=0, keepdims=True)], axis=0)

    pl.semaphore_wait(barrier, len(greeted))
    halo_f = halo(f_ext, HALO_F, 2 * [HALO_F] + 6 * [HALO_F_FAR], 2, 2)
    halo_v = halo(vx, HALO_V, 8 * [HALO_V], 1, 1)
    stats_y = [remote(stat_y.at[gy], stat_y.at[gy], STAT_Y, STAT_Y, neighbour(k, 0)) for k in range(1, N_GY)]
    stats_z = [remote(stat_z.at[gz], stat_z.at[gz], STAT_Z, STAT_Z, neighbour(0, k)) for k in range(1, N_GZ)]
    velocity = [
        remote(vy.at[own_z, Y1 - 1], vy.at[own_z, Y0 - 1], VEL, VEL, neighbour(1, 0)),
        remote(vz.at[Z1 - 1, own_y], vz.at[Z0 - 1, own_y], VEL, VEL, neighbour(0, 1)),
    ]
    send(stats_y)
    send(halo_f)

    def put_shifts(g, where):
        before, after = at_prev(g), at_next(g)
        put(smooth, where, before + 2.0 * g + after)
        put(diff, where, after - before)

    def shift_rows(g_ext, where):
        put_shifts(rows(g_ext, where), where)

    def sums_of(z, y, n):
        s = smooth[z, pl.ds(y - 1, n + 2)]
        d = diff[z, pl.ds(y - 1, n + 2)]

        def store():
            where = [(z, y, n)]
            put(sum_y, where, s[:-2] + 2.0 * s[1:-1] + s[2:])
            put(dif_y, where, s[2:] - s[:-2])
            put(sum_d, where, d[:-2] + 2.0 * d[1:-1] + d[2:])

        return store

    def put_sums(z, y, n):
        sums_of(z, y, n)()

    planes = (off, lo, hi, slope, scale)

    def planes_of(g_ext, dim):
        def stage(where):
            below, above = moved(where, -1, 0), moved(where, 1, 0)
            along_z = rows(sum_y, above) - rows(sum_y, below)
            along_y = rows(dif_y, below) + 2.0 * rows(dif_y, where) + rows(dif_y, above)
            along_x = rows(sum_d, below) + 2.0 * rows(sum_d, where) + rows(sum_d, above)
            slopes = [along_z, along_y, along_x]
            across = [slopes[k] for k in range(3) if k != dim]
            g = rows(g_ext, where)

            def store():
                for ref, value in zip(planes, plane(g, slopes[dim], *across)):
                    put(ref, where, value)

            return store

        return stage

    def put_planes(g_ext, dim, where):
        planes_of(g_ext, dim)(where)()

    def donors_x(where):
        found = [rows(ref, where) for ref in planes]
        q = rows(vx, where)
        others = [at_next(value) for value in found]
        before = at_prev(q)

        def store():
            upward = q > 0
            others[-1] = -others[-1]
            for ref, value, other in zip(planes, found, others):
                put(ref, where, jnp.where(upward, value, other))
            put(vx_diff, where, q - before)

        return store

    def donors(upward, here, there):
        picked = [jnp.where(upward, rows(ref, here), rows(ref, there)) for ref in planes[:-1]]
        return picked + [jnp.where(upward, rows(scale, here), -rows(scale, there))]

    inner = (Y0 + 1, NY - 2)

    loop(0, NZ // 2, lambda i: shift_rows(f_ext, [(Z0 + 2 * i, Y0, NY), (Z0 + 2 * i + 1, Y0, NY)]))
    loop(Z0, Z1, lambda z: put_sums(z, *inner))
    pipelined(NZ - 2, lambda i: [(Z0 + 1 + i, *inner)], planes_of(f_ext, 2), donors_x)
    send(halo_v)
    arrive(some(f_ext, NZ, 4), HALO_F)

    def shift_sides(i):
        z = Z0 + 4 * i
        shift_rows(f_ext, [w for k in range(4) for w in ((z + k, 0, 2), (z + k, Y1, 2))])

    def sums_side(z):
        put_sums(z, 1, 2)
        put_sums(z, Y1 - 1, 2)

    loop(0, NZ // 4, shift_sides)
    loop(Z0, Z1, sums_side)
    arrive(stat_y.at[pl.ds(0, N_GY - 1)], STAT_Y)
    stat_z[gz] = combined(stat_y, N_GY)
    send(stats_z)
    send(velocity)
    arrive(some(f_ext, 12, 4), HALO_F_FAR)

    loop(0, 2, lambda i: shift_rows(f_ext, [(i * Z1, 0, EY), (i * Z1 + 1, 0, EY)]))
    loop(0, 4, lambda i: put_sums(i + (i // 2) * (EZ - 4), 1, EY - 2))

    def sides(i):
        high = i // (NZ // 3 + 1)
        z, y = 1 + 3 * (i - high * (NZ // 3 + 1)), 1 + high * (Y1 - 2)
        return [(z + k, y, 2) for k in range(3)]

    def ends(i):
        return [(1 + i + (i // 2) * (NZ - 2), *inner)]

    loop(0, 4, lambda i: put_planes(f_ext, 2, ends(i)))
    arrive(some(vx, 13, 4), HALO_V)
    loop(0, 2, lambda i: donors_x([(1 + i * NZ + k, *inner) for k in range(2)])())
    pipelined(2 * (NZ // 3 + 1), sides, planes_of(f_ext, 2), donors_x)
    arrive(stat_z.at[pl.ds(0, N_GZ - 1)], STAT_Z)
    stats = combined(stat_z, N_GZ)
    umax = jnp.max(stats[0:1], axis=1, keepdims=True)
    share = jnp.sum(stats[1:2], axis=1, keepdims=True) * (4.0 / (N_GZ * NZ * N_GY * NY * J * LN))
    step = COURANT / ((umax + EPSILON) * (1.0 + share))
    dt_vec[...] = jnp.broadcast_to(step, (J, LN))
    dt_cell[...] = step

    def flow_x(where):
        found = [rows(ref, where) for ref in planes]
        q = rows(vx, where)
        return lambda: put(face, where, flow(*found, dt_vec[...] * q))

    def update_x(where):
        out = rows(face, where)
        before = at_prev(out)
        g, change = rows(f_ext, where), rows(vx_diff, where)
        return lambda: put(g1_ext, where, (g - out + before) / (1.0 - dt_vec[...] * change))

    def shifts_of(g_ext):
        def stage(where):
            g = rows(g_ext, where)
            before, after = at_prev(g), at_next(g)

            def store():
                put(smooth, where, before + 2.0 * g + after)
                put(diff, where, after - before)

            return store

        return stage

    dt_copy = pltpu.make_async_copy(dt_cell, dt_out, out_sem)
    x_stages = (flow_x, update_x, shifts_of(g1_ext))
    pipelined(
        NZ // 2 + 1,
        lambda i: [w for z in (1 + 2 * i, 2 + 2 * i) for w in ((z, 1, 3), (z, Y1 - 2, 3))],
        *x_stages,
    )

    dt_copy.start()

    def sums_edge(first, n):
        for z in range(n):
            put_sums(first + z, Y0, 1)
            put_sums(first + z, Y1 - 1, 1)

    def edges(first, n):
        return [w for k in range(n) for w in ((first + k, Y0, 1), (first + k, Y1 - 1, 1))]

    def half_faces_y(i):
        z = Z0 + 4 * i
        at_face = [w for k in range(4) for w in ((z + k, Y0 - 1, 1), (z + k, Y1 - 1, 1))]
        c = dt_vec[...] * rows(vy, at_face)
        out = flow(*[rows(ref, edges(z, 4)) for ref in planes], c)
        for k in range(4):
            edge_y[0, 4 * i + k] = jnp.where(c[2 * k + 1] > 0, out[2 * k + 1], 0.0)
            edge_y[1, 4 * i + k] = jnp.where(c[2 * k] < 0, out[2 * k], 0.0)

    flux_y = []
    for k in range(2):
        part = pl.ds(k * (NZ // 2), NZ // 2)
        flux_y += [
            remote(edge_y.at[0, part], edge_y.at[2, part], FLUX, FLUX, neighbour(1, 0)),
            remote(edge_y.at[1, part], edge_y.at[3, part], FLUX, FLUX, neighbour(-1, 0)),
        ]
    arrive(some(vy, 6, 4), VEL)
    loop(0, (NZ + 2) // 3, lambda i: sums_edge(Z0 - 1 + 3 * i, 3))
    for k in range(2):
        loop(2 * k, 2 * k + 2, lambda i: put_planes(g1_ext, 1, edges(Z0 + 4 * i, 4)))
        loop(2 * k, 2 * k + 2, half_faces_y)
        send(flux_y[2 * k : 2 * k + 2])

    def middle(i):
        return [(1 + 3 * i + k, Y0 + 2, NY - 4) for k in range(3)]

    def faces_y(where):
        c = dt_vec[...] * rows(vy, where)
        put(face, where, flow(*donors(c > 0, where, moved(where, 0, 1)), c))

    pipelined((NZ + 2) // 3, middle, *x_stages)
    loop(Z0 - 1, Z0 + 2, lambda z: put_sums(z, *inner))

    def y_inner(z):
        stores = planes_of(g1_ext, 1)([(z, *inner)]), sums_of(z + 2, *inner)
        for store in stores:
            store()

    loop(Z0, Z1 - 1, y_inner)
    put_planes(g1_ext, 1, [(Z1 - 1, *inner)])
    def faces_y_near(i):
        z = Z0 + 4 * i
        faces_y([w for k in range(4) for w in ((z + k, Y0, 1), (z + k, Y1 - 2, 1))])

    def update_y(where):
        before, q = moved(where, 0, -1), dt_vec[...]
        g = rows(g1_ext, where) - rows(face, where) + rows(face, before)
        put(g2_ext, where, g / (1.0 - q * (rows(vy, where) - rows(vy, before))))

    def update_y_edge(i):
        for k in range(4):
            z, at = Z0 + 4 * i + k, 4 * i + k
            face[z, Y0 - 1] = edge_y[2, at] - edge_y[1, at]
            face[z, Y1 - 1] = edge_y[0, at] - edge_y[3, at]
        update_y(edges(Z0 + 4 * i, 4))

    def rest_y(i):
        z = Z0 + 2 * lax.rem(7 * i, NZ // 2)
        faces_y([(z, Y0 + 1, NY - 3), (z + 1, Y0 + 1, NY - 3)])
        update_y([(z, *inner), (z + 1, *inner)])

    near = [HALO_G, HALO_G, HALO_G_NEAR, HALO_G_NEAR] + 4 * [HALO_G]
    halo_g = halo(g2_ext, HALO_G, near, 2, 1)
    loop(0, NZ // 4, faces_y_near)
    arrive(edge_y.at[pl.ds(2, 2)], FLUX)
    loop(0, NZ // 4, update_y_edge)
    send(halo_g[:2] + halo_g[4:])
    loop(0, 2, rest_y)
    send(halo_g[2:4])
    loop(2, NZ // 2, rest_y)

    def faces_z(where):
        c = dt_vec[...] * rows(vz, where)
        put(face, where, flow(*donors(c > 0, where, moved(where, 1, 0)), c))

    shift_rows(g2_ext, [(Z0, Y0, NY), (Z0 + 1, Y0, NY)])
    shift_rows(g2_ext, [(Z0 + 2, Y0, NY), (Z0 + 3, Y0, NY)])
    loop(Z0, Z0 + 3, lambda z: put_sums(z, *inner))

    def z_inner(z):
        stores = (
            shifts_of(g2_ext)([(z + 3, Y0, NY)]),
            planes_of(g2_ext, 0)([(z, *inner)]),
            sums_of(z + 2, *inner),
        )
        for store in reversed(stores):
            store()

    loop(Z0 + 1, Z1 - 3, z_inner)
    put_sums(Z1 - 1, *inner)
    loop(Z1 - 3, Z1 - 1, lambda z: put_planes(g2_ext, 0, [(z, *inner)]))
    loop(Z0 + 1, Z1 - 2, lambda z: faces_z([(z, *inner)]))
    arrive(some(g2_ext, 8, 4), HALO_G_NEAR)
    loop(0, 2, lambda i: shift_rows(g2_ext, [(i * Z1, Y0, NY), (i * Z1 + 1, Y0, NY)]))
    loop(0, 4, lambda i: put_sums(i + (i // 2) * (EZ - 4), *inner))
    loop(0, 4, lambda i: put_planes(g2_ext, 0, ends(i)))
    loop(0, 4, lambda i: faces_z([(1 + i + (i // 2) * (NZ - 3), *inner)]))
    def update_z(where):
        before, q = moved(where, -1, 0), dt_vec[...]
        g = rows(g2_ext, where) - rows(face, where) + rows(face, before)
        g = g / (1.0 - q * (rows(vz, where) - rows(vz, before)))
        for k, (z, y) in enumerate([(z, y + k) for z, y, n in where for k in range(n)]):
            out_ref[z - Z0, :, y - Y0, :] = g[k]

    loop(Z0, Z1, lambda z: update_z([(z, *inner)]))
    arrive(some(g2_ext, 10, 4), HALO_G)
    loop(0, 2, lambda i: shift_rows(
        g2_ext, [w for k in range(EZ // 2) for w in ((i * (EZ // 2) + k, Y0 - 1, 1), (i * (EZ // 2) + k, Y1, 1))]
    ))
    loop(0, EZ // 4, lambda i: sums_edge(4 * i, 4))
    loop(0, (NZ + 2) // 3, lambda i: put_planes(g2_ext, 0, edges(1 + 3 * i, 3)))
    loop(0, NZ // 3, lambda i: faces_z(edges(1 + 3 * i, 3)))
    faces_z(edges(Z1 - 2, 2))

    loop(0, NZ // 4, lambda i: update_z(edges(Z0 + 4 * i, 4)))
    left(some(f_ext, 14, 8), HALO_F)
    left(some(vx, 13, 4), HALO_V)
    left(some(g2_ext, 9, 8), HALO_G)
    left(some(vy, 6, 4), VEL)
    left(edge_y.at[pl.ds(0, 2)], FLUX)
    left(stat_y.at[pl.ds(0, N_GY - 1)], STAT_Y)
    left(stat_z.at[pl.ds(0, N_GZ - 1)], STAT_Z)
    dt_copy.wait()


def shards(*blocks):
    tiled = [b.reshape(NZ, NY, J, LN).transpose(0, 2, 1, 3) for b in blocks]
    row = (J, LN)
    ext = pltpu.VMEM((EZ, EY, *row), F32)
    anywhere = pl.BlockSpec(memory_space=pl.ANY)
    field, step = pl.pallas_call(
        kernel,
        out_shape=(pltpu.VMEM((NZ, J, NY, LN), F32), jax.ShapeDtypeStruct((1, 1), F32)),
        in_specs=[anywhere] * 4,
        out_specs=(pl.BlockSpec(memory_space=pltpu.VMEM), anywhere),
        scratch_shapes=[ext] * 18 + [
            pltpu.VMEM((4, NZ, *row), F32),
            pltpu.VMEM((N_GY, 2, LN), F32), pltpu.VMEM((N_GZ, 2, LN), F32),
            pltpu.VMEM(row, F32), pltpu.VMEM((1, 1), F32),
            pltpu.SemaphoreType.DMA((4,)), pltpu.SemaphoreType.DMA(()),
            pltpu.SemaphoreType.DMA((N_SEND,)), pltpu.SemaphoreType.DMA((N_RECV,)),
        ],
        compiler_params=pltpu.CompilerParams(collective_id=0, has_side_effects=True),
        name="advect",
    )(*tiled)
    return field.transpose(0, 2, 1, 3).reshape(NZ, NY, J * LN), step.reshape(())


def solution(mesh):
    spec = P("gz", "gy", None)
    return jax.shard_map(shards, mesh=mesh, in_specs=(spec,) * 4, out_specs=(spec, P()), check_vma=False)
```

```python
import jax
import jax.numpy as jnp
from jax import lax
from jax.experimental import pallas as pl
from jax.experimental.pallas import tpu as pltpu
from jax.sharding import PartitionSpec as P

NEWTON = 5
TILT_FLOOR = 3.2
TINY = 1e-18
COURANT = 0.45
EPSILON = 1e-6
THIRD = 1.0 / 3.0

NZ, NY, J, LN = 16, 8, 8, 128
N_GY, N_GZ = 16, 8
F32 = jnp.float32

EZ, EY = NZ + 4, NY + 4
Z0, Y0 = 2, 2
Z1, Y1 = Z0 + NZ, Y0 + NY

HALO_F, HALO_V, HALO_G, VEL, FLUX, STAT_Y, STAT_Z = range(7)
HALO_F_NEAR, HALO_F_FAR, HALO_G_NEAR = 7, 8, 9
N_SEND, N_RECV = 7, 10


def lanes(u):
    return lax.broadcasted_iota(jnp.int32, u.shape, u.ndim - 1)


def at_next(u):
    moved = pltpu.roll(u, LN - 1, u.ndim - 1)
    return jnp.where(lanes(u) == LN - 1, pltpu.roll(moved, J - 1, u.ndim - 2), moved)


def at_prev(u):
    moved = pltpu.roll(u, 1, u.ndim - 1)
    return jnp.where(lanes(u) == 0, pltpu.roll(moved, 1, u.ndim - 2), moved)


def plane(g, slope_d, slope_a, slope_b):
    tilt_a = jnp.abs(slope_a) + TILT_FLOOR
    tilt_b = jnp.abs(slope_b) + TILT_FLOOR
    lo, hi = jnp.minimum(tilt_a, tilt_b), jnp.maximum(tilt_a, tilt_b)
    slope_d = jnp.where(jnp.abs(slope_d) < TINY, TINY, slope_d)
    tilt_d = jnp.abs(slope_d)
    m1, rest = jnp.minimum(lo, tilt_d), jnp.maximum(lo, tilt_d)
    m2, m3 = jnp.minimum(rest, hi), jnp.maximum(rest, hi)
    lesser = jnp.maximum(jnp.minimum(g, 1.0 - g), 0.0)
    m12 = m1 * m2
    product = m12 * m3
    target = lesser * product
    both = target + target
    summed = lo + hi + tilt_d
    w = 0.5 * jnp.maximum(m1 + m2 - m3, 0.0)
    a = 0.5 * summed - (0.5 * product - target) / (m12 - w * w)
    for _ in range(NEWTON - 1):
        q0 = jnp.minimum(a, m1)
        r0 = a - q0
        p2 = jnp.maximum(a - m2, 0.0)
        q2 = jnp.minimum(p2, m1)
        r2 = p2 - q2
        p3 = jnp.maximum(a - m3, 0.0)
        s3 = p3 * p3
        value = q0 * (q0 * q0 * THIRD + a * r0) - q2 * (q2 * q2 * THIRD + p2 * r2) - s3 * (p3 * THIRD) - both
        rate = q0 * (a + r0) - q2 * (p2 + r2) - s3
        a = a - value / rate
    return jnp.where(g > 0.5, summed - a, a), lo, hi, slope_d, 0.5 / product


def cube_part(s, h):
    p = jnp.maximum(s, 0.0)
    q = jnp.minimum(p, h)
    r = p - q
    return q * (q * q * THIRD + p * r)


def flow(offset, lo, hi, slope_d, scale, c):
    signed = c * slope_d
    h = jnp.abs(signed)
    s = offset - jnp.where(signed < 0, jnp.abs(slope_d) - h, 0.0)
    t = s - hi
    return scale * ((cube_part(s, h) - cube_part(s - lo, h)) - (cube_part(t, h) - cube_part(t - lo, h)))


def rows(ref, where):
    parts = [ref[z, pl.ds(y, n)] for z, y, n in where]
    return parts[0] if len(parts) == 1 else jnp.concatenate(parts, axis=0)


def put(ref, where, value):
    start = 0
    for z, y, n in where:
        ref[z, pl.ds(y, n)] = value[start : start + n]
        start += n


def moved(where, dz, dy):
    return [(z + dz, y + dy, n) for z, y, n in where]


def loop(first, last, body):
    def step(i, carry):
        body(i)
        return carry

    lax.fori_loop(first, last, step, 0)


def pipelined(count, where_of, *stages):
    depth = len(stages)

    def run(i, live):
        for store in reversed([stages[k](where_of(i - k)) for k in live]):
            store()

    for i in range(depth - 1):
        run(i, range(i + 1))
    loop(depth - 1, count, lambda i: run(i, range(depth)))
    for i in range(count, count + depth - 1):
        run(i, range(i - count + 1, depth))


def kernel(
    f_hbm, vx_hbm, vy_hbm, vz_hbm, out_ref, dt_out,
    f_ext, g1_ext, g2_ext, vx, vy, vz, vx_diff, smooth, diff, sum_y, dif_y, sum_d,
    off, lo, hi, slope, scale, face, edge_y, stat_y, stat_z, dt_vec, dt_cell,
    load_sem, out_sem, send_sem, recv_sem,
):
    gy, gz = lax.axis_index("gy"), lax.axis_index("gz")

    def neighbour(dy, dz):
        return {"gy": lax.rem(gy + dy + N_GY, N_GY), "gz": lax.rem(gz + dz + N_GZ, N_GZ)}

    corners = [(1, 1), (1, -1), (-1, 1), (-1, -1)]
    own_z, own_y = pl.ds(Z0, NZ), pl.ds(Y0, NY)

    arrays = [(f_hbm, f_ext), (vx_hbm, vx), (vy_hbm, vy), (vz_hbm, vz)]

    def load(k):
        source, target = arrays[k]
        for y in range(NY):
            pltpu.make_async_copy(source.at[:, :, y, :], target.at[own_z, Y0 + y], load_sem.at[k]).start()

    load(0)
    barrier = pltpu.get_barrier_semaphore()
    greeted = [neighbour(k, 0) for k in range(1, N_GY)]
    greeted += [neighbour(0, k) for k in range(1, N_GZ)] + [neighbour(*c) for c in corners]
    for device in greeted:
        pl.semaphore_signal(barrier, inc=1, device_id=device, device_id_type=pl.DeviceIdType.MESH)
    for k in (1, 2, 3):
        load(k)

    def remote(source, target, sends, receives, device):
        return pltpu.make_async_remote_copy(
            src_ref=source, dst_ref=target, send_sem=send_sem.at[sends], recv_sem=recv_sem.at[receives],
            device_id=device, device_id_type=pl.DeviceIdType.MESH,
        )

    def halo(g, sends, receives, wide_z, wide_y):
        from_z = {1: pl.ds(Z1 - wide_z, wide_z), -1: pl.ds(Z0, wide_z), 0: own_z}
        from_y = {1: pl.ds(Y1 - wide_y, wide_y), -1: pl.ds(Y0, wide_y), 0: own_y}
        to_z = {1: pl.ds(Z0 - wide_z, wide_z), -1: pl.ds(Z1, wide_z), 0: own_z}
        to_y = {1: pl.ds(Y0 - wide_y, wide_y), -1: pl.ds(Y1, wide_y), 0: own_y}
        return [
            remote(g.at[from_z[dz], from_y[dy]], g.at[to_z[dz], to_y[dy]], sends, receives[k], neighbour(dy, dz))
            for k, (dy, dz) in enumerate([(1, 0), (-1, 0), (0, 1), (0, -1)] + corners)
        ]

    def send(copies):
        for copy in copies:
            copy.start()

    def arrive(part, receives):
        remote(part, part, 0, receives, neighbour(1, 0)).wait_recv()

    def left(part, sends):
        remote(part, part, sends, 0, neighbour(1, 0)).wait_send()

    def some(ref, z, y):
        return ref.at[pl.ds(0, z), pl.ds(0, y)]

    def loaded(k):
        source, target = arrays[k]
        pltpu.make_async_copy(source, target.at[own_z, own_y], load_sem.at[k]).wait()

    def scan_fraction(i, total):
        g = f_ext[i + Z0, own_y]
        return total + g * (1.0 - g)

    loaded(0)
    total = lax.fori_loop(0, NZ, scan_fraction, jnp.zeros((NY, J, LN), F32))
    peak = jnp.zeros((NY, J, LN), F32)
    for k in (1, 2, 3):
        loaded(k)
        speeds = arrays[k][1]
        peak = lax.fori_loop(0, NZ, lambda i, peak: jnp.maximum(peak, jnp.abs(speeds[i + Z0, own_y])), peak)
    top_row = lax.broadcasted_iota(jnp.int32, (2, LN), 0) == 0

    def combined(ref, n):
        top, add = ref[0], ref[0]
        for k in range(1, n):
            top, add = jnp.maximum(top, ref[k]), add + ref[k]
        return jnp.where(top_row, top, add)

    top, add = jnp.max(peak, axis=0), jnp.sum(total, axis=0)
    stat_y[gy] = jnp.concatenate([jnp.max(top, axis=0, keepdims=True), jnp.sum(add, axis=0, keepdims=True)], axis=0)

    pl.semaphore_wait(barrier, len(greeted))
    halo_f = halo(f_ext, HALO_F, 2 * [HALO_F] + 2 * [HALO_F_NEAR] + 4 * [HALO_F_FAR], 2, 2)
    halo_v = halo(vx, HALO_V, 8 * [HALO_V], 1, 1)
    stats_y = [remote(stat_y.at[gy], stat_y.at[gy], STAT_Y, STAT_Y, neighbour(k, 0)) for k in range(1, N_GY)]
    stats_z = [remote(stat_z.at[gz], stat_z.at[gz], STAT_Z, STAT_Z, neighbour(0, k)) for k in range(1, N_GZ)]
    velocity = [
        remote(vy.at[own_z, Y1 - 1], vy.at[own_z, Y0 - 1], VEL, VEL, neighbour(1, 0)),
        remote(vz.at[Z1 - 1, own_y], vz.at[Z0 - 1, own_y], VEL, VEL, neighbour(0, 1)),
    ]
    send(stats_y)
    send(halo_f[2:4] + halo_f[:2] + halo_f[4:])

    def put_shifts(g, where):
        before, after = at_prev(g), at_next(g)
        put(smooth, where, before + 2.0 * g + after)
        put(diff, where, after - before)

    def shift_rows(g_ext, where):
        put_shifts(rows(g_ext, where), where)

    def sums_of(z, y, n):
        s = smooth[z, pl.ds(y - 1, n + 2)]
        d = diff[z, pl.ds(y - 1, n + 2)]

        def store():
            where = [(z, y, n)]
            put(sum_y, where, s[:-2] + 2.0 * s[1:-1] + s[2:])
            put(dif_y, where, s[2:] - s[:-2])
            put(sum_d, where, d[:-2] + 2.0 * d[1:-1] + d[2:])

        return store

    def put_sums(z, y, n):
        sums_of(z, y, n)()

    planes = (off, lo, hi, slope, scale)

    def planes_of(g_ext, dim):
        def stage(where):
            below, above = moved(where, -1, 0), moved(where, 1, 0)
            along_z = rows(sum_y, above) - rows(sum_y, below)
            along_y = rows(dif_y, below) + 2.0 * rows(dif_y, where) + rows(dif_y, above)
            along_x = rows(sum_d, below) + 2.0 * rows(sum_d, where) + rows(sum_d, above)
            slopes = [along_z, along_y, along_x]
            across = [slopes[k] for k in range(3) if k != dim]
            g = rows(g_ext, where)

            def store():
                for ref, value in zip(planes, plane(g, slopes[dim], *across)):
                    put(ref, where, value)

            return store

        return stage

    def put_planes(g_ext, dim, where):
        planes_of(g_ext, dim)(where)()

    def donors_x(where):
        found = [rows(ref, where) for ref in planes]
        q = rows(vx, where)
        others = [at_next(value) for value in found]
        before = at_prev(q)

        def store():
            upward = q > 0
            others[-1] = -others[-1]
            for ref, value, other in zip(planes, found, others):
                put(ref, where, jnp.where(upward, value, other))
            put(vx_diff, where, q - before)

        return store

    def donors(upward, here, there):
        picked = [jnp.where(upward, rows(ref, here), rows(ref, there)) for ref in planes[:-1]]
        return picked + [jnp.where(upward, rows(scale, here), -rows(scale, there))]

    inner = (Y0 + 1, NY - 2)

    def pair(z):
        return [(z, *inner), (z + 1, *inner)]

    def shift_ends(g_ext):
        loop(0, 2, lambda i: shift_rows(g_ext, [(i * Z1, Y0, NY), (i * Z1 + 1, Y0, NY)]))
        loop(0, 4, lambda i: put_sums(i + (i // 2) * (EZ - 4), *inner))

    loop(0, NZ // 2, lambda i: shift_rows(f_ext, [(Z0 + 2 * i, Y0, NY), (Z0 + 2 * i + 1, Y0, NY)]))
    loop(Z0, Z1, lambda z: put_sums(z, *inner))
    pipelined(NZ // 2 - 1, lambda i: pair(Z0 + 1 + 2 * i), planes_of(f_ext, 2), donors_x)
    send(halo_v)
    arrive(some(f_ext, 8, 4), HALO_F_NEAR)
    shift_ends(f_ext)
    loop(0, 2, lambda i: put_planes(f_ext, 2, pair(1 + i * NZ)))
    arrive(some(f_ext, NZ, 4), HALO_F)

    def shift_sides(i):
        z = Z0 + 4 * i
        shift_rows(f_ext, [w for k in range(4) for w in ((z + k, 0, 2), (z + k, Y1, 2))])

    def sums_side(z):
        put_sums(z, 1, 2)
        put_sums(z, Y1 - 1, 2)

    loop(0, NZ // 4, shift_sides)
    loop(Z0, Z1, sums_side)
    arrive(stat_y.at[pl.ds(0, N_GY - 1)], STAT_Y)
    stat_z[gz] = combined(stat_y, N_GY)
    send(stats_z)
    send(velocity)
    arrive(some(f_ext, 4, 4), HALO_F_FAR)

    def shift_corners(i):
        z = i * Z1
        shift_rows(f_ext, [(z, 0, 2), (z, Y1, 2), (z + 1, 0, 2), (z + 1, Y1, 2)])

    def sides(i):
        high = i // 3
        z, y = 1 + 6 * (i - 3 * high), 1 + high * (Y1 - 2)
        return [(z + k, y, 2) for k in range(6)]

    loop(0, 2, shift_corners)
    loop(0, 4, lambda i: sums_side(i + (i // 2) * (EZ - 4)))
    arrive(some(vx, 13, 4), HALO_V)
    loop(0, 2, lambda i: donors_x(pair(1 + i * NZ))())
    pipelined(6, sides, planes_of(f_ext, 2), donors_x)
    arrive(stat_z.at[pl.ds(0, N_GZ - 1)], STAT_Z)
    stats = combined(stat_z, N_GZ)
    umax = jnp.max(stats[0:1], axis=1, keepdims=True)
    share = jnp.sum(stats[1:2], axis=1, keepdims=True) * (4.0 / (N_GZ * NZ * N_GY * NY * J * LN))
    step = COURANT / ((umax + EPSILON) * (1.0 + share))
    dt_vec[...] = jnp.broadcast_to(step, (J, LN))
    dt_cell[...] = step

    def flow_x(where):
        found = [rows(ref, where) for ref in planes]
        q = rows(vx, where)
        return lambda: put(face, where, flow(*found, dt_vec[...] * q))

    def update_x(where):
        out = rows(face, where)
        before = at_prev(out)
        g, change = rows(f_ext, where), rows(vx_diff, where)
        return lambda: put(g1_ext, where, (g - out + before) / (1.0 - dt_vec[...] * change))

    def shifts_of(g_ext):
        def stage(where):
            g = rows(g_ext, where)
            before, after = at_prev(g), at_next(g)

            def store():
                put(smooth, where, before + 2.0 * g + after)
                put(diff, where, after - before)

            return store

        return stage

    dt_copy = pltpu.make_async_copy(dt_cell, dt_out, out_sem)
    x_stages = (flow_x, update_x, shifts_of(g1_ext))
    pipelined(
        NZ // 2 + 1,
        lambda i: [w for z in (1 + 2 * i, 2 + 2 * i) for w in ((z, 1, 3), (z, Y1 - 2, 3))],
        *x_stages,
    )

    dt_copy.start()

    def sums_edge(first, n):
        for z in range(n):
            put_sums(first + z, Y0, 1)
            put_sums(first + z, Y1 - 1, 1)

    def edges(first, n):
        return [w for k in range(n) for w in ((first + k, Y0, 1), (first + k, Y1 - 1, 1))]

    def half_faces_y(i):
        z = Z0 + 4 * i
        at_face = [w for k in range(4) for w in ((z + k, Y0 - 1, 1), (z + k, Y1 - 1, 1))]
        c = dt_vec[...] * rows(vy, at_face)
        out = flow(*[rows(ref, edges(z, 4)) for ref in planes], c)
        for k in range(4):
            edge_y[0, 4 * i + k] = jnp.where(c[2 * k + 1] > 0, out[2 * k + 1], 0.0)
            edge_y[1, 4 * i + k] = jnp.where(c[2 * k] < 0, out[2 * k], 0.0)

    flux_y = []
    for k in range(2):
        part = pl.ds(k * (NZ // 2), NZ // 2)
        flux_y += [
            remote(edge_y.at[0, part], edge_y.at[2, part], FLUX, FLUX, neighbour(1, 0)),
            remote(edge_y.at[1, part], edge_y.at[3, part], FLUX, FLUX, neighbour(-1, 0)),
        ]
    arrive(some(vy, 6, 4), VEL)
    loop(0, (NZ + 2) // 3, lambda i: sums_edge(Z0 - 1 + 3 * i, 3))
    for k in range(2):
        put_planes(g1_ext, 1, edges(Z0 + k * (NZ // 2), NZ // 2))
        loop(2 * k, 2 * k + 2, half_faces_y)
        send(flux_y[2 * k : 2 * k + 2])

    def middle(i):
        return [(1 + 3 * i + k, Y0 + 2, NY - 4) for k in range(3)]

    def faces_y(where):
        c = dt_vec[...] * rows(vy, where)
        put(face, where, flow(*donors(c > 0, where, moved(where, 0, 1)), c))

    pipelined((NZ + 2) // 3, middle, *x_stages)
    loop(Z0 - 1, Z0 + 3, lambda z: put_sums(z, *inner))

    def y_inner(i):
        z = Z0 + 2 * i
        stores = planes_of(g1_ext, 1)(pair(z)), sums_of(z + 3, *inner), sums_of(z + 4, *inner)
        for store in stores:
            store()

    loop(0, NZ // 2 - 1, y_inner)
    put_planes(g1_ext, 1, pair(Z1 - 2))
    def faces_y_near(i):
        z = Z0 + 4 * i
        faces_y([w for k in range(4) for w in ((z + k, Y0, 1), (z + k, Y1 - 2, 1))])

    def update_y(where):
        before, q = moved(where, 0, -1), dt_vec[...]
        g = rows(g1_ext, where) - rows(face, where) + rows(face, before)
        put(g2_ext, where, g / (1.0 - q * (rows(vy, where) - rows(vy, before))))

    def update_y_edge(i):
        for k in range(4):
            z, at = Z0 + 4 * i + k, 4 * i + k
            face[z, Y0 - 1] = edge_y[2, at] - edge_y[1, at]
            face[z, Y1 - 1] = edge_y[0, at] - edge_y[3, at]
        update_y(edges(Z0 + 4 * i, 4))

    def rest_y(i):
        z = Z0 + 2 * lax.rem(7 * i, NZ // 2)
        faces_y([(z, Y0 + 1, NY - 3), (z + 1, Y0 + 1, NY - 3)])
        update_y([(z, *inner), (z + 1, *inner)])

    near = [HALO_G, HALO_G, HALO_G_NEAR, HALO_G_NEAR] + 4 * [HALO_G]
    halo_g = halo(g2_ext, HALO_G, near, 2, 1)
    loop(0, NZ // 4, faces_y_near)
    arrive(edge_y.at[pl.ds(2, 2)], FLUX)
    loop(0, NZ // 4, update_y_edge)
    send(halo_g[:2] + halo_g[4:])
    loop(0, 2, rest_y)
    send(halo_g[2:4])
    loop(2, NZ // 2, rest_y)

    def faces_z(where):
        c = dt_vec[...] * rows(vz, where)
        put(face, where, flow(*donors(c > 0, where, moved(where, 1, 0)), c))

    loop(0, 2, lambda i: shift_rows(g2_ext, [(Z0 + 3 * i + k, Y0, NY) for k in range(3)]))
    loop(Z0, Z0 + 4, lambda z: put_sums(z, *inner))

    def z_inner(i):
        z = Z0 + 1 + 2 * i
        stores = (
            shifts_of(g2_ext)([(z + 5, Y0, NY), (z + 6, Y0, NY)]),
            planes_of(g2_ext, 0)(pair(z)),
            sums_of(z + 3, *inner),
            sums_of(z + 4, *inner),
        )
        for store in reversed(stores):
            store()

    loop(0, NZ // 2 - 3, z_inner)
    put_sums(Z1 - 2, *inner)
    put_sums(Z1 - 1, *inner)
    loop(0, 2, lambda i: put_planes(g2_ext, 0, pair(Z1 - 5 + 2 * i)))
    loop(0, NZ // 2 - 2, lambda i: faces_z(pair(Z0 + 1 + 2 * i)))
    faces_z([(Z1 - 3, *inner)])
    arrive(some(g2_ext, 8, 4), HALO_G_NEAR)
    shift_ends(g2_ext)
    loop(0, 2, lambda i: put_planes(g2_ext, 0, pair(1 + i * NZ)))
    loop(0, 2, lambda i: faces_z(pair(1 + i * (NZ - 1))))

    def update_z(where):
        before, q = moved(where, -1, 0), dt_vec[...]
        g = rows(g2_ext, where) - rows(face, where) + rows(face, before)
        g = g / (1.0 - q * (rows(vz, where) - rows(vz, before)))
        for k, (z, y) in enumerate([(z, y + k) for z, y, n in where for k in range(n)]):
            out_ref[z - Z0, :, y - Y0, :] = g[k]

    loop(Z0, Z1, lambda z: update_z([(z, *inner)]))
    arrive(some(g2_ext, 10, 4), HALO_G)
    loop(0, 2, lambda i: shift_rows(
        g2_ext, [w for k in range(EZ // 2) for w in ((i * (EZ // 2) + k, Y0 - 1, 1), (i * (EZ // 2) + k, Y1, 1))]
    ))
    loop(0, EZ // 4, lambda i: sums_edge(4 * i, 4))
    loop(0, (NZ + 2) // 6, lambda i: put_planes(g2_ext, 0, edges(1 + 6 * i, 6)))
    loop(0, 2, lambda i: faces_z(edges(1 + 6 * i, 6)))
    faces_z(edges(Z1 - 5, 5))

    loop(0, NZ // 4, lambda i: update_z(edges(Z0 + 4 * i, 4)))
    left(some(f_ext, 14, 8), HALO_F)
    left(some(vx, 13, 4), HALO_V)
    left(some(g2_ext, 9, 8), HALO_G)
    left(some(vy, 6, 4), VEL)
    left(edge_y.at[pl.ds(0, 2)], FLUX)
    left(stat_y.at[pl.ds(0, N_GY - 1)], STAT_Y)
    left(stat_z.at[pl.ds(0, N_GZ - 1)], STAT_Z)
    dt_copy.wait()


def shards(*blocks):
    tiled = [b.reshape(NZ, NY, J, LN).transpose(0, 2, 1, 3) for b in blocks]
    row = (J, LN)
    ext = pltpu.VMEM((EZ, EY, *row), F32)
    anywhere = pl.BlockSpec(memory_space=pl.ANY)
    field, step = pl.pallas_call(
        kernel,
        out_shape=(pltpu.VMEM((NZ, J, NY, LN), F32), jax.ShapeDtypeStruct((1, 1), F32)),
        in_specs=[anywhere] * 4,
        out_specs=(pl.BlockSpec(memory_space=pltpu.VMEM), anywhere),
        scratch_shapes=[ext] * 18 + [
            pltpu.VMEM((4, NZ, *row), F32),
            pltpu.VMEM((N_GY, 2, LN), F32), pltpu.VMEM((N_GZ, 2, LN), F32),
            pltpu.VMEM(row, F32), pltpu.VMEM((1, 1), F32),
            pltpu.SemaphoreType.DMA((4,)), pltpu.SemaphoreType.DMA(()),
            pltpu.SemaphoreType.DMA((N_SEND,)), pltpu.SemaphoreType.DMA((N_RECV,)),
        ],
        compiler_params=pltpu.CompilerParams(collective_id=0, has_side_effects=True),
        name="advect",
    )(*tiled)
    return field.transpose(0, 2, 1, 3).reshape(NZ, NY, J * LN), step.reshape(())


def solution(mesh):
    spec = P("gz", "gy", None)
    return jax.shard_map(shards, mesh=mesh, in_specs=(spec,) * 4, out_specs=(spec, P()), check_vma=False)
```

```python
import jax
import jax.numpy as jnp
from jax import lax
from jax.experimental import pallas as pl
from jax.experimental.pallas import tpu as pltpu
from jax.sharding import PartitionSpec as P

NEWTON = 5
TILT_FLOOR = 3.2
TINY = 1e-18
COURANT = 0.45
EPSILON = 1e-6
THIRD = 1.0 / 3.0

NZ, NY, J, LN = 16, 8, 8, 128
N_GY, N_GZ = 16, 8
F32 = jnp.float32

EZ, EY = NZ + 4, NY + 4
Z0, Y0 = 2, 2
Z1, Y1 = Z0 + NZ, Y0 + NY

HALO_F, HALO_V, HALO_G, VEL, FLUX, STAT_Y, STAT_Z = range(7)
HALO_F_NEAR, HALO_F_FAR, HALO_G_NEAR = 7, 8, 9
N_SEND, N_RECV = 7, 10


def lanes(u):
    return lax.broadcasted_iota(jnp.int32, u.shape, u.ndim - 1)


def at_next(u):
    moved = pltpu.roll(u, LN - 1, u.ndim - 1)
    return jnp.where(lanes(u) == LN - 1, pltpu.roll(moved, J - 1, u.ndim - 2), moved)


def at_prev(u):
    moved = pltpu.roll(u, 1, u.ndim - 1)
    return jnp.where(lanes(u) == 0, pltpu.roll(moved, 1, u.ndim - 2), moved)


def plane(g, slope_d, slope_a, slope_b):
    tilt_a = jnp.abs(slope_a) + TILT_FLOOR
    tilt_b = jnp.abs(slope_b) + TILT_FLOOR
    lo, hi = jnp.minimum(tilt_a, tilt_b), jnp.maximum(tilt_a, tilt_b)
    slope_d = jnp.where(jnp.abs(slope_d) < TINY, TINY, slope_d)
    tilt_d = jnp.abs(slope_d)
    m1, rest = jnp.minimum(lo, tilt_d), jnp.maximum(lo, tilt_d)
    m2, m3 = jnp.minimum(rest, hi), jnp.maximum(rest, hi)
    lesser = jnp.maximum(jnp.minimum(g, 1.0 - g), 0.0)
    m12 = m1 * m2
    product = m12 * m3
    target = lesser * product
    both = target + target
    summed = lo + hi + tilt_d
    w = 0.5 * jnp.maximum(m1 + m2 - m3, 0.0)
    a = 0.5 * summed - (0.5 * product - target) / (m12 - w * w)
    for _ in range(NEWTON - 1):
        q0 = jnp.minimum(a, m1)
        r0 = a - q0
        p2 = jnp.maximum(a - m2, 0.0)
        q2 = jnp.minimum(p2, m1)
        r2 = p2 - q2
        p3 = jnp.maximum(a - m3, 0.0)
        s3 = p3 * p3
        value = q0 * (q0 * q0 * THIRD + a * r0) - q2 * (q2 * q2 * THIRD + p2 * r2) - s3 * (p3 * THIRD) - both
        rate = q0 * (a + r0) - q2 * (p2 + r2) - s3
        a = a - value / rate
    return jnp.where(g > 0.5, summed - a, a), lo, hi, slope_d, 0.5 / product


def cube_part(s, h):
    p = jnp.maximum(s, 0.0)
    q = jnp.minimum(p, h)
    r = p - q
    return q * (q * q * THIRD + p * r)


def flow(offset, lo, hi, slope_d, scale, c):
    signed = c * slope_d
    h = jnp.abs(signed)
    s = offset - jnp.where(signed < 0, jnp.abs(slope_d) - h, 0.0)
    t = s - hi
    return scale * ((cube_part(s, h) - cube_part(s - lo, h)) - (cube_part(t, h) - cube_part(t - lo, h)))


def rows(ref, where):
    parts = [ref[z, pl.ds(y, n)] for z, y, n in where]
    return parts[0] if len(parts) == 1 else jnp.concatenate(parts, axis=0)


def put(ref, where, value):
    start = 0
    for z, y, n in where:
        ref[z, pl.ds(y, n)] = value[start : start + n]
        start += n


def moved(where, dz, dy):
    return [(z + dz, y + dy, n) for z, y, n in where]


def loop(first, last, body):
    def step(i, carry):
        body(i)
        return carry

    lax.fori_loop(first, last, step, 0)


def pipelined(count, where_of, *stages):
    depth = len(stages)

    def run(i, live):
        for store in reversed([stages[k](where_of(i - k)) for k in live]):
            store()

    for i in range(depth - 1):
        run(i, range(i + 1))
    loop(depth - 1, count, lambda i: run(i, range(depth)))
    for i in range(count, count + depth - 1):
        run(i, range(i - count + 1, depth))


def kernel(
    f_hbm, vx_hbm, vy_hbm, vz_hbm, out_ref, dt_out,
    f_ext, g1_ext, g2_ext, vx, vy, vz, vx_diff, smooth, diff, sum_y, dif_y, sum_d,
    off, lo, hi, slope, scale, face, edge_y, stat_y, stat_z, dt_vec, dt_cell,
    load_sem, out_sem, send_sem, recv_sem,
):
    gy, gz = lax.axis_index("gy"), lax.axis_index("gz")

    def neighbour(dy, dz):
        return {"gy": lax.rem(gy + dy + N_GY, N_GY), "gz": lax.rem(gz + dz + N_GZ, N_GZ)}

    corners = [(1, 1), (1, -1), (-1, 1), (-1, -1)]
    own_z, own_y = pl.ds(Z0, NZ), pl.ds(Y0, NY)

    arrays = [(f_hbm, f_ext), (vx_hbm, vx), (vy_hbm, vy), (vz_hbm, vz)]

    def load(k):
        source, target = arrays[k]
        for y in range(NY):
            pltpu.make_async_copy(source.at[:, :, y, :], target.at[own_z, Y0 + y], load_sem.at[k]).start()

    load(0)
    barrier = pltpu.get_barrier_semaphore()
    greeted = [neighbour(k, 0) for k in range(1, N_GY)]
    greeted += [neighbour(0, k) for k in range(1, N_GZ)] + [neighbour(*c) for c in corners]
    for device in greeted:
        pl.semaphore_signal(barrier, inc=1, device_id=device, device_id_type=pl.DeviceIdType.MESH)
    for k in (1, 2, 3):
        load(k)

    def remote(source, target, sends, receives, device):
        return pltpu.make_async_remote_copy(
            src_ref=source, dst_ref=target, send_sem=send_sem.at[sends], recv_sem=recv_sem.at[receives],
            device_id=device, device_id_type=pl.DeviceIdType.MESH,
        )

    def halo(g, sends, receives, wide_z, wide_y):
        from_z = {1: pl.ds(Z1 - wide_z, wide_z), -1: pl.ds(Z0, wide_z), 0: own_z}
        from_y = {1: pl.ds(Y1 - wide_y, wide_y), -1: pl.ds(Y0, wide_y), 0: own_y}
        to_z = {1: pl.ds(Z0 - wide_z, wide_z), -1: pl.ds(Z1, wide_z), 0: own_z}
        to_y = {1: pl.ds(Y0 - wide_y, wide_y), -1: pl.ds(Y1, wide_y), 0: own_y}
        return [
            remote(g.at[from_z[dz], from_y[dy]], g.at[to_z[dz], to_y[dy]], sends, receives[k], neighbour(dy, dz))
            for k, (dy, dz) in enumerate([(1, 0), (-1, 0), (0, 1), (0, -1)] + corners)
        ]

    def send(copies):
        for copy in copies:
            copy.start()

    def arrive(part, receives):
        remote(part, part, 0, receives, neighbour(1, 0)).wait_recv()

    def left(part, sends):
        remote(part, part, sends, 0, neighbour(1, 0)).wait_send()

    def some(ref, z, y):
        return ref.at[pl.ds(0, z), pl.ds(0, y)]

    def loaded(k):
        source, target = arrays[k]
        pltpu.make_async_copy(source, target.at[own_z, own_y], load_sem.at[k]).wait()

    def scan_fraction(i, total):
        g = f_ext[i + Z0, own_y]
        return total + g * (1.0 - g)

    loaded(0)
    total = lax.fori_loop(0, NZ, scan_fraction, jnp.zeros((NY, J, LN), F32))
    peak = jnp.zeros((NY, J, LN), F32)
    for k in (1, 2, 3):
        loaded(k)
        speeds = arrays[k][1]
        peak = lax.fori_loop(0, NZ, lambda i, peak: jnp.maximum(peak, jnp.abs(speeds[i + Z0, own_y])), peak)
    top_row = lax.broadcasted_iota(jnp.int32, (2, LN), 0) == 0

    def combined(ref, n):
        top, add = ref[0], ref[0]
        for k in range(1, n):
            top, add = jnp.maximum(top, ref[k]), add + ref[k]
        return jnp.where(top_row, top, add)

    top, add = jnp.max(peak, axis=0), jnp.sum(total, axis=0)
    stat_y[gy] = jnp.concatenate([jnp.max(top, axis=0, keepdims=True), jnp.sum(add, axis=0, keepdims=True)], axis=0)

    pl.semaphore_wait(barrier, len(greeted))
    halo_f = halo(f_ext, HALO_F, 2 * [HALO_F] + 2 * [HALO_F_NEAR] + 4 * [HALO_F_FAR], 2, 2)
    halo_v = halo(vx, HALO_V, 8 * [HALO_V], 1, 1)
    stats_y = [remote(stat_y.at[gy], stat_y.at[gy], STAT_Y, STAT_Y, neighbour(k, 0)) for k in range(1, N_GY)]
    stats_z = [remote(stat_z.at[gz], stat_z.at[gz], STAT_Z, STAT_Z, neighbour(0, k)) for k in range(1, N_GZ)]
    velocity = [
        remote(vy.at[own_z, Y1 - 1], vy.at[own_z, Y0 - 1], VEL, VEL, neighbour(1, 0)),
        remote(vz.at[Z1 - 1, own_y], vz.at[Z0 - 1, own_y], VEL, VEL, neighbour(0, 1)),
    ]
    send(stats_y)
    send(halo_f[2:4] + halo_f[:2] + halo_f[4:])

    def put_shifts(g, where):
        before, after = at_prev(g), at_next(g)
        put(smooth, where, before + 2.0 * g + after)
        put(diff, where, after - before)

    def shift_rows(g_ext, where):
        put_shifts(rows(g_ext, where), where)

    def sums_of(z, y, n):
        s = smooth[z, pl.ds(y - 1, n + 2)]
        d = diff[z, pl.ds(y - 1, n + 2)]

        def store():
            where = [(z, y, n)]
            put(sum_y, where, s[:-2] + 2.0 * s[1:-1] + s[2:])
            put(dif_y, where, s[2:] - s[:-2])
            put(sum_d, where, d[:-2] + 2.0 * d[1:-1] + d[2:])

        return store

    def put_sums(z, y, n):
        sums_of(z, y, n)()

    planes = (off, lo, hi, slope, scale)

    def planes_of(g_ext, dim):
        def stage(where):
            below, above = moved(where, -1, 0), moved(where, 1, 0)
            along_z = rows(sum_y, above) - rows(sum_y, below)
            along_y = rows(dif_y, below) + 2.0 * rows(dif_y, where) + rows(dif_y, above)
            along_x = rows(sum_d, below) + 2.0 * rows(sum_d, where) + rows(sum_d, above)
            slopes = [along_z, along_y, along_x]
            across = [slopes[k] for k in range(3) if k != dim]
            g = rows(g_ext, where)

            def store():
                for ref, value in zip(planes, plane(g, slopes[dim], *across)):
                    put(ref, where, value)

            return store

        return stage

    def put_planes(g_ext, dim, where):
        planes_of(g_ext, dim)(where)()

    def donors_x(where):
        found = [rows(ref, where) for ref in planes]
        q = rows(vx, where)
        others = [at_next(value) for value in found]
        before = at_prev(q)

        def store():
            upward = q > 0
            others[-1] = -others[-1]
            for ref, value, other in zip(planes, found, others):
                put(ref, where, jnp.where(upward, value, other))
            put(vx_diff, where, q - before)

        return store

    def donors(upward, here, there):
        picked = [jnp.where(upward, rows(ref, here), rows(ref, there)) for ref in planes[:-1]]
        return picked + [jnp.where(upward, rows(scale, here), -rows(scale, there))]

    inner = (Y0 + 1, NY - 2)

    def pair(z):
        return [(z, *inner), (z + 1, *inner)]

    def shift_ends(g_ext):
        loop(0, 2, lambda i: shift_rows(g_ext, [(i * Z1, Y0, NY), (i * Z1 + 1, Y0, NY)]))
        loop(0, 4, lambda i: put_sums(i + (i // 2) * (EZ - 4), *inner))

    loop(0, NZ // 2, lambda i: shift_rows(f_ext, [(Z0 + 2 * i, Y0, NY), (Z0 + 2 * i + 1, Y0, NY)]))
    loop(Z0, Z1, lambda z: put_sums(z, *inner))
    pipelined(5, lambda i: [(Z0 + 1 + i, *inner)], planes_of(f_ext, 2), donors_x)
    send(halo_v)
    pipelined(NZ - 7, lambda i: [(Z0 + 6 + i, *inner)], planes_of(f_ext, 2), donors_x)
    arrive(some(f_ext, 8, 4), HALO_F_NEAR)
    shift_ends(f_ext)
    loop(0, 2, lambda i: put_planes(f_ext, 2, pair(1 + i * NZ)))
    arrive(some(f_ext, NZ, 4), HALO_F)

    def shift_sides(i):
        z = Z0 + 4 * i
        shift_rows(f_ext, [w for k in range(4) for w in ((z + k, 0, 2), (z + k, Y1, 2))])

    def sums_side(z):
        put_sums(z, 1, 2)
        put_sums(z, Y1 - 1, 2)

    loop(0, NZ // 4, shift_sides)
    loop(Z0, Z1, sums_side)
    arrive(stat_y.at[pl.ds(0, N_GY - 1)], STAT_Y)
    stat_z[gz] = combined(stat_y, N_GY)
    send(stats_z)
    send(velocity)
    arrive(some(f_ext, 4, 4), HALO_F_FAR)

    def shift_corners(i):
        z = i * Z1
        shift_rows(f_ext, [(z, 0, 2), (z, Y1, 2), (z + 1, 0, 2), (z + 1, Y1, 2)])

    def sides(i):
        high = i // 3
        z, y = 1 + 6 * (i - 3 * high), 1 + high * (Y1 - 2)
        return [(z + k, y, 2) for k in range(6)]

    loop(0, 2, shift_corners)
    loop(0, 4, lambda i: sums_side(i + (i // 2) * (EZ - 4)))
    loop(0, 6, lambda i: put_planes(f_ext, 2, sides(i)))
    arrive(some(vx, 13, 4), HALO_V)
    loop(0, 2, lambda i: donors_x(pair(1 + i * NZ))())
    loop(0, 6, lambda i: donors_x(sides(i))())
    arrive(stat_z.at[pl.ds(0, N_GZ - 1)], STAT_Z)
    stats = combined(stat_z, N_GZ)
    umax = jnp.max(stats[0:1], axis=1, keepdims=True)
    share = jnp.sum(stats[1:2], axis=1, keepdims=True) * (4.0 / (N_GZ * NZ * N_GY * NY * J * LN))
    step = COURANT / ((umax + EPSILON) * (1.0 + share))
    dt_vec[...] = jnp.broadcast_to(step, (J, LN))
    dt_cell[...] = step

    def flow_x(where):
        found = [rows(ref, where) for ref in planes]
        q = rows(vx, where)
        return lambda: put(face, where, flow(*found, dt_vec[...] * q))

    def update_x(where):
        out = rows(face, where)
        before = at_prev(out)
        g, change = rows(f_ext, where), rows(vx_diff, where)
        return lambda: put(g1_ext, where, (g - out + before) / (1.0 - dt_vec[...] * change))

    def shifts_of(g_ext):
        def stage(where):
            g = rows(g_ext, where)
            before, after = at_prev(g), at_next(g)

            def store():
                put(smooth, where, before + 2.0 * g + after)
                put(diff, where, after - before)

            return store

        return stage

    dt_copy = pltpu.make_async_copy(dt_cell, dt_out, out_sem)
    x_stages = (flow_x, update_x, shifts_of(g1_ext))
    pipelined(
        NZ // 2 + 1,
        lambda i: [w for z in (1 + 2 * i, 2 + 2 * i) for w in ((z, 1, 3), (z, Y1 - 2, 3))],
        *x_stages,
    )

    dt_copy.start()

    def sums_edge(first, n):
        for z in range(n):
            put_sums(first + z, Y0, 1)
            put_sums(first + z, Y1 - 1, 1)

    def edges(first, n):
        return [w for k in range(n) for w in ((first + k, Y0, 1), (first + k, Y1 - 1, 1))]

    def half_faces_y(i):
        z = Z0 + 4 * i
        at_face = [w for k in range(4) for w in ((z + k, Y0 - 1, 1), (z + k, Y1 - 1, 1))]
        c = dt_vec[...] * rows(vy, at_face)
        out = flow(*[rows(ref, edges(z, 4)) for ref in planes], c)
        for k in range(4):
            edge_y[0, 4 * i + k] = jnp.where(c[2 * k + 1] > 0, out[2 * k + 1], 0.0)
            edge_y[1, 4 * i + k] = jnp.where(c[2 * k] < 0, out[2 * k], 0.0)

    flux_y = []
    for k in range(2):
        part = pl.ds(k * (NZ // 2), NZ // 2)
        flux_y += [
            remote(edge_y.at[0, part], edge_y.at[2, part], FLUX, FLUX, neighbour(1, 0)),
            remote(edge_y.at[1, part], edge_y.at[3, part], FLUX, FLUX, neighbour(-1, 0)),
        ]
    arrive(some(vy, 6, 4), VEL)
    loop(0, (NZ + 2) // 3, lambda i: sums_edge(Z0 - 1 + 3 * i, 3))
    for k in range(2):
        put_planes(g1_ext, 1, edges(Z0 + k * (NZ // 2), NZ // 2))
        loop(2 * k, 2 * k + 2, half_faces_y)
        send(flux_y[2 * k : 2 * k + 2])

    def middle(i):
        return [(1 + 3 * i + k, Y0 + 2, NY - 4) for k in range(3)]

    def faces_y(where):
        c = dt_vec[...] * rows(vy, where)
        put(face, where, flow(*donors(c > 0, where, moved(where, 0, 1)), c))

    pipelined((NZ + 2) // 3, middle, *x_stages)
    loop(Z0 - 1, Z0 + 3, lambda z: put_sums(z, *inner))

    def y_inner(i):
        z = Z0 + 2 * i
        stores = planes_of(g1_ext, 1)(pair(z)), sums_of(z + 3, *inner), sums_of(z + 4, *inner)
        for store in stores:
            store()

    loop(0, NZ // 2 - 1, y_inner)
    put_planes(g1_ext, 1, pair(Z1 - 2))
    def faces_y_near(i):
        z = Z0 + 4 * i
        faces_y([w for k in range(4) for w in ((z + k, Y0, 1), (z + k, Y1 - 2, 1))])

    def update_y(where):
        before, q = moved(where, 0, -1), dt_vec[...]
        g = rows(g1_ext, where) - rows(face, where) + rows(face, before)
        put(g2_ext, where, g / (1.0 - q * (rows(vy, where) - rows(vy, before))))

    def update_y_edge(i):
        for k in range(4):
            z, at = Z0 + 4 * i + k, 4 * i + k
            face[z, Y0 - 1] = edge_y[2, at] - edge_y[1, at]
            face[z, Y1 - 1] = edge_y[0, at] - edge_y[3, at]
        update_y(edges(Z0 + 4 * i, 4))

    def rest_y(i):
        z = Z0 + 2 * lax.rem(7 * i, NZ // 2)
        faces_y([(z, Y0 + 1, NY - 3), (z + 1, Y0 + 1, NY - 3)])
        update_y([(z, *inner), (z + 1, *inner)])

    near = [HALO_G, HALO_G, HALO_G_NEAR, HALO_G_NEAR] + 4 * [HALO_G]
    halo_g = halo(g2_ext, HALO_G, near, 2, 1)
    loop(0, NZ // 4, faces_y_near)
    arrive(edge_y.at[pl.ds(2, 2)], FLUX)
    loop(0, NZ // 4, update_y_edge)
    send(halo_g[:2] + halo_g[4:])
    loop(0, 2, rest_y)
    send(halo_g[2:4])
    loop(2, NZ // 2, rest_y)

    def faces_z(where):
        c = dt_vec[...] * rows(vz, where)
        put(face, where, flow(*donors(c > 0, where, moved(where, 1, 0)), c))

    shift_rows(g2_ext, [(Z0, Y0, NY), (Z0 + 1, Y0, NY)])
    shift_rows(g2_ext, [(Z0 + 2, Y0, NY), (Z0 + 3, Y0, NY)])
    loop(Z0, Z0 + 3, lambda z: put_sums(z, *inner))

    def z_inner(z):
        stores = (
            shifts_of(g2_ext)([(z + 3, Y0, NY)]),
            planes_of(g2_ext, 0)([(z, *inner)]),
            sums_of(z + 2, *inner),
        )
        for store in reversed(stores):
            store()

    loop(Z0 + 1, Z1 - 3, z_inner)
    put_sums(Z1 - 1, *inner)
    put_planes(g2_ext, 0, pair(Z1 - 3))
    loop(0, NZ // 2 - 2, lambda i: faces_z(pair(Z0 + 1 + 2 * i)))
    faces_z([(Z1 - 3, *inner)])
    arrive(some(g2_ext, 8, 4), HALO_G_NEAR)
    shift_ends(g2_ext)
    loop(0, 2, lambda i: put_planes(g2_ext, 0, pair(1 + i * NZ)))
    loop(0, 2, lambda i: faces_z(pair(1 + i * (NZ - 1))))

    def update_z(where):
        before, q = moved(where, -1, 0), dt_vec[...]
        g = rows(g2_ext, where) - rows(face, where) + rows(face, before)
        g = g / (1.0 - q * (rows(vz, where) - rows(vz, before)))
        for k, (z, y) in enumerate([(z, y + k) for z, y, n in where for k in range(n)]):
            out_ref[z - Z0, :, y - Y0, :] = g[k]

    loop(Z0, Z1, lambda z: update_z([(z, *inner)]))
    arrive(some(g2_ext, 10, 4), HALO_G)
    loop(0, 2, lambda i: shift_rows(
        g2_ext, [w for k in range(EZ // 2) for w in ((i * (EZ // 2) + k, Y0 - 1, 1), (i * (EZ // 2) + k, Y1, 1))]
    ))
    loop(0, EZ // 4, lambda i: sums_edge(4 * i, 4))
    loop(0, (NZ + 2) // 6, lambda i: put_planes(g2_ext, 0, edges(1 + 6 * i, 6)))
    loop(0, 2, lambda i: faces_z(edges(1 + 6 * i, 6)))
    faces_z(edges(Z1 - 5, 5))

    loop(0, NZ // 4, lambda i: update_z(edges(Z0 + 4 * i, 4)))
    left(some(f_ext, 14, 8), HALO_F)
    left(some(vx, 13, 4), HALO_V)
    left(some(g2_ext, 9, 8), HALO_G)
    left(some(vy, 6, 4), VEL)
    left(edge_y.at[pl.ds(0, 2)], FLUX)
    left(stat_y.at[pl.ds(0, N_GY - 1)], STAT_Y)
    left(stat_z.at[pl.ds(0, N_GZ - 1)], STAT_Z)
    dt_copy.wait()


def shards(*blocks):
    tiled = [b.reshape(NZ, NY, J, LN).transpose(0, 2, 1, 3) for b in blocks]
    row = (J, LN)
    ext = pltpu.VMEM((EZ, EY, *row), F32)
    anywhere = pl.BlockSpec(memory_space=pl.ANY)
    field, step = pl.pallas_call(
        kernel,
        out_shape=(pltpu.VMEM((NZ, J, NY, LN), F32), jax.ShapeDtypeStruct((1, 1), F32)),
        in_specs=[anywhere] * 4,
        out_specs=(pl.BlockSpec(memory_space=pltpu.VMEM), anywhere),
        scratch_shapes=[ext] * 18 + [
            pltpu.VMEM((4, NZ, *row), F32),
            pltpu.VMEM((N_GY, 2, LN), F32), pltpu.VMEM((N_GZ, 2, LN), F32),
            pltpu.VMEM(row, F32), pltpu.VMEM((1, 1), F32),
            pltpu.SemaphoreType.DMA((4,)), pltpu.SemaphoreType.DMA(()),
            pltpu.SemaphoreType.DMA((N_SEND,)), pltpu.SemaphoreType.DMA((N_RECV,)),
        ],
        compiler_params=pltpu.CompilerParams(collective_id=0, has_side_effects=True),
        name="advect",
    )(*tiled)
    return field.transpose(0, 2, 1, 3).reshape(NZ, NY, J * LN), step.reshape(())


def solution(mesh):
    spec = P("gz", "gy", None)
    return jax.shard_map(shards, mesh=mesh, in_specs=(spec,) * 4, out_specs=(spec, P()), check_vma=False)
```

```python
import jax
import jax.numpy as jnp
from jax import lax
from jax.experimental import pallas as pl
from jax.experimental.pallas import tpu as pltpu
from jax.sharding import PartitionSpec as P

NEWTON = 5
TILT_FLOOR = 3.2
TINY = 1e-18
COURANT = 0.45
EPSILON = 1e-6
THIRD = 1.0 / 3.0

NZ, NY, J, LN = 16, 8, 8, 128
N_GY, N_GZ = 16, 8
F32 = jnp.float32

EZ, EY = NZ + 4, NY + 4
Z0, Y0 = 2, 2
Z1, Y1 = Z0 + NZ, Y0 + NY

HALO_F, HALO_V, HALO_G, VEL, FLUX, STAT_Y, STAT_Z = range(7)
HALO_F_NEAR, HALO_F_FAR, HALO_G_NEAR = 7, 8, 9
N_SEND, N_RECV = 7, 10


def lanes(u):
    return lax.broadcasted_iota(jnp.int32, u.shape, u.ndim - 1)


def at_next(u):
    moved = pltpu.roll(u, LN - 1, u.ndim - 1)
    return jnp.where(lanes(u) == LN - 1, pltpu.roll(moved, J - 1, u.ndim - 2), moved)


def at_prev(u):
    moved = pltpu.roll(u, 1, u.ndim - 1)
    return jnp.where(lanes(u) == 0, pltpu.roll(moved, 1, u.ndim - 2), moved)


def plane(g, slope_d, slope_a, slope_b):
    tilt_a = jnp.abs(slope_a) + TILT_FLOOR
    tilt_b = jnp.abs(slope_b) + TILT_FLOOR
    lo, hi = jnp.minimum(tilt_a, tilt_b), jnp.maximum(tilt_a, tilt_b)
    slope_d = jnp.where(jnp.abs(slope_d) < TINY, TINY, slope_d)
    tilt_d = jnp.abs(slope_d)
    m1, rest = jnp.minimum(lo, tilt_d), jnp.maximum(lo, tilt_d)
    m2, m3 = jnp.minimum(rest, hi), jnp.maximum(rest, hi)
    lesser = jnp.maximum(jnp.minimum(g, 1.0 - g), 0.0)
    m12 = m1 * m2
    product = m12 * m3
    target = lesser * product
    both = target + target
    summed = lo + hi + tilt_d
    w = 0.5 * jnp.maximum(m1 + m2 - m3, 0.0)
    a = 0.5 * summed - (0.5 * product - target) / (m12 - w * w)
    for _ in range(NEWTON - 1):
        q0 = jnp.minimum(a, m1)
        r0 = a - q0
        p2 = jnp.maximum(a - m2, 0.0)
        q2 = jnp.minimum(p2, m1)
        r2 = p2 - q2
        p3 = jnp.maximum(a - m3, 0.0)
        s3 = p3 * p3
        value = q0 * (q0 * q0 * THIRD + a * r0) - q2 * (q2 * q2 * THIRD + p2 * r2) - s3 * (p3 * THIRD) - both
        rate = q0 * (a + r0) - q2 * (p2 + r2) - s3
        a = a - value / rate
    return jnp.where(g > 0.5, summed - a, a), lo, hi, slope_d, 0.5 / product


def cube_part(s, h):
    p = jnp.maximum(s, 0.0)
    q = jnp.minimum(p, h)
    r = p - q
    return q * (q * q * THIRD + p * r)


def flow(offset, lo, hi, slope_d, scale, c):
    signed = c * slope_d
    h = jnp.abs(signed)
    s = offset - jnp.where(signed < 0, jnp.abs(slope_d) - h, 0.0)
    t = s - hi
    return scale * ((cube_part(s, h) - cube_part(s - lo, h)) - (cube_part(t, h) - cube_part(t - lo, h)))


def rows(ref, where):
    parts = [ref[z, pl.ds(y, n)] for z, y, n in where]
    return parts[0] if len(parts) == 1 else jnp.concatenate(parts, axis=0)


def put(ref, where, value):
    start = 0
    for z, y, n in where:
        ref[z, pl.ds(y, n)] = value[start : start + n]
        start += n


def moved(where, dz, dy):
    return [(z + dz, y + dy, n) for z, y, n in where]


def loop(first, last, body):
    def step(i, carry):
        body(i)
        return carry

    lax.fori_loop(first, last, step, 0)


def pipelined(count, where_of, *stages):
    depth = len(stages)

    def run(i, live):
        for store in reversed([stages[k](where_of(i - k)) for k in live]):
            store()

    for i in range(depth - 1):
        run(i, range(i + 1))
    loop(depth - 1, count, lambda i: run(i, range(depth)))
    for i in range(count, count + depth - 1):
        run(i, range(i - count + 1, depth))


def kernel(
    f_hbm, vx_hbm, vy_hbm, vz_hbm, out_ref, dt_out,
    f_ext, g1_ext, g2_ext, vx, vy, vz, vx_diff, smooth, diff, sum_y, dif_y, sum_d,
    off, lo, hi, slope, scale, face, edge_y, stat_y, stat_z, dt_vec, dt_cell,
    load_sem, out_sem, send_sem, recv_sem,
):
    gy, gz = lax.axis_index("gy"), lax.axis_index("gz")

    def neighbour(dy, dz):
        return {"gy": lax.rem(gy + dy + N_GY, N_GY), "gz": lax.rem(gz + dz + N_GZ, N_GZ)}

    corners = [(1, 1), (1, -1), (-1, 1), (-1, -1)]
    own_z, own_y = pl.ds(Z0, NZ), pl.ds(Y0, NY)

    arrays = [(f_hbm, f_ext), (vx_hbm, vx), (vy_hbm, vy), (vz_hbm, vz)]

    def load(k):
        source, target = arrays[k]
        for y in range(NY):
            pltpu.make_async_copy(source.at[:, :, y, :], target.at[own_z, Y0 + y], load_sem.at[k]).start()

    load(0)
    barrier = pltpu.get_barrier_semaphore()
    greeted = [neighbour(k, 0) for k in range(1, N_GY)]
    greeted += [neighbour(0, k) for k in range(1, N_GZ)] + [neighbour(*c) for c in corners]
    for device in greeted:
        pl.semaphore_signal(barrier, inc=1, device_id=device, device_id_type=pl.DeviceIdType.MESH)
    for k in (1, 2, 3):
        load(k)

    def remote(source, target, sends, receives, device):
        return pltpu.make_async_remote_copy(
            src_ref=source, dst_ref=target, send_sem=send_sem.at[sends], recv_sem=recv_sem.at[receives],
            device_id=device, device_id_type=pl.DeviceIdType.MESH,
        )

    def halo(g, sends, receives, wide_z, wide_y):
        from_z = {1: pl.ds(Z1 - wide_z, wide_z), -1: pl.ds(Z0, wide_z), 0: own_z}
        from_y = {1: pl.ds(Y1 - wide_y, wide_y), -1: pl.ds(Y0, wide_y), 0: own_y}
        to_z = {1: pl.ds(Z0 - wide_z, wide_z), -1: pl.ds(Z1, wide_z), 0: own_z}
        to_y = {1: pl.ds(Y0 - wide_y, wide_y), -1: pl.ds(Y1, wide_y), 0: own_y}
        return [
            remote(g.at[from_z[dz], from_y[dy]], g.at[to_z[dz], to_y[dy]], sends, receives[k], neighbour(dy, dz))
            for k, (dy, dz) in enumerate([(1, 0), (-1, 0), (0, 1), (0, -1)] + corners)
        ]

    def send(copies):
        for copy in copies:
            copy.start()

    def arrive(part, receives):
        remote(part, part, 0, receives, neighbour(1, 0)).wait_recv()

    def left(part, sends):
        remote(part, part, sends, 0, neighbour(1, 0)).wait_send()

    def some(ref, z, y):
        return ref.at[pl.ds(0, z), pl.ds(0, y)]

    def loaded(k):
        source, target = arrays[k]
        pltpu.make_async_copy(source, target.at[own_z, own_y], load_sem.at[k]).wait()

    def scan_fraction(i, total):
        g = f_ext[i + Z0, own_y]
        return total + g * (1.0 - g)

    loaded(0)
    total = lax.fori_loop(0, NZ, scan_fraction, jnp.zeros((NY, J, LN), F32))
    peak = jnp.zeros((NY, J, LN), F32)
    for k in (1, 2, 3):
        loaded(k)
        speeds = arrays[k][1]
        peak = lax.fori_loop(0, NZ, lambda i, peak: jnp.maximum(peak, jnp.abs(speeds[i + Z0, own_y])), peak)
    top_row = lax.broadcasted_iota(jnp.int32, (2, LN), 0) == 0

    def combined(ref, n):
        top, add = ref[0], ref[0]
        for k in range(1, n):
            top, add = jnp.maximum(top, ref[k]), add + ref[k]
        return jnp.where(top_row, top, add)

    top, add = jnp.max(peak, axis=0), jnp.sum(total, axis=0)
    stat_y[gy] = jnp.concatenate([jnp.max(top, axis=0, keepdims=True), jnp.sum(add, axis=0, keepdims=True)], axis=0)

    pl.semaphore_wait(barrier, len(greeted))
    halo_f = halo(f_ext, HALO_F, 2 * [HALO_F] + 2 * [HALO_F_NEAR] + 4 * [HALO_F_FAR], 2, 2)
    halo_v = halo(vx, HALO_V, 8 * [HALO_V], 1, 1)
    stats_y = [remote(stat_y.at[gy], stat_y.at[gy], STAT_Y, STAT_Y, neighbour(k, 0)) for k in range(1, N_GY)]
    stats_z = [remote(stat_z.at[gz], stat_z.at[gz], STAT_Z, STAT_Z, neighbour(0, k)) for k in range(1, N_GZ)]
    velocity = [
        remote(vy.at[own_z, Y1 - 1], vy.at[own_z, Y0 - 1], VEL, VEL, neighbour(1, 0)),
        remote(vz.at[Z1 - 1, own_y], vz.at[Z0 - 1, own_y], VEL, VEL, neighbour(0, 1)),
    ]
    send(stats_y)
    send(halo_f[2:4] + halo_f[:2] + halo_f[4:])

    def put_shifts(g, where):
        before, after = at_prev(g), at_next(g)
        put(smooth, where, before + 2.0 * g + after)
        put(diff, where, after - before)

    def shift_rows(g_ext, where):
        put_shifts(rows(g_ext, where), where)

    def sums_of(z, y, n):
        s = smooth[z, pl.ds(y - 1, n + 2)]
        d = diff[z, pl.ds(y - 1, n + 2)]

        def store():
            where = [(z, y, n)]
            put(sum_y, where, s[:-2] + 2.0 * s[1:-1] + s[2:])
            put(dif_y, where, s[2:] - s[:-2])
            put(sum_d, where, d[:-2] + 2.0 * d[1:-1] + d[2:])

        return store

    def put_sums(z, y, n):
        sums_of(z, y, n)()

    planes = (off, lo, hi, slope, scale)

    def planes_of(g_ext, dim):
        def stage(where):
            below, above = moved(where, -1, 0), moved(where, 1, 0)
            along_z = rows(sum_y, above) - rows(sum_y, below)
            along_y = rows(dif_y, below) + 2.0 * rows(dif_y, where) + rows(dif_y, above)
            along_x = rows(sum_d, below) + 2.0 * rows(sum_d, where) + rows(sum_d, above)
            slopes = [along_z, along_y, along_x]
            across = [slopes[k] for k in range(3) if k != dim]
            g = rows(g_ext, where)

            def store():
                for ref, value in zip(planes, plane(g, slopes[dim], *across)):
                    put(ref, where, value)

            return store

        return stage

    def put_planes(g_ext, dim, where):
        planes_of(g_ext, dim)(where)()

    def donors_x(where):
        found = [rows(ref, where) for ref in planes]
        q = rows(vx, where)
        others = [at_next(value) for value in found]
        before = at_prev(q)

        def store():
            upward = q > 0
            others[-1] = -others[-1]
            for ref, value, other in zip(planes, found, others):
                put(ref, where, jnp.where(upward, value, other))
            put(vx_diff, where, q - before)

        return store

    def donors(upward, here, there):
        picked = [jnp.where(upward, rows(ref, here), rows(ref, there)) for ref in planes[:-1]]
        return picked + [jnp.where(upward, rows(scale, here), -rows(scale, there))]

    inner = (Y0 + 1, NY - 2)

    def pair(z):
        return [(z, *inner), (z + 1, *inner)]

    def shift_ends(g_ext):
        loop(0, 2, lambda i: shift_rows(g_ext, [(i * Z1, Y0, NY), (i * Z1 + 1, Y0, NY)]))
        loop(0, 4, lambda i: put_sums(i + (i // 2) * (EZ - 4), *inner))

    loop(0, NZ // 2, lambda i: shift_rows(f_ext, [(Z0 + 2 * i, Y0, NY), (Z0 + 2 * i + 1, Y0, NY)]))
    loop(Z0, Z1, lambda z: put_sums(z, *inner))
    pipelined(5, lambda i: [(Z0 + 1 + i, *inner)], planes_of(f_ext, 2), donors_x)
    send(halo_v)
    pipelined(NZ - 7, lambda i: [(Z0 + 6 + i, *inner)], planes_of(f_ext, 2), donors_x)
    arrive(some(f_ext, 8, 4), HALO_F_NEAR)
    shift_ends(f_ext)
    loop(0, 2, lambda i: put_planes(f_ext, 2, pair(1 + i * NZ)))
    arrive(some(f_ext, NZ, 4), HALO_F)
    arrive(stat_y.at[pl.ds(0, N_GY - 1)], STAT_Y)
    stat_z[gz] = combined(stat_y, N_GY)
    send(stats_z)

    def shift_sides(i):
        z = Z0 + 4 * i
        shift_rows(f_ext, [w for k in range(4) for w in ((z + k, 0, 2), (z + k, Y1, 2))])

    def sums_side(z):
        put_sums(z, 1, 2)
        put_sums(z, Y1 - 1, 2)

    loop(0, NZ // 4, shift_sides)
    loop(Z0, Z1, sums_side)
    def shift_corners(i):
        z = i * Z1
        shift_rows(f_ext, [(z, 0, 2), (z, Y1, 2), (z + 1, 0, 2), (z + 1, Y1, 2)])

    def side(zs, high):
        return [(z, 1 + high * (Y1 - 2), 2) for z in zs]

    def sides(i):
        high = i // 2
        first = 3 + 6 * (i - 2 * high)
        return side([first + k for k in range(6)], high)

    def side_ends(high):
        return side([1, 2, NZ - 1, NZ, NZ + 1, NZ + 2], high)

    send(velocity)
    loop(0, 4, lambda i: put_planes(f_ext, 2, sides(i)))
    arrive(some(f_ext, 4, 4), HALO_F_FAR)
    loop(0, 2, shift_corners)
    loop(0, 4, lambda i: sums_side(i + (i // 2) * (EZ - 4)))
    loop(0, 2, lambda i: put_planes(f_ext, 2, side_ends(i)))
    arrive(some(vx, 13, 4), HALO_V)
    loop(0, 2, lambda i: donors_x(pair(1 + i * NZ))())
    loop(0, 2, lambda i: donors_x(side_ends(i))())
    loop(0, 4, lambda i: donors_x(sides(i))())
    arrive(stat_z.at[pl.ds(0, N_GZ - 1)], STAT_Z)
    stats = combined(stat_z, N_GZ)
    umax = jnp.max(stats[0:1], axis=1, keepdims=True)
    share = jnp.sum(stats[1:2], axis=1, keepdims=True) * (4.0 / (N_GZ * NZ * N_GY * NY * J * LN))
    step = COURANT / ((umax + EPSILON) * (1.0 + share))
    dt_vec[...] = jnp.broadcast_to(step, (J, LN))
    dt_cell[...] = step

    def flow_x(where):
        found = [rows(ref, where) for ref in planes]
        q = rows(vx, where)
        return lambda: put(face, where, flow(*found, dt_vec[...] * q))

    def update_x(where):
        out = rows(face, where)
        before = at_prev(out)
        g, change = rows(f_ext, where), rows(vx_diff, where)
        return lambda: put(g1_ext, where, (g - out + before) / (1.0 - dt_vec[...] * change))

    def shifts_of(g_ext):
        def stage(where):
            g = rows(g_ext, where)
            before, after = at_prev(g), at_next(g)

            def store():
                put(smooth, where, before + 2.0 * g + after)
                put(diff, where, after - before)

            return store

        return stage

    dt_copy = pltpu.make_async_copy(dt_cell, dt_out, out_sem)
    x_stages = (flow_x, update_x, shifts_of(g1_ext))
    pipelined(
        NZ // 2 + 1,
        lambda i: [w for z in (1 + 2 * i, 2 + 2 * i) for w in ((z, 1, 3), (z, Y1 - 2, 3))],
        *x_stages,
    )

    dt_copy.start()

    def sums_edge(first, n):
        for z in range(n):
            put_sums(first + z, Y0, 1)
            put_sums(first + z, Y1 - 1, 1)

    def edges(first, n):
        return [w for k in range(n) for w in ((first + k, Y0, 1), (first + k, Y1 - 1, 1))]

    def half_faces_y(i):
        z = Z0 + 4 * i
        at_face = [w for k in range(4) for w in ((z + k, Y0 - 1, 1), (z + k, Y1 - 1, 1))]
        c = dt_vec[...] * rows(vy, at_face)
        out = flow(*[rows(ref, edges(z, 4)) for ref in planes], c)
        for k in range(4):
            edge_y[0, 4 * i + k] = jnp.where(c[2 * k + 1] > 0, out[2 * k + 1], 0.0)
            edge_y[1, 4 * i + k] = jnp.where(c[2 * k] < 0, out[2 * k], 0.0)

    flux_y = []
    for k in range(2):
        part = pl.ds(k * (NZ // 2), NZ // 2)
        flux_y += [
            remote(edge_y.at[0, part], edge_y.at[2, part], FLUX, FLUX, neighbour(1, 0)),
            remote(edge_y.at[1, part], edge_y.at[3, part], FLUX, FLUX, neighbour(-1, 0)),
        ]
    arrive(some(vy, 6, 4), VEL)
    loop(0, (NZ + 2) // 3, lambda i: sums_edge(Z0 - 1 + 3 * i, 3))
    for k in range(2):
        put_planes(g1_ext, 1, edges(Z0 + k * (NZ // 2), NZ // 2))
        loop(2 * k, 2 * k + 2, half_faces_y)
        send(flux_y[2 * k : 2 * k + 2])

    def middle(i):
        return [(1 + 3 * i + k, Y0 + 2, NY - 4) for k in range(3)]

    def faces_y(where):
        c = dt_vec[...] * rows(vy, where)
        put(face, where, flow(*donors(c > 0, where, moved(where, 0, 1)), c))

    pipelined((NZ + 2) // 3, middle, *x_stages)
    loop(Z0 - 1, Z0 + 3, lambda z: put_sums(z, *inner))

    def y_inner(i):
        z = Z0 + 2 * i
        stores = planes_of(g1_ext, 1)(pair(z)), sums_of(z + 3, *inner), sums_of(z + 4, *inner)
        for store in stores:
            store()

    loop(0, NZ // 2 - 1, y_inner)
    put_planes(g1_ext, 1, pair(Z1 - 2))
    def faces_y_near(i):
        z = Z0 + 4 * i
        faces_y([w for k in range(4) for w in ((z + k, Y0, 1), (z + k, Y1 - 2, 1))])

    def update_y(where):
        before, q = moved(where, 0, -1), dt_vec[...]
        g = rows(g1_ext, where) - rows(face, where) + rows(face, before)
        put(g2_ext, where, g / (1.0 - q * (rows(vy, where) - rows(vy, before))))

    def update_y_edge(i):
        for k in range(4):
            z, at = Z0 + 4 * i + k, 4 * i + k
            face[z, Y0 - 1] = edge_y[2, at] - edge_y[1, at]
            face[z, Y1 - 1] = edge_y[0, at] - edge_y[3, at]
        update_y(edges(Z0 + 4 * i, 4))

    def rest_y(i):
        z = Z0 + 2 * lax.rem(7 * i, NZ // 2)
        faces_y([(z, Y0 + 1, NY - 3), (z + 1, Y0 + 1, NY - 3)])
        update_y([(z, *inner), (z + 1, *inner)])

    near = [HALO_G, HALO_G, HALO_G_NEAR, HALO_G_NEAR] + 4 * [HALO_G]
    halo_g = halo(g2_ext, HALO_G, near, 2, 1)
    loop(0, NZ // 4, faces_y_near)
    arrive(edge_y.at[pl.ds(2, 2)], FLUX)
    loop(0, NZ // 4, update_y_edge)
    send(halo_g[:2] + halo_g[4:])
    loop(0, 2, rest_y)
    send(halo_g[2:4])
    loop(2, NZ // 2, rest_y)

    def faces_z(where):
        c = dt_vec[...] * rows(vz, where)
        put(face, where, flow(*donors(c > 0, where, moved(where, 1, 0)), c))

    shift_rows(g2_ext, [(Z0, Y0, NY), (Z0 + 1, Y0, NY)])
    shift_rows(g2_ext, [(Z0 + 2, Y0, NY), (Z0 + 3, Y0, NY)])
    loop(Z0, Z0 + 3, lambda z: put_sums(z, *inner))

    def z_inner(z):
        stores = (
            shifts_of(g2_ext)([(z + 3, Y0, NY)]),
            planes_of(g2_ext, 0)([(z, *inner)]),
            sums_of(z + 2, *inner),
        )
        for store in reversed(stores):
            store()

    loop(Z0 + 1, Z1 - 3, z_inner)
    put_sums(Z1 - 1, *inner)
    put_planes(g2_ext, 0, pair(Z1 - 3))
    loop(0, NZ // 2 - 2, lambda i: faces_z(pair(Z0 + 1 + 2 * i)))
    faces_z([(Z1 - 3, *inner)])
    arrive(some(g2_ext, 8, 4), HALO_G_NEAR)
    shift_ends(g2_ext)
    loop(0, 2, lambda i: put_planes(g2_ext, 0, pair(1 + i * NZ)))
    loop(0, 2, lambda i: faces_z(pair(1 + i * (NZ - 1))))

    def update_z(where):
        before, q = moved(where, -1, 0), dt_vec[...]
        g = rows(g2_ext, where) - rows(face, where) + rows(face, before)
        g = g / (1.0 - q * (rows(vz, where) - rows(vz, before)))
        for k, (z, y) in enumerate([(z, y + k) for z, y, n in where for k in range(n)]):
            out_ref[z - Z0, pl.ds(y - Y0, J, stride=NY), :] = g[k]

    loop(Z0, Z1, lambda z: update_z([(z, *inner)]))
    arrive(some(g2_ext, 10, 4), HALO_G)
    loop(0, 2, lambda i: shift_rows(
        g2_ext, [w for k in range(EZ // 2) for w in ((i * (EZ // 2) + k, Y0 - 1, 1), (i * (EZ // 2) + k, Y1, 1))]
    ))
    loop(0, EZ // 4, lambda i: sums_edge(4 * i, 4))
    loop(0, (NZ + 2) // 6, lambda i: put_planes(g2_ext, 0, edges(1 + 6 * i, 6)))
    loop(0, 2, lambda i: faces_z(edges(1 + 6 * i, 6)))
    faces_z(edges(Z1 - 5, 5))

    loop(0, NZ // 4, lambda i: update_z(edges(Z0 + 4 * i, 4)))
    left(some(f_ext, 14, 8), HALO_F)
    left(some(vx, 13, 4), HALO_V)
    left(some(g2_ext, 9, 8), HALO_G)
    left(some(vy, 6, 4), VEL)
    left(edge_y.at[pl.ds(0, 2)], FLUX)
    left(stat_y.at[pl.ds(0, N_GY - 1)], STAT_Y)
    left(stat_z.at[pl.ds(0, N_GZ - 1)], STAT_Z)
    dt_copy.wait()


def shards(*blocks):
    tiled = [b.reshape(NZ, NY, J, LN).transpose(0, 2, 1, 3) for b in blocks]
    row = (J, LN)
    ext = pltpu.VMEM((EZ, EY, *row), F32)
    anywhere = pl.BlockSpec(memory_space=pl.ANY)
    field, step = pl.pallas_call(
        kernel,
        out_shape=(pltpu.VMEM((NZ, J * NY, LN), F32), jax.ShapeDtypeStruct((1, 1), F32)),
        in_specs=[anywhere] * 4,
        out_specs=(pl.BlockSpec(memory_space=pltpu.VMEM), anywhere),
        scratch_shapes=[ext] * 18 + [
            pltpu.VMEM((4, NZ, *row), F32),
            pltpu.VMEM((N_GY, 2, LN), F32), pltpu.VMEM((N_GZ, 2, LN), F32),
            pltpu.VMEM(row, F32), pltpu.VMEM((1, 1), F32),
            pltpu.SemaphoreType.DMA((4,)), pltpu.SemaphoreType.DMA(()),
            pltpu.SemaphoreType.DMA((N_SEND,)), pltpu.SemaphoreType.DMA((N_RECV,)),
        ],
        compiler_params=pltpu.CompilerParams(collective_id=0, has_side_effects=True),
        name="advect",
    )(*tiled)
    return field.reshape(NZ, J, NY, LN).transpose(0, 2, 1, 3).reshape(NZ, NY, J * LN), step.reshape(())


def solution(mesh):
    spec = P("gz", "gy", None)
    return jax.shard_map(shards, mesh=mesh, in_specs=(spec,) * 4, out_specs=(spec, P()), check_vma=False)
```

```python
import jax
import jax.numpy as jnp
from jax import lax
from jax.experimental import pallas as pl
from jax.experimental.pallas import tpu as pltpu
from jax.sharding import PartitionSpec as P

NEWTON = 5
TILT_FLOOR = 3.2
TINY = 1e-18
COURANT = 0.45
EPSILON = 1e-6
THIRD = 1.0 / 3.0

NZ, NY, J, LN = 16, 8, 8, 128
N_GY, N_GZ = 16, 8
F32 = jnp.float32

EZ, EY = NZ + 4, NY + 4
Z0, Y0 = 2, 2
Z1, Y1 = Z0 + NZ, Y0 + NY

HALO_F, HALO_V, HALO_G, VEL, FLUX, STAT_Y, STAT_Z = range(7)
HALO_F_NEAR, HALO_F_FAR, HALO_G_NEAR = 7, 8, 9
N_SEND, N_RECV = 7, 10


def lanes(u):
    return lax.broadcasted_iota(jnp.int32, u.shape, u.ndim - 1)


def at_next(u):
    moved = pltpu.roll(u, LN - 1, u.ndim - 1)
    return jnp.where(lanes(u) == LN - 1, pltpu.roll(moved, J - 1, u.ndim - 2), moved)


def at_prev(u):
    moved = pltpu.roll(u, 1, u.ndim - 1)
    return jnp.where(lanes(u) == 0, pltpu.roll(moved, 1, u.ndim - 2), moved)


def plane(g, slope_d, slope_a, slope_b):
    tilt_a = jnp.abs(slope_a) + TILT_FLOOR
    tilt_b = jnp.abs(slope_b) + TILT_FLOOR
    lo, hi = jnp.minimum(tilt_a, tilt_b), jnp.maximum(tilt_a, tilt_b)
    slope_d = jnp.where(jnp.abs(slope_d) < TINY, TINY, slope_d)
    tilt_d = jnp.abs(slope_d)
    m1, rest = jnp.minimum(lo, tilt_d), jnp.maximum(lo, tilt_d)
    m2, m3 = jnp.minimum(rest, hi), jnp.maximum(rest, hi)
    lesser = jnp.maximum(jnp.minimum(g, 1.0 - g), 0.0)
    m12 = m1 * m2
    product = m12 * m3
    target = lesser * product
    both = target + target
    summed = lo + hi + tilt_d
    w = 0.5 * jnp.maximum(m1 + m2 - m3, 0.0)
    a = 0.5 * summed - (0.5 * product - target) / (m12 - w * w)
    for _ in range(NEWTON - 1):
        q0 = jnp.minimum(a, m1)
        r0 = a - q0
        p2 = jnp.maximum(a - m2, 0.0)
        q2 = jnp.minimum(p2, m1)
        r2 = p2 - q2
        p3 = jnp.maximum(a - m3, 0.0)
        s3 = p3 * p3
        value = q0 * (q0 * q0 * THIRD + a * r0) - q2 * (q2 * q2 * THIRD + p2 * r2) - s3 * (p3 * THIRD) - both
        rate = q0 * (a + r0) - q2 * (p2 + r2) - s3
        a = a - value / rate
    return jnp.where(g > 0.5, summed - a, a), lo, hi, slope_d, 0.5 / product


def cube_part(s, h):
    p = jnp.maximum(s, 0.0)
    q = jnp.minimum(p, h)
    r = p - q
    return q * (q * q * THIRD + p * r)


def flow(offset, lo, hi, slope_d, scale, c):
    signed = c * slope_d
    h = jnp.abs(signed)
    s = offset - jnp.where(signed < 0, jnp.abs(slope_d) - h, 0.0)
    t = s - hi
    return scale * ((cube_part(s, h) - cube_part(s - lo, h)) - (cube_part(t, h) - cube_part(t - lo, h)))


def rows(ref, where):
    parts = [ref[z, pl.ds(y, n)] for z, y, n in where]
    return parts[0] if len(parts) == 1 else jnp.concatenate(parts, axis=0)


def put(ref, where, value):
    start = 0
    for z, y, n in where:
        ref[z, pl.ds(y, n)] = value[start : start + n]
        start += n


def moved(where, dz, dy):
    return [(z + dz, y + dy, n) for z, y, n in where]


def loop(first, last, body):
    def step(i, carry):
        body(i)
        return carry

    lax.fori_loop(first, last, step, 0)


def pipelined(count, where_of, *stages):
    depth = len(stages)

    def run(i, live):
        for store in reversed([stages[k](where_of(i - k)) for k in live]):
            store()

    for i in range(depth - 1):
        run(i, range(i + 1))
    loop(depth - 1, count, lambda i: run(i, range(depth)))
    for i in range(count, count + depth - 1):
        run(i, range(i - count + 1, depth))


def kernel(
    f_hbm, vx_hbm, vy_hbm, vz_hbm, out_ref, dt_out,
    f_ext, g1_ext, g2_ext, vx, vy, vz, vx_diff, smooth, diff, sum_y, dif_y, sum_d,
    off, lo, hi, slope, scale, face, edge_y, stat_y, stat_z, speeds, dt_vec, dt_cell,
    load_sem, out_sem, send_sem, recv_sem,
):
    gy, gz = lax.axis_index("gy"), lax.axis_index("gz")

    def neighbour(dy, dz):
        return {"gy": lax.rem(gy + dy + N_GY, N_GY), "gz": lax.rem(gz + dz + N_GZ, N_GZ)}

    corners = [(1, 1), (1, -1), (-1, 1), (-1, -1)]
    own_z, own_y = pl.ds(Z0, NZ), pl.ds(Y0, NY)

    arrays = [(f_hbm, f_ext), (vx_hbm, vx), (vy_hbm, vy), (vz_hbm, vz)]

    def load(k):
        source, target = arrays[k]
        for y in range(NY):
            pltpu.make_async_copy(source.at[:, :, y, :], target.at[own_z, Y0 + y], load_sem.at[k]).start()

    load(0)
    whole = [
        pltpu.make_async_copy(arrays[k + 1][0], speeds.at[k], load_sem.at[4 + k]) for k in range(3)
    ]
    for copy in whole:
        copy.start()
    barrier = pltpu.get_barrier_semaphore()
    greeted = [neighbour(k, 0) for k in range(1, N_GY)]
    greeted += [neighbour(0, k) for k in range(1, N_GZ)] + [neighbour(*c) for c in corners]
    for device in greeted:
        pl.semaphore_signal(barrier, inc=1, device_id=device, device_id_type=pl.DeviceIdType.MESH)

    def remote(source, target, sends, receives, device):
        return pltpu.make_async_remote_copy(
            src_ref=source, dst_ref=target, send_sem=send_sem.at[sends], recv_sem=recv_sem.at[receives],
            device_id=device, device_id_type=pl.DeviceIdType.MESH,
        )

    def halo(g, sends, receives, wide_z, wide_y):
        from_z = {1: pl.ds(Z1 - wide_z, wide_z), -1: pl.ds(Z0, wide_z), 0: own_z}
        from_y = {1: pl.ds(Y1 - wide_y, wide_y), -1: pl.ds(Y0, wide_y), 0: own_y}
        to_z = {1: pl.ds(Z0 - wide_z, wide_z), -1: pl.ds(Z1, wide_z), 0: own_z}
        to_y = {1: pl.ds(Y0 - wide_y, wide_y), -1: pl.ds(Y1, wide_y), 0: own_y}
        return [
            remote(g.at[from_z[dz], from_y[dy]], g.at[to_z[dz], to_y[dy]], sends, receives[k], neighbour(dy, dz))
            for k, (dy, dz) in enumerate([(1, 0), (-1, 0), (0, 1), (0, -1)] + corners)
        ]

    def send(copies):
        for copy in copies:
            copy.start()

    def arrive(part, receives):
        remote(part, part, 0, receives, neighbour(1, 0)).wait_recv()

    def left(part, sends):
        remote(part, part, sends, 0, neighbour(1, 0)).wait_send()

    def some(ref, z, y):
        return ref.at[pl.ds(0, z), pl.ds(0, y)]

    def loaded(k):
        source, target = arrays[k]
        pltpu.make_async_copy(source, target.at[own_z, own_y], load_sem.at[k]).wait()

    def scan_fraction(i, total):
        g = f_ext[i + Z0, own_y]
        return total + g * (1.0 - g)

    loaded(0)
    total = lax.fori_loop(0, NZ, scan_fraction, jnp.zeros((NY, J, LN), F32))
    peak = jnp.zeros((NY, J, LN), F32)
    for k in range(3):
        whole[k].wait()
        peak = lax.fori_loop(0, NZ, lambda z, peak: jnp.maximum(peak, jnp.abs(speeds[k, z])), peak)
    top_row = lax.broadcasted_iota(jnp.int32, (2, LN), 0) == 0

    def combined(ref, n):
        top, add = ref[0], ref[0]
        for k in range(1, n):
            top, add = jnp.maximum(top, ref[k]), add + ref[k]
        return jnp.where(top_row, top, add)

    top, add = jnp.max(peak, axis=0), jnp.sum(total, axis=0)
    stat_y[gy] = jnp.concatenate([jnp.max(top, axis=0, keepdims=True), jnp.sum(add, axis=0, keepdims=True)], axis=0)

    pl.semaphore_wait(barrier, len(greeted))
    halo_f = halo(f_ext, HALO_F, 2 * [HALO_F] + 2 * [HALO_F_NEAR] + 4 * [HALO_F_FAR], 2, 2)
    halo_v = halo(vx, HALO_V, 8 * [HALO_V], 1, 1)
    stats_y = [remote(stat_y.at[gy], stat_y.at[gy], STAT_Y, STAT_Y, neighbour(k, 0)) for k in range(1, N_GY)]
    stats_z = [remote(stat_z.at[gz], stat_z.at[gz], STAT_Z, STAT_Z, neighbour(0, k)) for k in range(1, N_GZ)]
    velocity = [
        remote(vy.at[own_z, Y1 - 1], vy.at[own_z, Y0 - 1], VEL, VEL, neighbour(1, 0)),
        remote(vz.at[Z1 - 1, own_y], vz.at[Z0 - 1, own_y], VEL, VEL, neighbour(0, 1)),
    ]
    send(stats_y)
    send(halo_f[2:4] + halo_f[:2] + halo_f[4:])
    for k in (1, 2, 3):
        load(k)

    def put_shifts(g, where):
        before, after = at_prev(g), at_next(g)
        put(smooth, where, before + 2.0 * g + after)
        put(diff, where, after - before)

    def shift_rows(g_ext, where):
        put_shifts(rows(g_ext, where), where)

    def sums_of(z, y, n):
        s = smooth[z, pl.ds(y - 1, n + 2)]
        d = diff[z, pl.ds(y - 1, n + 2)]

        def store():
            where = [(z, y, n)]
            put(sum_y, where, s[:-2] + 2.0 * s[1:-1] + s[2:])
            put(dif_y, where, s[2:] - s[:-2])
            put(sum_d, where, d[:-2] + 2.0 * d[1:-1] + d[2:])

        return store

    def put_sums(z, y, n):
        sums_of(z, y, n)()

    planes = (off, lo, hi, slope, scale)

    def planes_of(g_ext, dim):
        def stage(where):
            below, above = moved(where, -1, 0), moved(where, 1, 0)
            along_z = rows(sum_y, above) - rows(sum_y, below)
            along_y = rows(dif_y, below) + 2.0 * rows(dif_y, where) + rows(dif_y, above)
            along_x = rows(sum_d, below) + 2.0 * rows(sum_d, where) + rows(sum_d, above)
            slopes = [along_z, along_y, along_x]
            across = [slopes[k] for k in range(3) if k != dim]
            g = rows(g_ext, where)

            def store():
                for ref, value in zip(planes, plane(g, slopes[dim], *across)):
                    put(ref, where, value)

            return store

        return stage

    def put_planes(g_ext, dim, where):
        planes_of(g_ext, dim)(where)()

    def donors_x(where):
        found = [rows(ref, where) for ref in planes]
        q = rows(vx, where)
        others = [at_next(value) for value in found]
        before = at_prev(q)

        def store():
            upward = q > 0
            others[-1] = -others[-1]
            for ref, value, other in zip(planes, found, others):
                put(ref, where, jnp.where(upward, value, other))
            put(vx_diff, where, q - before)

        return store

    def donors(upward, here, there):
        picked = [jnp.where(upward, rows(ref, here), rows(ref, there)) for ref in planes[:-1]]
        return picked + [jnp.where(upward, rows(scale, here), -rows(scale, there))]

    inner = (Y0 + 1, NY - 2)

    def pair(z):
        return [(z, *inner), (z + 1, *inner)]

    def shift_ends(g_ext):
        loop(0, 2, lambda i: shift_rows(g_ext, [(i * Z1, Y0, NY), (i * Z1 + 1, Y0, NY)]))
        loop(0, 4, lambda i: put_sums(i + (i // 2) * (EZ - 4), *inner))

    loop(0, NZ // 2, lambda i: shift_rows(f_ext, [(Z0 + 2 * i, Y0, NY), (Z0 + 2 * i + 1, Y0, NY)]))
    loop(Z0, Z1, lambda z: put_sums(z, *inner))
    loaded(1)
    pipelined(5, lambda i: [(Z0 + 1 + i, *inner)], planes_of(f_ext, 2), donors_x)
    send(halo_v)
    pipelined(NZ - 7, lambda i: [(Z0 + 6 + i, *inner)], planes_of(f_ext, 2), donors_x)
    arrive(some(f_ext, 8, 4), HALO_F_NEAR)
    shift_ends(f_ext)
    loop(0, 2, lambda i: put_planes(f_ext, 2, pair(1 + i * NZ)))
    arrive(some(f_ext, NZ, 4), HALO_F)
    arrive(stat_y.at[pl.ds(0, N_GY - 1)], STAT_Y)
    stat_z[gz] = combined(stat_y, N_GY)
    send(stats_z)

    def shift_sides(i):
        z = Z0 + 4 * i
        shift_rows(f_ext, [w for k in range(4) for w in ((z + k, 0, 2), (z + k, Y1, 2))])

    def sums_side(z):
        put_sums(z, 1, 2)
        put_sums(z, Y1 - 1, 2)

    loop(0, NZ // 4, shift_sides)
    loop(Z0, Z1, sums_side)
    def shift_corners(i):
        z = i * Z1
        shift_rows(f_ext, [(z, 0, 2), (z, Y1, 2), (z + 1, 0, 2), (z + 1, Y1, 2)])

    def side(zs, high):
        return [(z, 1 + high * (Y1 - 2), 2) for z in zs]

    def sides(i):
        high = i // 2
        first = 3 + 6 * (i - 2 * high)
        return side([first + k for k in range(6)], high)

    def side_ends(high):
        return side([1, 2, NZ - 1, NZ, NZ + 1, NZ + 2], high)

    loaded(2)
    loaded(3)
    send(velocity)
    loop(0, 4, lambda i: put_planes(f_ext, 2, sides(i)))
    arrive(some(f_ext, 4, 4), HALO_F_FAR)
    loop(0, 2, shift_corners)
    loop(0, 4, lambda i: sums_side(i + (i // 2) * (EZ - 4)))
    loop(0, 2, lambda i: put_planes(f_ext, 2, side_ends(i)))
    arrive(some(vx, 13, 4), HALO_V)
    loop(0, 2, lambda i: donors_x(pair(1 + i * NZ))())
    loop(0, 2, lambda i: donors_x(side_ends(i))())
    loop(0, 4, lambda i: donors_x(sides(i))())
    arrive(stat_z.at[pl.ds(0, N_GZ - 1)], STAT_Z)
    stats = combined(stat_z, N_GZ)
    umax = jnp.max(stats[0:1], axis=1, keepdims=True)
    share = jnp.sum(stats[1:2], axis=1, keepdims=True) * (4.0 / (N_GZ * NZ * N_GY * NY * J * LN))
    step = COURANT / ((umax + EPSILON) * (1.0 + share))
    dt_vec[...] = jnp.broadcast_to(step, (J, LN))
    dt_cell[...] = step

    def flow_x(where):
        found = [rows(ref, where) for ref in planes]
        q = rows(vx, where)
        return lambda: put(face, where, flow(*found, dt_vec[...] * q))

    def update_x(where):
        out = rows(face, where)
        before = at_prev(out)
        g, change = rows(f_ext, where), rows(vx_diff, where)
        return lambda: put(g1_ext, where, (g - out + before) / (1.0 - dt_vec[...] * change))

    def shifts_of(g_ext):
        def stage(where):
            g = rows(g_ext, where)
            before, after = at_prev(g), at_next(g)

            def store():
                put(smooth, where, before + 2.0 * g + after)
                put(diff, where, after - before)

            return store

        return stage

    dt_copy = pltpu.make_async_copy(dt_cell, dt_out, out_sem)
    x_stages = (flow_x, update_x, shifts_of(g1_ext))
    pipelined(
        NZ // 2 + 1,
        lambda i: [w for z in (1 + 2 * i, 2 + 2 * i) for w in ((z, 1, 3), (z, Y1 - 2, 3))],
        *x_stages,
    )

    dt_copy.start()

    def sums_edge(first, n):
        for z in range(n):
            put_sums(first + z, Y0, 1)
            put_sums(first + z, Y1 - 1, 1)

    def edges(first, n):
        return [w for k in range(n) for w in ((first + k, Y0, 1), (first + k, Y1 - 1, 1))]

    def half_faces_y(i):
        z = Z0 + 4 * i
        at_face = [w for k in range(4) for w in ((z + k, Y0 - 1, 1), (z + k, Y1 - 1, 1))]
        c = dt_vec[...] * rows(vy, at_face)
        out = flow(*[rows(ref, edges(z, 4)) for ref in planes], c)
        for k in range(4):
            edge_y[0, 4 * i + k] = jnp.where(c[2 * k + 1] > 0, out[2 * k + 1], 0.0)
            edge_y[1, 4 * i + k] = jnp.where(c[2 * k] < 0, out[2 * k], 0.0)

    flux_y = []
    for k in range(2):
        part = pl.ds(k * (NZ // 2), NZ // 2)
        flux_y += [
            remote(edge_y.at[0, part], edge_y.at[2, part], FLUX, FLUX, neighbour(1, 0)),
            remote(edge_y.at[1, part], edge_y.at[3, part], FLUX, FLUX, neighbour(-1, 0)),
        ]
    arrive(some(vy, 6, 4), VEL)
    loop(0, (NZ + 2) // 3, lambda i: sums_edge(Z0 - 1 + 3 * i, 3))
    for k in range(2):
        put_planes(g1_ext, 1, edges(Z0 + k * (NZ // 2), NZ // 2))
        loop(2 * k, 2 * k + 2, half_faces_y)
        send(flux_y[2 * k : 2 * k + 2])

    def middle(i):
        return [(1 + 3 * i + k, Y0 + 2, NY - 4) for k in range(3)]

    def faces_y(where):
        c = dt_vec[...] * rows(vy, where)
        put(face, where, flow(*donors(c > 0, where, moved(where, 0, 1)), c))

    pipelined((NZ + 2) // 3, middle, *x_stages)
    def y_sums(i):
        for store in [sums_of(Z0 - 1 + 3 * i + k, *inner) for k in range(3)]:
            store()

    def y_near(i):
        z = Z0 + 8 * i
        put_planes(g1_ext, 1, [w for k in range(8) for w in ((z + k, Y0 + 1, 1), (z + k, Y1 - 2, 1))])

    def y_middle(i):
        put_planes(g1_ext, 1, [(Z0 + 4 * i + k, Y0 + 2, NY - 4) for k in range(4)])

    loop(0, (NZ + 2) // 3, y_sums)
    loop(0, 2, y_near)
    loop(0, 2, lambda i: y_middle(3 * i))
    def faces_y_near(i):
        z = Z0 + 4 * i
        faces_y([w for k in range(4) for w in ((z + k, Y0, 1), (z + k, Y1 - 2, 1))])

    def update_y(where):
        before, q = moved(where, 0, -1), dt_vec[...]
        g = rows(g1_ext, where) - rows(face, where) + rows(face, before)
        put(g2_ext, where, g / (1.0 - q * (rows(vy, where) - rows(vy, before))))

    def update_y_edge(i):
        for k in range(4):
            z, at = Z0 + 4 * i + k, 4 * i + k
            face[z, Y0 - 1] = edge_y[2, at] - edge_y[1, at]
            face[z, Y1 - 1] = edge_y[0, at] - edge_y[3, at]
        update_y(edges(Z0 + 4 * i, 4))

    def rest_y(i):
        z = Z0 + 2 * lax.rem(7 * i, NZ // 2)
        faces_y([(z, Y0 + 1, NY - 3), (z + 1, Y0 + 1, NY - 3)])
        update_y([(z, *inner), (z + 1, *inner)])

    near = [HALO_G, HALO_G, HALO_G_NEAR, HALO_G_NEAR] + 4 * [HALO_G]
    halo_g = halo(g2_ext, HALO_G, near, 2, 1)
    loop(0, NZ // 4, faces_y_near)
    arrive(edge_y.at[pl.ds(2, 2)], FLUX)
    loop(0, NZ // 4, update_y_edge)
    send(halo_g[:2] + halo_g[4:])
    loop(0, 2, rest_y)
    send(halo_g[2:4])
    loop(1, 3, y_middle)
    loop(2, NZ // 2, rest_y)

    def faces_z(where):
        c = dt_vec[...] * rows(vz, where)
        put(face, where, flow(*donors(c > 0, where, moved(where, 1, 0)), c))

    shift_rows(g2_ext, [(Z0, Y0, NY), (Z0 + 1, Y0, NY)])
    shift_rows(g2_ext, [(Z0 + 2, Y0, NY), (Z0 + 3, Y0, NY)])
    loop(Z0, Z0 + 3, lambda z: put_sums(z, *inner))

    def z_inner(z):
        stores = (
            shifts_of(g2_ext)([(z + 3, Y0, NY)]),
            planes_of(g2_ext, 0)([(z, *inner)]),
            sums_of(z + 2, *inner),
        )
        for store in reversed(stores):
            store()

    loop(Z0 + 1, Z1 - 3, z_inner)
    put_sums(Z1 - 1, *inner)
    put_planes(g2_ext, 0, pair(Z1 - 3))
    loop(0, NZ // 2 - 2, lambda i: faces_z(pair(Z0 + 1 + 2 * i)))
    faces_z([(Z1 - 3, *inner)])
    arrive(some(g2_ext, 8, 4), HALO_G_NEAR)
    shift_ends(g2_ext)
    loop(0, 2, lambda i: put_planes(g2_ext, 0, pair(1 + i * NZ)))
    loop(0, 2, lambda i: faces_z(pair(1 + i * (NZ - 1))))

    def update_z(where):
        before, q = moved(where, -1, 0), dt_vec[...]
        g = rows(g2_ext, where) - rows(face, where) + rows(face, before)
        g = g / (1.0 - q * (rows(vz, where) - rows(vz, before)))
        for k, (z, y) in enumerate([(z, y + k) for z, y, n in where for k in range(n)]):
            out_ref[z - Z0, pl.ds(y - Y0, J, stride=NY), :] = g[k]

    loop(Z0, Z1, lambda z: update_z([(z, *inner)]))
    arrive(some(g2_ext, 10, 4), HALO_G)
    loop(0, 2, lambda i: shift_rows(
        g2_ext, [w for k in range(EZ // 2) for w in ((i * (EZ // 2) + k, Y0 - 1, 1), (i * (EZ // 2) + k, Y1, 1))]
    ))
    loop(0, EZ // 4, lambda i: sums_edge(4 * i, 4))
    loop(0, (NZ + 2) // 6, lambda i: put_planes(g2_ext, 0, edges(1 + 6 * i, 6)))
    loop(0, 2, lambda i: faces_z(edges(1 + 6 * i, 6)))
    faces_z(edges(Z1 - 5, 5))

    loop(0, NZ // 4, lambda i: update_z(edges(Z0 + 4 * i, 4)))
    left(some(f_ext, 14, 8), HALO_F)
    left(some(vx, 13, 4), HALO_V)
    left(some(g2_ext, 9, 8), HALO_G)
    left(some(vy, 6, 4), VEL)
    left(edge_y.at[pl.ds(0, 2)], FLUX)
    left(stat_y.at[pl.ds(0, N_GY - 1)], STAT_Y)
    left(stat_z.at[pl.ds(0, N_GZ - 1)], STAT_Z)
    dt_copy.wait()


def shards(*blocks):
    tiled = [b.reshape(NZ, NY, J, LN).transpose(0, 2, 1, 3) for b in blocks]
    row = (J, LN)
    ext = pltpu.VMEM((EZ, EY, *row), F32)
    anywhere = pl.BlockSpec(memory_space=pl.ANY)
    field, step = pl.pallas_call(
        kernel,
        out_shape=(pltpu.VMEM((NZ, J * NY, LN), F32), jax.ShapeDtypeStruct((1, 1), F32)),
        in_specs=[anywhere] * 4,
        out_specs=(pl.BlockSpec(memory_space=pltpu.VMEM), anywhere),
        scratch_shapes=[ext] * 18 + [
            pltpu.VMEM((4, NZ, *row), F32),
            pltpu.VMEM((N_GY, 2, LN), F32), pltpu.VMEM((N_GZ, 2, LN), F32),
            pltpu.VMEM((3, NZ, J, NY, LN), F32),
            pltpu.VMEM(row, F32), pltpu.VMEM((1, 1), F32),
            pltpu.SemaphoreType.DMA((7,)), pltpu.SemaphoreType.DMA(()),
            pltpu.SemaphoreType.DMA((N_SEND,)), pltpu.SemaphoreType.DMA((N_RECV,)),
        ],
        compiler_params=pltpu.CompilerParams(collective_id=0, has_side_effects=True),
        name="advect",
    )(*tiled)
    return field.reshape(NZ, J, NY, LN).transpose(0, 2, 1, 3).reshape(NZ, NY, J * LN), step.reshape(())


def solution(mesh):
    spec = P("gz", "gy", None)
    return jax.shard_map(shards, mesh=mesh, in_specs=(spec,) * 4, out_specs=(spec, P()), check_vma=False)
```

```python
import jax
import jax.numpy as jnp
from jax import lax
from jax.experimental import pallas as pl
from jax.experimental.pallas import tpu as pltpu
from jax.sharding import PartitionSpec as P

NEWTON = 5
TILT_FLOOR = 3.2
TINY = 1e-18
COURANT = 0.45
EPSILON = 1e-6
THIRD = 1.0 / 3.0

NZ, NY, J, LN = 16, 8, 8, 128
N_GY, N_GZ = 16, 8
F32 = jnp.float32

EZ, EY = NZ + 4, NY + 4
Z0, Y0 = 2, 2
Z1, Y1 = Z0 + NZ, Y0 + NY

HALO_F, HALO_V, HALO_G, VEL, FLUX, STAT_Y, STAT_Z = range(7)
HALO_F_NEAR, HALO_F_FAR, HALO_G_NEAR = 7, 8, 9
N_SEND, N_RECV = 7, 10


def lanes(u):
    return lax.broadcasted_iota(jnp.int32, u.shape, u.ndim - 1)


def at_next(u):
    moved = pltpu.roll(u, LN - 1, u.ndim - 1)
    return jnp.where(lanes(u) == LN - 1, pltpu.roll(moved, J - 1, u.ndim - 2), moved)


def at_prev(u):
    moved = pltpu.roll(u, 1, u.ndim - 1)
    return jnp.where(lanes(u) == 0, pltpu.roll(moved, 1, u.ndim - 2), moved)


def plane(g, slope_d, slope_a, slope_b):
    tilt_a = jnp.abs(slope_a) + TILT_FLOOR
    tilt_b = jnp.abs(slope_b) + TILT_FLOOR
    lo, hi = jnp.minimum(tilt_a, tilt_b), jnp.maximum(tilt_a, tilt_b)
    slope_d = jnp.where(jnp.abs(slope_d) < TINY, TINY, slope_d)
    tilt_d = jnp.abs(slope_d)
    m1, rest = jnp.minimum(lo, tilt_d), jnp.maximum(lo, tilt_d)
    m2, m3 = jnp.minimum(rest, hi), jnp.maximum(rest, hi)
    lesser = jnp.maximum(jnp.minimum(g, 1.0 - g), 0.0)
    m12 = m1 * m2
    product = m12 * m3
    target = lesser * product
    both = target + target
    summed = lo + hi + tilt_d
    w = 0.5 * jnp.maximum(m1 + m2 - m3, 0.0)
    a = 0.5 * summed - (0.5 * product - target) / (m12 - w * w)
    for _ in range(NEWTON - 1):
        q0 = jnp.minimum(a, m1)
        r0 = a - q0
        p2 = jnp.maximum(a - m2, 0.0)
        q2 = jnp.minimum(p2, m1)
        r2 = p2 - q2
        p3 = jnp.maximum(a - m3, 0.0)
        s3 = p3 * p3
        value = q0 * (q0 * q0 * THIRD + a * r0) - q2 * (q2 * q2 * THIRD + p2 * r2) - s3 * (p3 * THIRD) - both
        rate = q0 * (a + r0) - q2 * (p2 + r2) - s3
        a = a - value / rate
    return jnp.where(g > 0.5, summed - a, a), lo, hi, slope_d, 0.5 / product


def cube_part(s, h):
    p = jnp.maximum(s, 0.0)
    q = jnp.minimum(p, h)
    r = p - q
    return q * (q * q * THIRD + p * r)


def flow(offset, lo, hi, slope_d, scale, c):
    signed = c * slope_d
    h = jnp.abs(signed)
    s = offset - jnp.where(signed < 0, jnp.abs(slope_d) - h, 0.0)
    t = s - hi
    return scale * ((cube_part(s, h) - cube_part(s - lo, h)) - (cube_part(t, h) - cube_part(t - lo, h)))


def rows(ref, where):
    parts = [ref[z, pl.ds(y, n)] for z, y, n in where]
    return parts[0] if len(parts) == 1 else jnp.concatenate(parts, axis=0)


def put(ref, where, value):
    start = 0
    for z, y, n in where:
        ref[z, pl.ds(y, n)] = value[start : start + n]
        start += n


def moved(where, dz, dy):
    return [(z + dz, y + dy, n) for z, y, n in where]


def loop(first, last, body):
    def step(i, carry):
        body(i)
        return carry

    lax.fori_loop(first, last, step, 0)


def pipelined(count, where_of, *stages):
    depth = len(stages)

    def run(i, live):
        for store in reversed([stages[k](where_of(i - k)) for k in live]):
            store()

    for i in range(depth - 1):
        run(i, range(i + 1))
    loop(depth - 1, count, lambda i: run(i, range(depth)))
    for i in range(count, count + depth - 1):
        run(i, range(i - count + 1, depth))


def kernel(
    f_hbm, vx_hbm, vy_hbm, vz_hbm, out_ref, dt_out,
    f_ext, g1_ext, g2_ext, vx, vy, vz, vx_diff, smooth, diff, sum_y, dif_y, sum_d,
    off, lo, hi, slope, scale, face, edge_y, stat_y, stat_z, dt_vec, dt_cell,
    load_sem, out_sem, send_sem, recv_sem,
):
    gy, gz = lax.axis_index("gy"), lax.axis_index("gz")

    def neighbour(dy, dz):
        return {"gy": lax.rem(gy + dy + N_GY, N_GY), "gz": lax.rem(gz + dz + N_GZ, N_GZ)}

    corners = [(1, 1), (1, -1), (-1, 1), (-1, -1)]
    own_z, own_y = pl.ds(Z0, NZ), pl.ds(Y0, NY)

    arrays = [(f_hbm, f_ext), (vx_hbm, vx), (vy_hbm, vy), (vz_hbm, vz)]

    def load(k):
        source, target = arrays[k]
        for y in range(NY):
            pltpu.make_async_copy(source.at[:, :, y, :], target.at[own_z, Y0 + y], load_sem.at[k]).start()

    load(0)
    barrier = pltpu.get_barrier_semaphore()
    greeted = [neighbour(k, 0) for k in range(1, N_GY)]
    greeted += [neighbour(0, k) for k in range(1, N_GZ)] + [neighbour(*c) for c in corners]
    for device in greeted:
        pl.semaphore_signal(barrier, inc=1, device_id=device, device_id_type=pl.DeviceIdType.MESH)
    for k in (1, 2, 3):
        load(k)

    def remote(source, target, sends, receives, device):
        return pltpu.make_async_remote_copy(
            src_ref=source, dst_ref=target, send_sem=send_sem.at[sends], recv_sem=recv_sem.at[receives],
            device_id=device, device_id_type=pl.DeviceIdType.MESH,
        )

    def halo(g, sends, receives, wide_z, wide_y):
        from_z = {1: pl.ds(Z1 - wide_z, wide_z), -1: pl.ds(Z0, wide_z), 0: own_z}
        from_y = {1: pl.ds(Y1 - wide_y, wide_y), -1: pl.ds(Y0, wide_y), 0: own_y}
        to_z = {1: pl.ds(Z0 - wide_z, wide_z), -1: pl.ds(Z1, wide_z), 0: own_z}
        to_y = {1: pl.ds(Y0 - wide_y, wide_y), -1: pl.ds(Y1, wide_y), 0: own_y}
        return [
            remote(g.at[from_z[dz], from_y[dy]], g.at[to_z[dz], to_y[dy]], sends, receives[k], neighbour(dy, dz))
            for k, (dy, dz) in enumerate([(1, 0), (-1, 0), (0, 1), (0, -1)] + corners)
        ]

    def send(copies):
        for copy in copies:
            copy.start()

    def arrive(part, receives):
        remote(part, part, 0, receives, neighbour(1, 0)).wait_recv()

    def left(part, sends):
        remote(part, part, sends, 0, neighbour(1, 0)).wait_send()

    def some(ref, z, y):
        return ref.at[pl.ds(0, z), pl.ds(0, y)]

    def loaded(k):
        source, target = arrays[k]
        pltpu.make_async_copy(source, target.at[own_z, own_y], load_sem.at[k]).wait()

    def scan_fraction(i, total):
        g = f_ext[i + Z0, own_y]
        return total + g * (1.0 - g)

    loaded(0)
    total = lax.fori_loop(0, NZ, scan_fraction, jnp.zeros((NY, J, LN), F32))
    peak = jnp.zeros((NY, J, LN), F32)
    for k in (1, 2, 3):
        loaded(k)
        speeds = arrays[k][1]
        peak = lax.fori_loop(0, NZ, lambda i, peak: jnp.maximum(peak, jnp.abs(speeds[i + Z0, own_y])), peak)
    top_row = lax.broadcasted_iota(jnp.int32, (2, LN), 0) == 0

    def combined(ref, n):
        top, add = ref[0], ref[0]
        for k in range(1, n):
            top, add = jnp.maximum(top, ref[k]), add + ref[k]
        return jnp.where(top_row, top, add)

    top, add = jnp.max(peak, axis=0), jnp.sum(total, axis=0)
    stat_y[gy] = jnp.concatenate([jnp.max(top, axis=0, keepdims=True), jnp.sum(add, axis=0, keepdims=True)], axis=0)

    pl.semaphore_wait(barrier, len(greeted))
    halo_f = halo(f_ext, HALO_F, 2 * [HALO_F] + 2 * [HALO_F_NEAR] + 4 * [HALO_F_FAR], 2, 2)
    halo_v = halo(vx, HALO_V, 8 * [HALO_V], 1, 1)
    stats_y = [remote(stat_y.at[gy], stat_y.at[gy], STAT_Y, STAT_Y, neighbour(k, 0)) for k in range(1, N_GY)]
    stats_z = [remote(stat_z.at[gz], stat_z.at[gz], STAT_Z, STAT_Z, neighbour(0, k)) for k in range(1, N_GZ)]
    velocity = [
        remote(vy.at[own_z, Y1 - 1], vy.at[own_z, Y0 - 1], VEL, VEL, neighbour(1, 0)),
        remote(vz.at[Z1 - 1, own_y], vz.at[Z0 - 1, own_y], VEL, VEL, neighbour(0, 1)),
    ]
    send(stats_y)
    send(halo_f[2:4] + halo_f[:2] + halo_f[4:])

    def put_shifts(g, where):
        before, after = at_prev(g), at_next(g)
        put(smooth, where, before + 2.0 * g + after)
        put(diff, where, after - before)

    def shift_rows(g_ext, where):
        put_shifts(rows(g_ext, where), where)

    def sums_of(z, y, n):
        s = smooth[z, pl.ds(y - 1, n + 2)]
        d = diff[z, pl.ds(y - 1, n + 2)]

        def store():
            where = [(z, y, n)]
            put(sum_y, where, s[:-2] + 2.0 * s[1:-1] + s[2:])
            put(dif_y, where, s[2:] - s[:-2])
            put(sum_d, where, d[:-2] + 2.0 * d[1:-1] + d[2:])

        return store

    def put_sums(z, y, n):
        sums_of(z, y, n)()

    planes = (off, lo, hi, slope, scale)

    def planes_of(g_ext, dim):
        def stage(where):
            below, above = moved(where, -1, 0), moved(where, 1, 0)
            along_z = rows(sum_y, above) - rows(sum_y, below)
            along_y = rows(dif_y, below) + 2.0 * rows(dif_y, where) + rows(dif_y, above)
            along_x = rows(sum_d, below) + 2.0 * rows(sum_d, where) + rows(sum_d, above)
            slopes = [along_z, along_y, along_x]
            across = [slopes[k] for k in range(3) if k != dim]
            g = rows(g_ext, where)

            def store():
                for ref, value in zip(planes, plane(g, slopes[dim], *across)):
                    put(ref, where, value)

            return store

        return stage

    def put_planes(g_ext, dim, where):
        planes_of(g_ext, dim)(where)()

    def donors_x(where):
        found = [rows(ref, where) for ref in planes]
        q = rows(vx, where)
        others = [at_next(value) for value in found]
        before = at_prev(q)

        def store():
            upward = q > 0
            others[-1] = -others[-1]
            for ref, value, other in zip(planes, found, others):
                put(ref, where, jnp.where(upward, value, other))
            put(vx_diff, where, q - before)

        return store

    def donors(upward, here, there):
        picked = [jnp.where(upward, rows(ref, here), rows(ref, there)) for ref in planes[:-1]]
        return picked + [jnp.where(upward, rows(scale, here), -rows(scale, there))]

    inner = (Y0 + 1, NY - 2)

    def pair(z):
        return [(z, *inner), (z + 1, *inner)]

    def shift_ends(g_ext):
        loop(0, 2, lambda i: shift_rows(g_ext, [(i * Z1, Y0, NY), (i * Z1 + 1, Y0, NY)]))
        loop(0, 4, lambda i: put_sums(i + (i // 2) * (EZ - 4), *inner))

    loop(0, NZ // 2, lambda i: shift_rows(f_ext, [(Z0 + 2 * i, Y0, NY), (Z0 + 2 * i + 1, Y0, NY)]))
    loop(Z0, Z1, lambda z: put_sums(z, *inner))
    pipelined(5, lambda i: [(Z0 + 1 + i, *inner)], planes_of(f_ext, 2), donors_x)
    send(halo_v)
    pipelined(NZ - 7, lambda i: [(Z0 + 6 + i, *inner)], planes_of(f_ext, 2), donors_x)
    arrive(some(f_ext, 8, 4), HALO_F_NEAR)
    shift_ends(f_ext)
    loop(0, 2, lambda i: put_planes(f_ext, 2, pair(1 + i * NZ)))
    donors_x([(Z0, *inner), (Z1 - 1, *inner)])()
    arrive(some(f_ext, NZ, 4), HALO_F)
    arrive(stat_y.at[pl.ds(0, N_GY - 1)], STAT_Y)
    stat_z[gz] = combined(stat_y, N_GY)
    send(stats_z)

    def shift_sides(i):
        z = Z0 + 4 * i
        shift_rows(f_ext, [w for k in range(4) for w in ((z + k, 0, 2), (z + k, Y1, 2))])

    def sums_side(z):
        put_sums(z, 1, 2)
        put_sums(z, Y1 - 1, 2)

    loop(0, NZ // 4, shift_sides)
    loop(Z0, Z1, sums_side)
    def shift_corners(i):
        z = i * Z1
        shift_rows(f_ext, [(z, 0, 2), (z, Y1, 2), (z + 1, 0, 2), (z + 1, Y1, 2)])

    def column(zs, y):
        return [(z, y, 1) for z in zs]

    def own_columns(i):
        first, high = 3 + 6 * (i - 2 * (i // 2)), i // 2
        return column([first + k for k in range(6)], Y0 + high * (NY - 1))

    def next_columns(i):
        first, high = 3 + 6 * (i - 2 * (i // 2)), i // 2
        return column([first + k for k in range(6)], Y0 - 1 + high * (NY + 1))

    def end_columns(i):
        return column([1, 2, NZ - 1, NZ, NZ + 1, NZ + 2], 1 + i + (i // 2) * (NY - 2))

    planes_x = planes_of(f_ext, 2)
    send(velocity)
    pipelined(4, own_columns, planes_x, donors_x)
    arrive(some(vx, 13, 4), HALO_V)
    pipelined(4, next_columns, planes_x, donors_x)
    arrive(some(f_ext, 4, 4), HALO_F_FAR)
    loop(0, 2, shift_corners)
    loop(0, 4, lambda i: sums_side(i + (i // 2) * (EZ - 4)))
    pipelined(4, end_columns, planes_x, donors_x)
    donors_x([(1, *inner), (NZ + 2, *inner)])()
    arrive(stat_z.at[pl.ds(0, N_GZ - 1)], STAT_Z)
    stats = combined(stat_z, N_GZ)
    umax = jnp.max(stats[0:1], axis=1, keepdims=True)
    share = jnp.sum(stats[1:2], axis=1, keepdims=True) * (4.0 / (N_GZ * NZ * N_GY * NY * J * LN))
    step = COURANT / ((umax + EPSILON) * (1.0 + share))
    dt_vec[...] = jnp.broadcast_to(step, (J, LN))
    dt_cell[...] = step

    def flow_x(where):
        found = [rows(ref, where) for ref in planes]
        q = rows(vx, where)
        return lambda: put(face, where, flow(*found, dt_vec[...] * q))

    def update_x(where):
        out = rows(face, where)
        before = at_prev(out)
        g, change = rows(f_ext, where), rows(vx_diff, where)
        return lambda: put(g1_ext, where, (g - out + before) / (1.0 - dt_vec[...] * change))

    def shifts_of(g_ext):
        def stage(where):
            g = rows(g_ext, where)
            before, after = at_prev(g), at_next(g)

            def store():
                put(smooth, where, before + 2.0 * g + after)
                put(diff, where, after - before)

            return store

        return stage

    dt_copy = pltpu.make_async_copy(dt_cell, dt_out, out_sem)
    x_stages = (flow_x, update_x, shifts_of(g1_ext))
    pipelined(
        NZ // 2 + 1,
        lambda i: [w for z in (1 + 2 * i, 2 + 2 * i) for w in ((z, 1, 3), (z, Y1 - 2, 3))],
        *x_stages,
    )

    dt_copy.start()

    def sums_edge(first, n):
        for z in range(n):
            put_sums(first + z, Y0, 1)
            put_sums(first + z, Y1 - 1, 1)

    def edges(first, n):
        return [w for k in range(n) for w in ((first + k, Y0, 1), (first + k, Y1 - 1, 1))]

    def half_faces_y(i):
        z = Z0 + 4 * i
        at_face = [w for k in range(4) for w in ((z + k, Y0 - 1, 1), (z + k, Y1 - 1, 1))]
        c = dt_vec[...] * rows(vy, at_face)
        out = flow(*[rows(ref, edges(z, 4)) for ref in planes], c)
        for k in range(4):
            edge_y[0, 4 * i + k] = jnp.where(c[2 * k + 1] > 0, out[2 * k + 1], 0.0)
            edge_y[1, 4 * i + k] = jnp.where(c[2 * k] < 0, out[2 * k], 0.0)

    flux_y = []
    for k in range(2):
        part = pl.ds(k * (NZ // 2), NZ // 2)
        flux_y += [
            remote(edge_y.at[0, part], edge_y.at[2, part], FLUX, FLUX, neighbour(1, 0)),
            remote(edge_y.at[1, part], edge_y.at[3, part], FLUX, FLUX, neighbour(-1, 0)),
        ]
    arrive(some(vy, 6, 4), VEL)
    loop(0, (NZ + 2) // 3, lambda i: sums_edge(Z0 - 1 + 3 * i, 3))
    for k in range(2):
        put_planes(g1_ext, 1, edges(Z0 + k * (NZ // 2), NZ // 2))
        loop(2 * k, 2 * k + 2, half_faces_y)
        send(flux_y[2 * k : 2 * k + 2])

    def middle(i):
        return [(1 + 3 * i + k, Y0 + 2, NY - 4) for k in range(3)]

    def faces_y(where):
        c = dt_vec[...] * rows(vy, where)
        put(face, where, flow(*donors(c > 0, where, moved(where, 0, 1)), c))

    pipelined((NZ + 2) // 3, middle, *x_stages)
    loop(Z0 - 1, Z0 + 3, lambda z: put_sums(z, *inner))

    def y_inner(i):
        z = Z0 + 2 * i
        stores = planes_of(g1_ext, 1)(pair(z)), sums_of(z + 3, *inner), sums_of(z + 4, *inner)
        for store in stores:
            store()

    loop(0, NZ // 2 - 1, y_inner)
    put_planes(g1_ext, 1, pair(Z1 - 2))
    def faces_y_near(i):
        z = Z0 + 4 * i
        faces_y([w for k in range(4) for w in ((z + k, Y0, 1), (z + k, Y1 - 2, 1))])

    def update_y(where):
        before, q = moved(where, 0, -1), dt_vec[...]
        g = rows(g1_ext, where) - rows(face, where) + rows(face, before)
        put(g2_ext, where, g / (1.0 - q * (rows(vy, where) - rows(vy, before))))

    def update_y_edge(i):
        for k in range(4):
            z, at = Z0 + 4 * i + k, 4 * i + k
            face[z, Y0 - 1] = edge_y[2, at] - edge_y[1, at]
            face[z, Y1 - 1] = edge_y[0, at] - edge_y[3, at]
        update_y(edges(Z0 + 4 * i, 4))

    def rest_y(i):
        z = Z0 + 2 * lax.rem(7 * i, NZ // 2)
        faces_y([(z, Y0 + 1, NY - 3), (z + 1, Y0 + 1, NY - 3)])
        update_y([(z, *inner), (z + 1, *inner)])

    near = [HALO_G, HALO_G, HALO_G_NEAR, HALO_G_NEAR] + 4 * [HALO_G]
    halo_g = halo(g2_ext, HALO_G, near, 2, 1)
    loop(0, NZ // 4, faces_y_near)
    arrive(edge_y.at[pl.ds(2, 2)], FLUX)
    loop(0, NZ // 4, update_y_edge)
    send(halo_g[:2] + halo_g[4:])
    loop(0, 2, rest_y)
    send(halo_g[2:4])
    loop(2, NZ // 2, rest_y)

    def faces_z(where):
        c = dt_vec[...] * rows(vz, where)
        put(face, where, flow(*donors(c > 0, where, moved(where, 1, 0)), c))

    shift_rows(g2_ext, [(Z0, Y0, NY), (Z0 + 1, Y0, NY)])
    shift_rows(g2_ext, [(Z0 + 2, Y0, NY), (Z0 + 3, Y0, NY)])
    loop(Z0, Z0 + 3, lambda z: put_sums(z, *inner))

    def z_inner(z):
        stores = (
            shifts_of(g2_ext)([(z + 3, Y0, NY)]),
            planes_of(g2_ext, 0)([(z, *inner)]),
            sums_of(z + 2, *inner),
        )
        for store in reversed(stores):
            store()

    loop(Z0 + 1, Z1 - 3, z_inner)
    put_sums(Z1 - 1, *inner)
    put_planes(g2_ext, 0, pair(Z1 - 3))
    loop(0, NZ // 2 - 2, lambda i: faces_z(pair(Z0 + 1 + 2 * i)))
    faces_z([(Z1 - 3, *inner)])
    arrive(some(g2_ext, 8, 4), HALO_G_NEAR)
    shift_ends(g2_ext)
    loop(0, 2, lambda i: put_planes(g2_ext, 0, pair(1 + i * NZ)))
    loop(0, 2, lambda i: faces_z(pair(1 + i * (NZ - 1))))

    def update_z(where):
        before, q = moved(where, -1, 0), dt_vec[...]
        g = rows(g2_ext, where) - rows(face, where) + rows(face, before)
        g = g / (1.0 - q * (rows(vz, where) - rows(vz, before)))
        for k, (z, y) in enumerate([(z, y + k) for z, y, n in where for k in range(n)]):
            out_ref[z - Z0, pl.ds(y - Y0, J, stride=NY), :] = g[k]

    loop(Z0, Z1, lambda z: update_z([(z, *inner)]))
    arrive(some(g2_ext, 10, 4), HALO_G)
    loop(0, 2, lambda i: shift_rows(
        g2_ext, [w for k in range(EZ // 2) for w in ((i * (EZ // 2) + k, Y0 - 1, 1), (i * (EZ // 2) + k, Y1, 1))]
    ))
    loop(0, EZ // 4, lambda i: sums_edge(4 * i, 4))
    loop(0, (NZ + 2) // 6, lambda i: put_planes(g2_ext, 0, edges(1 + 6 * i, 6)))
    loop(0, 2, lambda i: faces_z(edges(1 + 6 * i, 6)))
    faces_z(edges(Z1 - 5, 5))

    loop(0, NZ // 4, lambda i: update_z(edges(Z0 + 4 * i, 4)))
    left(some(f_ext, 14, 8), HALO_F)
    left(some(vx, 13, 4), HALO_V)
    left(some(g2_ext, 9, 8), HALO_G)
    left(some(vy, 6, 4), VEL)
    left(edge_y.at[pl.ds(0, 2)], FLUX)
    left(stat_y.at[pl.ds(0, N_GY - 1)], STAT_Y)
    left(stat_z.at[pl.ds(0, N_GZ - 1)], STAT_Z)
    dt_copy.wait()


def shards(*blocks):
    tiled = [b.reshape(NZ, NY, J, LN).transpose(0, 2, 1, 3) for b in blocks]
    row = (J, LN)
    ext = pltpu.VMEM((EZ, EY, *row), F32)
    anywhere = pl.BlockSpec(memory_space=pl.ANY)
    field, step = pl.pallas_call(
        kernel,
        out_shape=(pltpu.VMEM((NZ, J * NY, LN), F32), jax.ShapeDtypeStruct((1, 1), F32)),
        in_specs=[anywhere] * 4,
        out_specs=(pl.BlockSpec(memory_space=pltpu.VMEM), anywhere),
        scratch_shapes=[ext] * 18 + [
            pltpu.VMEM((4, NZ, *row), F32),
            pltpu.VMEM((N_GY, 2, LN), F32), pltpu.VMEM((N_GZ, 2, LN), F32),
            pltpu.VMEM(row, F32), pltpu.VMEM((1, 1), F32),
            pltpu.SemaphoreType.DMA((4,)), pltpu.SemaphoreType.DMA(()),
            pltpu.SemaphoreType.DMA((N_SEND,)), pltpu.SemaphoreType.DMA((N_RECV,)),
        ],
        compiler_params=pltpu.CompilerParams(collective_id=0, has_side_effects=True),
        name="advect",
    )(*tiled)
    return field.reshape(NZ, J, NY, LN).transpose(0, 2, 1, 3).reshape(NZ, NY, J * LN), step.reshape(())


def solution(mesh):
    spec = P("gz", "gy", None)
    return jax.shard_map(shards, mesh=mesh, in_specs=(spec,) * 4, out_specs=(spec, P()), check_vma=False)
```

```python
import jax
import jax.numpy as jnp
from jax import lax
from jax.experimental import pallas as pl
from jax.experimental.pallas import tpu as pltpu
from jax.sharding import PartitionSpec as P

NEWTON = 5
TILT_FLOOR = 3.2
TINY = 1e-18
COURANT = 0.45
EPSILON = 1e-6
THIRD = 1.0 / 3.0

NZ, NY, J, LN = 16, 8, 8, 128
N_GY, N_GZ = 16, 8
F32 = jnp.float32

EZ, EY = NZ + 4, NY + 4
Z0, Y0 = 2, 2
Z1, Y1 = Z0 + NZ, Y0 + NY

HALO_F, HALO_V, HALO_G, VEL, FLUX, STAT_Y, STAT_Z = range(7)
HALO_F_NEAR, HALO_F_FAR, HALO_G_NEAR = 7, 8, 9
N_SEND, N_RECV = 7, 10


def lanes(u):
    return lax.broadcasted_iota(jnp.int32, u.shape, u.ndim - 1)


def at_next(u):
    moved = pltpu.roll(u, LN - 1, u.ndim - 1)
    return jnp.where(lanes(u) == LN - 1, pltpu.roll(moved, J - 1, u.ndim - 2), moved)


def at_prev(u):
    moved = pltpu.roll(u, 1, u.ndim - 1)
    return jnp.where(lanes(u) == 0, pltpu.roll(moved, 1, u.ndim - 2), moved)


def plane(g, slope_d, slope_a, slope_b):
    tilt_a = jnp.abs(slope_a) + TILT_FLOOR
    tilt_b = jnp.abs(slope_b) + TILT_FLOOR
    lo, hi = jnp.minimum(tilt_a, tilt_b), jnp.maximum(tilt_a, tilt_b)
    slope_d = jnp.where(jnp.abs(slope_d) < TINY, TINY, slope_d)
    tilt_d = jnp.abs(slope_d)
    m1, rest = jnp.minimum(lo, tilt_d), jnp.maximum(lo, tilt_d)
    m2, m3 = jnp.minimum(rest, hi), jnp.maximum(rest, hi)
    lesser = jnp.maximum(jnp.minimum(g, 1.0 - g), 0.0)
    m12 = m1 * m2
    product = m12 * m3
    target = lesser * product
    both = target + target
    summed = lo + hi + tilt_d
    w = 0.5 * jnp.maximum(m1 + m2 - m3, 0.0)
    a = 0.5 * summed - (0.5 * product - target) / (m12 - w * w)
    for _ in range(NEWTON - 1):
        q0 = jnp.minimum(a, m1)
        r0 = a - q0
        p2 = jnp.maximum(a - m2, 0.0)
        q2 = jnp.minimum(p2, m1)
        r2 = p2 - q2
        p3 = jnp.maximum(a - m3, 0.0)
        s3 = p3 * p3
        value = q0 * (q0 * q0 * THIRD + a * r0) - q2 * (q2 * q2 * THIRD + p2 * r2) - s3 * (p3 * THIRD) - both
        rate = q0 * (a + r0) - q2 * (p2 + r2) - s3
        a = a - value / rate
    return jnp.where(g > 0.5, summed - a, a), lo, hi, slope_d, 0.5 / product


def cube_part(s, h):
    p = jnp.maximum(s, 0.0)
    q = jnp.minimum(p, h)
    r = p - q
    return q * (q * q * THIRD + p * r)


def flow(offset, lo, hi, slope_d, scale, c):
    signed = c * slope_d
    h = jnp.abs(signed)
    s = offset - jnp.where(signed < 0, jnp.abs(slope_d) - h, 0.0)
    t = s - hi
    return scale * ((cube_part(s, h) - cube_part(s - lo, h)) - (cube_part(t, h) - cube_part(t - lo, h)))


def rows(ref, where):
    parts = [ref[z, pl.ds(y, n)] for z, y, n in where]
    return parts[0] if len(parts) == 1 else jnp.concatenate(parts, axis=0)


def put(ref, where, value):
    start = 0
    for z, y, n in where:
        ref[z, pl.ds(y, n)] = value[start : start + n]
        start += n


def moved(where, dz, dy):
    return [(z + dz, y + dy, n) for z, y, n in where]


def loop(first, last, body):
    def step(i, carry):
        body(i)
        return carry

    lax.fori_loop(first, last, step, 0)


def pipelined(count, where_of, *stages):
    depth = len(stages)

    def run(i, live):
        for store in reversed([stages[k](where_of(i - k)) for k in live]):
            store()

    for i in range(depth - 1):
        run(i, range(i + 1))
    loop(depth - 1, count, lambda i: run(i, range(depth)))
    for i in range(count, count + depth - 1):
        run(i, range(i - count + 1, depth))


def kernel(
    f_hbm, vx_hbm, vy_hbm, vz_hbm, out_ref, dt_out,
    f_ext, g1_ext, g2_ext, vx, vy, vz, vx_diff, smooth, diff, sum_y, dif_y, sum_d,
    off, lo, hi, slope, scale, face, edge_y, stat_y, stat_z, dt_vec, dt_cell,
    load_sem, out_sem, send_sem, recv_sem,
):
    gy, gz = lax.axis_index("gy"), lax.axis_index("gz")

    def neighbour(dy, dz):
        return {"gy": lax.rem(gy + dy + N_GY, N_GY), "gz": lax.rem(gz + dz + N_GZ, N_GZ)}

    corners = [(1, 1), (1, -1), (-1, 1), (-1, -1)]
    own_z, own_y = pl.ds(Z0, NZ), pl.ds(Y0, NY)

    arrays = [(f_hbm, f_ext), (vx_hbm, vx), (vy_hbm, vy), (vz_hbm, vz)]

    def load(k):
        source, target = arrays[k]
        for y in range(NY):
            pltpu.make_async_copy(source.at[:, :, y, :], target.at[own_z, Y0 + y], load_sem.at[k]).start()

    load(0)
    barrier = pltpu.get_barrier_semaphore()
    greeted = [neighbour(k, 0) for k in range(1, N_GY)]
    greeted += [neighbour(0, k) for k in range(1, N_GZ)] + [neighbour(*c) for c in corners]
    for device in greeted:
        pl.semaphore_signal(barrier, inc=1, device_id=device, device_id_type=pl.DeviceIdType.MESH)
    for k in (1, 2, 3):
        load(k)

    def remote(source, target, sends, receives, device):
        return pltpu.make_async_remote_copy(
            src_ref=source, dst_ref=target, send_sem=send_sem.at[sends], recv_sem=recv_sem.at[receives],
            device_id=device, device_id_type=pl.DeviceIdType.MESH,
        )

    def halo(g, sends, receives, wide_z, wide_y):
        from_z = {1: pl.ds(Z1 - wide_z, wide_z), -1: pl.ds(Z0, wide_z), 0: own_z}
        from_y = {1: pl.ds(Y1 - wide_y, wide_y), -1: pl.ds(Y0, wide_y), 0: own_y}
        to_z = {1: pl.ds(Z0 - wide_z, wide_z), -1: pl.ds(Z1, wide_z), 0: own_z}
        to_y = {1: pl.ds(Y0 - wide_y, wide_y), -1: pl.ds(Y1, wide_y), 0: own_y}
        return [
            remote(g.at[from_z[dz], from_y[dy]], g.at[to_z[dz], to_y[dy]], sends, receives[k], neighbour(dy, dz))
            for k, (dy, dz) in enumerate([(1, 0), (-1, 0), (0, 1), (0, -1)] + corners)
        ]

    def send(copies):
        for copy in copies:
            copy.start()

    def arrive(part, receives):
        remote(part, part, 0, receives, neighbour(1, 0)).wait_recv()

    def left(part, sends):
        remote(part, part, sends, 0, neighbour(1, 0)).wait_send()

    def some(ref, z, y):
        return ref.at[pl.ds(0, z), pl.ds(0, y)]

    def loaded(k):
        source, target = arrays[k]
        pltpu.make_async_copy(source, target.at[own_z, own_y], load_sem.at[k]).wait()

    def scan_fraction(i, total):
        g = f_ext[i + Z0, own_y]
        return total + g * (1.0 - g)

    loaded(0)
    total = lax.fori_loop(0, NZ, scan_fraction, jnp.zeros((NY, J, LN), F32))
    peak = jnp.zeros((NY, J, LN), F32)
    for k in (1, 2, 3):
        loaded(k)
        speeds = arrays[k][1]
        peak = lax.fori_loop(0, NZ, lambda i, peak: jnp.maximum(peak, jnp.abs(speeds[i + Z0, own_y])), peak)
    top_row = lax.broadcasted_iota(jnp.int32, (2, LN), 0) == 0

    def combined(ref, n):
        top, add = ref[0], ref[0]
        for k in range(1, n):
            top, add = jnp.maximum(top, ref[k]), add + ref[k]
        return jnp.where(top_row, top, add)

    top, add = jnp.max(peak, axis=0), jnp.sum(total, axis=0)
    stat_y[gy] = jnp.concatenate([jnp.max(top, axis=0, keepdims=True), jnp.sum(add, axis=0, keepdims=True)], axis=0)

    pl.semaphore_wait(barrier, len(greeted))
    halo_f = halo(f_ext, HALO_F, 2 * [HALO_F] + 2 * [HALO_F_NEAR] + 4 * [HALO_F_FAR], 2, 2)
    halo_v = halo(vx, HALO_V, 8 * [HALO_V], 1, 1)
    stats_y = [remote(stat_y.at[gy], stat_y.at[gy], STAT_Y, STAT_Y, neighbour(k, 0)) for k in range(1, N_GY)]
    stats_z = [remote(stat_z.at[gz], stat_z.at[gz], STAT_Z, STAT_Z, neighbour(0, k)) for k in range(1, N_GZ)]
    velocity = [
        remote(vy.at[own_z, Y1 - 1], vy.at[own_z, Y0 - 1], VEL, VEL, neighbour(1, 0)),
        remote(vz.at[Z1 - 1, own_y], vz.at[Z0 - 1, own_y], VEL, VEL, neighbour(0, 1)),
    ]
    send(stats_y)
    send(halo_f[2:4] + halo_f[:2] + halo_f[4:])

    def put_shifts(g, where):
        before, after = at_prev(g), at_next(g)
        put(smooth, where, before + 2.0 * g + after)
        put(diff, where, after - before)

    def shift_rows(g_ext, where):
        put_shifts(rows(g_ext, where), where)

    def sums_of(z, y, n):
        s = smooth[z, pl.ds(y - 1, n + 2)]
        d = diff[z, pl.ds(y - 1, n + 2)]

        def store():
            where = [(z, y, n)]
            put(sum_y, where, s[:-2] + 2.0 * s[1:-1] + s[2:])
            put(dif_y, where, s[2:] - s[:-2])
            put(sum_d, where, d[:-2] + 2.0 * d[1:-1] + d[2:])

        return store

    def put_sums(z, y, n):
        sums_of(z, y, n)()

    planes = (off, lo, hi, slope, scale)

    def planes_of(g_ext, dim):
        def stage(where):
            below, above = moved(where, -1, 0), moved(where, 1, 0)
            along_z = rows(sum_y, above) - rows(sum_y, below)
            along_y = rows(dif_y, below) + 2.0 * rows(dif_y, where) + rows(dif_y, above)
            along_x = rows(sum_d, below) + 2.0 * rows(sum_d, where) + rows(sum_d, above)
            slopes = [along_z, along_y, along_x]
            across = [slopes[k] for k in range(3) if k != dim]
            g = rows(g_ext, where)

            def store():
                for ref, value in zip(planes, plane(g, slopes[dim], *across)):
                    put(ref, where, value)

            return store

        return stage

    def put_planes(g_ext, dim, where):
        planes_of(g_ext, dim)(where)()

    def donors_x(where):
        found = [rows(ref, where) for ref in planes]
        q = rows(vx, where)
        others = [at_next(value) for value in found]
        before = at_prev(q)

        def store():
            upward = q > 0
            others[-1] = -others[-1]
            for ref, value, other in zip(planes, found, others):
                put(ref, where, jnp.where(upward, value, other))
            put(vx_diff, where, q - before)

        return store

    def donors(upward, here, there):
        picked = [jnp.where(upward, rows(ref, here), rows(ref, there)) for ref in planes[:-1]]
        return picked + [jnp.where(upward, rows(scale, here), -rows(scale, there))]

    inner = (Y0 + 1, NY - 2)

    def pair(z):
        return [(z, *inner), (z + 1, *inner)]

    def shift_ends(g_ext):
        loop(0, 2, lambda i: shift_rows(g_ext, [(i * Z1, Y0, NY), (i * Z1 + 1, Y0, NY)]))
        loop(0, 4, lambda i: put_sums(i + (i // 2) * (EZ - 4), *inner))

    loop(0, NZ // 2, lambda i: shift_rows(f_ext, [(Z0 + 2 * i, Y0, NY), (Z0 + 2 * i + 1, Y0, NY)]))
    loop(Z0, Z1, lambda z: put_sums(z, *inner))
    pipelined(5, lambda i: [(Z0 + 1 + i, *inner)], planes_of(f_ext, 2), donors_x)
    send(halo_v)
    pipelined(NZ - 7, lambda i: [(Z0 + 6 + i, *inner)], planes_of(f_ext, 2), donors_x)
    arrive(some(f_ext, 8, 4), HALO_F_NEAR)
    shift_ends(f_ext)
    loop(0, 2, lambda i: put_planes(f_ext, 2, pair(1 + i * NZ)))
    donors_x([(Z0, *inner), (Z1 - 1, *inner)])()
    arrive(some(f_ext, NZ, 4), HALO_F)
    arrive(stat_y.at[pl.ds(0, N_GY - 1)], STAT_Y)
    stat_z[gz] = combined(stat_y, N_GY)
    send(stats_z)

    def shift_sides(i):
        z = Z0 + 4 * i
        shift_rows(f_ext, [w for k in range(4) for w in ((z + k, 0, 2), (z + k, Y1, 2))])

    def sums_side(z):
        put_sums(z, 1, 2)
        put_sums(z, Y1 - 1, 2)

    loop(0, NZ // 4, shift_sides)
    loop(Z0, Z1, sums_side)
    def shift_corners(i):
        z = i * Z1
        shift_rows(f_ext, [(z, 0, 2), (z, Y1, 2), (z + 1, 0, 2), (z + 1, Y1, 2)])

    def column(zs, y):
        return [(z, y, 1) for z in zs]

    def own_columns(i):
        first, high = 3 + 6 * (i - 2 * (i // 2)), i // 2
        return column([first + k for k in range(6)], Y0 + high * (NY - 1))

    def next_column(high):
        return column([Z0 + 1 + k for k in range(12)], Y0 - 1 + high * (NY + 1))

    def end_columns(high):
        return [(z, 1 + high * (Y1 - 2), 2) for z in (1, 2, NZ - 1, NZ, NZ + 1, NZ + 2)]

    planes_x = planes_of(f_ext, 2)
    send(velocity)
    pipelined(4, own_columns, planes_x, donors_x)
    loop(0, 2, lambda i: put_planes(f_ext, 2, next_column(i)))
    arrive(some(f_ext, 4, 4), HALO_F_FAR)
    loop(0, 2, shift_corners)
    loop(0, 4, lambda i: sums_side(i + (i // 2) * (EZ - 4)))
    loop(0, 2, lambda i: put_planes(f_ext, 2, end_columns(i)))
    arrive(some(vx, 13, 4), HALO_V)
    loop(0, 2, lambda i: donors_x(next_column(i))())
    loop(0, 2, lambda i: donors_x(end_columns(i))())
    donors_x([(1, *inner), (NZ + 2, *inner)])()
    arrive(stat_z.at[pl.ds(0, N_GZ - 1)], STAT_Z)
    stats = combined(stat_z, N_GZ)
    umax = jnp.max(stats[0:1], axis=1, keepdims=True)
    share = jnp.sum(stats[1:2], axis=1, keepdims=True) * (4.0 / (N_GZ * NZ * N_GY * NY * J * LN))
    step = COURANT / ((umax + EPSILON) * (1.0 + share))
    dt_vec[...] = jnp.broadcast_to(step, (J, LN))
    dt_cell[...] = step

    def flow_x(where):
        found = [rows(ref, where) for ref in planes]
        q = rows(vx, where)
        return lambda: put(face, where, flow(*found, dt_vec[...] * q))

    def update_x(where):
        out = rows(face, where)
        before = at_prev(out)
        g, change = rows(f_ext, where), rows(vx_diff, where)
        return lambda: put(g1_ext, where, (g - out + before) / (1.0 - dt_vec[...] * change))

    def shifts_of(g_ext):
        def stage(where):
            g = rows(g_ext, where)
            before, after = at_prev(g), at_next(g)

            def store():
                put(smooth, where, before + 2.0 * g + after)
                put(diff, where, after - before)

            return store

        return stage

    dt_copy = pltpu.make_async_copy(dt_cell, dt_out, out_sem)
    x_stages = (flow_x, update_x, shifts_of(g1_ext))
    pipelined(
        NZ // 2 + 1,
        lambda i: [w for z in (1 + 2 * i, 2 + 2 * i) for w in ((z, 1, 3), (z, Y1 - 2, 3))],
        *x_stages,
    )

    dt_copy.start()

    def sums_edge(first, n):
        for z in range(n):
            put_sums(first + z, Y0, 1)
            put_sums(first + z, Y1 - 1, 1)

    def edges(first, n):
        return [w for k in range(n) for w in ((first + k, Y0, 1), (first + k, Y1 - 1, 1))]

    def half_faces_y(i):
        z = Z0 + 4 * i
        at_face = [w for k in range(4) for w in ((z + k, Y0 - 1, 1), (z + k, Y1 - 1, 1))]
        c = dt_vec[...] * rows(vy, at_face)
        out = flow(*[rows(ref, edges(z, 4)) for ref in planes], c)
        for k in range(4):
            edge_y[0, 4 * i + k] = jnp.where(c[2 * k + 1] > 0, out[2 * k + 1], 0.0)
            edge_y[1, 4 * i + k] = jnp.where(c[2 * k] < 0, out[2 * k], 0.0)

    flux_y = []
    for k in range(2):
        part = pl.ds(k * (NZ // 2), NZ // 2)
        flux_y += [
            remote(edge_y.at[0, part], edge_y.at[2, part], FLUX, FLUX, neighbour(1, 0)),
            remote(edge_y.at[1, part], edge_y.at[3, part], FLUX, FLUX, neighbour(-1, 0)),
        ]
    arrive(some(vy, 6, 4), VEL)
    loop(0, (NZ + 2) // 3, lambda i: sums_edge(Z0 - 1 + 3 * i, 3))
    for k in range(2):
        put_planes(g1_ext, 1, edges(Z0 + k * (NZ // 2), NZ // 2))
        loop(2 * k, 2 * k + 2, half_faces_y)
        send(flux_y[2 * k : 2 * k + 2])

    def middle(i):
        return [(1 + 3 * i + k, Y0 + 2, NY - 4) for k in range(3)]

    def faces_y(where):
        c = dt_vec[...] * rows(vy, where)
        put(face, where, flow(*donors(c > 0, where, moved(where, 0, 1)), c))

    pipelined((NZ + 2) // 3, middle, *x_stages)
    loop(Z0 - 1, Z0 + 3, lambda z: put_sums(z, *inner))

    def y_inner(i):
        z = Z0 + 2 * i
        stores = planes_of(g1_ext, 1)(pair(z)), sums_of(z + 3, *inner), sums_of(z + 4, *inner)
        for store in stores:
            store()

    loop(0, NZ // 2 - 1, y_inner)
    put_planes(g1_ext, 1, pair(Z1 - 2))
    def faces_y_near(i):
        z = Z0 + 4 * i
        faces_y([w for k in range(4) for w in ((z + k, Y0, 1), (z + k, Y1 - 2, 1))])

    def update_y(where):
        before, q = moved(where, 0, -1), dt_vec[...]
        g = rows(g1_ext, where) - rows(face, where) + rows(face, before)
        put(g2_ext, where, g / (1.0 - q * (rows(vy, where) - rows(vy, before))))

    def update_y_edge(i):
        for k in range(4):
            z, at = Z0 + 4 * i + k, 4 * i + k
            face[z, Y0 - 1] = edge_y[2, at] - edge_y[1, at]
            face[z, Y1 - 1] = edge_y[0, at] - edge_y[3, at]
        update_y(edges(Z0 + 4 * i, 4))

    def rest_y(i):
        z = Z0 + 2 * lax.rem(7 * i, NZ // 2)
        faces_y([(z, Y0 + 1, NY - 3), (z + 1, Y0 + 1, NY - 3)])
        update_y([(z, *inner), (z + 1, *inner)])

    near = [HALO_G, HALO_G, HALO_G_NEAR, HALO_G_NEAR] + 4 * [HALO_G]
    halo_g = halo(g2_ext, HALO_G, near, 2, 1)
    loop(0, NZ // 4, faces_y_near)
    arrive(edge_y.at[pl.ds(2, 2)], FLUX)
    loop(0, NZ // 4, update_y_edge)
    send(halo_g[:2] + halo_g[4:])
    loop(0, 2, rest_y)
    send(halo_g[2:4])
    loop(2, NZ // 2, rest_y)

    def faces_z(where):
        c = dt_vec[...] * rows(vz, where)
        put(face, where, flow(*donors(c > 0, where, moved(where, 1, 0)), c))

    shift_rows(g2_ext, [(Z0, Y0, NY), (Z0 + 1, Y0, NY)])
    shift_rows(g2_ext, [(Z0 + 2, Y0, NY), (Z0 + 3, Y0, NY)])
    loop(Z0, Z0 + 3, lambda z: put_sums(z, *inner))

    def z_inner(z):
        stores = (
            shifts_of(g2_ext)([(z + 3, Y0, NY)]),
            planes_of(g2_ext, 0)([(z, *inner)]),
            sums_of(z + 2, *inner),
        )
        for store in reversed(stores):
            store()

    loop(Z0 + 1, Z1 - 3, z_inner)
    put_sums(Z1 - 1, *inner)
    put_planes(g2_ext, 0, pair(Z1 - 3))
    loop(0, NZ // 2 - 2, lambda i: faces_z(pair(Z0 + 1 + 2 * i)))
    faces_z([(Z1 - 3, *inner)])
    arrive(some(g2_ext, 8, 4), HALO_G_NEAR)
    shift_ends(g2_ext)
    loop(0, 2, lambda i: put_planes(g2_ext, 0, pair(1 + i * NZ)))
    loop(0, 2, lambda i: faces_z(pair(1 + i * (NZ - 1))))

    def update_z(where):
        before, q = moved(where, -1, 0), dt_vec[...]
        g = rows(g2_ext, where) - rows(face, where) + rows(face, before)
        g = g / (1.0 - q * (rows(vz, where) - rows(vz, before)))
        for k, (z, y) in enumerate([(z, y + k) for z, y, n in where for k in range(n)]):
            out_ref[z - Z0, pl.ds(y - Y0, J, stride=NY), :] = g[k]

    loop(Z0, Z1, lambda z: update_z([(z, *inner)]))
    arrive(some(g2_ext, 10, 4), HALO_G)
    loop(0, 2, lambda i: shift_rows(
        g2_ext, [w for k in range(EZ // 2) for w in ((i * (EZ // 2) + k, Y0 - 1, 1), (i * (EZ // 2) + k, Y1, 1))]
    ))
    loop(0, EZ // 4, lambda i: sums_edge(4 * i, 4))
    loop(0, (NZ + 2) // 6, lambda i: put_planes(g2_ext, 0, edges(1 + 6 * i, 6)))
    loop(0, 2, lambda i: faces_z(edges(1 + 6 * i, 6)))
    faces_z(edges(Z1 - 5, 5))

    loop(0, NZ // 4, lambda i: update_z(edges(Z0 + 4 * i, 4)))
    left(some(f_ext, 14, 8), HALO_F)
    left(some(vx, 13, 4), HALO_V)
    left(some(g2_ext, 9, 8), HALO_G)
    left(some(vy, 6, 4), VEL)
    left(edge_y.at[pl.ds(0, 2)], FLUX)
    left(stat_y.at[pl.ds(0, N_GY - 1)], STAT_Y)
    left(stat_z.at[pl.ds(0, N_GZ - 1)], STAT_Z)
    dt_copy.wait()


def shards(*blocks):
    tiled = [b.reshape(NZ, NY, J, LN).transpose(0, 2, 1, 3) for b in blocks]
    row = (J, LN)
    ext = pltpu.VMEM((EZ, EY, *row), F32)
    anywhere = pl.BlockSpec(memory_space=pl.ANY)
    field, step = pl.pallas_call(
        kernel,
        out_shape=(pltpu.VMEM((NZ, J * NY, LN), F32), jax.ShapeDtypeStruct((1, 1), F32)),
        in_specs=[anywhere] * 4,
        out_specs=(pl.BlockSpec(memory_space=pltpu.VMEM), anywhere),
        scratch_shapes=[ext] * 18 + [
            pltpu.VMEM((4, NZ, *row), F32),
            pltpu.VMEM((N_GY, 2, LN), F32), pltpu.VMEM((N_GZ, 2, LN), F32),
            pltpu.VMEM(row, F32), pltpu.VMEM((1, 1), F32),
            pltpu.SemaphoreType.DMA((4,)), pltpu.SemaphoreType.DMA(()),
            pltpu.SemaphoreType.DMA((N_SEND,)), pltpu.SemaphoreType.DMA((N_RECV,)),
        ],
        compiler_params=pltpu.CompilerParams(collective_id=0, has_side_effects=True),
        name="advect",
    )(*tiled)
    return field.reshape(NZ, J, NY, LN).transpose(0, 2, 1, 3).reshape(NZ, NY, J * LN), step.reshape(())


def solution(mesh):
    spec = P("gz", "gy", None)
    return jax.shard_map(shards, mesh=mesh, in_specs=(spec,) * 4, out_specs=(spec, P()), check_vma=False)
```

```python
import jax
import jax.numpy as jnp
from jax import lax
from jax.experimental import pallas as pl
from jax.experimental.pallas import tpu as pltpu
from jax.sharding import PartitionSpec as P

NEWTON = 5
TILT_FLOOR = 3.2
TINY = 1e-18
COURANT = 0.45
EPSILON = 1e-6
THIRD = 1.0 / 3.0

NZ, NY, J, LN = 16, 8, 8, 128
N_GY, N_GZ = 16, 8
F32 = jnp.float32

EZ, EY = NZ + 4, NY + 4
Z0, Y0 = 2, 2
Z1, Y1 = Z0 + NZ, Y0 + NY

HALO_F, HALO_V, HALO_G, VEL, FLUX, STAT_Y, STAT_Z = range(7)
HALO_F_NEAR, HALO_F_FAR, HALO_G_NEAR = 7, 8, 9
N_SEND, N_RECV = 7, 10


def lanes(u):
    return lax.broadcasted_iota(jnp.int32, u.shape, u.ndim - 1)


def at_next(u):
    moved = pltpu.roll(u, LN - 1, u.ndim - 1)
    return jnp.where(lanes(u) == LN - 1, pltpu.roll(moved, J - 1, u.ndim - 2), moved)


def at_prev(u):
    moved = pltpu.roll(u, 1, u.ndim - 1)
    return jnp.where(lanes(u) == 0, pltpu.roll(moved, 1, u.ndim - 2), moved)


def plane(g, slope_d, slope_a, slope_b):
    tilt_a = jnp.abs(slope_a) + TILT_FLOOR
    tilt_b = jnp.abs(slope_b) + TILT_FLOOR
    lo, hi = jnp.minimum(tilt_a, tilt_b), jnp.maximum(tilt_a, tilt_b)
    slope_d = jnp.where(jnp.abs(slope_d) < TINY, TINY, slope_d)
    tilt_d = jnp.abs(slope_d)
    m1, rest = jnp.minimum(lo, tilt_d), jnp.maximum(lo, tilt_d)
    m2, m3 = jnp.minimum(rest, hi), jnp.maximum(rest, hi)
    lesser = jnp.maximum(jnp.minimum(g, 1.0 - g), 0.0)
    m12 = m1 * m2
    product = m12 * m3
    target = lesser * product
    both = target + target
    summed = lo + hi + tilt_d
    w = 0.5 * jnp.maximum(m1 + m2 - m3, 0.0)
    a = 0.5 * summed - (0.5 * product - target) / (m12 - w * w)
    for _ in range(NEWTON - 1):
        q0 = jnp.minimum(a, m1)
        r0 = a - q0
        p2 = jnp.maximum(a - m2, 0.0)
        q2 = jnp.minimum(p2, m1)
        r2 = p2 - q2
        p3 = jnp.maximum(a - m3, 0.0)
        s3 = p3 * p3
        value = q0 * (q0 * q0 * THIRD + a * r0) - q2 * (q2 * q2 * THIRD + p2 * r2) - s3 * (p3 * THIRD) - both
        rate = q0 * (a + r0) - q2 * (p2 + r2) - s3
        a = a - value / rate
    return jnp.where(g > 0.5, summed - a, a), lo, hi, slope_d, 0.5 / product


def cube_part(s, h):
    p = jnp.maximum(s, 0.0)
    q = jnp.minimum(p, h)
    r = p - q
    return q * (q * q * THIRD + p * r)


def flow(offset, lo, hi, slope_d, scale, c):
    signed = c * slope_d
    h = jnp.abs(signed)
    s = offset - jnp.where(signed < 0, jnp.abs(slope_d) - h, 0.0)
    t = s - hi
    return scale * ((cube_part(s, h) - cube_part(s - lo, h)) - (cube_part(t, h) - cube_part(t - lo, h)))


def rows(ref, where):
    parts = [ref[z, pl.ds(y, n)] for z, y, n in where]
    return parts[0] if len(parts) == 1 else jnp.concatenate(parts, axis=0)


def put(ref, where, value):
    start = 0
    for z, y, n in where:
        ref[z, pl.ds(y, n)] = value[start : start + n]
        start += n


def moved(where, dz, dy):
    return [(z + dz, y + dy, n) for z, y, n in where]


def loop(first, last, body):
    def step(i, carry):
        body(i)
        return carry

    lax.fori_loop(first, last, step, 0)


def pipelined(count, where_of, *stages):
    depth = len(stages)

    def run(i, live):
        for store in reversed([stages[k](where_of(i - k)) for k in live]):
            store()

    for i in range(depth - 1):
        run(i, range(i + 1))
    loop(depth - 1, count, lambda i: run(i, range(depth)))
    for i in range(count, count + depth - 1):
        run(i, range(i - count + 1, depth))


def kernel(
    f_hbm, vx_hbm, vy_hbm, vz_hbm, out_ref, dt_out,
    f_ext, g1_ext, g2_ext, vx, vy, vz, vx_diff, smooth, diff, sum_y, dif_y, sum_d,
    off, lo, hi, slope, scale, face, edge_y, stat_y, stat_z, dt_vec, dt_cell,
    load_sem, out_sem, send_sem, recv_sem,
):
    gy, gz = lax.axis_index("gy"), lax.axis_index("gz")

    def neighbour(dy, dz):
        return {"gy": lax.rem(gy + dy + N_GY, N_GY), "gz": lax.rem(gz + dz + N_GZ, N_GZ)}

    corners = [(1, 1), (1, -1), (-1, 1), (-1, -1)]
    own_z, own_y = pl.ds(Z0, NZ), pl.ds(Y0, NY)

    arrays = [(f_hbm, f_ext), (vx_hbm, vx), (vy_hbm, vy), (vz_hbm, vz)]

    def load(k):
        source, target = arrays[k]
        for y in range(NY):
            pltpu.make_async_copy(source.at[:, :, y, :], target.at[own_z, Y0 + y], load_sem.at[k]).start()

    load(0)
    barrier = pltpu.get_barrier_semaphore()
    greeted = [neighbour(k, 0) for k in range(1, N_GY)]
    greeted += [neighbour(0, k) for k in range(1, N_GZ)] + [neighbour(*c) for c in corners]
    for device in greeted:
        pl.semaphore_signal(barrier, inc=1, device_id=device, device_id_type=pl.DeviceIdType.MESH)
    for k in (1, 2, 3):
        load(k)

    def remote(source, target, sends, receives, device):
        return pltpu.make_async_remote_copy(
            src_ref=source, dst_ref=target, send_sem=send_sem.at[sends], recv_sem=recv_sem.at[receives],
            device_id=device, device_id_type=pl.DeviceIdType.MESH,
        )

    def halo(g, sends, receives, wide_z, wide_y):
        from_z = {1: pl.ds(Z1 - wide_z, wide_z), -1: pl.ds(Z0, wide_z), 0: own_z}
        from_y = {1: pl.ds(Y1 - wide_y, wide_y), -1: pl.ds(Y0, wide_y), 0: own_y}
        to_z = {1: pl.ds(Z0 - wide_z, wide_z), -1: pl.ds(Z1, wide_z), 0: own_z}
        to_y = {1: pl.ds(Y0 - wide_y, wide_y), -1: pl.ds(Y1, wide_y), 0: own_y}
        return [
            remote(g.at[from_z[dz], from_y[dy]], g.at[to_z[dz], to_y[dy]], sends, receives[k], neighbour(dy, dz))
            for k, (dy, dz) in enumerate([(1, 0), (-1, 0), (0, 1), (0, -1)] + corners)
        ]

    def send(copies):
        for copy in copies:
            copy.start()

    def arrive(part, receives):
        remote(part, part, 0, receives, neighbour(1, 0)).wait_recv()

    def left(part, sends):
        remote(part, part, sends, 0, neighbour(1, 0)).wait_send()

    def some(ref, z, y):
        return ref.at[pl.ds(0, z), pl.ds(0, y)]

    def loaded(k):
        source, target = arrays[k]
        pltpu.make_async_copy(source, target.at[own_z, own_y], load_sem.at[k]).wait()

    def scan_fraction(i, total):
        g = f_ext[i + Z0, own_y]
        return total + g * (1.0 - g)

    loaded(0)
    total = lax.fori_loop(0, NZ, scan_fraction, jnp.zeros((NY, J, LN), F32))
    peak = jnp.zeros((NY, J, LN), F32)
    for k in (1, 2, 3):
        loaded(k)
        speeds = arrays[k][1]
        peak = lax.fori_loop(0, NZ, lambda i, peak: jnp.maximum(peak, jnp.abs(speeds[i + Z0, own_y])), peak)
    top_row = lax.broadcasted_iota(jnp.int32, (2, LN), 0) == 0

    def combined(ref, n):
        top, add = ref[0], ref[0]
        for k in range(1, n):
            top, add = jnp.maximum(top, ref[k]), add + ref[k]
        return jnp.where(top_row, top, add)

    top, add = jnp.max(peak, axis=0), jnp.sum(total, axis=0)
    stat_y[gy] = jnp.concatenate([jnp.max(top, axis=0, keepdims=True), jnp.sum(add, axis=0, keepdims=True)], axis=0)

    pl.semaphore_wait(barrier, len(greeted))
    halo_f = halo(f_ext, HALO_F, 2 * [HALO_F] + 2 * [HALO_F_NEAR] + 4 * [HALO_F_FAR], 2, 2)
    halo_v = halo(vx, HALO_V, 8 * [HALO_V], 1, 1)
    stats_y = [remote(stat_y.at[gy], stat_y.at[gy], STAT_Y, STAT_Y, neighbour(k, 0)) for k in range(1, N_GY)]
    stats_z = [remote(stat_z.at[gz], stat_z.at[gz], STAT_Z, STAT_Z, neighbour(0, k)) for k in range(1, N_GZ)]
    velocity = [
        remote(vy.at[own_z, Y1 - 1], vy.at[own_z, Y0 - 1], VEL, VEL, neighbour(1, 0)),
        remote(vz.at[Z1 - 1, own_y], vz.at[Z0 - 1, own_y], VEL, VEL, neighbour(0, 1)),
    ]
    send(stats_y)
    send(halo_f[2:4] + halo_f[:2] + halo_f[4:])

    def put_shifts(g, where):
        before, after = at_prev(g), at_next(g)
        put(smooth, where, before + 2.0 * g + after)
        put(diff, where, after - before)

    def shift_rows(g_ext, where):
        put_shifts(rows(g_ext, where), where)

    def sums_of(z, y, n):
        s = smooth[z, pl.ds(y - 1, n + 2)]
        d = diff[z, pl.ds(y - 1, n + 2)]

        def store():
            where = [(z, y, n)]
            put(sum_y, where, s[:-2] + 2.0 * s[1:-1] + s[2:])
            put(dif_y, where, s[2:] - s[:-2])
            put(sum_d, where, d[:-2] + 2.0 * d[1:-1] + d[2:])

        return store

    def put_sums(z, y, n):
        sums_of(z, y, n)()

    planes = (off, lo, hi, slope, scale)

    def planes_of(g_ext, dim):
        def stage(where):
            below, above = moved(where, -1, 0), moved(where, 1, 0)
            along_z = rows(sum_y, above) - rows(sum_y, below)
            along_y = rows(dif_y, below) + 2.0 * rows(dif_y, where) + rows(dif_y, above)
            along_x = rows(sum_d, below) + 2.0 * rows(sum_d, where) + rows(sum_d, above)
            slopes = [along_z, along_y, along_x]
            across = [slopes[k] for k in range(3) if k != dim]
            g = rows(g_ext, where)

            def store():
                for ref, value in zip(planes, plane(g, slopes[dim], *across)):
                    put(ref, where, value)

            return store

        return stage

    def put_planes(g_ext, dim, where):
        planes_of(g_ext, dim)(where)()

    def donors_x(where):
        found = [rows(ref, where) for ref in planes]
        q = rows(vx, where)
        others = [at_next(value) for value in found]
        before = at_prev(q)

        def store():
            upward = q > 0
            others[-1] = -others[-1]
            for ref, value, other in zip(planes, found, others):
                put(ref, where, jnp.where(upward, value, other))
            put(vx_diff, where, q - before)

        return store

    def donors(upward, here, there):
        picked = [jnp.where(upward, rows(ref, here), rows(ref, there)) for ref in planes[:-1]]
        return picked + [jnp.where(upward, rows(scale, here), -rows(scale, there))]

    inner = (Y0 + 1, NY - 2)

    def pair(z):
        return [(z, *inner), (z + 1, *inner)]

    def shift_ends(g_ext):
        loop(0, 2, lambda i: shift_rows(g_ext, [(i * Z1, Y0, NY), (i * Z1 + 1, Y0, NY)]))
        loop(0, 4, lambda i: put_sums(i + (i // 2) * (EZ - 4), *inner))

    loop(0, NZ // 2, lambda i: shift_rows(f_ext, [(Z0 + 2 * i, Y0, NY), (Z0 + 2 * i + 1, Y0, NY)]))
    loop(Z0, Z1, lambda z: put_sums(z, *inner))
    pipelined(5, lambda i: [(Z0 + 1 + i, *inner)], planes_of(f_ext, 2), donors_x)
    send(halo_v)
    pipelined(NZ - 7, lambda i: [(Z0 + 6 + i, *inner)], planes_of(f_ext, 2), donors_x)
    send(velocity)
    arrive(some(f_ext, 8, 4), HALO_F_NEAR)
    shift_ends(f_ext)
    loop(0, 2, lambda i: put_planes(f_ext, 2, pair(1 + i * NZ)))
    donors_x([(Z0, *inner), (Z1 - 1, *inner)])()
    arrive(some(f_ext, NZ, 4), HALO_F)
    arrive(stat_y.at[pl.ds(0, N_GY - 1)], STAT_Y)
    stat_z[gz] = combined(stat_y, N_GY)
    send(stats_z)

    def shift_sides(i):
        z = Z0 + 4 * i
        shift_rows(f_ext, [w for k in range(4) for w in ((z + k, 0, 2), (z + k, Y1, 2))])

    def sums_side(z):
        put_sums(z, 1, 2)
        put_sums(z, Y1 - 1, 2)

    loop(0, NZ // 4, shift_sides)
    loop(Z0, Z1, sums_side)
    def shift_corners(i):
        z = i * Z1
        shift_rows(f_ext, [(z, 0, 2), (z, Y1, 2), (z + 1, 0, 2), (z + 1, Y1, 2)])

    def column(zs, y):
        return [(z, y, 1) for z in zs]

    def own_columns(i):
        first, high = 3 + 6 * (i - 2 * (i // 2)), i // 2
        return column([first + k for k in range(6)], Y0 + high * (NY - 1))

    def next_column(high):
        return column([Z0 + 1 + k for k in range(12)], Y0 - 1 + high * (NY + 1))

    def end_columns(high):
        return [(z, 1 + high * (Y1 - 2), 2) for z in (1, 2, NZ - 1, NZ, NZ + 1, NZ + 2)]

    planes_x = planes_of(f_ext, 2)
    pipelined(4, own_columns, planes_x, donors_x)
    loop(0, 2, lambda i: put_planes(f_ext, 2, next_column(i)))
    arrive(some(f_ext, 4, 4), HALO_F_FAR)
    loop(0, 2, shift_corners)
    loop(0, 4, lambda i: sums_side(i + (i // 2) * (EZ - 4)))
    loop(0, 2, lambda i: put_planes(f_ext, 2, end_columns(i)))
    arrive(some(vx, 13, 4), HALO_V)
    loop(0, 2, lambda i: donors_x(next_column(i))())
    loop(0, 2, lambda i: donors_x(end_columns(i))())
    donors_x([(1, *inner), (NZ + 2, *inner)])()
    arrive(stat_z.at[pl.ds(0, N_GZ - 1)], STAT_Z)
    stats = combined(stat_z, N_GZ)
    umax = jnp.max(stats[0:1], axis=1, keepdims=True)
    share = jnp.sum(stats[1:2], axis=1, keepdims=True) * (4.0 / (N_GZ * NZ * N_GY * NY * J * LN))
    step = COURANT / ((umax + EPSILON) * (1.0 + share))
    dt_vec[...] = jnp.broadcast_to(step, (J, LN))
    dt_cell[...] = step

    def flow_x(where):
        found = [rows(ref, where) for ref in planes]
        q = rows(vx, where)
        return lambda: put(face, where, flow(*found, dt_vec[...] * q))

    def update_x(where):
        out = rows(face, where)
        before = at_prev(out)
        g, change = rows(f_ext, where), rows(vx_diff, where)
        return lambda: put(g1_ext, where, (g - out + before) / (1.0 - dt_vec[...] * change))

    def shifts_of(g_ext):
        def stage(where):
            g = rows(g_ext, where)
            before, after = at_prev(g), at_next(g)

            def store():
                put(smooth, where, before + 2.0 * g + after)
                put(diff, where, after - before)

            return store

        return stage

    dt_copy = pltpu.make_async_copy(dt_cell, dt_out, out_sem)
    x_stages = (flow_x, update_x, shifts_of(g1_ext))
    pipelined(
        NZ // 2 + 1,
        lambda i: [w for z in (1 + 2 * i, 2 + 2 * i) for w in ((z, 1, 3), (z, Y1 - 2, 3))],
        *x_stages,
    )

    dt_copy.start()

    def sums_edge(first, n):
        for z in range(n):
            put_sums(first + z, Y0, 1)
            put_sums(first + z, Y1 - 1, 1)

    def edges(first, n):
        return [w for k in range(n) for w in ((first + k, Y0, 1), (first + k, Y1 - 1, 1))]

    def half_faces_y(i):
        z = Z0 + 4 * i
        at_face = [w for k in range(4) for w in ((z + k, Y0 - 1, 1), (z + k, Y1 - 1, 1))]
        c = dt_vec[...] * rows(vy, at_face)
        out = flow(*[rows(ref, edges(z, 4)) for ref in planes], c)
        for k in range(4):
            edge_y[0, 4 * i + k] = jnp.where(c[2 * k + 1] > 0, out[2 * k + 1], 0.0)
            edge_y[1, 4 * i + k] = jnp.where(c[2 * k] < 0, out[2 * k], 0.0)

    flux_y = []
    for k in range(2):
        part = pl.ds(k * (NZ // 2), NZ // 2)
        flux_y += [
            remote(edge_y.at[0, part], edge_y.at[2, part], FLUX, FLUX, neighbour(1, 0)),
            remote(edge_y.at[1, part], edge_y.at[3, part], FLUX, FLUX, neighbour(-1, 0)),
        ]
    loop(0, (NZ + 2) // 3, lambda i: sums_edge(Z0 - 1 + 3 * i, 3))
    for k in range(2):
        put_planes(g1_ext, 1, edges(Z0 + k * (NZ // 2), NZ // 2))
    arrive(some(vy, 6, 4), VEL)
    for k in range(2):
        loop(2 * k, 2 * k + 2, half_faces_y)
        send(flux_y[2 * k : 2 * k + 2])

    def middle(i):
        return [(1 + 3 * i + k, Y0 + 2, NY - 4) for k in range(3)]

    def faces_y(where):
        c = dt_vec[...] * rows(vy, where)
        put(face, where, flow(*donors(c > 0, where, moved(where, 0, 1)), c))

    pipelined((NZ + 2) // 3, middle, *x_stages)
    loop(Z0 - 1, Z0 + 3, lambda z: put_sums(z, *inner))

    def y_inner(i):
        z = Z0 + 2 * i
        stores = planes_of(g1_ext, 1)(pair(z)), sums_of(z + 3, *inner), sums_of(z + 4, *inner)
        for store in stores:
            store()

    loop(0, NZ // 2 - 1, y_inner)
    put_planes(g1_ext, 1, pair(Z1 - 2))
    def faces_y_near(i):
        z = Z0 + 4 * i
        faces_y([w for k in range(4) for w in ((z + k, Y0, 1), (z + k, Y1 - 2, 1))])

    def update_y(where):
        before, q = moved(where, 0, -1), dt_vec[...]
        g = rows(g1_ext, where) - rows(face, where) + rows(face, before)
        put(g2_ext, where, g / (1.0 - q * (rows(vy, where) - rows(vy, before))))

    def update_y_edge(i):
        for k in range(4):
            z, at = Z0 + 4 * i + k, 4 * i + k
            face[z, Y0 - 1] = edge_y[2, at] - edge_y[1, at]
            face[z, Y1 - 1] = edge_y[0, at] - edge_y[3, at]
        update_y(edges(Z0 + 4 * i, 4))

    def rest_y(i):
        z = Z0 + 2 * lax.rem(7 * i, NZ // 2)
        faces_y([(z, Y0 + 1, NY - 3), (z + 1, Y0 + 1, NY - 3)])
        update_y([(z, *inner), (z + 1, *inner)])

    near = [HALO_G, HALO_G, HALO_G_NEAR, HALO_G_NEAR] + 4 * [HALO_G]
    halo_g = halo(g2_ext, HALO_G, near, 2, 1)
    loop(0, NZ // 4, faces_y_near)
    arrive(edge_y.at[pl.ds(2, 2)], FLUX)
    loop(0, NZ // 4, update_y_edge)
    send(halo_g[:2] + halo_g[4:])
    loop(0, 2, rest_y)
    send(halo_g[2:4])
    loop(2, NZ // 2, rest_y)

    def faces_z(where):
        c = dt_vec[...] * rows(vz, where)
        put(face, where, flow(*donors(c > 0, where, moved(where, 1, 0)), c))

    shift_rows(g2_ext, [(Z0, Y0, NY), (Z0 + 1, Y0, NY)])
    shift_rows(g2_ext, [(Z0 + 2, Y0, NY), (Z0 + 3, Y0, NY)])
    loop(Z0, Z0 + 3, lambda z: put_sums(z, *inner))

    def z_inner(z):
        stores = (
            shifts_of(g2_ext)([(z + 3, Y0, NY)]),
            planes_of(g2_ext, 0)([(z, *inner)]),
            sums_of(z + 2, *inner),
        )
        for store in reversed(stores):
            store()

    loop(Z0 + 1, Z1 - 3, z_inner)
    put_sums(Z1 - 1, *inner)
    put_planes(g2_ext, 0, pair(Z1 - 3))
    loop(0, NZ // 2 - 2, lambda i: faces_z(pair(Z0 + 1 + 2 * i)))
    faces_z([(Z1 - 3, *inner)])
    arrive(some(g2_ext, 8, 4), HALO_G_NEAR)
    shift_ends(g2_ext)
    loop(0, 2, lambda i: put_planes(g2_ext, 0, pair(1 + i * NZ)))
    loop(0, 2, lambda i: faces_z(pair(1 + i * (NZ - 1))))

    def update_z(where):
        before, q = moved(where, -1, 0), dt_vec[...]
        g = rows(g2_ext, where) - rows(face, where) + rows(face, before)
        g = g / (1.0 - q * (rows(vz, where) - rows(vz, before)))
        for k, (z, y) in enumerate([(z, y + k) for z, y, n in where for k in range(n)]):
            out_ref[z - Z0, pl.ds(y - Y0, J, stride=NY), :] = g[k]

    loop(Z0, Z1, lambda z: update_z([(z, *inner)]))
    arrive(some(g2_ext, 10, 4), HALO_G)
    loop(0, 2, lambda i: shift_rows(
        g2_ext, [w for k in range(EZ // 2) for w in ((i * (EZ // 2) + k, Y0 - 1, 1), (i * (EZ // 2) + k, Y1, 1))]
    ))
    loop(0, EZ // 4, lambda i: sums_edge(4 * i, 4))
    loop(0, (NZ + 2) // 6, lambda i: put_planes(g2_ext, 0, edges(1 + 6 * i, 6)))
    loop(0, 2, lambda i: faces_z(edges(1 + 6 * i, 6)))
    faces_z(edges(Z1 - 5, 5))

    loop(0, NZ // 4, lambda i: update_z(edges(Z0 + 4 * i, 4)))
    left(some(f_ext, 14, 8), HALO_F)
    left(some(vx, 13, 4), HALO_V)
    left(some(g2_ext, 9, 8), HALO_G)
    left(some(vy, 6, 4), VEL)
    left(edge_y.at[pl.ds(0, 2)], FLUX)
    left(stat_y.at[pl.ds(0, N_GY - 1)], STAT_Y)
    left(stat_z.at[pl.ds(0, N_GZ - 1)], STAT_Z)
    dt_copy.wait()


def shards(*blocks):
    tiled = [b.reshape(NZ, NY, J, LN).transpose(0, 2, 1, 3) for b in blocks]
    row = (J, LN)
    ext = pltpu.VMEM((EZ, EY, *row), F32)
    anywhere = pl.BlockSpec(memory_space=pl.ANY)
    field, step = pl.pallas_call(
        kernel,
        out_shape=(pltpu.VMEM((NZ, J * NY, LN), F32), jax.ShapeDtypeStruct((1, 1), F32)),
        in_specs=[anywhere] * 4,
        out_specs=(pl.BlockSpec(memory_space=pltpu.VMEM), anywhere),
        scratch_shapes=[ext] * 18 + [
            pltpu.VMEM((4, NZ, *row), F32),
            pltpu.VMEM((N_GY, 2, LN), F32), pltpu.VMEM((N_GZ, 2, LN), F32),
            pltpu.VMEM(row, F32), pltpu.VMEM((1, 1), F32),
            pltpu.SemaphoreType.DMA((4,)), pltpu.SemaphoreType.DMA(()),
            pltpu.SemaphoreType.DMA((N_SEND,)), pltpu.SemaphoreType.DMA((N_RECV,)),
        ],
        compiler_params=pltpu.CompilerParams(collective_id=0, has_side_effects=True),
        name="advect",
    )(*tiled)
    return field.reshape(NZ, J, NY, LN).transpose(0, 2, 1, 3).reshape(NZ, NY, J * LN), step.reshape(())


def solution(mesh):
    spec = P("gz", "gy", None)
    return jax.shard_map(shards, mesh=mesh, in_specs=(spec,) * 4, out_specs=(spec, P()), check_vma=False)
```

```python
import jax
import jax.numpy as jnp
from jax import lax
from jax.experimental import pallas as pl
from jax.experimental.pallas import tpu as pltpu
from jax.sharding import PartitionSpec as P

NEWTON = 5
TILT_FLOOR = 3.2
TINY = 1e-18
COURANT = 0.45
EPSILON = 1e-6
THIRD = 1.0 / 3.0

NZ, NY, J, LN = 16, 8, 8, 128
N_GY, N_GZ = 16, 8
F32 = jnp.float32

EZ, EY = NZ + 4, NY + 4
Z0, Y0 = 2, 2
Z1, Y1 = Z0 + NZ, Y0 + NY

HALO_F, HALO_V, HALO_G, VEL, FLUX, STAT_Y, STAT_Z = range(7)
HALO_F_NEAR, HALO_F_FAR, HALO_G_NEAR = 7, 8, 9
N_SEND, N_RECV = 7, 10


def lanes(u):
    return lax.broadcasted_iota(jnp.int32, u.shape, u.ndim - 1)


def at_next(u):
    moved = pltpu.roll(u, LN - 1, u.ndim - 1)
    return jnp.where(lanes(u) == LN - 1, pltpu.roll(moved, J - 1, u.ndim - 2), moved)


def at_prev(u):
    moved = pltpu.roll(u, 1, u.ndim - 1)
    return jnp.where(lanes(u) == 0, pltpu.roll(moved, 1, u.ndim - 2), moved)


def plane(g, slope_d, slope_a, slope_b):
    tilt_a = jnp.abs(slope_a) + TILT_FLOOR
    tilt_b = jnp.abs(slope_b) + TILT_FLOOR
    lo, hi = jnp.minimum(tilt_a, tilt_b), jnp.maximum(tilt_a, tilt_b)
    slope_d = jnp.where(jnp.abs(slope_d) < TINY, TINY, slope_d)
    tilt_d = jnp.abs(slope_d)
    m1, rest = jnp.minimum(lo, tilt_d), jnp.maximum(lo, tilt_d)
    m2, m3 = jnp.minimum(rest, hi), jnp.maximum(rest, hi)
    lesser = jnp.maximum(jnp.minimum(g, 1.0 - g), 0.0)
    m12 = m1 * m2
    product = m12 * m3
    target = lesser * product
    both = target + target
    summed = lo + hi + tilt_d
    w = 0.5 * jnp.maximum(m1 + m2 - m3, 0.0)
    a = 0.5 * summed - (0.5 * product - target) / (m12 - w * w)
    for _ in range(NEWTON - 1):
        q0 = jnp.minimum(a, m1)
        r0 = a - q0
        p2 = jnp.maximum(a - m2, 0.0)
        q2 = jnp.minimum(p2, m1)
        r2 = p2 - q2
        p3 = jnp.maximum(a - m3, 0.0)
        s3 = p3 * p3
        value = q0 * (q0 * q0 * THIRD + a * r0) - q2 * (q2 * q2 * THIRD + p2 * r2) - s3 * (p3 * THIRD) - both
        rate = q0 * (a + r0) - q2 * (p2 + r2) - s3
        a = a - value / rate
    return jnp.where(g > 0.5, summed - a, a), lo, hi, slope_d, 0.5 / product


def cube_part(s, h):
    p = jnp.maximum(s, 0.0)
    q = jnp.minimum(p, h)
    r = p - q
    return q * (q * q * THIRD + p * r)


def flow(offset, lo, hi, slope_d, scale, c):
    signed = c * slope_d
    h = jnp.abs(signed)
    s = offset - jnp.where(signed < 0, jnp.abs(slope_d) - h, 0.0)
    t = s - hi
    return scale * ((cube_part(s, h) - cube_part(s - lo, h)) - (cube_part(t, h) - cube_part(t - lo, h)))


def rows(ref, where):
    parts = [ref[z, pl.ds(y, n)] for z, y, n in where]
    return parts[0] if len(parts) == 1 else jnp.concatenate(parts, axis=0)


def put(ref, where, value):
    start = 0
    for z, y, n in where:
        ref[z, pl.ds(y, n)] = value[start : start + n]
        start += n


def moved(where, dz, dy):
    return [(z + dz, y + dy, n) for z, y, n in where]


def loop(first, last, body):
    def step(i, carry):
        body(i)
        return carry

    lax.fori_loop(first, last, step, 0)


def pipelined(count, where_of, *stages):
    depth = len(stages)

    def run(i, live):
        for store in reversed([stages[k](where_of(i - k)) for k in live]):
            store()

    for i in range(depth - 1):
        run(i, range(i + 1))
    loop(depth - 1, count, lambda i: run(i, range(depth)))
    for i in range(count, count + depth - 1):
        run(i, range(i - count + 1, depth))


def kernel(
    f_hbm, vx_hbm, vy_hbm, vz_hbm, out_ref, dt_out,
    f_ext, g1_ext, g2_ext, vx, vy, vz, vx_diff, smooth, diff, sum_y, dif_y, sum_d,
    off, lo, hi, slope, scale, face, edge_y, stat_y, stat_z, dt_vec, dt_cell,
    load_sem, out_sem, send_sem, recv_sem,
):
    gy, gz = lax.axis_index("gy"), lax.axis_index("gz")

    def neighbour(dy, dz):
        return {"gy": lax.rem(gy + dy + N_GY, N_GY), "gz": lax.rem(gz + dz + N_GZ, N_GZ)}

    corners = [(1, 1), (1, -1), (-1, 1), (-1, -1)]
    own_z, own_y = pl.ds(Z0, NZ), pl.ds(Y0, NY)

    arrays = [(f_hbm, f_ext), (vx_hbm, vx), (vy_hbm, vy), (vz_hbm, vz)]

    def load(k):
        source, target = arrays[k]
        for y in range(NY):
            pltpu.make_async_copy(source.at[:, :, y, :], target.at[own_z, Y0 + y], load_sem.at[k]).start()

    load(0)
    barrier = pltpu.get_barrier_semaphore()
    greeted = [neighbour(k, 0) for k in range(1, N_GY)]
    greeted += [neighbour(0, k) for k in range(1, N_GZ)] + [neighbour(*c) for c in corners]
    for device in greeted:
        pl.semaphore_signal(barrier, inc=1, device_id=device, device_id_type=pl.DeviceIdType.MESH)
    for k in (1, 2, 3):
        load(k)

    def remote(source, target, sends, receives, device):
        return pltpu.make_async_remote_copy(
            src_ref=source, dst_ref=target, send_sem=send_sem.at[sends], recv_sem=recv_sem.at[receives],
            device_id=device, device_id_type=pl.DeviceIdType.MESH,
        )

    def halo(g, sends, receives, wide_z, wide_y):
        from_z = {1: pl.ds(Z1 - wide_z, wide_z), -1: pl.ds(Z0, wide_z), 0: own_z}
        from_y = {1: pl.ds(Y1 - wide_y, wide_y), -1: pl.ds(Y0, wide_y), 0: own_y}
        to_z = {1: pl.ds(Z0 - wide_z, wide_z), -1: pl.ds(Z1, wide_z), 0: own_z}
        to_y = {1: pl.ds(Y0 - wide_y, wide_y), -1: pl.ds(Y1, wide_y), 0: own_y}
        return [
            remote(g.at[from_z[dz], from_y[dy]], g.at[to_z[dz], to_y[dy]], sends, receives[k], neighbour(dy, dz))
            for k, (dy, dz) in enumerate([(1, 0), (-1, 0), (0, 1), (0, -1)] + corners)
        ]

    def send(copies):
        for copy in copies:
            copy.start()

    def arrive(part, receives):
        remote(part, part, 0, receives, neighbour(1, 0)).wait_recv()

    def left(part, sends):
        remote(part, part, sends, 0, neighbour(1, 0)).wait_send()

    def some(ref, z, y):
        return ref.at[pl.ds(0, z), pl.ds(0, y)]

    def loaded(k):
        source, target = arrays[k]
        pltpu.make_async_copy(source, target.at[own_z, own_y], load_sem.at[k]).wait()

    def scan_fraction(i, total):
        g = f_ext[i + Z0, own_y]
        return total + g * (1.0 - g)

    loaded(0)
    total = lax.fori_loop(0, NZ, scan_fraction, jnp.zeros((NY, J, LN), F32))
    peak = jnp.zeros((NY, J, LN), F32)
    for k in (1, 2, 3):
        loaded(k)
        speeds = arrays[k][1]
        peak = lax.fori_loop(0, NZ, lambda i, peak: jnp.maximum(peak, jnp.abs(speeds[i + Z0, own_y])), peak)
    top_row = lax.broadcasted_iota(jnp.int32, (2, LN), 0) == 0

    def combined(ref, n):
        top, add = ref[0], ref[0]
        for k in range(1, n):
            top, add = jnp.maximum(top, ref[k]), add + ref[k]
        return jnp.where(top_row, top, add)

    top, add = jnp.max(peak, axis=0), jnp.sum(total, axis=0)
    stat_y[gy] = jnp.concatenate([jnp.max(top, axis=0, keepdims=True), jnp.sum(add, axis=0, keepdims=True)], axis=0)

    pl.semaphore_wait(barrier, len(greeted))
    halo_f = halo(f_ext, HALO_F, 2 * [HALO_F] + 2 * [HALO_F_NEAR] + 4 * [HALO_F_FAR], 2, 2)
    halo_v = halo(vx, HALO_V, 8 * [HALO_V], 1, 1)
    stats_y = [remote(stat_y.at[gy], stat_y.at[gy], STAT_Y, STAT_Y, neighbour(k, 0)) for k in range(1, N_GY)]
    stats_z = [remote(stat_z.at[gz], stat_z.at[gz], STAT_Z, STAT_Z, neighbour(0, k)) for k in range(1, N_GZ)]
    velocity = [
        remote(vy.at[own_z, Y1 - 1], vy.at[own_z, Y0 - 1], VEL, VEL, neighbour(1, 0)),
        remote(vz.at[Z1 - 1, own_y], vz.at[Z0 - 1, own_y], VEL, VEL, neighbour(0, 1)),
    ]
    send(stats_y)
    send(halo_f[2:4] + halo_f[:2] + halo_f[4:])

    def put_shifts(g, where):
        before, after = at_prev(g), at_next(g)
        put(smooth, where, before + 2.0 * g + after)
        put(diff, where, after - before)

    def shift_rows(g_ext, where):
        put_shifts(rows(g_ext, where), where)

    def sums_of(z, y, n):
        s = smooth[z, pl.ds(y - 1, n + 2)]
        d = diff[z, pl.ds(y - 1, n + 2)]

        def store():
            where = [(z, y, n)]
            put(sum_y, where, s[:-2] + 2.0 * s[1:-1] + s[2:])
            put(dif_y, where, s[2:] - s[:-2])
            put(sum_d, where, d[:-2] + 2.0 * d[1:-1] + d[2:])

        return store

    def put_sums(z, y, n):
        sums_of(z, y, n)()

    planes = (off, lo, hi, slope, scale)

    def planes_of(g_ext, dim):
        def stage(where):
            below, above = moved(where, -1, 0), moved(where, 1, 0)
            along_z = rows(sum_y, above) - rows(sum_y, below)
            along_y = rows(dif_y, below) + 2.0 * rows(dif_y, where) + rows(dif_y, above)
            along_x = rows(sum_d, below) + 2.0 * rows(sum_d, where) + rows(sum_d, above)
            slopes = [along_z, along_y, along_x]
            across = [slopes[k] for k in range(3) if k != dim]
            g = rows(g_ext, where)

            def store():
                for ref, value in zip(planes, plane(g, slopes[dim], *across)):
                    put(ref, where, value)

            return store

        return stage

    def put_planes(g_ext, dim, where):
        planes_of(g_ext, dim)(where)()

    def donors_x(where):
        found = [rows(ref, where) for ref in planes]
        q = rows(vx, where)
        others = [at_next(value) for value in found]
        before = at_prev(q)

        def store():
            upward = q > 0
            others[-1] = -others[-1]
            for ref, value, other in zip(planes, found, others):
                put(ref, where, jnp.where(upward, value, other))
            put(vx_diff, where, q - before)

        return store

    def donors(upward, here, there):
        picked = [jnp.where(upward, rows(ref, here), rows(ref, there)) for ref in planes[:-1]]
        return picked + [jnp.where(upward, rows(scale, here), -rows(scale, there))]

    inner = (Y0 + 1, NY - 2)

    def pair(z):
        return [(z, *inner), (z + 1, *inner)]

    def shift_ends(g_ext):
        loop(0, 2, lambda i: shift_rows(g_ext, [(i * Z1, Y0, NY), (i * Z1 + 1, Y0, NY)]))
        loop(0, 4, lambda i: put_sums(i + (i // 2) * (EZ - 4), *inner))

    loop(0, NZ // 2, lambda i: shift_rows(f_ext, [(Z0 + 2 * i, Y0, NY), (Z0 + 2 * i + 1, Y0, NY)]))
    loop(Z0, Z1, lambda z: put_sums(z, *inner))
    pipelined(5, lambda i: [(Z0 + 1 + i, *inner)], planes_of(f_ext, 2), donors_x)
    send(halo_v)
    pipelined(NZ - 7, lambda i: [(Z0 + 6 + i, *inner)], planes_of(f_ext, 2), donors_x)
    send(velocity)
    arrive(some(f_ext, 8, 4), HALO_F_NEAR)
    shift_ends(f_ext)
    loop(0, 2, lambda i: put_planes(f_ext, 2, pair(1 + i * NZ)))
    donors_x([(Z0, *inner), (Z1 - 1, *inner)])()
    arrive(some(f_ext, NZ, 4), HALO_F)
    arrive(stat_y.at[pl.ds(0, N_GY - 1)], STAT_Y)
    stat_z[gz] = combined(stat_y, N_GY)
    send(stats_z)

    def shift_sides(i):
        z = Z0 + 4 * i
        shift_rows(f_ext, [w for k in range(4) for w in ((z + k, 0, 2), (z + k, Y1, 2))])

    def sums_side(z):
        put_sums(z, 1, 2)
        put_sums(z, Y1 - 1, 2)

    loop(0, NZ // 4, shift_sides)
    loop(Z0, Z1, sums_side)
    def shift_corners(i):
        z = i * Z1
        shift_rows(f_ext, [(z, 0, 2), (z, Y1, 2), (z + 1, 0, 2), (z + 1, Y1, 2)])

    def column(zs, y):
        return [(z, y, 1) for z in zs]

    def own_columns(i):
        first, high = 3 + 6 * (i - 2 * (i // 2)), i // 2
        return column([first + k for k in range(6)], Y0 + high * (NY - 1))

    def next_column(high):
        return column([Z0 + 1 + k for k in range(12)], Y0 - 1 + high * (NY + 1))

    def end_columns(high):
        return [(z, 1 + high * (Y1 - 2), 2) for z in (1, 2, NZ - 1, NZ, NZ + 1, NZ + 2)]

    planes_x = planes_of(f_ext, 2)
    pipelined(4, own_columns, planes_x, donors_x)
    loop(0, 2, lambda i: put_planes(f_ext, 2, next_column(i)))
    arrive(some(f_ext, 4, 4), HALO_F_FAR)
    loop(0, 2, shift_corners)
    loop(0, 4, lambda i: sums_side(i + (i // 2) * (EZ - 4)))
    loop(0, 2, lambda i: put_planes(f_ext, 2, end_columns(i)))
    arrive(some(vx, 13, 4), HALO_V)
    loop(0, 2, lambda i: donors_x(next_column(i))())
    loop(0, 2, lambda i: donors_x(end_columns(i))())
    donors_x([(1, *inner), (NZ + 2, *inner)])()
    arrive(stat_z.at[pl.ds(0, N_GZ - 1)], STAT_Z)
    stats = combined(stat_z, N_GZ)
    umax = jnp.max(stats[0:1], axis=1, keepdims=True)
    share = jnp.sum(stats[1:2], axis=1, keepdims=True) * (4.0 / (N_GZ * NZ * N_GY * NY * J * LN))
    step = COURANT / ((umax + EPSILON) * (1.0 + share))
    dt_vec[...] = jnp.broadcast_to(step, (J, LN))
    dt_cell[...] = step

    def flow_x(where):
        found = [rows(ref, where) for ref in planes]
        q = rows(vx, where)
        return lambda: put(face, where, flow(*found, dt_vec[...] * q))

    def update_x(where):
        out = rows(face, where)
        before = at_prev(out)
        g, change = rows(f_ext, where), rows(vx_diff, where)
        return lambda: put(g1_ext, where, (g - out + before) / (1.0 - dt_vec[...] * change))

    def shifts_of(g_ext):
        def stage(where):
            g = rows(g_ext, where)
            before, after = at_prev(g), at_next(g)

            def store():
                put(smooth, where, before + 2.0 * g + after)
                put(diff, where, after - before)

            return store

        return stage

    dt_copy = pltpu.make_async_copy(dt_cell, dt_out, out_sem)
    x_stages = (flow_x, update_x, shifts_of(g1_ext))
    pipelined(
        NZ // 2 + 1,
        lambda i: [w for z in (1 + 2 * i, 2 + 2 * i) for w in ((z, 1, 3), (z, Y1 - 2, 3))],
        *x_stages,
    )

    dt_copy.start()

    def sums_edge(first, n):
        for z in range(n):
            put_sums(first + z, Y0, 1)
            put_sums(first + z, Y1 - 1, 1)

    def edges(first, n):
        return [w for k in range(n) for w in ((first + k, Y0, 1), (first + k, Y1 - 1, 1))]

    def half_faces_y(i):
        z = Z0 + 4 * i
        at_face = [w for k in range(4) for w in ((z + k, Y0 - 1, 1), (z + k, Y1 - 1, 1))]
        c = dt_vec[...] * rows(vy, at_face)
        out = flow(*[rows(ref, edges(z, 4)) for ref in planes], c)
        for k in range(4):
            edge_y[0, 4 * i + k] = jnp.where(c[2 * k + 1] > 0, out[2 * k + 1], 0.0)
            edge_y[1, 4 * i + k] = jnp.where(c[2 * k] < 0, out[2 * k], 0.0)

    flux_y = []
    for k in range(2):
        part = pl.ds(k * (NZ // 2), NZ // 2)
        flux_y += [
            remote(edge_y.at[0, part], edge_y.at[2, part], FLUX, FLUX, neighbour(1, 0)),
            remote(edge_y.at[1, part], edge_y.at[3, part], FLUX, FLUX, neighbour(-1, 0)),
        ]
    loop(0, (NZ + 2) // 3, lambda i: sums_edge(Z0 - 1 + 3 * i, 3))
    for k in range(2):
        put_planes(g1_ext, 1, edges(Z0 + k * (NZ // 2), NZ // 2))
        if k == 0:
            arrive(some(vy, 6, 4), VEL)
        loop(2 * k, 2 * k + 2, half_faces_y)
        send(flux_y[2 * k : 2 * k + 2])

    def middle(i):
        return [(1 + 3 * i + k, Y0 + 2, NY - 4) for k in range(3)]

    def faces_y(where):
        c = dt_vec[...] * rows(vy, where)
        put(face, where, flow(*donors(c > 0, where, moved(where, 0, 1)), c))

    pipelined((NZ + 2) // 3, middle, *x_stages)
    loop(Z0 - 1, Z0 + 3, lambda z: put_sums(z, *inner))

    def y_inner(i):
        z = Z0 + 2 * i
        stores = planes_of(g1_ext, 1)(pair(z)), sums_of(z + 3, *inner), sums_of(z + 4, *inner)
        for store in stores:
            store()

    loop(0, NZ // 2 - 1, y_inner)
    put_planes(g1_ext, 1, pair(Z1 - 2))
    def faces_y_near(i):
        z = Z0 + 4 * i
        faces_y([w for k in range(4) for w in ((z + k, Y0, 1), (z + k, Y1 - 2, 1))])

    def update_y(where):
        before, q = moved(where, 0, -1), dt_vec[...]
        g = rows(g1_ext, where) - rows(face, where) + rows(face, before)
        put(g2_ext, where, g / (1.0 - q * (rows(vy, where) - rows(vy, before))))

    def update_y_edge(i):
        for k in range(4):
            z, at = Z0 + 4 * i + k, 4 * i + k
            face[z, Y0 - 1] = edge_y[2, at] - edge_y[1, at]
            face[z, Y1 - 1] = edge_y[0, at] - edge_y[3, at]
        update_y(edges(Z0 + 4 * i, 4))

    def rest_y(i):
        z = Z0 + 2 * lax.rem(7 * i, NZ // 2)
        faces_y([(z, Y0 + 1, NY - 3), (z + 1, Y0 + 1, NY - 3)])
        update_y([(z, *inner), (z + 1, *inner)])

    near = [HALO_G, HALO_G, HALO_G_NEAR, HALO_G_NEAR] + 4 * [HALO_G]
    halo_g = halo(g2_ext, HALO_G, near, 2, 1)
    loop(0, NZ // 4, faces_y_near)
    loop(NZ // 2 - 3, NZ // 2, rest_y)
    arrive(edge_y.at[pl.ds(2, 2)], FLUX)
    loop(0, NZ // 4, update_y_edge)
    send(halo_g[:2] + halo_g[4:])
    loop(0, 2, rest_y)
    send(halo_g[2:4])
    loop(2, NZ // 2 - 3, rest_y)

    def faces_z(where):
        c = dt_vec[...] * rows(vz, where)
        put(face, where, flow(*donors(c > 0, where, moved(where, 1, 0)), c))

    shift_rows(g2_ext, [(Z0, Y0, NY), (Z0 + 1, Y0, NY)])
    shift_rows(g2_ext, [(Z0 + 2, Y0, NY), (Z0 + 3, Y0, NY)])
    loop(Z0, Z0 + 3, lambda z: put_sums(z, *inner))

    def z_inner(z):
        stores = (
            shifts_of(g2_ext)([(z + 3, Y0, NY)]),
            planes_of(g2_ext, 0)([(z, *inner)]),
            sums_of(z + 2, *inner),
        )
        for store in reversed(stores):
            store()

    loop(Z0 + 1, Z1 - 3, z_inner)
    put_sums(Z1 - 1, *inner)
    put_planes(g2_ext, 0, pair(Z1 - 3))
    loop(0, NZ // 2 - 2, lambda i: faces_z(pair(Z0 + 1 + 2 * i)))
    faces_z([(Z1 - 3, *inner)])
    arrive(some(g2_ext, 8, 4), HALO_G_NEAR)
    shift_ends(g2_ext)
    loop(0, 2, lambda i: put_planes(g2_ext, 0, pair(1 + i * NZ)))
    loop(0, 2, lambda i: faces_z(pair(1 + i * (NZ - 1))))

    def update_z(where):
        before, q = moved(where, -1, 0), dt_vec[...]
        g = rows(g2_ext, where) - rows(face, where) + rows(face, before)
        g = g / (1.0 - q * (rows(vz, where) - rows(vz, before)))
        for k, (z, y) in enumerate([(z, y + k) for z, y, n in where for k in range(n)]):
            out_ref[z - Z0, pl.ds(y - Y0, J, stride=NY), :] = g[k]

    loop(Z0, Z1, lambda z: update_z([(z, *inner)]))
    arrive(some(g2_ext, 10, 4), HALO_G)
    loop(0, 2, lambda i: shift_rows(
        g2_ext, [w for k in range(EZ // 2) for w in ((i * (EZ // 2) + k, Y0 - 1, 1), (i * (EZ // 2) + k, Y1, 1))]
    ))
    loop(0, EZ // 4, lambda i: sums_edge(4 * i, 4))
    loop(0, (NZ + 2) // 6, lambda i: put_planes(g2_ext, 0, edges(1 + 6 * i, 6)))
    loop(0, 2, lambda i: faces_z(edges(1 + 6 * i, 6)))
    faces_z(edges(Z1 - 5, 5))

    loop(0, NZ // 4, lambda i: update_z(edges(Z0 + 4 * i, 4)))
    left(some(f_ext, 14, 8), HALO_F)
    left(some(vx, 13, 4), HALO_V)
    left(some(g2_ext, 9, 8), HALO_G)
    left(some(vy, 6, 4), VEL)
    left(edge_y.at[pl.ds(0, 2)], FLUX)
    left(stat_y.at[pl.ds(0, N_GY - 1)], STAT_Y)
    left(stat_z.at[pl.ds(0, N_GZ - 1)], STAT_Z)
    dt_copy.wait()


def shards(*blocks):
    tiled = [b.reshape(NZ, NY, J, LN).transpose(0, 2, 1, 3) for b in blocks]
    row = (J, LN)
    ext = pltpu.VMEM((EZ, EY, *row), F32)
    anywhere = pl.BlockSpec(memory_space=pl.ANY)
    field, step = pl.pallas_call(
        kernel,
        out_shape=(pltpu.VMEM((NZ, J * NY, LN), F32), jax.ShapeDtypeStruct((1, 1), F32)),
        in_specs=[anywhere] * 4,
        out_specs=(pl.BlockSpec(memory_space=pltpu.VMEM), anywhere),
        scratch_shapes=[ext] * 18 + [
            pltpu.VMEM((4, NZ, *row), F32),
            pltpu.VMEM((N_GY, 2, LN), F32), pltpu.VMEM((N_GZ, 2, LN), F32),
            pltpu.VMEM(row, F32), pltpu.VMEM((1, 1), F32),
            pltpu.SemaphoreType.DMA((4,)), pltpu.SemaphoreType.DMA(()),
            pltpu.SemaphoreType.DMA((N_SEND,)), pltpu.SemaphoreType.DMA((N_RECV,)),
        ],
        compiler_params=pltpu.CompilerParams(collective_id=0, has_side_effects=True),
        name="advect",
    )(*tiled)
    return field.reshape(NZ, J, NY, LN).transpose(0, 2, 1, 3).reshape(NZ, NY, J * LN), step.reshape(())


def solution(mesh):
    spec = P("gz", "gy", None)
    return jax.shard_map(shards, mesh=mesh, in_specs=(spec,) * 4, out_specs=(spec, P()), check_vma=False)
```

```python
import jax
import jax.numpy as jnp
from jax import lax
from jax.experimental import pallas as pl
from jax.experimental.pallas import tpu as pltpu
from jax.sharding import PartitionSpec as P

NEWTON = 5
TILT_FLOOR = 3.2
TINY = 1e-18
COURANT = 0.45
EPSILON = 1e-6
THIRD = 1.0 / 3.0

NZ, NY, J, LN = 16, 8, 8, 128
N_GY, N_GZ = 16, 8
F32 = jnp.float32

EZ, EY = NZ + 4, NY + 4
Z0, Y0 = 2, 2
Z1, Y1 = Z0 + NZ, Y0 + NY

HALO_F, HALO_V, HALO_G, VEL, FLUX, STAT_Y, STAT_Z = range(7)
HALO_F_NEAR, HALO_F_FAR, HALO_G_NEAR = 7, 8, 9
N_SEND, N_RECV = 7, 10


def lanes(u):
    return lax.broadcasted_iota(jnp.int32, u.shape, u.ndim - 1)


def at_next(u):
    moved = pltpu.roll(u, LN - 1, u.ndim - 1)
    return jnp.where(lanes(u) == LN - 1, pltpu.roll(moved, J - 1, u.ndim - 2), moved)


def at_prev(u):
    moved = pltpu.roll(u, 1, u.ndim - 1)
    return jnp.where(lanes(u) == 0, pltpu.roll(moved, 1, u.ndim - 2), moved)


def plane(g, slope_d, slope_a, slope_b):
    tilt_a = jnp.abs(slope_a) + TILT_FLOOR
    tilt_b = jnp.abs(slope_b) + TILT_FLOOR
    lo, hi = jnp.minimum(tilt_a, tilt_b), jnp.maximum(tilt_a, tilt_b)
    slope_d = jnp.where(jnp.abs(slope_d) < TINY, TINY, slope_d)
    tilt_d = jnp.abs(slope_d)
    m1, rest = jnp.minimum(lo, tilt_d), jnp.maximum(lo, tilt_d)
    m2, m3 = jnp.minimum(rest, hi), jnp.maximum(rest, hi)
    lesser = jnp.maximum(jnp.minimum(g, 1.0 - g), 0.0)
    m12 = m1 * m2
    product = m12 * m3
    target = lesser * product
    both = target + target
    summed = lo + hi + tilt_d
    w = 0.5 * jnp.maximum(m1 + m2 - m3, 0.0)
    a = 0.5 * summed - (0.5 * product - target) / (m12 - w * w)
    for _ in range(NEWTON - 1):
        q0 = jnp.minimum(a, m1)
        r0 = a - q0
        p2 = jnp.maximum(a - m2, 0.0)
        q2 = jnp.minimum(p2, m1)
        r2 = p2 - q2
        p3 = jnp.maximum(a - m3, 0.0)
        s3 = p3 * p3
        value = q0 * (q0 * q0 * THIRD + a * r0) - q2 * (q2 * q2 * THIRD + p2 * r2) - s3 * (p3 * THIRD) - both
        rate = q0 * (a + r0) - q2 * (p2 + r2) - s3
        a = a - value / rate
    return jnp.where(g > 0.5, summed - a, a), lo, hi, slope_d, 0.5 / product


def cube_part(s, h):
    p = jnp.maximum(s, 0.0)
    q = jnp.minimum(p, h)
    r = p - q
    return q * (q * q * THIRD + p * r)


def flow(offset, lo, hi, slope_d, scale, c):
    signed = c * slope_d
    h = jnp.abs(signed)
    s = offset - jnp.where(signed < 0, jnp.abs(slope_d) - h, 0.0)
    t = s - hi
    return scale * ((cube_part(s, h) - cube_part(s - lo, h)) - (cube_part(t, h) - cube_part(t - lo, h)))


def rows(ref, where):
    parts = [ref[z, pl.ds(y, n)] for z, y, n in where]
    return parts[0] if len(parts) == 1 else jnp.concatenate(parts, axis=0)


def put(ref, where, value):
    start = 0
    for z, y, n in where:
        ref[z, pl.ds(y, n)] = value[start : start + n]
        start += n


def moved(where, dz, dy):
    return [(z + dz, y + dy, n) for z, y, n in where]


def loop(first, last, body):
    def step(i, carry):
        body(i)
        return carry

    lax.fori_loop(first, last, step, 0)


def pipelined(count, where_of, *stages):
    depth = len(stages)

    def run(i, live):
        for store in reversed([stages[k](where_of(i - k)) for k in live]):
            store()

    for i in range(depth - 1):
        run(i, range(i + 1))
    loop(depth - 1, count, lambda i: run(i, range(depth)))
    for i in range(count, count + depth - 1):
        run(i, range(i - count + 1, depth))


def kernel(
    f_hbm, vx_hbm, vy_hbm, vz_hbm, out_ref, dt_out,
    f_ext, g1_ext, g2_ext, vx, vy, vz, vx_diff, smooth, diff, sum_y, dif_y, sum_d,
    off, lo, hi, slope, scale, face, edge_y, stat_y, stat_z, dt_vec, dt_cell,
    load_sem, out_sem, send_sem, recv_sem,
):
    gy, gz = lax.axis_index("gy"), lax.axis_index("gz")

    def neighbour(dy, dz):
        return {"gy": lax.rem(gy + dy + N_GY, N_GY), "gz": lax.rem(gz + dz + N_GZ, N_GZ)}

    corners = [(1, 1), (1, -1), (-1, 1), (-1, -1)]
    own_z, own_y = pl.ds(Z0, NZ), pl.ds(Y0, NY)

    arrays = [(f_hbm, f_ext), (vx_hbm, vx), (vy_hbm, vy), (vz_hbm, vz)]

    def load(k):
        source, target = arrays[k]
        for y in range(NY):
            pltpu.make_async_copy(source.at[:, :, y, :], target.at[own_z, Y0 + y], load_sem.at[k]).start()

    load(0)
    barrier = pltpu.get_barrier_semaphore()
    greeted = [neighbour(k, 0) for k in range(1, N_GY)]
    greeted += [neighbour(0, k) for k in range(1, N_GZ)] + [neighbour(*c) for c in corners]
    for device in greeted:
        pl.semaphore_signal(barrier, inc=1, device_id=device, device_id_type=pl.DeviceIdType.MESH)
    for k in (1, 2, 3):
        load(k)

    def remote(source, target, sends, receives, device):
        return pltpu.make_async_remote_copy(
            src_ref=source, dst_ref=target, send_sem=send_sem.at[sends], recv_sem=recv_sem.at[receives],
            device_id=device, device_id_type=pl.DeviceIdType.MESH,
        )

    def halo(g, sends, receives, wide_z, wide_y):
        from_z = {1: pl.ds(Z1 - wide_z, wide_z), -1: pl.ds(Z0, wide_z), 0: own_z}
        from_y = {1: pl.ds(Y1 - wide_y, wide_y), -1: pl.ds(Y0, wide_y), 0: own_y}
        to_z = {1: pl.ds(Z0 - wide_z, wide_z), -1: pl.ds(Z1, wide_z), 0: own_z}
        to_y = {1: pl.ds(Y0 - wide_y, wide_y), -1: pl.ds(Y1, wide_y), 0: own_y}
        return [
            remote(g.at[from_z[dz], from_y[dy]], g.at[to_z[dz], to_y[dy]], sends, receives[k], neighbour(dy, dz))
            for k, (dy, dz) in enumerate([(1, 0), (-1, 0), (0, 1), (0, -1)] + corners)
        ]

    def send(copies):
        for copy in copies:
            copy.start()

    def arrive(part, receives):
        remote(part, part, 0, receives, neighbour(1, 0)).wait_recv()

    def left(part, sends):
        remote(part, part, sends, 0, neighbour(1, 0)).wait_send()

    def some(ref, z, y):
        return ref.at[pl.ds(0, z), pl.ds(0, y)]

    def loaded(k):
        source, target = arrays[k]
        pltpu.make_async_copy(source, target.at[own_z, own_y], load_sem.at[k]).wait()

    def scan_fraction(i, total):
        g = f_ext[i + Z0, own_y]
        return total + g * (1.0 - g)

    loaded(0)
    total = lax.fori_loop(0, NZ, scan_fraction, jnp.zeros((NY, J, LN), F32))
    peak = jnp.zeros((NY, J, LN), F32)
    for k in (1, 2, 3):
        loaded(k)
        speeds = arrays[k][1]
        peak = lax.fori_loop(0, NZ, lambda i, peak: jnp.maximum(peak, jnp.abs(speeds[i + Z0, own_y])), peak)
    top_row = lax.broadcasted_iota(jnp.int32, (2, LN), 0) == 0

    def combined(ref, n):
        top, add = ref[0], ref[0]
        for k in range(1, n):
            top, add = jnp.maximum(top, ref[k]), add + ref[k]
        return jnp.where(top_row, top, add)

    top, add = jnp.max(peak, axis=0), jnp.sum(total, axis=0)
    stat_y[gy] = jnp.concatenate([jnp.max(top, axis=0, keepdims=True), jnp.sum(add, axis=0, keepdims=True)], axis=0)

    pl.semaphore_wait(barrier, len(greeted))
    halo_f = halo(f_ext, HALO_F, 2 * [HALO_F] + 2 * [HALO_F_NEAR] + 4 * [HALO_F_FAR], 2, 2)
    halo_v = halo(vx, HALO_V, 8 * [HALO_V], 1, 1)
    stats_y = [remote(stat_y.at[gy], stat_y.at[gy], STAT_Y, STAT_Y, neighbour(k, 0)) for k in range(1, N_GY)]
    stats_z = [remote(stat_z.at[gz], stat_z.at[gz], STAT_Z, STAT_Z, neighbour(0, k)) for k in range(1, N_GZ)]
    velocity = [
        remote(vy.at[own_z, Y1 - 1], vy.at[own_z, Y0 - 1], VEL, VEL, neighbour(1, 0)),
        remote(vz.at[Z1 - 1, own_y], vz.at[Z0 - 1, own_y], VEL, VEL, neighbour(0, 1)),
    ]
    send(stats_y)
    send(halo_f[2:4] + halo_f[:2] + halo_f[4:])

    def put_shifts(g, where):
        before, after = at_prev(g), at_next(g)
        put(smooth, where, before + 2.0 * g + after)
        put(diff, where, after - before)

    def shift_rows(g_ext, where):
        put_shifts(rows(g_ext, where), where)

    def sums_of(z, y, n):
        s = smooth[z, pl.ds(y - 1, n + 2)]
        d = diff[z, pl.ds(y - 1, n + 2)]

        def store():
            where = [(z, y, n)]
            put(sum_y, where, s[:-2] + 2.0 * s[1:-1] + s[2:])
            put(dif_y, where, s[2:] - s[:-2])
            put(sum_d, where, d[:-2] + 2.0 * d[1:-1] + d[2:])

        return store

    def put_sums(z, y, n):
        sums_of(z, y, n)()

    planes = (off, lo, hi, slope, scale)

    def planes_of(g_ext, dim):
        def stage(where):
            below, above = moved(where, -1, 0), moved(where, 1, 0)
            along_z = rows(sum_y, above) - rows(sum_y, below)
            along_y = rows(dif_y, below) + 2.0 * rows(dif_y, where) + rows(dif_y, above)
            along_x = rows(sum_d, below) + 2.0 * rows(sum_d, where) + rows(sum_d, above)
            slopes = [along_z, along_y, along_x]
            across = [slopes[k] for k in range(3) if k != dim]
            g = rows(g_ext, where)

            def store():
                for ref, value in zip(planes, plane(g, slopes[dim], *across)):
                    put(ref, where, value)

            return store

        return stage

    def put_planes(g_ext, dim, where):
        planes_of(g_ext, dim)(where)()

    def donors_x(where):
        found = [rows(ref, where) for ref in planes]
        q = rows(vx, where)
        others = [at_next(value) for value in found]
        before = at_prev(q)

        def store():
            upward = q > 0
            others[-1] = -others[-1]
            for ref, value, other in zip(planes, found, others):
                put(ref, where, jnp.where(upward, value, other))
            put(vx_diff, where, q - before)

        return store

    def donors(upward, here, there):
        picked = [jnp.where(upward, rows(ref, here), rows(ref, there)) for ref in planes[:-1]]
        return picked + [jnp.where(upward, rows(scale, here), -rows(scale, there))]

    inner = (Y0 + 1, NY - 2)

    def pair(z):
        return [(z, *inner), (z + 1, *inner)]

    def shift_ends(g_ext):
        loop(0, 2, lambda i: shift_rows(g_ext, [(i * Z1, Y0, NY), (i * Z1 + 1, Y0, NY)]))
        loop(0, 4, lambda i: put_sums(i + (i // 2) * (EZ - 4), *inner))

    loop(0, NZ // 2, lambda i: shift_rows(f_ext, [(Z0 + 2 * i, Y0, NY), (Z0 + 2 * i + 1, Y0, NY)]))
    loop(Z0, Z1, lambda z: put_sums(z, *inner))
    pipelined(5, lambda i: [(Z0 + 1 + i, *inner)], planes_of(f_ext, 2), donors_x)
    send(halo_v)
    pipelined(NZ - 7, lambda i: [(Z0 + 6 + i, *inner)], planes_of(f_ext, 2), donors_x)
    send(velocity)
    arrive(some(f_ext, 8, 4), HALO_F_NEAR)
    shift_ends(f_ext)
    loop(0, 2, lambda i: put_planes(f_ext, 2, pair(1 + i * NZ)))
    donors_x([(Z0, *inner), (Z1 - 1, *inner)])()
    arrive(stat_y.at[pl.ds(0, N_GY - 1)], STAT_Y)
    stat_z[gz] = combined(stat_y, N_GY)
    send(stats_z)
    arrive(some(f_ext, NZ, 4), HALO_F)

    def shift_sides(i):
        z = Z0 + 4 * i
        shift_rows(f_ext, [w for k in range(4) for w in ((z + k, 0, 2), (z + k, Y1, 2))])

    def sums_side(z):
        put_sums(z, 1, 2)
        put_sums(z, Y1 - 1, 2)

    loop(0, NZ // 4, shift_sides)
    loop(Z0, Z1, sums_side)
    def shift_corners(i):
        z = i * Z1
        shift_rows(f_ext, [(z, 0, 2), (z, Y1, 2), (z + 1, 0, 2), (z + 1, Y1, 2)])

    def column(zs, y):
        return [(z, y, 1) for z in zs]

    def own_columns(i):
        first, high = 3 + 6 * (i - 2 * (i // 2)), i // 2
        return column([first + k for k in range(6)], Y0 + high * (NY - 1))

    def next_column(high):
        return column([Z0 + 1 + k for k in range(12)], Y0 - 1 + high * (NY + 1))

    def end_columns(high):
        return [(z, 1 + high * (Y1 - 2), 2) for z in (1, 2, NZ - 1, NZ, NZ + 1, NZ + 2)]

    planes_x = planes_of(f_ext, 2)
    pipelined(4, own_columns, planes_x, donors_x)
    loop(0, 2, lambda i: put_planes(f_ext, 2, next_column(i)))
    arrive(some(f_ext, 4, 4), HALO_F_FAR)
    loop(0, 2, shift_corners)
    loop(0, 4, lambda i: sums_side(i + (i // 2) * (EZ - 4)))
    loop(0, 2, lambda i: put_planes(f_ext, 2, end_columns(i)))
    arrive(some(vx, 13, 4), HALO_V)
    loop(0, 2, lambda i: donors_x(next_column(i))())
    loop(0, 2, lambda i: donors_x(end_columns(i))())
    donors_x([(1, *inner), (NZ + 2, *inner)])()
    arrive(stat_z.at[pl.ds(0, N_GZ - 1)], STAT_Z)
    stats = combined(stat_z, N_GZ)
    umax = jnp.max(stats[0:1], axis=1, keepdims=True)
    share = jnp.sum(stats[1:2], axis=1, keepdims=True) * (4.0 / (N_GZ * NZ * N_GY * NY * J * LN))
    step = COURANT / ((umax + EPSILON) * (1.0 + share))
    dt_vec[...] = jnp.broadcast_to(step, (J, LN))
    dt_cell[...] = step

    def flow_x(where):
        found = [rows(ref, where) for ref in planes]
        q = rows(vx, where)
        return lambda: put(face, where, flow(*found, dt_vec[...] * q))

    def update_x(where):
        out = rows(face, where)
        before = at_prev(out)
        g, change = rows(f_ext, where), rows(vx_diff, where)
        return lambda: put(g1_ext, where, (g - out + before) / (1.0 - dt_vec[...] * change))

    def shifts_of(g_ext):
        def stage(where):
            g = rows(g_ext, where)
            before, after = at_prev(g), at_next(g)

            def store():
                put(smooth, where, before + 2.0 * g + after)
                put(diff, where, after - before)

            return store

        return stage

    dt_copy = pltpu.make_async_copy(dt_cell, dt_out, out_sem)
    x_stages = (flow_x, update_x, shifts_of(g1_ext))
    pipelined(
        NZ // 2 + 1,
        lambda i: [w for z in (1 + 2 * i, 2 + 2 * i) for w in ((z, 1, 3), (z, Y1 - 2, 3))],
        *x_stages,
    )

    dt_copy.start()

    def sums_edge(first, n):
        for z in range(n):
            put_sums(first + z, Y0, 1)
            put_sums(first + z, Y1 - 1, 1)

    def edges(first, n):
        return [w for k in range(n) for w in ((first + k, Y0, 1), (first + k, Y1 - 1, 1))]

    def half_faces_y(i):
        z = Z0 + 4 * i
        at_face = [w for k in range(4) for w in ((z + k, Y0 - 1, 1), (z + k, Y1 - 1, 1))]
        c = dt_vec[...] * rows(vy, at_face)
        out = flow(*[rows(ref, edges(z, 4)) for ref in planes], c)
        for k in range(4):
            edge_y[0, 4 * i + k] = jnp.where(c[2 * k + 1] > 0, out[2 * k + 1], 0.0)
            edge_y[1, 4 * i + k] = jnp.where(c[2 * k] < 0, out[2 * k], 0.0)

    flux_y = []
    for k in range(2):
        part = pl.ds(k * (NZ // 2), NZ // 2)
        flux_y += [
            remote(edge_y.at[0, part], edge_y.at[2, part], FLUX, FLUX, neighbour(1, 0)),
            remote(edge_y.at[1, part], edge_y.at[3, part], FLUX, FLUX, neighbour(-1, 0)),
        ]
    loop(0, (NZ + 2) // 3, lambda i: sums_edge(Z0 - 1 + 3 * i, 3))
    for k in range(2):
        put_planes(g1_ext, 1, edges(Z0 + k * (NZ // 2), NZ // 2))
    arrive(some(vy, 6, 4), VEL)
    for k in range(2):
        loop(2 * k, 2 * k + 2, half_faces_y)
        send(flux_y[2 * k : 2 * k + 2])

    def middle(i):
        return [(1 + 3 * i + k, Y0 + 2, NY - 4) for k in range(3)]

    def faces_y(where):
        c = dt_vec[...] * rows(vy, where)
        put(face, where, flow(*donors(c > 0, where, moved(where, 0, 1)), c))

    pipelined((NZ + 2) // 3, middle, *x_stages)
    loop(Z0 - 1, Z0 + 3, lambda z: put_sums(z, *inner))

    def y_inner(i):
        z = Z0 + 2 * i
        stores = planes_of(g1_ext, 1)(pair(z)), sums_of(z + 3, *inner), sums_of(z + 4, *inner)
        for store in stores:
            store()

    loop(0, NZ // 2 - 1, y_inner)
    put_planes(g1_ext, 1, pair(Z1 - 2))
    def faces_y_near(i):
        z = Z0 + 4 * i
        faces_y([w for k in range(4) for w in ((z + k, Y0, 1), (z + k, Y1 - 2, 1))])

    def update_y(where):
        before, q = moved(where, 0, -1), dt_vec[...]
        g = rows(g1_ext, where) - rows(face, where) + rows(face, before)
        put(g2_ext, where, g / (1.0 - q * (rows(vy, where) - rows(vy, before))))

    def update_y_edge(i):
        for k in range(4):
            z, at = Z0 + 4 * i + k, 4 * i + k
            face[z, Y0 - 1] = edge_y[2, at] - edge_y[1, at]
            face[z, Y1 - 1] = edge_y[0, at] - edge_y[3, at]
        update_y(edges(Z0 + 4 * i, 4))

    def rest_y(i):
        z = Z0 + 2 * lax.rem(7 * i, NZ // 2)
        faces_y([(z, Y0 + 1, NY - 3), (z + 1, Y0 + 1, NY - 3)])
        update_y([(z, *inner), (z + 1, *inner)])

    near = [HALO_G, HALO_G, HALO_G_NEAR, HALO_G_NEAR] + 4 * [HALO_G]
    halo_g = halo(g2_ext, HALO_G, near, 2, 1)
    loop(0, NZ // 4, faces_y_near)
    arrive(edge_y.at[pl.ds(2, 2)], FLUX)
    loop(0, NZ // 4, update_y_edge)
    send(halo_g[:2] + halo_g[4:])
    loop(0, 2, rest_y)
    send(halo_g[2:4])
    loop(2, NZ // 2, rest_y)

    def faces_z(where):
        c = dt_vec[...] * rows(vz, where)
        put(face, where, flow(*donors(c > 0, where, moved(where, 1, 0)), c))

    shift_rows(g2_ext, [(Z0, Y0, NY), (Z0 + 1, Y0, NY)])
    shift_rows(g2_ext, [(Z0 + 2, Y0, NY), (Z0 + 3, Y0, NY)])
    loop(Z0, Z0 + 3, lambda z: put_sums(z, *inner))

    def z_inner(z):
        stores = (
            shifts_of(g2_ext)([(z + 3, Y0, NY)]),
            planes_of(g2_ext, 0)([(z, *inner)]),
            sums_of(z + 2, *inner),
        )
        for store in reversed(stores):
            store()

    loop(Z0 + 1, Z1 - 3, z_inner)
    put_sums(Z1 - 1, *inner)
    put_planes(g2_ext, 0, pair(Z1 - 3))
    loop(0, NZ // 2 - 2, lambda i: faces_z(pair(Z0 + 1 + 2 * i)))
    faces_z([(Z1 - 3, *inner)])
    arrive(some(g2_ext, 8, 4), HALO_G_NEAR)
    shift_ends(g2_ext)
    loop(0, 2, lambda i: put_planes(g2_ext, 0, pair(1 + i * NZ)))
    loop(0, 2, lambda i: faces_z(pair(1 + i * (NZ - 1))))

    def update_z(where):
        before, q = moved(where, -1, 0), dt_vec[...]
        g = rows(g2_ext, where) - rows(face, where) + rows(face, before)
        g = g / (1.0 - q * (rows(vz, where) - rows(vz, before)))
        for k, (z, y) in enumerate([(z, y + k) for z, y, n in where for k in range(n)]):
            out_ref[z - Z0, pl.ds(y - Y0, J, stride=NY), :] = g[k]

    loop(Z0, Z1, lambda z: update_z([(z, *inner)]))
    arrive(some(g2_ext, 10, 4), HALO_G)
    loop(0, 2, lambda i: shift_rows(
        g2_ext, [w for k in range(EZ // 2) for w in ((i * (EZ // 2) + k, Y0 - 1, 1), (i * (EZ // 2) + k, Y1, 1))]
    ))
    loop(0, EZ // 4, lambda i: sums_edge(4 * i, 4))
    loop(0, (NZ + 2) // 6, lambda i: put_planes(g2_ext, 0, edges(1 + 6 * i, 6)))
    loop(0, 2, lambda i: faces_z(edges(1 + 6 * i, 6)))
    faces_z(edges(Z1 - 5, 5))

    loop(0, NZ // 4, lambda i: update_z(edges(Z0 + 4 * i, 4)))
    left(some(f_ext, 14, 8), HALO_F)
    left(some(vx, 13, 4), HALO_V)
    left(some(g2_ext, 9, 8), HALO_G)
    left(some(vy, 6, 4), VEL)
    left(edge_y.at[pl.ds(0, 2)], FLUX)
    left(stat_y.at[pl.ds(0, N_GY - 1)], STAT_Y)
    left(stat_z.at[pl.ds(0, N_GZ - 1)], STAT_Z)
    dt_copy.wait()


def shards(*blocks):
    tiled = [b.reshape(NZ, NY, J, LN).transpose(0, 2, 1, 3) for b in blocks]
    row = (J, LN)
    ext = pltpu.VMEM((EZ, EY, *row), F32)
    anywhere = pl.BlockSpec(memory_space=pl.ANY)
    field, step = pl.pallas_call(
        kernel,
        out_shape=(pltpu.VMEM((NZ, J * NY, LN), F32), jax.ShapeDtypeStruct((1, 1), F32)),
        in_specs=[anywhere] * 4,
        out_specs=(pl.BlockSpec(memory_space=pltpu.VMEM), anywhere),
        scratch_shapes=[ext] * 18 + [
            pltpu.VMEM((4, NZ, *row), F32),
            pltpu.VMEM((N_GY, 2, LN), F32), pltpu.VMEM((N_GZ, 2, LN), F32),
            pltpu.VMEM(row, F32), pltpu.VMEM((1, 1), F32),
            pltpu.SemaphoreType.DMA((4,)), pltpu.SemaphoreType.DMA(()),
            pltpu.SemaphoreType.DMA((N_SEND,)), pltpu.SemaphoreType.DMA((N_RECV,)),
        ],
        compiler_params=pltpu.CompilerParams(collective_id=0, has_side_effects=True),
        name="advect",
    )(*tiled)
    return field.reshape(NZ, J, NY, LN).transpose(0, 2, 1, 3).reshape(NZ, NY, J * LN), step.reshape(())


def solution(mesh):
    spec = P("gz", "gy", None)
    return jax.shard_map(shards, mesh=mesh, in_specs=(spec,) * 4, out_specs=(spec, P()), check_vma=False)
```

```python
import jax
import jax.numpy as jnp
from jax import lax
from jax.experimental import pallas as pl
from jax.experimental.pallas import tpu as pltpu
from jax.sharding import PartitionSpec as P

NEWTON = 5
TILT_FLOOR = 3.2
TINY = 1e-18
COURANT = 0.45
EPSILON = 1e-6
THIRD = 1.0 / 3.0

NZ, NY, J, LN = 16, 8, 8, 128
N_GY, N_GZ = 16, 8
F32 = jnp.float32

EZ, EY = NZ + 4, NY + 4
Z0, Y0 = 2, 2
Z1, Y1 = Z0 + NZ, Y0 + NY

HALO_F, HALO_V, HALO_G, VEL, FLUX, STAT_Y, STAT_Z = range(7)
HALO_F_NEAR, HALO_F_FAR, HALO_G_NEAR = 7, 8, 9
N_SEND, N_RECV = 7, 10


def lanes(u):
    return lax.broadcasted_iota(jnp.int32, u.shape, u.ndim - 1)


def at_next(u):
    moved = pltpu.roll(u, LN - 1, u.ndim - 1)
    return jnp.where(lanes(u) == LN - 1, pltpu.roll(moved, J - 1, u.ndim - 2), moved)


def at_prev(u):
    moved = pltpu.roll(u, 1, u.ndim - 1)
    return jnp.where(lanes(u) == 0, pltpu.roll(moved, 1, u.ndim - 2), moved)


def plane(g, slope_d, slope_a, slope_b):
    tilt_a = jnp.abs(slope_a) + TILT_FLOOR
    tilt_b = jnp.abs(slope_b) + TILT_FLOOR
    lo, hi = jnp.minimum(tilt_a, tilt_b), jnp.maximum(tilt_a, tilt_b)
    slope_d = jnp.where(jnp.abs(slope_d) < TINY, TINY, slope_d)
    tilt_d = jnp.abs(slope_d)
    m1, rest = jnp.minimum(lo, tilt_d), jnp.maximum(lo, tilt_d)
    m2, m3 = jnp.minimum(rest, hi), jnp.maximum(rest, hi)
    lesser = jnp.maximum(jnp.minimum(g, 1.0 - g), 0.0)
    m12 = m1 * m2
    product = m12 * m3
    target = lesser * product
    both = target + target
    summed = lo + hi + tilt_d
    w = 0.5 * jnp.maximum(m1 + m2 - m3, 0.0)
    a = 0.5 * summed - (0.5 * product - target) / (m12 - w * w)
    for _ in range(NEWTON - 1):
        q0 = jnp.minimum(a, m1)
        r0 = a - q0
        p2 = jnp.maximum(a - m2, 0.0)
        q2 = jnp.minimum(p2, m1)
        r2 = p2 - q2
        p3 = jnp.maximum(a - m3, 0.0)
        s3 = p3 * p3
        value = q0 * (q0 * q0 * THIRD + a * r0) - q2 * (q2 * q2 * THIRD + p2 * r2) - s3 * (p3 * THIRD) - both
        rate = q0 * (a + r0) - q2 * (p2 + r2) - s3
        a = a - value / rate
    return jnp.where(g > 0.5, summed - a, a), lo, hi, slope_d, 0.5 / product


def cube_part(s, h):
    p = jnp.maximum(s, 0.0)
    q = jnp.minimum(p, h)
    r = p - q
    return q * (q * q * THIRD + p * r)


def flow(offset, lo, hi, slope_d, scale, c):
    signed = c * slope_d
    h = jnp.abs(signed)
    s = offset - jnp.where(signed < 0, jnp.abs(slope_d) - h, 0.0)
    t = s - hi
    return scale * ((cube_part(s, h) - cube_part(s - lo, h)) - (cube_part(t, h) - cube_part(t - lo, h)))


def rows(ref, where):
    parts = [ref[z, pl.ds(y, n)] for z, y, n in where]
    return parts[0] if len(parts) == 1 else jnp.concatenate(parts, axis=0)


def put(ref, where, value):
    start = 0
    for z, y, n in where:
        ref[z, pl.ds(y, n)] = value[start : start + n]
        start += n


def moved(where, dz, dy):
    return [(z + dz, y + dy, n) for z, y, n in where]


def loop(first, last, body):
    def step(i, carry):
        body(i)
        return carry

    lax.fori_loop(first, last, step, 0)


def pipelined(count, where_of, *stages):
    depth = len(stages)

    def run(i, live):
        for store in reversed([stages[k](where_of(i - k)) for k in live]):
            store()

    for i in range(depth - 1):
        run(i, range(i + 1))
    loop(depth - 1, count, lambda i: run(i, range(depth)))
    for i in range(count, count + depth - 1):
        run(i, range(i - count + 1, depth))


def kernel(
    f_hbm, vx_hbm, vy_hbm, vz_hbm, out_ref, dt_out,
    f_ext, g1_ext, g2_ext, vx, vy, vz, vx_diff, smooth, diff, sum_y, dif_y, sum_d,
    off, lo, hi, slope, scale, face, edge_y, stat_y, stat_z, dt_vec, dt_cell,
    load_sem, out_sem, send_sem, recv_sem,
):
    gy, gz = lax.axis_index("gy"), lax.axis_index("gz")

    def neighbour(dy, dz):
        return {"gy": lax.rem(gy + dy + N_GY, N_GY), "gz": lax.rem(gz + dz + N_GZ, N_GZ)}

    corners = [(1, 1), (1, -1), (-1, 1), (-1, -1)]
    own_z, own_y = pl.ds(Z0, NZ), pl.ds(Y0, NY)

    arrays = [(f_hbm, f_ext), (vx_hbm, vx), (vy_hbm, vy), (vz_hbm, vz)]

    def load(k):
        source, target = arrays[k]
        for y in range(NY):
            pltpu.make_async_copy(source.at[:, :, y, :], target.at[own_z, Y0 + y], load_sem.at[k]).start()

    load(0)
    barrier = pltpu.get_barrier_semaphore()
    greeted = [neighbour(k, 0) for k in range(1, N_GY)]
    greeted += [neighbour(0, k) for k in range(1, N_GZ)] + [neighbour(*c) for c in corners]
    for device in greeted:
        pl.semaphore_signal(barrier, inc=1, device_id=device, device_id_type=pl.DeviceIdType.MESH)
    for k in (1, 2, 3):
        load(k)

    def remote(source, target, sends, receives, device):
        return pltpu.make_async_remote_copy(
            src_ref=source, dst_ref=target, send_sem=send_sem.at[sends], recv_sem=recv_sem.at[receives],
            device_id=device, device_id_type=pl.DeviceIdType.MESH,
        )

    def halo(g, sends, receives, wide_z, wide_y):
        from_z = {1: pl.ds(Z1 - wide_z, wide_z), -1: pl.ds(Z0, wide_z), 0: own_z}
        from_y = {1: pl.ds(Y1 - wide_y, wide_y), -1: pl.ds(Y0, wide_y), 0: own_y}
        to_z = {1: pl.ds(Z0 - wide_z, wide_z), -1: pl.ds(Z1, wide_z), 0: own_z}
        to_y = {1: pl.ds(Y0 - wide_y, wide_y), -1: pl.ds(Y1, wide_y), 0: own_y}
        return [
            remote(g.at[from_z[dz], from_y[dy]], g.at[to_z[dz], to_y[dy]], sends, receives[k], neighbour(dy, dz))
            for k, (dy, dz) in enumerate([(1, 0), (-1, 0), (0, 1), (0, -1)] + corners)
        ]

    def send(copies):
        for copy in copies:
            copy.start()

    def arrive(part, receives):
        remote(part, part, 0, receives, neighbour(1, 0)).wait_recv()

    def left(part, sends):
        remote(part, part, sends, 0, neighbour(1, 0)).wait_send()

    def some(ref, z, y):
        return ref.at[pl.ds(0, z), pl.ds(0, y)]

    def loaded(k):
        source, target = arrays[k]
        pltpu.make_async_copy(source, target.at[own_z, own_y], load_sem.at[k]).wait()

    def scan_fraction(i, total):
        g = f_ext[i + Z0, own_y]
        return total + g * (1.0 - g)

    loaded(0)
    total = lax.fori_loop(0, NZ, scan_fraction, jnp.zeros((NY, J, LN), F32))
    peak = jnp.zeros((NY, J, LN), F32)
    for k in (1, 2, 3):
        loaded(k)
        speeds = arrays[k][1]
        peak = lax.fori_loop(0, NZ, lambda i, peak: jnp.maximum(peak, jnp.abs(speeds[i + Z0, own_y])), peak)
    top_row = lax.broadcasted_iota(jnp.int32, (2, LN), 0) == 0

    def combined(ref, n):
        top, add = ref[0], ref[0]
        for k in range(1, n):
            top, add = jnp.maximum(top, ref[k]), add + ref[k]
        return jnp.where(top_row, top, add)

    top, add = jnp.max(peak, axis=0), jnp.sum(total, axis=0)
    stat_y[gy] = jnp.concatenate([jnp.max(top, axis=0, keepdims=True), jnp.sum(add, axis=0, keepdims=True)], axis=0)

    pl.semaphore_wait(barrier, len(greeted))
    halo_f = halo(f_ext, HALO_F, 2 * [HALO_F] + 2 * [HALO_F_NEAR] + 4 * [HALO_F_FAR], 2, 2)
    halo_v = halo(vx, HALO_V, 8 * [HALO_V], 1, 1)
    stats_y = [remote(stat_y.at[gy], stat_y.at[gy], STAT_Y, STAT_Y, neighbour(k, 0)) for k in range(1, N_GY)]
    stats_z = [remote(stat_z.at[gz], stat_z.at[gz], STAT_Z, STAT_Z, neighbour(0, k)) for k in range(1, N_GZ)]
    velocity = [
        remote(vy.at[own_z, Y1 - 1], vy.at[own_z, Y0 - 1], VEL, VEL, neighbour(1, 0)),
        remote(vz.at[Z1 - 1, own_y], vz.at[Z0 - 1, own_y], VEL, VEL, neighbour(0, 1)),
    ]
    send(stats_y)
    send(halo_f[2:4] + halo_f[:2] + halo_f[4:])

    def put_shifts(g, where):
        before, after = at_prev(g), at_next(g)
        put(smooth, where, before + 2.0 * g + after)
        put(diff, where, after - before)

    def shift_rows(g_ext, where):
        put_shifts(rows(g_ext, where), where)

    def sums_of(z, y, n):
        s = smooth[z, pl.ds(y - 1, n + 2)]
        d = diff[z, pl.ds(y - 1, n + 2)]

        def store():
            where = [(z, y, n)]
            put(sum_y, where, s[:-2] + 2.0 * s[1:-1] + s[2:])
            put(dif_y, where, s[2:] - s[:-2])
            put(sum_d, where, d[:-2] + 2.0 * d[1:-1] + d[2:])

        return store

    def put_sums(z, y, n):
        sums_of(z, y, n)()

    planes = (off, lo, hi, slope, scale)

    def planes_of(g_ext, dim):
        def stage(where):
            below, above = moved(where, -1, 0), moved(where, 1, 0)
            along_z = rows(sum_y, above) - rows(sum_y, below)
            along_y = rows(dif_y, below) + 2.0 * rows(dif_y, where) + rows(dif_y, above)
            along_x = rows(sum_d, below) + 2.0 * rows(sum_d, where) + rows(sum_d, above)
            slopes = [along_z, along_y, along_x]
            across = [slopes[k] for k in range(3) if k != dim]
            g = rows(g_ext, where)

            def store():
                for ref, value in zip(planes, plane(g, slopes[dim], *across)):
                    put(ref, where, value)

            return store

        return stage

    def put_planes(g_ext, dim, where):
        planes_of(g_ext, dim)(where)()

    def donors_x(where):
        found = [rows(ref, where) for ref in planes]
        q = rows(vx, where)
        others = [at_next(value) for value in found]
        before = at_prev(q)

        def store():
            upward = q > 0
            others[-1] = -others[-1]
            for ref, value, other in zip(planes, found, others):
                put(ref, where, jnp.where(upward, value, other))
            put(vx_diff, where, q - before)

        return store

    def donors(upward, here, there):
        picked = [jnp.where(upward, rows(ref, here), rows(ref, there)) for ref in planes[:-1]]
        return picked + [jnp.where(upward, rows(scale, here), -rows(scale, there))]

    inner = (Y0 + 1, NY - 2)

    def pair(z):
        return [(z, *inner), (z + 1, *inner)]

    def shift_ends(g_ext):
        loop(0, 2, lambda i: shift_rows(g_ext, [(i * Z1, Y0, NY), (i * Z1 + 1, Y0, NY)]))
        loop(0, 4, lambda i: put_sums(i + (i // 2) * (EZ - 4), *inner))

    loop(0, NZ // 2, lambda i: shift_rows(f_ext, [(Z0 + 2 * i, Y0, NY), (Z0 + 2 * i + 1, Y0, NY)]))
    loop(Z0, Z1, lambda z: put_sums(z, *inner))
    pipelined(5, lambda i: [(Z0 + 1 + i, *inner)], planes_of(f_ext, 2), donors_x)
    send(halo_v)
    pipelined(NZ - 7, lambda i: [(Z0 + 6 + i, *inner)], planes_of(f_ext, 2), donors_x)
    send(velocity)
    arrive(some(f_ext, 8, 4), HALO_F_NEAR)
    shift_ends(f_ext)
    loop(0, 2, lambda i: put_planes(f_ext, 2, pair(1 + i * NZ)))
    donors_x([(Z0, *inner), (Z1 - 1, *inner)])()
    arrive(some(f_ext, NZ, 4), HALO_F)
    arrive(stat_y.at[pl.ds(0, N_GY - 1)], STAT_Y)
    stat_z[gz] = combined(stat_y, N_GY)
    send(stats_z)

    def shift_sides(i):
        z = Z0 + 4 * i
        shift_rows(f_ext, [w for k in range(4) for w in ((z + k, 0, 2), (z + k, Y1, 2))])

    def sums_side(z):
        put_sums(z, 1, 2)
        put_sums(z, Y1 - 1, 2)

    loop(0, NZ // 4, shift_sides)
    loop(Z0, Z1, sums_side)
    def shift_corners(i):
        z = i * Z1
        shift_rows(f_ext, [(z, 0, 2), (z, Y1, 2), (z + 1, 0, 2), (z + 1, Y1, 2)])

    def column(zs, y):
        return [(z, y, 1) for z in zs]

    def own_columns(i):
        first, high = 3 + 6 * (i - 2 * (i // 2)), i // 2
        return column([first + k for k in range(6)], Y0 + high * (NY - 1))

    def next_column(high):
        return column([Z0 + 1 + k for k in range(12)], Y0 - 1 + high * (NY + 1))

    def end_columns(high):
        return [(z, 1 + high * (Y1 - 2), 2) for z in (1, 2, NZ - 1, NZ, NZ + 1, NZ + 2)]

    planes_x = planes_of(f_ext, 2)
    pipelined(4, own_columns, planes_x, donors_x)
    loop(0, 2, lambda i: put_planes(f_ext, 2, next_column(i)))
    arrive(some(f_ext, 4, 4), HALO_F_FAR)
    loop(0, 2, shift_corners)
    loop(0, 4, lambda i: sums_side(i + (i // 2) * (EZ - 4)))
    loop(0, 2, lambda i: put_planes(f_ext, 2, end_columns(i)))
    arrive(some(vx, 13, 4), HALO_V)
    loop(0, 2, lambda i: donors_x(next_column(i))())
    loop(0, 2, lambda i: donors_x(end_columns(i))())
    donors_x([(1, *inner), (NZ + 2, *inner)])()
    arrive(stat_z.at[pl.ds(0, N_GZ - 1)], STAT_Z)
    stats = combined(stat_z, N_GZ)
    umax = jnp.max(stats[0:1], axis=1, keepdims=True)
    share = jnp.sum(stats[1:2], axis=1, keepdims=True) * (4.0 / (N_GZ * NZ * N_GY * NY * J * LN))
    step = COURANT / ((umax + EPSILON) * (1.0 + share))
    dt_vec[...] = jnp.broadcast_to(step, (J, LN))
    dt_cell[...] = step

    def flow_x(where):
        found = [rows(ref, where) for ref in planes]
        q = rows(vx, where)
        return lambda: put(face, where, flow(*found, dt_vec[...] * q))

    def update_x(where):
        out = rows(face, where)
        before = at_prev(out)
        g, change = rows(f_ext, where), rows(vx_diff, where)
        return lambda: put(g1_ext, where, (g - out + before) / (1.0 - dt_vec[...] * change))

    def shifts_of(g_ext):
        def stage(where):
            g = rows(g_ext, where)
            before, after = at_prev(g), at_next(g)

            def store():
                put(smooth, where, before + 2.0 * g + after)
                put(diff, where, after - before)

            return store

        return stage

    dt_copy = pltpu.make_async_copy(dt_cell, dt_out, out_sem)
    x_stages = (flow_x, update_x, shifts_of(g1_ext))
    pipelined(
        NZ // 2 + 1,
        lambda i: [w for z in (1 + 2 * i, 2 + 2 * i) for w in ((z, 1, 3), (z, Y1 - 2, 3))],
        *x_stages,
    )

    dt_copy.start()

    def sums_edge(first, n):
        for z in range(n):
            put_sums(first + z, Y0, 1)
            put_sums(first + z, Y1 - 1, 1)

    def edges(first, n):
        return [w for k in range(n) for w in ((first + k, Y0, 1), (first + k, Y1 - 1, 1))]

    def half_faces_y(i):
        z = Z0 + 4 * i
        at_face = [w for k in range(4) for w in ((z + k, Y0 - 1, 1), (z + k, Y1 - 1, 1))]
        c = dt_vec[...] * rows(vy, at_face)
        out = flow(*[rows(ref, edges(z, 4)) for ref in planes], c)
        for k in range(4):
            edge_y[0, 4 * i + k] = jnp.where(c[2 * k + 1] > 0, out[2 * k + 1], 0.0)
            edge_y[1, 4 * i + k] = jnp.where(c[2 * k] < 0, out[2 * k], 0.0)

    flux_y = []
    for k in range(2):
        part = pl.ds(k * (NZ // 2), NZ // 2)
        flux_y += [
            remote(edge_y.at[0, part], edge_y.at[2, part], FLUX, FLUX, neighbour(1, 0)),
            remote(edge_y.at[1, part], edge_y.at[3, part], FLUX, FLUX, neighbour(-1, 0)),
        ]
    loop(0, (NZ + 2) // 3, lambda i: sums_edge(Z0 - 1 + 3 * i, 3))
    for k in range(2):
        put_planes(g1_ext, 1, edges(Z0 + k * (NZ // 2), NZ // 2))
        if k == 0:
            arrive(some(vy, 6, 4), VEL)
        loop(2 * k, 2 * k + 2, half_faces_y)
        send(flux_y[2 * k : 2 * k + 2])

    def middle(i):
        return [(1 + 3 * i + k, Y0 + 2, NY - 4) for k in range(3)]

    def faces_y(where):
        c = dt_vec[...] * rows(vy, where)
        put(face, where, flow(*donors(c > 0, where, moved(where, 0, 1)), c))

    pipelined((NZ + 2) // 3, middle, *x_stages)
    loop(Z0 - 1, Z0 + 3, lambda z: put_sums(z, *inner))

    def y_inner(i):
        z = Z0 + 2 * i
        stores = planes_of(g1_ext, 1)(pair(z)), sums_of(z + 3, *inner), sums_of(z + 4, *inner)
        for store in stores:
            store()

    loop(0, NZ // 2 - 1, y_inner)
    put_planes(g1_ext, 1, pair(Z1 - 2))
    def faces_y_near(i):
        z = Z0 + 4 * i
        faces_y([w for k in range(4) for w in ((z + k, Y0, 1), (z + k, Y1 - 2, 1))])

    def update_y(where):
        before, q = moved(where, 0, -1), dt_vec[...]
        g = rows(g1_ext, where) - rows(face, where) + rows(face, before)
        put(g2_ext, where, g / (1.0 - q * (rows(vy, where) - rows(vy, before))))

    def update_y_edge(i):
        for k in range(4):
            z, at = Z0 + 4 * i + k, 4 * i + k
            face[z, Y0 - 1] = edge_y[2, at] - edge_y[1, at]
            face[z, Y1 - 1] = edge_y[0, at] - edge_y[3, at]
        update_y(edges(Z0 + 4 * i, 4))

    def rest_y(i):
        z = Z0 + 2 * lax.rem(7 * i, NZ // 2)
        faces_y([(z, Y0 + 1, NY - 3), (z + 1, Y0 + 1, NY - 3)])
        update_y([(z, *inner), (z + 1, *inner)])

    near = [HALO_G, HALO_G, HALO_G_NEAR, HALO_G_NEAR] + 4 * [HALO_G]
    halo_g = halo(g2_ext, HALO_G, near, 2, 1)
    loop(0, NZ // 4, faces_y_near)
    arrive(edge_y.at[pl.ds(2, 2)], FLUX)
    loop(0, NZ // 4, update_y_edge)
    send(halo_g[:2] + halo_g[4:])
    loop(0, 2, rest_y)
    send(halo_g[2:4])
    loop(2, NZ // 2, rest_y)

    def faces_z(where):
        c = dt_vec[...] * rows(vz, where)
        put(face, where, flow(*donors(c > 0, where, moved(where, 1, 0)), c))

    shift_rows(g2_ext, [(Z0, Y0, NY), (Z0 + 1, Y0, NY)])
    shift_rows(g2_ext, [(Z0 + 2, Y0, NY), (Z0 + 3, Y0, NY)])
    loop(Z0, Z0 + 3, lambda z: put_sums(z, *inner))

    def z_inner(z):
        stores = (
            shifts_of(g2_ext)([(z + 3, Y0, NY)]),
            planes_of(g2_ext, 0)([(z, *inner)]),
            sums_of(z + 2, *inner),
        )
        for store in reversed(stores):
            store()

    loop(Z0 + 1, Z1 - 3, z_inner)
    put_sums(Z1 - 1, *inner)
    put_planes(g2_ext, 0, pair(Z1 - 3))
    loop(0, NZ // 2 - 2, lambda i: faces_z(pair(Z0 + 1 + 2 * i)))
    faces_z([(Z1 - 3, *inner)])
    arrive(some(g2_ext, 8, 4), HALO_G_NEAR)
    shift_ends(g2_ext)
    loop(0, 2, lambda i: put_planes(g2_ext, 0, pair(1 + i * NZ)))
    loop(0, 2, lambda i: faces_z(pair(1 + i * (NZ - 1))))

    def update_z(where):
        before, q = moved(where, -1, 0), dt_vec[...]
        g = rows(g2_ext, where) - rows(face, where) + rows(face, before)
        g = g / (1.0 - q * (rows(vz, where) - rows(vz, before)))
        for k, (z, y) in enumerate([(z, y + k) for z, y, n in where for k in range(n)]):
            out_ref[z - Z0, pl.ds(y - Y0, J, stride=NY), :] = g[k]

    loop(Z0, Z1, lambda z: update_z([(z, *inner)]))
    arrive(some(g2_ext, 10, 4), HALO_G)
    loop(0, 2, lambda i: shift_rows(
        g2_ext, [w for k in range(EZ // 2) for w in ((i * (EZ // 2) + k, Y0 - 1, 1), (i * (EZ // 2) + k, Y1, 1))]
    ))
    loop(0, EZ // 4, lambda i: sums_edge(4 * i, 4))
    loop(0, (NZ + 2) // 6, lambda i: put_planes(g2_ext, 0, edges(1 + 6 * i, 6)))
    loop(0, 2, lambda i: faces_z(edges(1 + 6 * i, 6)))
    faces_z(edges(Z1 - 5, 5))

    loop(0, NZ // 4, lambda i: update_z(edges(Z0 + 4 * i, 4)))
    left(some(f_ext, 14, 8), HALO_F)
    left(some(vx, 13, 4), HALO_V)
    left(some(g2_ext, 9, 8), HALO_G)
    left(some(vy, 6, 4), VEL)
    left(edge_y.at[pl.ds(0, 2)], FLUX)
    left(stat_y.at[pl.ds(0, N_GY - 1)], STAT_Y)
    left(stat_z.at[pl.ds(0, N_GZ - 1)], STAT_Z)
    dt_copy.wait()


def shards(*blocks):
    tiled = [b.reshape(NZ, NY, J, LN).transpose(0, 2, 1, 3) for b in blocks]
    row = (J, LN)
    ext = pltpu.VMEM((EZ, EY, *row), F32)
    anywhere = pl.BlockSpec(memory_space=pl.ANY)
    field, step = pl.pallas_call(
        kernel,
        out_shape=(pltpu.VMEM((NZ, J * NY, LN), F32), jax.ShapeDtypeStruct((1, 1), F32)),
        in_specs=[anywhere] * 4,
        out_specs=(pl.BlockSpec(memory_space=pltpu.VMEM), anywhere),
        scratch_shapes=[ext] * 18 + [
            pltpu.VMEM((4, NZ, *row), F32),
            pltpu.VMEM((N_GY, 2, LN), F32), pltpu.VMEM((N_GZ, 2, LN), F32),
            pltpu.VMEM(row, F32), pltpu.VMEM((1, 1), F32),
            pltpu.SemaphoreType.DMA((4,)), pltpu.SemaphoreType.DMA(()),
            pltpu.SemaphoreType.DMA((N_SEND,)), pltpu.SemaphoreType.DMA((N_RECV,)),
        ],
        compiler_params=pltpu.CompilerParams(collective_id=0, has_side_effects=True),
        name="advect",
    )(*tiled)
    return field.reshape(NZ, J, NY, LN).transpose(0, 2, 1, 3).reshape(NZ, NY, J * LN), step.reshape(())


def solution(mesh):
    spec = P("gz", "gy", None)
    return jax.shard_map(shards, mesh=mesh, in_specs=(spec,) * 4, out_specs=(spec, P()), check_vma=False)
```
